32 devices in a mesh: dp: 8 (over y, x, core), mp: 4 (over z).
Axes of the slice: x: 2, y: 2, z: 4, core: 2. Of those that a mesh axis runs over, the one named last changes fastest.
Arguments:
- inputs: bfloat16 [8192, 2048], P(('dp', 'mp')), may hold values from -6 to 6
- segments: int32 [8, 1024], P('dp'), may hold values from 0 to 5, never falling along the last dimension, each value on 1 to 512 neighbouring positions
- first_norm_gain: float32 [2048], replicated, may hold values from 0.1 to 1.9
- w_query: bfloat16 [2048, 2048], P('dp', 'mp'), may hold values from -0.125 to 0.125
- w_key: bfloat16 [2048, 2048], P('dp', 'mp'), may hold values from -0.125 to 0.125
- w_value: bfloat16 [2048, 3456], P('dp', 'mp'), may hold values from -0.125 to 0.125
- w_gate: bfloat16 [2048, 3456], P('dp', 'mp'), may hold values from -0.125 to 0.125
- w_out: bfloat16 [3456, 2048], P('mp', 'dp'), may hold values from -0.21875 to 0.21875
- second_norm_gain: float32 [2048], replicated, may hold values from 0.1 to 1.9
- w_glu_gate: bfloat16 [2048, 3456], P('dp', 'mp'), may hold values from -0.125 to 0.125
- w_glu_up: bfloat16 [2048, 3456], P('dp', 'mp'), may hold values from -0.125 to 0.125
- w_down: bfloat16 [3456, 2048], P('mp', 'dp'), may hold values from -0.21875 to 0.21875
- cotangent: bfloat16 [8192, 2048], P(('dp', 'mp')), may hold values from -9 to 9
Outputs:
- outputs: bfloat16 [8192, 2048], P(('dp', 'mp'))
- input_gradient: float32 [8192, 2048], P(('dp', 'mp'))
- grad_norm1_gain: float32 [2048], replicated
- grad_w_query: float32 [2048, 2048], P('dp', 'mp')
- grad_w_key: float32 [2048, 2048], P('dp', 'mp')
- grad_w_value: float32 [2048, 3456], P('dp', 'mp')
- grad_w_gate: float32 [2048, 3456], P('dp', 'mp')
- grad_w_out: float32 [3456, 2048], P('mp', 'dp')
- grad_norm2_gain: float32 [2048], replicated
- grad_w_glu_gate: float32 [2048, 3456], P('dp', 'mp')
- grad_w_glu_up: float32 [2048, 3456], P('dp', 'mp')
- grad_w_down: float32 [3456, 2048], P('mp', 'dp')
The draws below stay inside these ranges and needn't reach their ends.
Inputs may be any that keep to these rules, and one draw needn't show every extreme that they name: `segments`: within a sequence the document numbers never fall; each document holds 1 to 512 tokens and one holds exactly 512.
All inputs are finite; a program needn't handle non-finite values.
Results may differ from the reference program's by a relative error of at most 0.024.
Values may be sent and summed in bfloat16 or wider, within the bound.
A program may use at most 256 MiB of HBM per device.

```python
import math
import jax
import jax.numpy as jnp
import numpy as np
from jax import lax

D = 2048
H = 8
HK = 256
HV = 432
FF = 3456
LEN = 1024
DOCS = 6
DK = 2048
DV = 3456
DOC_MOST = 512
SEQS = 8
TOKENS = 8192
N_MP = 4


def draw_cotangent(key, part):
    place = jnp.arange(TOKENS, dtype=jnp.float32) / max(TOKENS - 1, 1)
    noise = jnp.clip(jax.random.normal(key, (TOKENS, D), jnp.float32), -5.0, 5.0)
    scaling = 0.6 * jnp.power(3.0, place)
    return (noise * scaling[:, None]).astype(jnp.bfloat16)


def shard_levels(rng, extent, cuts, smallest, top_value):
    level, own = 1.0, jax.random.fold_in(rng, 6)
    for position, shards_of in cuts:
        draws = jnp.exp(jax.random.uniform(jax.random.fold_in(own, position), (shards_of,), jnp.float32, smallest / len(cuts), top_value / len(cuts)))
        level = level * jnp.repeat(draws, extent[position] // shards_of).reshape([-1 if axis == position else 1 for axis in range(len(extent))])
    return level


def split_up(number_of, total, most, lean):
    weights = [(1 << 20) // math.isqrt(grade ** lean) + 1 for grade in range(2, number_of + 1)]
    spare, holding = total - most - (number_of - 1), [1] * (number_of - 1)
    while spare > 0:
        free = [i for i in range(number_of - 1) if holding[i] < most]
        whole, remaining = sum([weights[i] for i in free]), spare
        for i in free:
            addition = min(most - holding[i], max(1, remaining * weights[i] // whole), spare)
            holding[i] = holding[i] + addition
            spare = spare - addition
    return np.array([most] + holding)


def ragged_sizes(stream_key, amount, total, most, skew):
    if amount == 2:
        one = jax.random.randint(stream_key, (), max(1, total - most), min(most, total - 1) + 1)
        return jnp.stack([one, total - one])
    lengths = jnp.asarray(split_up(amount, total, most, skew), jnp.int32)
    pairs = (amount - 1) // 2
    giver, receiver = lengths[1:1 + 2 * pairs:2], lengths[2:2 + 2 * pairs:2]
    room = jnp.minimum(giver - 1, most - receiver)
    passed = jax.random.randint(jax.random.fold_in(stream_key, 1), (pairs,), 0, 1 << 20) % (room + 1)
    lengths = lengths.at[1:1 + 2 * pairs:2].set(giver - passed).at[2:2 + 2 * pairs:2].set(receiver + passed)
    return lengths[jax.random.permutation(jax.random.fold_in(stream_key, 2), amount)]


def normal_values(rng, dims, scale, bound, pieces=(), kind=jnp.bfloat16):
    drawn = jax.random.normal(rng, dims, jnp.float32) * scale
    if len(pieces) > 0:
        drawn = shard_levels(rng, dims, pieces, -0.22, 0.18) * drawn
    return jnp.clip(drawn, min=-bound, max=bound).astype(kind)


def setup_inputs(seed: int = 0) -> dict:
    key_of = jax.random.split(jax.random.key(seed), 14)
    inputs = normal_values(key_of[0], (TOKENS, D), 1.0, 6.0, ((0, 32),))
    segments = jax.vmap(lambda own: jnp.searchsorted(jnp.cumsum(ragged_sizes(own, DOCS, LEN, DOC_MOST, 1)), jnp.arange(LEN), side="right"))(jax.random.split(key_of[1], SEQS)).reshape((SEQS, LEN)).astype(jnp.int32)
    first_norm_gain = jnp.clip(1.0 + 0.18 * jax.random.normal(key_of[2], (D,), jnp.float32), 0.1, 1.9)
    w_query = normal_values(key_of[3], (D, DK), D ** -0.5, 0.125, ((0, 8), (1, 4)))
    w_key = normal_values(key_of[4], (D, DK), D ** -0.5, 0.125, ((0, 8), (1, 4)))
    w_value = normal_values(key_of[5], (D, DV), D ** -0.5, 0.125, ((0, 8), (1, 4)))
    w_gate = normal_values(key_of[6], (D, DV), D ** -0.5, 0.125, ((0, 8), (1, 4)))
    w_out = normal_values(key_of[7], (DV, D), (DV // 4) ** -0.5, 0.21875, ((0, 4), (1, 8)))
    second_norm_gain = jnp.clip(1.0 + 0.18 * jax.random.normal(key_of[8], (D,), jnp.float32), 0.1, 1.9)
    w_glu_gate = normal_values(key_of[9], (D, FF), D ** -0.5, 0.125, ((0, 8), (1, 4)))
    w_glu_up = normal_values(key_of[10], (D, FF), D ** -0.5, 0.125, ((0, 8), (1, 4)))
    w_down = normal_values(key_of[11], (FF, D), (FF // 4) ** -0.5, 0.21875, ((0, 4), (1, 8)))
    cotangent = draw_cotangent(jax.random.fold_in(key_of[13], 71), 0)
    return {"inputs": inputs, "segments": segments, "first_norm_gain": first_norm_gain, "w_query": w_query, "w_key": w_key, "w_value": w_value, "w_gate": w_gate, "w_out": w_out, "second_norm_gain": second_norm_gain, "w_glu_gate": w_glu_gate, "w_glu_up": w_glu_up, "w_down": w_down, "cotangent": cotangent}


epsilon = 1e-05
group_epsilon = 1.0

def apply_layer_norm(values_in, offset):
    centre = lax.optimization_barrier(jnp.mean(values_in, axis=-1, keepdims=True))
    centred = values_in - centre
    variance = lax.optimization_barrier(jnp.mean(centred * centred, axis=-1, keepdims=True))
    scaling = lax.rsqrt(variance + offset)
    return (centred * scaling, scaling)

def norm_backward_rule(grad_hat, normed_hat, scaling):
    first_mean = lax.optimization_barrier(jnp.mean(grad_hat, axis=-1, keepdims=True))
    second_mean = lax.optimization_barrier(jnp.mean(grad_hat * normed_hat, axis=-1, keepdims=True))
    return scaling * (grad_hat - first_mean - normed_hat * second_mean)

def glu_act(gate_pre, up_pre):
    return jax.nn.gelu(gate_pre, approximate=True) * up_pre

def decay_mask(seg_row, head_start, head_count):
    places = jnp.arange(LEN)
    distance = places[:, None] - places[None, :]
    allowed = (distance >= 0) & (seg_row[:, None] == seg_row[None, :])
    heads = (head_start + jnp.arange(head_count)).astype(jnp.float32)
    log_gamma = jnp.log1p(-jnp.exp2(-5.0 - heads))
    exponent = jnp.where(allowed[None], distance[None].astype(jnp.float32) * log_gamma[:, None, None], 0.0)
    return jnp.where(allowed[None], jnp.exp(exponent), 0.0)

def retain_weights(query_heads, key_heads, mask):
    scores = jnp.einsum('thk,shk->hts', query_heads.astype(jnp.float32), key_heads.astype(jnp.float32)) * mask
    return scores.astype(jnp.bfloat16)

def retain(query_heads, key_heads, value_heads, mask):
    weights = retain_weights(query_heads, key_heads, mask)
    return jnp.einsum('hts,shv->thv', weights.astype(jnp.float32), value_heads.astype(jnp.float32))

def retain_back(query_heads, key_heads, value_heads, mask, grad_out):
    weights = retain_weights(query_heads, key_heads, mask)
    grad_f = grad_out.astype(jnp.float32)
    grad_value = jnp.einsum('hts,thv->shv', weights.astype(jnp.float32), grad_f).astype(jnp.bfloat16)
    grad_weights = jnp.einsum('thv,shv->hts', grad_f, value_heads.astype(jnp.float32))
    grad_scores = (grad_weights * mask).astype(jnp.bfloat16).astype(jnp.float32)
    grad_query = jnp.einsum('hts,shk->thk', grad_scores, key_heads.astype(jnp.float32)).astype(jnp.bfloat16)
    grad_key = (jnp.einsum('hts,thk->shk', grad_scores, query_heads.astype(jnp.float32)) * HK ** (-0.5)).astype(jnp.bfloat16)
    return (grad_query, grad_key, grad_value)

def group_sum(pairs):
    running = jnp.zeros((N_MP, LEN, D), jnp.float32)
    for left_side, right_side in pairs:
        columns = left_side.shape[1]
        left_groups = left_side.reshape(LEN, N_MP, columns // N_MP).astype(jnp.float32)
        right_groups = right_side.reshape(N_MP, columns // N_MP, D).astype(jnp.float32)
        running = running + jnp.einsum('lgc,gcd->gld', left_groups, right_groups)
    rounded = lax.optimization_barrier(running.astype(jnp.bfloat16))
    return lax.optimization_barrier(jnp.sum(rounded.astype(jnp.float32), axis=0))

def one_sequence(seq_in, seg_row, sequence_output_gradient, params):
    first_norm_gain, w_query, w_key, w_value, w_gate, w_out, second_norm_gain, w_glu_gate, w_glu_up, w_down = params
    inputs_float = seq_in.astype(jnp.float32)
    first_standardized, first_inverse_scale = apply_layer_norm(inputs_float, epsilon)
    first_normed_rows = (first_standardized * first_norm_gain).astype(jnp.bfloat16)
    query_all = jnp.dot(first_normed_rows, w_query, preferred_element_type=jnp.float32).astype(jnp.bfloat16)
    key_all = (jnp.dot(first_normed_rows, w_key, preferred_element_type=jnp.float32) * HK ** (-0.5)).astype(jnp.bfloat16)
    value_all = jnp.dot(first_normed_rows, w_value, preferred_element_type=jnp.float32).astype(jnp.bfloat16)
    gate_pre = jnp.dot(first_normed_rows, w_gate, preferred_element_type=jnp.float32)
    mask = decay_mask(seg_row, 0, H)
    query_heads = query_all.reshape(LEN, H, HK)
    key_heads = key_all.reshape(LEN, H, HK)
    value_heads = value_all.reshape(LEN, H, HV)
    retained = retain(query_heads, key_heads, value_heads, mask)
    normalized, scale_group = apply_layer_norm(retained, group_epsilon)
    normal_flat = normalized.reshape(LEN, DV)
    swish = jax.nn.silu(gate_pre)
    gated = (swish * normal_flat).astype(jnp.bfloat16)
    middle_state = inputs_float + group_sum([(gated, w_out)])
    second_standardized, second_inverse_scale = apply_layer_norm(middle_state, epsilon)
    second_normed_rows = (second_standardized * second_norm_gain).astype(jnp.bfloat16)
    glu_gate = jnp.dot(second_normed_rows, w_glu_gate, preferred_element_type=jnp.float32)
    glu_up = jnp.dot(second_normed_rows, w_glu_up, preferred_element_type=jnp.float32)
    hidden = glu_act(glu_gate, glu_up).astype(jnp.bfloat16)
    outputs = (middle_state + group_sum([(hidden, w_down)])).astype(jnp.bfloat16)
    d_hidden = jnp.dot(sequence_output_gradient, w_down.T, preferred_element_type=jnp.float32)
    unused, pullback = jax.vjp(glu_act, glu_gate, glu_up)
    d_glu_gate, d_glu_up = pullback(d_hidden)
    d_glu_gate = d_glu_gate.astype(jnp.bfloat16)
    d_glu_up = d_glu_up.astype(jnp.bfloat16)
    grad_w_down = jnp.dot(hidden.T, sequence_output_gradient, preferred_element_type=jnp.float32)
    grad_w_glu_gate = jnp.dot(second_normed_rows.T, d_glu_gate, preferred_element_type=jnp.float32)
    grad_w_glu_up = jnp.dot(second_normed_rows.T, d_glu_up, preferred_element_type=jnp.float32)
    second_normed_gradient = group_sum([(d_glu_gate, w_glu_gate.T), (d_glu_up, w_glu_up.T)])
    second_gain_gradient = lax.optimization_barrier(jnp.sum(second_standardized * second_normed_gradient, axis=0))
    middle_gradient = sequence_output_gradient.astype(jnp.float32) + norm_backward_rule(second_normed_gradient * second_norm_gain, second_standardized, second_inverse_scale)
    d_mid_round = middle_gradient.astype(jnp.bfloat16)
    grad_w_out = jnp.dot(gated.T, d_mid_round, preferred_element_type=jnp.float32)
    d_gated = jnp.dot(d_mid_round, w_out.T, preferred_element_type=jnp.float32)
    sigmoid_gate = jax.nn.sigmoid(gate_pre)
    d_gate_pre = (d_gated * normal_flat * (sigmoid_gate + gate_pre * sigmoid_gate * (1.0 - sigmoid_gate))).astype(jnp.bfloat16)
    d_normalized = (d_gated * swish).reshape(LEN, H, HV)
    d_retained = norm_backward_rule(d_normalized, normalized, scale_group).astype(jnp.bfloat16)
    d_query, d_key, d_value = retain_back(query_heads, key_heads, value_heads, mask, d_retained)
    d_query = d_query.reshape(LEN, DK)
    d_key = d_key.reshape(LEN, DK)
    d_value = d_value.reshape(LEN, DV)
    grad_w_query = jnp.dot(first_normed_rows.T, d_query, preferred_element_type=jnp.float32)
    grad_w_key = jnp.dot(first_normed_rows.T, d_key, preferred_element_type=jnp.float32)
    grad_w_value = jnp.dot(first_normed_rows.T, d_value, preferred_element_type=jnp.float32)
    grad_w_gate = jnp.dot(first_normed_rows.T, d_gate_pre, preferred_element_type=jnp.float32)
    first_normed_gradient = group_sum([(d_query, w_query.T), (d_key, w_key.T), (d_value, w_value.T), (d_gate_pre, w_gate.T)])
    first_gain_gradient = lax.optimization_barrier(jnp.sum(first_standardized * first_normed_gradient, axis=0))
    input_gradient = middle_gradient + norm_backward_rule(first_normed_gradient * first_norm_gain, first_standardized, first_inverse_scale)
    grads = (first_gain_gradient, grad_w_query, grad_w_key, grad_w_value, grad_w_gate, grad_w_out, second_gain_gradient, grad_w_glu_gate, grad_w_glu_up, grad_w_down)
    return (outputs, input_gradient, grads)

def reference(inputs, segments, first_norm_gain, w_query, w_key, w_value, w_gate, w_out, second_norm_gain, w_glu_gate, w_glu_up, w_down, cotangent):
    params = (first_norm_gain, w_query, w_key, w_value, w_gate, w_out, second_norm_gain, w_glu_gate, w_glu_up, w_down)
    seq_inputs = inputs.reshape(SEQS, LEN, D)
    seq_cots = cotangent.reshape(SEQS, LEN, D)

    def step_one(running, item):
        seq_in, seg_row, sequence_output_gradient = item
        outputs, input_gradient, grads = one_sequence(seq_in, seg_row, sequence_output_gradient, params)
        return (jax.tree.map(jnp.add, running, grads), (outputs, input_gradient))
    starting = tuple((jnp.zeros(weight.shape, jnp.float32) for weight in params))
    totals, results = lax.scan(step_one, starting, (seq_inputs, segments, seq_cots))
    out_seqs, grad_seqs = results
    return (out_seqs.reshape(TOKENS, D), grad_seqs.reshape(TOKENS, D), totals[0], totals[1], totals[2], totals[3], totals[4], totals[5], totals[6], totals[7], totals[8], totals[9])
```

```python
import jax
import jax.numpy as jnp
from jax import lax
from jax.sharding import PartitionSpec as P

H = 8
HK = 256
HV = 432
LEN = 1024
CHUNKS = 2

epsilon = 1e-05
group_epsilon = 1.0
BF = jnp.bfloat16
F32 = jnp.float32


def layer_norm(values_in, offset):
    centre = jnp.mean(values_in, axis=-1, keepdims=True)
    centred = values_in - centre
    variance = jnp.mean(centred * centred, axis=-1, keepdims=True)
    scaling = lax.rsqrt(variance + offset)
    return (centred * scaling, scaling)


def norm_back(grad_hat, normed_hat, scaling):
    first_mean = jnp.mean(grad_hat, axis=-1, keepdims=True)
    second_mean = jnp.mean(grad_hat * normed_hat, axis=-1, keepdims=True)
    return scaling * (grad_hat - first_mean - normed_hat * second_mean)


def glu_act(gate_pre, up_pre):
    return jax.nn.gelu(gate_pre, approximate=True) * up_pre


def dot_nt(a, b):
    return lax.dot_general(a, b, (((1,), (1,)), ((), ())), preferred_element_type=F32)


def dot_nn(a, b):
    return lax.dot_general(a, b, (((1,), (0,)), ((), ())), preferred_element_type=F32)


def dot_tn(a, b):
    return lax.dot_general(a, b, (((0,), (0,)), ((), ())), preferred_element_type=F32)


def line_gather(own, n, place):
    right, left = [None], [None]
    r = l = own
    for step in range(1, n):
        r = lax.ppermute(r, "mp", [(i, i + 1) for i in range(step - 1, n - 1)])
        l = lax.ppermute(l, "mp", [(i, i - 1) for i in range(1, n - step + 1)])
        right.append(r)
        left.append(l)
    return [own] + [jnp.where(place >= k, right[k], left[n - k]) for k in range(1, n)]


def line_scatter(slots, n):
    r = l = None
    for step in range(1, n):
        send_r, send_l = slots[step], slots[n - step]
        if r is not None:
            send_r = (send_r.astype(F32) + r.astype(F32)).astype(BF)
            send_l = (send_l.astype(F32) + l.astype(F32)).astype(BF)
        r = lax.ppermute(send_r, "mp", [(i, i + 1) for i in range(step)])
        l = lax.ppermute(send_l, "mp", [(i, i - 1) for i in range(n - step, n)])
    return slots[0].astype(F32) + r.astype(F32) + l.astype(F32)


def body(
    inputs,
    segments,
    first_norm_gain,
    w_query,
    w_key,
    w_value,
    w_gate,
    w_out,
    second_norm_gain,
    w_glu_gate,
    w_glu_up,
    w_down,
    cotangent,
):
    n = lax.axis_size("mp")
    place = lax.axis_index("mp")
    heads = H // n
    head_start = place * heads
    rows, width = inputs.shape
    piece = rows // CHUNKS
    per = n * piece
    nk, nv, nf = heads * HK, heads * HV, w_down.shape[0]

    pack_one = jnp.concatenate([w_query.T, w_key.T, w_value.T, w_gate.T], axis=0)
    weight_one = lax.all_gather(pack_one, "dp", axis=1, tiled=True)
    out_weight = lax.all_gather(w_out, "dp", axis=1, tiled=True)
    pack_two = jnp.concatenate([w_glu_gate.T, w_glu_up.T, w_down], axis=0)
    weight_two = lax.all_gather(pack_two, "dp", axis=1, tiled=True)
    glu_weight, down_weight = weight_two[: 2 * nf], weight_two[2 * nf :]

    def cut(array):
        return [array[h * piece : (h + 1) * piece] for h in range(CHUNKS)]

    def gather(block):
        return jnp.concatenate(line_gather(block, n, place), axis=0)

    def scatter(part):
        return line_scatter([part[k * piece : (k + 1) * piece] for k in range(n)], n)

    inputs_cut = [c.astype(F32) for c in cut(inputs)]
    first_hat, first_scale, first_rows = [], [], []
    for x in inputs_cut:
        hat, scale = layer_norm(x, epsilon)
        first_hat.append(hat)
        first_scale.append(scale)
        first_rows.append((hat * first_norm_gain).astype(BF))
    rows_one = jnp.concatenate([gather(block) for block in first_rows], axis=0)
    tokens = rows_one.shape[0]

    slot_shard = lax.rem(place - jnp.arange(n) + n, n)
    places = (
        slot_shard[None, :, None] * rows
        + jnp.arange(CHUNKS)[:, None, None] * piece
        + jnp.arange(piece)[None, None, :]
    ).reshape(tokens)
    seg = segments.reshape(n, CHUNKS, piece)[::-1]
    seg = lax.dynamic_slice_in_dim(jnp.concatenate([seg, seg], axis=0), n - 1 - place, n, axis=0)
    seg = seg.transpose(1, 0, 2).reshape(tokens)

    query_key = dot_nt(rows_one, weight_one[: 2 * nk]).astype(BF)
    value = dot_nt(rows_one, weight_one[2 * nk : 2 * nk + nv]).astype(BF)
    gate_pre = dot_nt(rows_one, weight_one[2 * nk + nv :])
    query = query_key[:, :nk].reshape(tokens, heads, HK)
    key = query_key[:, nk:].reshape(tokens, heads, HK)
    value = value.reshape(tokens, heads, HV)

    distance = places[:, None] - places[None, :]
    allowed = (distance >= 0) & (seg[:, None] == seg[None, :])
    log_gamma = jnp.log1p(-jnp.exp2(-5.0 - (head_start + jnp.arange(heads)).astype(F32)))
    exponent = jnp.where(
        allowed[None], distance[None].astype(F32) * log_gamma[:, None, None], 0.0
    )
    mask = jnp.where(allowed[None], jnp.exp(exponent), 0.0) * HK ** (-0.5)

    scores = (jnp.einsum("thk,shk->hts", query, key, preferred_element_type=F32) * mask).astype(BF)
    retained = jnp.einsum("hts,shv->thv", scores, value, preferred_element_type=F32)
    normalized, scale_group = layer_norm(retained, group_epsilon)
    normal_flat = normalized.reshape(tokens, nv)
    swish = jax.nn.silu(gate_pre)
    gated = (swish * normal_flat).astype(BF)

    cot_cut = cut(cotangent)
    cot_rows = [gather(c) for c in cot_cut]

    def group(array, h):
        return array[h * per : (h + 1) * per]

    outputs, second_gain, middle_grad = [], [], []
    rows_two, hidden_all, d_glu_all, mid_rows = [], [], [], []
    for h in range(CHUNKS):
        attn_part = dot_nn(group(gated, h), out_weight).astype(BF)
        middle = inputs_cut[h] + scatter(attn_part)
        hat, scale = layer_norm(middle, epsilon)
        rows_h = gather((hat * second_norm_gain).astype(BF))
        rows_two.append(rows_h)
        glu = dot_nt(rows_h, glu_weight)
        glu_gate, glu_up = glu[:, :nf], glu[:, nf:]
        d_hidden = dot_nt(cot_rows[h], down_weight)
        hidden, pullback = jax.vjp(glu_act, glu_gate, glu_up)
        hidden = hidden.astype(BF)
        d_glu = jnp.concatenate([d.astype(BF) for d in pullback(d_hidden)], axis=1)
        hidden_all.append(hidden)
        d_glu_all.append(d_glu)
        second_grad = scatter(dot_nn(d_glu, glu_weight).astype(BF))
        second_gain.append(jnp.sum(hat * second_grad, axis=0))
        grad_h = cot_cut[h].astype(F32) + norm_back(second_grad * second_norm_gain, hat, scale)
        middle_grad.append(grad_h)
        mid_rows.append(gather(grad_h.astype(BF)))
        outputs.append(middle + scatter(dot_nn(hidden, down_weight).astype(BF)))

    cot_all = jnp.concatenate(cot_rows, axis=0)
    grads_two = jnp.concatenate(
        [
            dot_tn(jnp.concatenate(d_glu_all, axis=0), jnp.concatenate(rows_two, axis=0)),
            dot_tn(jnp.concatenate(hidden_all, axis=0), cot_all),
        ],
        axis=0,
    ).astype(BF)
    summed_two = lax.psum_scatter(grads_two, "dp", scatter_dimension=1, tiled=True).astype(F32)

    mid_all = jnp.concatenate(mid_rows, axis=0)
    d_gated = dot_nt(mid_all, out_weight)
    sigmoid_gate = jax.nn.sigmoid(gate_pre)
    d_gate_pre = (
        d_gated * normal_flat * (sigmoid_gate + gate_pre * sigmoid_gate * (1.0 - sigmoid_gate))
    ).astype(BF)
    d_normalized = (d_gated * swish).reshape(tokens, heads, HV)
    d_retained = norm_back(d_normalized, normalized, scale_group).astype(BF)
    grads_out = jnp.concatenate(
        [dot_tn(gated, mid_all).astype(BF), dot_tn(d_gate_pre, rows_one).astype(BF)], axis=0
    )
    summed_out = lax.psum_scatter(grads_out, "dp", scatter_dimension=1, tiled=True).astype(F32)

    d_value = jnp.einsum("hts,thv->shv", scores, d_retained, preferred_element_type=F32).astype(BF)
    d_scores = (
        jnp.einsum("thv,shv->hts", d_retained, value, preferred_element_type=F32) * mask
    ).astype(BF)
    d_query = jnp.einsum("hts,shk->thk", d_scores, key, preferred_element_type=F32).astype(BF)
    d_key = jnp.einsum("hts,thk->shk", d_scores, query, preferred_element_type=F32).astype(BF)
    d_qkv = jnp.concatenate(
        [d_query.reshape(tokens, nk), d_key.reshape(tokens, nk), d_value.reshape(tokens, nv)], axis=1
    )
    grads_one = dot_tn(d_qkv, rows_one).astype(BF)
    summed_one = lax.psum_scatter(grads_one, "dp", scatter_dimension=1, tiled=True).astype(F32)

    d_one = jnp.concatenate([d_qkv, d_gate_pre], axis=1)
    input_gradient, first_gain = [], []
    for h in range(CHUNKS):
        first_grad = scatter(dot_nn(group(d_one, h), weight_one).astype(BF))
        first_gain.append(jnp.sum(first_hat[h] * first_grad, axis=0))
        input_gradient.append(
            middle_grad[h] + norm_back(first_grad * first_norm_gain, first_hat[h], first_scale[h])
        )

    gains = lax.psum(jnp.stack([sum(first_gain), sum(second_gain)]), ("dp", "mp"))
    return (
        jnp.concatenate(outputs, axis=0).astype(BF),
        jnp.concatenate(input_gradient, axis=0),
        gains[0],
        summed_one[:nk].T,
        summed_one[nk : 2 * nk].T,
        summed_one[2 * nk :].T,
        summed_out[nv:].T,
        summed_out[:nv],
        gains[1],
        summed_two[:nf].T,
        summed_two[nf : 2 * nf].T,
        summed_two[2 * nf :],
    )


def solution(mesh):
    split = P(("dp", "mp"), None)
    wide, tall = P("dp", "mp"), P("mp", "dp")
    return jax.shard_map(
        body,
        mesh=mesh,
        in_specs=(
            split, P("dp", None), P(), wide, wide, wide, wide, tall, P(), wide, wide, tall, split,
        ),
        out_specs=(
            split, split, P(), wide, wide, wide, wide, tall, P(), wide, wide, tall,
        ),
        check_vma=False,
    )
```

```python
import functools

import jax
import jax.numpy as jnp
from jax import lax
from jax.experimental import pallas as pl
from jax.experimental.pallas import tpu as pltpu
from jax.sharding import PartitionSpec as P

H = 8
HK = 256
HV = 432
LEN = 1024
CHUNKS = 2
LANES = 128
VMEM_MOST = 66_000_000

epsilon = 1e-05
group_epsilon = 1.0
BF = jnp.bfloat16
F32 = jnp.float32


def layer_norm(values_in, offset):
    centre = jnp.mean(values_in, axis=-1, keepdims=True)
    centred = values_in - centre
    variance = jnp.mean(centred * centred, axis=-1, keepdims=True)
    scaling = lax.rsqrt(variance + offset)
    return (centred * scaling, scaling)


def norm_back(grad_hat, normed_hat, scaling):
    first_mean = jnp.mean(grad_hat, axis=-1, keepdims=True)
    second_mean = jnp.mean(grad_hat * normed_hat, axis=-1, keepdims=True)
    return scaling * (grad_hat - first_mean - normed_hat * second_mean)


def glu_act(gate_pre, up_pre):
    return jax.nn.gelu(gate_pre, approximate=True) * up_pre


def dot_nt(a, b):
    return lax.dot_general(a, b, (((1,), (1,)), ((), ())), preferred_element_type=F32)


def dot_nn(a, b):
    return lax.dot_general(a, b, (((1,), (0,)), ((), ())), preferred_element_type=F32)


def dot_tn(a, b):
    return lax.dot_general(a, b, (((0,), (0,)), ((), ())), preferred_element_type=F32)


MESH = pl.DeviceIdType.MESH


class Line:
    def __init__(self, n, send_sem, recv_sem):
        self.n, self.send_sem, self.recv_sem = n, send_sem, recv_sem
        self.place = lax.axis_index("mp")
        self.used = 0
        self.sent = []

    def enter(self):
        barrier = pltpu.get_barrier_semaphore()
        n, place = self.n, self.place

        @pl.when(place >= 1)
        def _():
            pl.semaphore_signal(barrier, inc=1, device_id={"mp": place - 1}, device_id_type=MESH)

        @pl.when(place <= n - 2)
        def _():
            pl.semaphore_signal(barrier, inc=1, device_id={"mp": place + 1}, device_id_type=MESH)

        pl.semaphore_wait(barrier, jnp.minimum(place, 1) + jnp.minimum(n - 1 - place, 1))

    def copy(self, src, dst, index, toward):
        return pltpu.make_async_remote_copy(
            src_ref=src,
            dst_ref=dst,
            send_sem=self.send_sem.at[index],
            recv_sem=self.recv_sem.at[index],
            device_id={"mp": self.place + toward},
            device_id_type=MESH,
        )

    def leave(self):
        for condition, copy in self.sent:
            pl.when(condition)(copy.wait_send)


class Gather:
    def __init__(self, line, slot):
        self.line, self.slot, self.step_no = line, slot, 0
        self.base = line.used
        line.used += 2 * (line.n - 1)
        n = line.n
        self.right = [
            line.copy(slot(s - 1), slot(s), self.base + s - 1, 1) for s in range(1, n)
        ]
        self.left = [
            line.copy(slot((n - s + 1) % n), slot(n - s), self.base + n - 2 + s, -1)
            for s in range(1, n)
        ]

    def arrive(self, s):
        n, place = self.line.n, self.line.place
        pl.when(place >= s)(self.right[s - 1].wait_recv)
        pl.when(place <= n - 1 - s)(self.left[s - 1].wait_recv)

    def step(self):
        self.step_no += 1
        s, n, place = self.step_no, self.line.n, self.line.place
        if s > 1:
            self.arrive(s - 1)
        if s < n:
            to_right = (place >= s - 1) & (place <= n - 2)
            to_left = (place <= n - s) & (place >= 1)
            pl.when(to_right)(self.right[s - 1].start)
            pl.when(to_left)(self.left[s - 1].start)
            self.line.sent += [(to_right, self.right[s - 1]), (to_left, self.left[s - 1])]


class Scatter:
    def __init__(self, line, slot, from_left, from_right, add):
        self.line, self.slot, self.add, self.step_no = line, slot, add, 0
        self.from_left, self.from_right = from_left, from_right
        self.base = line.used
        line.used += 2 * (line.n - 1)
        n = line.n
        self.right = [
            line.copy(slot(s), from_left(s), self.base + s - 1, 1) for s in range(1, n)
        ]
        self.left = [
            line.copy(slot(n - s), from_right(s), self.base + n - 2 + s, -1) for s in range(1, n)
        ]
        self.mine = []

    def step(self):
        self.step_no += 1
        s, n, place = self.step_no, self.line.n, self.line.place
        to_right, to_left = place <= s - 1, place >= n - s
        if s > 1:

            @pl.when(to_right & (place >= 1))
            def _():
                self.right[s - 2].wait_recv()
                self.add(self.slot(s), self.from_left(s - 1))

            @pl.when(to_left & (place <= n - 2))
            def _():
                self.left[s - 2].wait_recv()
                self.add(self.slot(n - s), self.from_right(s - 1))

        pl.when(to_right)(self.right[s - 1].start)
        pl.when(to_left)(self.left[s - 1].start)
        self.mine += [(to_right, self.right[s - 1]), (to_left, self.left[s - 1])]

    def finish(self):
        n, place = self.line.n, self.line.place

        @pl.when(place >= 1)
        def _():
            self.right[n - 2].wait_recv()

        @pl.when(place <= n - 2)
        def _():
            self.left[n - 2].wait_recv()

    def drain(self):
        for condition, copy in self.mine:
            pl.when(condition)(copy.wait_send)


ANY = pl.BlockSpec(memory_space=pl.ANY)
VM = pl.BlockSpec(memory_space=pltpu.VMEM)
BLOCK = 16


def blocks(count, step):
    def run(i, carry):
        step(lambda base=0: pl.ds(pl.multiple_of(base + i * BLOCK, BLOCK), BLOCK))
        return carry

    lax.fori_loop(0, count // BLOCK, run, 0)


def add_into(target, extra):
    def step(at):
        target[at(), :] = (target[at(), :].astype(F32) + extra[at(), :].astype(F32)).astype(BF)

    blocks(target.shape[0], step)


def product_tiles(target, left, right, tile):
    def step(j, carry):
        at = pl.ds(pl.multiple_of(j * tile, tile), tile)
        target[:, at] = dot_nn(left[...], right[:, at]).astype(BF)
        return carry

    lax.fori_loop(0, right.shape[1] // tile, step, 0)


def gather_kernel(n, own, out, send_sem, recv_sem, copy_sem):
    line = Line(n, send_sem, recv_sem)
    piece = own.shape[0] // CHUNKS
    per = n * piece
    line.enter()
    local, gathers = [], []
    for h in range(CHUNKS):
        mine = own.at[pl.ds(h * piece, piece)]
        keep = pltpu.make_async_copy(mine, out.at[pl.ds(h * per, piece)], copy_sem.at[h])
        keep.start()
        local.append(keep)

        def slot(k, h=h, mine=mine):
            return mine if k == 0 else out.at[pl.ds(h * per + k * piece, piece)]

        gathers.append(Gather(line, slot))
    for _ in range(n):
        for g in gathers:
            g.step()
    for keep in local:
        keep.wait()
    line.leave()


def gather_rows(own, n):
    rows, width = own.shape
    count = CHUNKS * 2 * (n - 1)
    return pl.pallas_call(
        functools.partial(gather_kernel, n),
        out_shape=jax.ShapeDtypeStruct((n * rows, width), own.dtype),
        in_specs=[VM],
        out_specs=ANY,
        scratch_shapes=[
            pltpu.SemaphoreType.DMA((count,)),
            pltpu.SemaphoreType.DMA((count,)),
            pltpu.SemaphoreType.DMA((CHUNKS,)),
        ],
        compiler_params=pltpu.CompilerParams(collective_id=0, has_side_effects=True),
        name="gather_rows",
    )(own)


def no_neighbour_zero(n, place, from_left, from_right):
    @pl.when(place == 0)
    def _():
        from_left[...] = jnp.zeros_like(from_left)

    @pl.when(place == n - 1)
    def _():
        from_right[...] = jnp.zeros_like(from_right)


def middle_kernel(
    n, gated, wo, wg, wd, own, cot, gain,
    rows_out, cot_out, mid_out, hidden_out, glu_out, outputs, d_middle, gain_out,
    gated_v, wo_v, wg_v, wd_v, own_v, cot_v, rows_v, hidden_v, glu_v, part, part_two,
    left_a, right_a, left_b, right_b, middle, stage, copy_sem, send_sem, recv_sem,
):
    line = Line(n, send_sem, recv_sem)
    place = line.place
    count, width = own.shape
    piece = count // CHUNKS
    per = n * piece
    wide = hidden_v.shape[1]
    copies = []

    def local(src, dst):
        c = pltpu.make_async_copy(src, dst, copy_sem.at[len(copies)])
        copies.append(c)
        c.start()
        return c

    def rows_at(ref, h, k=0, size=piece):
        return ref.at[pl.ds(h * per + k * piece, size)]

    load_cot = [
        local(cot.at[pl.ds(h * piece, piece)], rows_at(cot_v, h)) for h in range(CHUNKS)
    ]
    load_gated = local(gated, gated_v)
    load_wo = local(wo, wo_v)
    load_own = local(own, own_v)
    load_wg = local(wg, wg_v)
    load_wd = local(wd, wd_v)
    line.enter()
    for h in range(CHUNKS):
        no_neighbour_zero(n, place, left_a.at[h, n - 2], right_a.at[h, n - 2])
        no_neighbour_zero(n, place, left_b.at[h, n - 2], right_b.at[h, n - 2])
    gain_out[...] = jnp.zeros_like(gain_out)

    def scatter(buf, lefts, rights, h):
        return Scatter(
            line,
            lambda k: rows_at(buf, h, k),
            lambda s: lefts.at[h, s - 1],
            lambda s: rights.at[h, s - 1],
            add_into,
        )

    gather_cot = [Gather(line, functools.partial(rows_at, cot_v, h)) for h in range(CHUNKS)]
    gather_two = [Gather(line, functools.partial(rows_at, rows_v, h)) for h in range(CHUNKS)]

    def mid_slot(h, k):
        return stage.at[h] if k == 0 else rows_at(mid_out, h, k)

    gather_mid = [Gather(line, functools.partial(mid_slot, h)) for h in range(CHUNKS)]
    scatter_one = [scatter(part, left_a, right_a, h) for h in range(CHUNKS)]
    scatter_two = [scatter(part_two, left_b, right_b, h) for h in range(CHUNKS)]
    scatter_grad = [scatter(part, left_a, right_a, h) for h in range(CHUNKS)]

    def chunk(ref, h):
        return ref.at[pl.ds(h * per, per)]

    def out_product(h):
        product_tiles(chunk(part, h), chunk(gated_v, h), wo_v, 2 * LANES)

    def finish_one(h):
        scatter_one[h].finish()

        def step(at):
            src = at(h * per)
            mine = at(h * piece)
            total = (
                own_v[mine, :].astype(F32)
                + part[src, :].astype(F32)
                + left_a[h, n - 2, at(), :].astype(F32)
                + right_a[h, n - 2, at(), :].astype(F32)
            )
            middle[mine, :] = total
            hat, _ = layer_norm(total, epsilon)
            rows_v[src, :] = (hat * gain[...]).astype(BF)

        blocks(piece, step)

    def glu_tiles(h, first, last):
        def step(j, carry):
            pair = pl.ds(pl.multiple_of(j * 2 * LANES, 2 * LANES), 2 * LANES)
            at = pl.ds(pl.multiple_of(j * LANES, LANES), LANES)
            whole = pl.ds(h * per, per)
            both = dot_nt(rows_v[whole, :], wg_v[pair, :])
            d_hidden = dot_nt(cot_v[whole, :], wd_v[at, :])
            u, up = both[:, :LANES], both[:, LANES:]
            c = 0.7978845608028654
            t = jnp.tanh(c * (u + 0.044715 * (u * u * u)))
            half = 0.5 * (1.0 + t)
            act = u * half
            slope = half + 0.5 * u * (1.0 - t * t) * (c * (1.0 + 3 * 0.044715 * (u * u)))
            hidden_v[whole, at] = (act * up).astype(BF)
            glu_v[whole, pair] = jnp.concatenate(
                [(d_hidden * up * slope).astype(BF), (d_hidden * act).astype(BF)], axis=1
            )
            return carry

        lax.fori_loop(first, last, step, 0)

    def grad_product(h):
        product_tiles(chunk(part, h), chunk(glu_v, h), wg_v, 2 * LANES)

    def down_product(h):
        product_tiles(chunk(part_two, h), chunk(hidden_v, h), wd_v, 2 * LANES)

    def finish_grad(h):
        scatter_grad[h].finish()

        def step(at):
            src = at(h * per)
            mine = at(h * piece)
            grad = (
                part[src, :].astype(F32)
                + left_a[h, n - 2, at(), :].astype(F32)
                + right_a[h, n - 2, at(), :].astype(F32)
            )
            hat, scale = layer_norm(middle[mine, :], epsilon)
            gain_out[...] += jnp.sum((hat * grad).reshape(BLOCK // 8, 8, width), axis=0)
            d_mid = cot_v[src, :].astype(F32) + norm_back(grad * gain[...], hat, scale)
            d_middle[mine, :] = d_mid
            stage[h, at(), :] = d_mid.astype(BF)

        blocks(piece, step)
        local(stage.at[h], rows_at(mid_out, h))

    def finish_two(h):
        scatter_two[h].finish()

        def step(at):
            src = at(h * per)
            mine = at(h * piece)
            outputs[mine, :] = (
                middle[mine, :]
                + part_two[src, :].astype(F32)
                + left_b[h, n - 2, at(), :].astype(F32)
                + right_b[h, n - 2, at(), :].astype(F32)
            ).astype(BF)

        blocks(piece, step)

    assert CHUNKS == 2
    tiles = wide // LANES
    cut = tiles // 2
    cot_a, cot_b = gather_cot
    two_a, two_b = gather_two
    mid_a, mid_b = gather_mid
    one_a, one_b = scatter_one
    grad_a, grad_b = scatter_grad
    down_a, down_b = scatter_two

    load_cot[0].wait()
    load_cot[1].wait()
    cot_a.step()
    load_gated.wait()
    load_wo.wait()
    out_product(0)
    one_a.step()
    out_product(1)
    one_b.step()
    for i in range(n - 2):
        one_a.step()
        if i > 0:
            one_b.step()
        cot_a.step()
    load_own.wait()
    finish_one(0)
    two_a.step()
    one_b.step()
    cot_a.step()
    two_a.step()
    finish_one(1)
    two_b.step()
    for _ in range(n - 3):
        two_a.step()
        two_b.step()
    load_wg.wait()
    load_wd.wait()
    two_a.step()
    cot_b.step()
    glu_tiles(0, 0, cut)
    two_b.step()
    cot_b.step()
    glu_tiles(0, cut, tiles)
    for _ in range(n - 3):
        cot_b.step()
    one_a.drain()
    grad_product(0)
    grad_a.step()
    down_product(0)
    grad_a.step()
    two_b.step()
    cot_b.step()
    one_b.drain()
    down_a.step()
    glu_tiles(1, 0, cut)
    for _ in range(n - 3):
        grad_a.step()
    down_a.step()
    glu_tiles(1, cut, tiles)
    finish_grad(0)
    mid_a.step()
    grad_product(1)
    grad_b.step()
    mid_a.step()
    down_product(1)
    grad_b.step()
    for _ in range(n - 3):
        grad_b.step()
        mid_a.step()
        down_a.step()
    down_b.step()
    finish_grad(1)
    mid_b.step()
    mid_a.step()
    for c in range(CHUNKS):
        local(chunk(rows_v, c), chunk(rows_out, c))
        local(chunk(cot_v, c), chunk(cot_out, c))
        local(chunk(hidden_v, c), chunk(hidden_out, c))
        local(chunk(glu_v, c), chunk(glu_out, c))
    finish_two(0)
    for _ in range(n - 2):
        mid_b.step()
        down_b.step()
    mid_b.step()
    finish_two(1)
    for item in gather_cot + gather_two + gather_mid:
        assert item.step_no == n
    for item in scatter_one + scatter_two + scatter_grad:
        assert item.step_no == n - 1
    for group in (scatter_grad, scatter_two):
        for item in group:
            item.drain()
    for item in copies[2 + 5 :]:
        item.wait()
    line.leave()


def middle_call(gated, wo, wg, wd, own, cot, gain, n):
    rows, width = own.shape
    tokens, nv = gated.shape
    wide = wd.shape[0]
    piece = rows // CHUNKS
    sems = CHUNKS * 6 * 2 * (n - 1)
    hop = (CHUNKS, n - 1, piece, width)
    shape = jax.ShapeDtypeStruct
    return pl.pallas_call(
        functools.partial(middle_kernel, n),
        out_shape=(
            shape((tokens, width), BF),
            shape((tokens, width), BF),
            shape((tokens, width), BF),
            shape((tokens, wide), BF),
            shape((tokens, 2 * wide), BF),
            shape((rows, width), BF),
            shape((rows, width), F32),
            shape((8, width), F32),
        ),
        in_specs=[ANY] * 6 + [VM],
        out_specs=(ANY,) * 5 + (VM,) * 3,
        scratch_shapes=[
            pltpu.VMEM((tokens, nv), BF),
            pltpu.VMEM((nv, width), BF),
            pltpu.VMEM((2 * wide, width), BF),
            pltpu.VMEM((wide, width), BF),
            pltpu.VMEM((rows, width), BF),
            pltpu.VMEM((tokens, width), BF),
            pltpu.VMEM((tokens, width), BF),
            pltpu.VMEM((tokens, wide), BF),
            pltpu.VMEM((tokens, 2 * wide), BF),
            pltpu.VMEM((tokens, width), BF),
            pltpu.VMEM((tokens, width), BF),
            pltpu.VMEM(hop, BF),
            pltpu.VMEM(hop, BF),
            pltpu.VMEM(hop, BF),
            pltpu.VMEM(hop, BF),
            pltpu.VMEM((rows, width), F32),
            pltpu.VMEM((CHUNKS, piece, width), BF),
            pltpu.SemaphoreType.DMA((7 + 5 * CHUNKS,)),
            pltpu.SemaphoreType.DMA((sems,)),
            pltpu.SemaphoreType.DMA((sems,)),
        ],
        compiler_params=pltpu.CompilerParams(
            collective_id=1, has_side_effects=True, vmem_limit_bytes=VMEM_MOST
        ),
        name="middle",
    )(gated, wo, wg, wd, own, cot, gain)


def last_kernel(
    n, grads, weight, out, grads_v, weight_v, part, lefts, rights, copy_sem, send_sem, recv_sem
):
    line = Line(n, send_sem, recv_sem)
    count, width = out.shape
    piece = count // CHUNKS
    per = n * piece
    load = [
        pltpu.make_async_copy(
            grads.at[pl.ds(h * per, per)], grads_v.at[pl.ds(h * per, per)], copy_sem.at[h]
        )
        for h in range(CHUNKS)
    ]
    load_weight = pltpu.make_async_copy(weight, weight_v, copy_sem.at[CHUNKS])
    for item in load + [load_weight]:
        item.start()
    line.enter()
    for h in range(CHUNKS):
        no_neighbour_zero(n, line.place, lefts.at[h, n - 2], rights.at[h, n - 2])
    scatters = [
        Scatter(
            line,
            lambda k, h=h: part.at[pl.ds(h * per + k * piece, piece)],
            lambda s, h=h: lefts.at[h, s - 1],
            lambda s, h=h: rights.at[h, s - 1],
            add_into,
        )
        for h in range(CHUNKS)
    ]

    def finish(h):
        scatters[h].finish()

        def step(at):
            src = at(h * per)
            out[at(h * piece), :] = (
                part[src, :].astype(F32)
                + lefts[h, n - 2, at(), :].astype(F32)
                + rights[h, n - 2, at(), :].astype(F32)
            )

        blocks(piece, step)

    load_weight.wait()
    for h in range(CHUNKS):
        load[h].wait()
        rows = pl.ds(h * per, per)
        product_tiles(part.at[rows], grads_v.at[rows], weight_v, 2 * LANES)
        scatters[h].step()
    for _ in range(n - 2):
        for h in range(CHUNKS):
            scatters[h].step()
    for h in range(CHUNKS):
        finish(h)
    for h in range(CHUNKS):
        scatters[h].drain()


def last_call(grads, weight, n):
    tokens, deep = grads.shape
    width = weight.shape[1]
    rows = tokens // n
    sems = CHUNKS * 2 * (n - 1)
    hop = (CHUNKS, n - 1, rows // CHUNKS, width)
    return pl.pallas_call(
        functools.partial(last_kernel, n),
        out_shape=jax.ShapeDtypeStruct((rows, width), F32),
        in_specs=[ANY, ANY],
        out_specs=VM,
        scratch_shapes=[
            pltpu.VMEM((tokens, deep), BF),
            pltpu.VMEM((deep, width), BF),
            pltpu.VMEM((tokens, width), BF),
            pltpu.VMEM(hop, BF),
            pltpu.VMEM(hop, BF),
            pltpu.SemaphoreType.DMA((CHUNKS + 1,)),
            pltpu.SemaphoreType.DMA((sems,)),
            pltpu.SemaphoreType.DMA((sems,)),
        ],
        compiler_params=pltpu.CompilerParams(
            collective_id=2, has_side_effects=True, vmem_limit_bytes=VMEM_MOST
        ),
        name="last",
    )(grads, weight)


def pad_rows(array, count):
    return jnp.pad(array, ((0, count - array.shape[0]), (0, 0)))


def pad_columns(array, count):
    return jnp.pad(array, ((0, 0), (0, count - array.shape[1])))


def body(
    inputs,
    segments,
    first_norm_gain,
    w_query,
    w_key,
    w_value,
    w_gate,
    w_out,
    second_norm_gain,
    w_glu_gate,
    w_glu_up,
    w_down,
    cotangent,
):
    n = lax.axis_size("mp")
    place = lax.axis_index("mp")
    heads = H // n
    head_start = place * heads
    rows, width = inputs.shape
    shard = w_query.shape[0]
    piece = rows // CHUNKS
    nk, nv, nf = heads * HK, heads * HV, w_down.shape[0]
    n_one = 2 * nk + 2 * nv
    one_wide = -(-n_one // (2 * LANES)) * 2 * LANES
    v_wide, f_wide = -(-nv // LANES) * LANES, -(-nf // LANES) * LANES
    f_tiles = f_wide // LANES

    pack_one = pad_rows(
        jnp.concatenate([w_query.T, w_key.T, w_value.T, w_gate.T], axis=0), one_wide
    )
    weight_one = lax.all_gather(pack_one, "dp", axis=1, tiled=True)
    out_weight = lax.all_gather(pad_rows(w_out, v_wide), "dp", axis=1, tiled=True)
    glu_pack = jnp.stack(
        [
            pad_rows(w_glu_gate.T, f_wide).reshape(f_tiles, LANES, shard),
            pad_rows(w_glu_up.T, f_wide).reshape(f_tiles, LANES, shard),
        ],
        axis=1,
    ).reshape(2 * f_wide, shard)
    pack_two = jnp.concatenate([glu_pack, pad_rows(w_down, f_wide)], axis=0)
    weight_two = lax.all_gather(pack_two, "dp", axis=1, tiled=True)
    glu_weight, down_weight = weight_two[: 2 * f_wide], weight_two[2 * f_wide :]

    first_hat, first_scale = layer_norm(inputs.astype(F32), epsilon)
    rows_one = gather_rows((first_hat * first_norm_gain).astype(BF), n)
    tokens = rows_one.shape[0]

    slot_shard = lax.rem(place - jnp.arange(n) + n, n)
    places = (
        slot_shard[None, :, None] * rows
        + jnp.arange(CHUNKS)[:, None, None] * piece
        + jnp.arange(piece)[None, None, :]
    ).reshape(tokens)
    seg = segments.reshape(n, CHUNKS, piece)[::-1]
    seg = lax.dynamic_slice_in_dim(jnp.concatenate([seg, seg], axis=0), n - 1 - place, n, axis=0)
    seg = seg.transpose(1, 0, 2).reshape(tokens)

    query_key = dot_nt(rows_one, weight_one[: 2 * nk]).astype(BF)
    value = dot_nt(rows_one, weight_one[2 * nk : 2 * nk + nv]).astype(BF)
    gate_pre = dot_nt(rows_one, weight_one[2 * nk + nv : n_one])
    query = query_key[:, :nk].reshape(tokens, heads, HK)
    key = query_key[:, nk:].reshape(tokens, heads, HK)
    value = value.reshape(tokens, heads, HV)

    distance = places[:, None] - places[None, :]
    allowed = (distance >= 0) & (seg[:, None] == seg[None, :])
    log_gamma = jnp.log1p(-jnp.exp2(-5.0 - (head_start + jnp.arange(heads)).astype(F32)))
    exponent = jnp.where(
        allowed[None], distance[None].astype(F32) * log_gamma[:, None, None], 0.0
    )
    mask = jnp.where(allowed[None], jnp.exp(exponent), 0.0) * HK ** (-0.5)

    scores = (jnp.einsum("thk,shk->hts", query, key, preferred_element_type=F32) * mask).astype(BF)
    retained = jnp.einsum("hts,shv->thv", scores, value, preferred_element_type=F32)
    normalized, scale_group = layer_norm(retained, group_epsilon)
    normal_flat = normalized.reshape(tokens, nv)
    swish = jax.nn.silu(gate_pre)
    gated = pad_columns((swish * normal_flat).astype(BF), v_wide)

    rows_two, cot_rows, mid_rows, hidden, d_glu, outputs, middle_grad, second_gain = middle_call(
        gated, out_weight, glu_weight, down_weight, inputs, cotangent, second_norm_gain[None], n
    )

    grads_two = jnp.concatenate([dot_tn(d_glu, rows_two), dot_tn(hidden, cot_rows)], axis=0).astype(BF)
    summed_two = lax.psum_scatter(grads_two, "dp", scatter_dimension=1, tiled=True).astype(F32)
    glu_sum = summed_two[: 2 * f_wide].reshape(f_tiles, 2, LANES, shard)

    d_gated = dot_nt(mid_rows, out_weight[:nv])
    sigmoid_gate = jax.nn.sigmoid(gate_pre)
    d_gate_pre = (
        d_gated * normal_flat * (sigmoid_gate + gate_pre * sigmoid_gate * (1.0 - sigmoid_gate))
    ).astype(BF)
    d_normalized = (d_gated * swish).reshape(tokens, heads, HV)
    d_retained = norm_back(d_normalized, normalized, scale_group).astype(BF)
    grads_out = jnp.concatenate(
        [dot_tn(gated[:, :nv], mid_rows).astype(BF), dot_tn(d_gate_pre, rows_one).astype(BF)], axis=0
    )
    summed_out = lax.psum_scatter(grads_out, "dp", scatter_dimension=1, tiled=True).astype(F32)

    d_value = jnp.einsum("hts,thv->shv", scores, d_retained, preferred_element_type=F32).astype(BF)
    d_scores = (
        jnp.einsum("thv,shv->hts", d_retained, value, preferred_element_type=F32) * mask
    ).astype(BF)
    d_query = jnp.einsum("hts,shk->thk", d_scores, key, preferred_element_type=F32).astype(BF)
    d_key = jnp.einsum("hts,thk->shk", d_scores, query, preferred_element_type=F32).astype(BF)
    d_qkv = jnp.concatenate(
        [d_query.reshape(tokens, nk), d_key.reshape(tokens, nk), d_value.reshape(tokens, nv)], axis=1
    )
    grads_one = dot_tn(d_qkv, rows_one).astype(BF)
    summed_one = lax.psum_scatter(grads_one, "dp", scatter_dimension=1, tiled=True).astype(F32)

    d_one = pad_columns(jnp.concatenate([d_qkv, d_gate_pre], axis=1), one_wide)
    first_grad = last_call(d_one, weight_one, n)
    first_gain = jnp.sum(first_hat * first_grad, axis=0)
    input_gradient = middle_grad + norm_back(first_grad * first_norm_gain, first_hat, first_scale)

    gains = lax.psum(jnp.stack([first_gain, jnp.sum(second_gain, axis=0)]), ("dp", "mp"))
    return (
        outputs,
        input_gradient,
        gains[0],
        summed_one[:nk].T,
        summed_one[nk : 2 * nk].T,
        summed_one[2 * nk :].T,
        summed_out[nv:].T,
        summed_out[:nv],
        gains[1],
        glu_sum[:, 0].reshape(f_wide, shard)[:nf].T,
        glu_sum[:, 1].reshape(f_wide, shard)[:nf].T,
        summed_two[2 * f_wide : 2 * f_wide + nf],
    )


def solution(mesh):
    split = P(("dp", "mp"), None)
    wide, tall = P("dp", "mp"), P("mp", "dp")
    return jax.shard_map(
        body,
        mesh=mesh,
        in_specs=(
            split, P("dp", None), P(), wide, wide, wide, wide, tall, P(), wide, wide, tall, split,
        ),
        out_specs=(
            split, split, P(), wide, wide, wide, wide, tall, P(), wide, wide, tall,
        ),
        check_vma=False,
    )
```

```python
import functools

import jax
import jax.numpy as jnp
from jax import lax
from jax.experimental import pallas as pl
from jax.experimental.pallas import tpu as pltpu
from jax.sharding import PartitionSpec as P

H = 8
HK = 256
HV = 432
LEN = 1024
CHUNKS = 4
LANES = 128
VMEM_MOST = 66_000_000

epsilon = 1e-05
group_epsilon = 1.0
BF = jnp.bfloat16
F32 = jnp.float32


def layer_norm(values_in, offset):
    centre = jnp.mean(values_in, axis=-1, keepdims=True)
    centred = values_in - centre
    variance = jnp.mean(centred * centred, axis=-1, keepdims=True)
    scaling = lax.rsqrt(variance + offset)
    return (centred * scaling, scaling)


def norm_back(grad_hat, normed_hat, scaling):
    first_mean = jnp.mean(grad_hat, axis=-1, keepdims=True)
    second_mean = jnp.mean(grad_hat * normed_hat, axis=-1, keepdims=True)
    return scaling * (grad_hat - first_mean - normed_hat * second_mean)


def glu_act(gate_pre, up_pre):
    return jax.nn.gelu(gate_pre, approximate=True) * up_pre


def dot_nt(a, b):
    return lax.dot_general(a, b, (((1,), (1,)), ((), ())), preferred_element_type=F32)


def dot_nn(a, b):
    return lax.dot_general(a, b, (((1,), (0,)), ((), ())), preferred_element_type=F32)


def dot_tn(a, b):
    return lax.dot_general(a, b, (((0,), (0,)), ((), ())), preferred_element_type=F32)


MESH = pl.DeviceIdType.MESH


class Line:
    def __init__(self, n, send_sem, recv_sem):
        self.n, self.send_sem, self.recv_sem = n, send_sem, recv_sem
        self.place = lax.axis_index("mp")
        self.used = 0
        self.sent = []

    def enter(self):
        barrier = pltpu.get_barrier_semaphore()
        n, place = self.n, self.place

        @pl.when(place >= 1)
        def _():
            pl.semaphore_signal(barrier, inc=1, device_id={"mp": place - 1}, device_id_type=MESH)

        @pl.when(place <= n - 2)
        def _():
            pl.semaphore_signal(barrier, inc=1, device_id={"mp": place + 1}, device_id_type=MESH)

        pl.semaphore_wait(barrier, jnp.minimum(place, 1) + jnp.minimum(n - 1 - place, 1))

    def copy(self, src, dst, index, toward):
        return pltpu.make_async_remote_copy(
            src_ref=src,
            dst_ref=dst,
            send_sem=self.send_sem.at[index],
            recv_sem=self.recv_sem.at[index],
            device_id={"mp": self.place + toward},
            device_id_type=MESH,
        )

    def leave(self):
        for condition, copy in self.sent:
            pl.when(condition)(copy.wait_send)


class Gather:
    def __init__(self, line, slot):
        self.line, self.slot, self.step_no = line, slot, 0
        self.base = line.used
        line.used += 2 * (line.n - 1)
        n = line.n
        self.right = [
            line.copy(slot(s - 1), slot(s), self.base + s - 1, 1) for s in range(1, n)
        ]
        self.left = [
            line.copy(slot((n - s + 1) % n), slot(n - s), self.base + n - 2 + s, -1)
            for s in range(1, n)
        ]

    def arrive(self, s):
        n, place = self.line.n, self.line.place
        pl.when(place >= s)(self.right[s - 1].wait_recv)
        pl.when(place <= n - 1 - s)(self.left[s - 1].wait_recv)

    def step(self):
        self.step_no += 1
        s, n, place = self.step_no, self.line.n, self.line.place
        if s > 1:
            self.arrive(s - 1)
        if s < n:
            to_right = (place >= s - 1) & (place <= n - 2)
            to_left = (place <= n - s) & (place >= 1)
            pl.when(to_right)(self.right[s - 1].start)
            pl.when(to_left)(self.left[s - 1].start)
            self.line.sent += [(to_right, self.right[s - 1]), (to_left, self.left[s - 1])]


class Scatter:
    def __init__(self, line, slot, from_left, from_right, add):
        self.line, self.slot, self.add, self.step_no = line, slot, add, 0
        self.from_left, self.from_right = from_left, from_right
        self.base = line.used
        line.used += 2 * (line.n - 1)
        n = line.n
        self.right = [
            line.copy(slot(s), from_left(s), self.base + s - 1, 1) for s in range(1, n)
        ]
        self.left = [
            line.copy(slot(n - s), from_right(s), self.base + n - 2 + s, -1) for s in range(1, n)
        ]
        self.mine = []

    def step(self):
        self.step_no += 1
        s, n, place = self.step_no, self.line.n, self.line.place
        to_right, to_left = place <= s - 1, place >= n - s
        if s > 1:

            @pl.when(to_right & (place >= 1))
            def _():
                self.right[s - 2].wait_recv()
                self.add(self.slot(s), self.from_left(s - 1))

            @pl.when(to_left & (place <= n - 2))
            def _():
                self.left[s - 2].wait_recv()
                self.add(self.slot(n - s), self.from_right(s - 1))

        pl.when(to_right)(self.right[s - 1].start)
        pl.when(to_left)(self.left[s - 1].start)
        self.mine += [(to_right, self.right[s - 1]), (to_left, self.left[s - 1])]

    def finish(self):
        n, place = self.line.n, self.line.place

        @pl.when(place >= 1)
        def _():
            self.right[n - 2].wait_recv()

        @pl.when(place <= n - 2)
        def _():
            self.left[n - 2].wait_recv()

    def drain(self):
        for condition, copy in self.mine:
            pl.when(condition)(copy.wait_send)


ANY = pl.BlockSpec(memory_space=pl.ANY)
VM = pl.BlockSpec(memory_space=pltpu.VMEM)
BLOCK = 16


def blocks(count, step):
    def run(i, carry):
        step(lambda base=0: pl.ds(pl.multiple_of(base + i * BLOCK, BLOCK), BLOCK))
        return carry

    lax.fori_loop(0, count // BLOCK, run, 0)


def add_into(target, extra):
    def step(at):
        target[at(), :] = (target[at(), :].astype(F32) + extra[at(), :].astype(F32)).astype(BF)

    blocks(target.shape[0], step)


def product_tiles(target, left, right, tile):
    def step(j, carry):
        at = pl.ds(pl.multiple_of(j * tile, tile), tile)
        target[:, at] = dot_nn(left[...], right[:, at]).astype(BF)
        return carry

    lax.fori_loop(0, right.shape[1] // tile, step, 0)


def gather_kernel(n, own, out, send_sem, recv_sem, copy_sem):
    line = Line(n, send_sem, recv_sem)
    piece = own.shape[0] // CHUNKS
    per = n * piece
    line.enter()
    local, gathers = [], []
    for h in range(CHUNKS):
        mine = own.at[pl.ds(h * piece, piece)]
        keep = pltpu.make_async_copy(mine, out.at[pl.ds(h * per, piece)], copy_sem.at[h])
        keep.start()
        local.append(keep)

        def slot(k, h=h, mine=mine):
            return mine if k == 0 else out.at[pl.ds(h * per + k * piece, piece)]

        gathers.append(Gather(line, slot))
    for _ in range(n):
        for g in gathers:
            g.step()
    for keep in local:
        keep.wait()
    line.leave()


def gather_rows(own, n):
    rows, width = own.shape
    count = CHUNKS * 2 * (n - 1)
    return pl.pallas_call(
        functools.partial(gather_kernel, n),
        out_shape=jax.ShapeDtypeStruct((n * rows, width), own.dtype),
        in_specs=[VM],
        out_specs=ANY,
        scratch_shapes=[
            pltpu.SemaphoreType.DMA((count,)),
            pltpu.SemaphoreType.DMA((count,)),
            pltpu.SemaphoreType.DMA((CHUNKS,)),
        ],
        compiler_params=pltpu.CompilerParams(collective_id=0, has_side_effects=True),
        name="gather_rows",
    )(own)


def no_neighbour_zero(n, place, from_left, from_right):
    @pl.when(place == 0)
    def _():
        from_left[...] = jnp.zeros_like(from_left)

    @pl.when(place == n - 1)
    def _():
        from_right[...] = jnp.zeros_like(from_right)


(COT, OUT, ONE, END_ONE, TWO, GLU, GRAD, GRAD_SUM, END_GRAD, MID, DOWN, DOWN_SUM, END_DOWN) = range(13)

DUE = {
    OUT: (-2.23, 1.66, 0), ONE: (-1.99, 1.12, 1.03), END_ONE: (1.46, 1.37, 0), TWO: (0.73, 1.15, 0.94),
    COT: (0.35, 1.39, 1.02), GLU: (1.14, -1.37, 1.55), GRAD: (3.09, 2.02, 0),
    GRAD_SUM: (3.48, 1.71, 0.74), END_GRAD: (7.02, -2.12, 0), MID: (5.68, 0.86, 1.11),
    DOWN: (1.3, 0.36, 0), DOWN_SUM: (1.87, 1.35, 0.95), END_DOWN: (7.9, 2.17, 0),
}
TUNED = {
    (4, 4): [
        0, 4, 8, 0, 5, 8, 1, 0, 8, 9, 6, 1, 12, 9, 16, 9, 10, 16, 0, 3,
        10, 16, 7, 11, 1, 13, 17, 16, 20, 10, 20, 11, 1, 17, 40, 14, 2, 11, 18, 24,
        17, 2, 28, 44, 15, 19, 17, 21, 2, 18, 28, 44, 21, 41, 18, 19, 3, 2, 45, 28,
        25, 29, 18, 45, 22, 3, 29, 22, 42, 29, 32, 19, 46, 26, 36, 46, 3, 33, 19, 44,
        30, 23, 36, 23, 37, 45, 30, 46, 30, 37, 43, 27, 31, 47, 36, 34, 38, 36, 31, 47,
        50, 37, 37, 38, 31, 48, 47, 35, 38, 39, 49, 39, 38, 39, 51, 39,
    ],
}


def middle_order(n):
    if (n, CHUNKS) in TUNED:
        return [divmod(code, CHUNKS) for code in TUNED[n, CHUNKS]]
    count = {k: 1 for k in DUE}
    count.update({COT: n, TWO: n, MID: n, ONE: n - 1, GRAD_SUM: n - 1, DOWN_SUM: n - 1, GLU: 2})
    needs = {
        ONE: [OUT], END_ONE: [ONE], TWO: [END_ONE], GLU: [TWO, COT], GRAD: [GLU], GRAD_SUM: [GRAD],
        END_GRAD: [GRAD_SUM], MID: [END_GRAD], DOWN: [GLU], DOWN_SUM: [DOWN], END_DOWN: [DOWN_SUM],
    }
    todo = sorted(
        (first + h * later + s * 3 / (n - 1) * each, k, h, s)
        for k, (first, later, each) in DUE.items()
        for h in range(CHUNKS)
        for s in range(count[k])
    )
    taken, order = {}, []
    while todo:
        for item in todo:
            _, k, h, s = item
            ready = taken.get((k, h), 0) == s and all(
                taken.get((need, h), 0) == count[need] for need in needs.get(k, [])
            )
            if ready:
                break
        todo.remove(item)
        taken[k, h] = s + 1
        order.append((k, h))
    return order


def middle_kernel(
    n, gated, weights, own, cot, gain,
    rows_out, cot_out, mid_out, hidden_out, glu_out, outputs, d_middle, gain_out,
    gated_v, wo_v, wg_v, wd_v, own_v, cot_v, rows_v, hidden_v, glu_v, part, part_two,
    left_a, right_a, left_b, right_b, middle, stage, copy_sem, send_sem, recv_sem,
):
    line = Line(n, send_sem, recv_sem)
    place = line.place
    count, width = own.shape
    piece = count // CHUNKS
    per = n * piece
    wide = hidden_v.shape[1]
    copies = []

    def local(src, dst):
        c = pltpu.make_async_copy(src, dst, copy_sem.at[len(copies)])
        copies.append(c)
        c.start()
        return c

    def rows_at(ref, h, k=0, size=piece):
        return ref.at[pl.ds(h * per + k * piece, size)]

    load_cot = [
        local(cot.at[pl.ds(h * piece, piece)], rows_at(cot_v, h)) for h in range(CHUNKS)
    ]
    load_gated = local(gated, gated_v)
    load_wo = local(weights.at[pl.ds(3 * wide, wo_v.shape[0])], wo_v)
    load_own = local(own, own_v)
    load_wg = local(weights.at[pl.ds(0, 2 * wide)], wg_v)
    load_wd = local(weights.at[pl.ds(2 * wide, wide)], wd_v)
    line.enter()
    for h in range(CHUNKS):
        no_neighbour_zero(n, place, left_a.at[h, n - 2], right_a.at[h, n - 2])
        no_neighbour_zero(n, place, left_b.at[h, n - 2], right_b.at[h, n - 2])
    gain_out[...] = jnp.zeros_like(gain_out)

    def scatter(buf, lefts, rights, h):
        return Scatter(
            line,
            lambda k: rows_at(buf, h, k),
            lambda s: lefts.at[h, s - 1],
            lambda s: rights.at[h, s - 1],
            add_into,
        )

    gather_cot = [Gather(line, functools.partial(rows_at, cot_v, h)) for h in range(CHUNKS)]
    gather_two = [Gather(line, functools.partial(rows_at, rows_v, h)) for h in range(CHUNKS)]

    def mid_slot(h, k):
        return stage.at[h] if k == 0 else rows_at(mid_out, h, k)

    gather_mid = [Gather(line, functools.partial(mid_slot, h)) for h in range(CHUNKS)]
    scatter_one = [scatter(part, left_a, right_a, h) for h in range(CHUNKS)]
    scatter_two = [scatter(part_two, left_b, right_b, h) for h in range(CHUNKS)]
    scatter_grad = [scatter(part, left_a, right_a, h) for h in range(CHUNKS)]

    def chunk(ref, h):
        return ref.at[pl.ds(h * per, per)]

    def out_product(h):
        product_tiles(chunk(part, h), chunk(gated_v, h), wo_v, 2 * LANES)

    def finish_one(h):
        scatter_one[h].finish()

        def step(at):
            src = at(h * per)
            mine = at(h * piece)
            total = (
                own_v[mine, :].astype(F32)
                + part[src, :].astype(F32)
                + left_a[h, n - 2, at(), :].astype(F32)
                + right_a[h, n - 2, at(), :].astype(F32)
            )
            middle[mine, :] = total
            hat, _ = layer_norm(total, epsilon)
            rows_v[src, :] = (hat * gain[...]).astype(BF)

        blocks(piece, step)

    def glu_tiles(h, first, last):
        def step(j, carry):
            pair = pl.ds(pl.multiple_of(j * 2 * LANES, 2 * LANES), 2 * LANES)
            at = pl.ds(pl.multiple_of(j * LANES, LANES), LANES)
            whole = pl.ds(h * per, per)
            both = dot_nt(rows_v[whole, :], wg_v[pair, :])
            d_hidden = dot_nt(cot_v[whole, :], wd_v[at, :])
            u, up = both[:, :LANES], both[:, LANES:]
            c = 0.7978845608028654
            t = jnp.tanh(c * (u + 0.044715 * (u * u * u)))
            half = 0.5 * (1.0 + t)
            act = u * half
            slope = half + 0.5 * u * (1.0 - t * t) * (c * (1.0 + 3 * 0.044715 * (u * u)))
            hidden_v[whole, at] = (act * up).astype(BF)
            glu_v[whole, pair] = jnp.concatenate(
                [(d_hidden * up * slope).astype(BF), (d_hidden * act).astype(BF)], axis=1
            )
            return carry

        lax.fori_loop(first, last, step, 0)

    def grad_product(h):
        product_tiles(chunk(part, h), chunk(glu_v, h), wg_v, 2 * LANES)

    def down_product(h):
        product_tiles(chunk(part_two, h), chunk(hidden_v, h), wd_v, 2 * LANES)

    def finish_grad(h):
        scatter_grad[h].finish()

        def step(at):
            src = at(h * per)
            mine = at(h * piece)
            grad = (
                part[src, :].astype(F32)
                + left_a[h, n - 2, at(), :].astype(F32)
                + right_a[h, n - 2, at(), :].astype(F32)
            )
            hat, scale = layer_norm(middle[mine, :], epsilon)
            gain_out[...] += jnp.sum((hat * grad).reshape(BLOCK // 8, 8, width), axis=0)
            d_mid = cot_v[src, :].astype(F32) + norm_back(grad * gain[...], hat, scale)
            d_middle[mine, :] = d_mid
            stage[h, at(), :] = d_mid.astype(BF)

        blocks(piece, step)
        local(stage.at[h], rows_at(mid_out, h))

    def finish_two(h):
        scatter_two[h].finish()

        def step(at):
            src = at(h * per)
            mine = at(h * piece)
            outputs[mine, :] = (
                middle[mine, :]
                + part_two[src, :].astype(F32)
                + left_b[h, n - 2, at(), :].astype(F32)
                + right_b[h, n - 2, at(), :].astype(F32)
            ).astype(BF)

        blocks(piece, step)

    tiles = wide // LANES
    cut = tiles // 2

    def wait_for(items):
        for item in items:
            item.wait()
        items.clear()

    first_loads, own_load = [load_gated, load_wo], [load_own]
    later_loads = [load_wg, load_wd]

    def out_action(h):
        wait_for(first_loads)
        out_product(h)

    def finish_one_action(h):
        wait_for(own_load)
        finish_one(h)

    def glu_action(h):
        wait_for(later_loads)
        if h in begun:
            glu_tiles(h, cut, tiles)
        else:
            begun.add(h)
            glu_tiles(h, 0, cut)

    def grad_action(h):
        scatter_one[h].drain()
        grad_product(h)

    begun = set()
    actions = {
        COT: lambda h: gather_cot[h].step(),
        OUT: out_action,
        ONE: lambda h: scatter_one[h].step(),
        END_ONE: finish_one_action,
        TWO: lambda h: gather_two[h].step(),
        GLU: glu_action,
        GRAD: grad_action,
        GRAD_SUM: lambda h: scatter_grad[h].step(),
        END_GRAD: finish_grad,
        MID: lambda h: gather_mid[h].step(),
        DOWN: down_product,
        DOWN_SUM: lambda h: scatter_two[h].step(),
        END_DOWN: finish_two,
    }
    for item in load_cot:
        item.wait()
    for kind, h in middle_order(n):
        actions[kind](h)
    for c in range(CHUNKS):
        local(chunk(rows_v, c), chunk(rows_out, c))
        local(chunk(cot_v, c), chunk(cot_out, c))
        local(chunk(hidden_v, c), chunk(hidden_out, c))
        local(chunk(glu_v, c), chunk(glu_out, c))
    for item in gather_cot + gather_two + gather_mid:
        assert item.step_no == n
    for item in scatter_one + scatter_two + scatter_grad:
        assert item.step_no == n - 1
    for group in (scatter_grad, scatter_two):
        for item in group:
            item.drain()
    for item in copies[CHUNKS + 5 :]:
        item.wait()
    line.leave()


def middle_call(gated, weights, own, cot, gain, n):
    rows, width = own.shape
    tokens, nv = gated.shape
    wide = (weights.shape[0] - nv) // 3
    piece = rows // CHUNKS
    sems = CHUNKS * 6 * 2 * (n - 1)
    hop = (CHUNKS, n - 1, piece, width)
    shape = jax.ShapeDtypeStruct
    return pl.pallas_call(
        functools.partial(middle_kernel, n),
        out_shape=(
            shape((tokens, width), BF),
            shape((tokens, width), BF),
            shape((tokens, width), BF),
            shape((tokens, wide), BF),
            shape((tokens, 2 * wide), BF),
            shape((rows, width), BF),
            shape((rows, width), F32),
            shape((8, width), F32),
        ),
        in_specs=[ANY] * 4 + [VM],
        out_specs=(ANY,) * 5 + (VM,) * 3,
        scratch_shapes=[
            pltpu.VMEM((tokens, nv), BF),
            pltpu.VMEM((nv, width), BF),
            pltpu.VMEM((2 * wide, width), BF),
            pltpu.VMEM((wide, width), BF),
            pltpu.VMEM((rows, width), BF),
            pltpu.VMEM((tokens, width), BF),
            pltpu.VMEM((tokens, width), BF),
            pltpu.VMEM((tokens, wide), BF),
            pltpu.VMEM((tokens, 2 * wide), BF),
            pltpu.VMEM((tokens, width), BF),
            pltpu.VMEM((tokens, width), BF),
            pltpu.VMEM(hop, BF),
            pltpu.VMEM(hop, BF),
            pltpu.VMEM(hop, BF),
            pltpu.VMEM(hop, BF),
            pltpu.VMEM((rows, width), F32),
            pltpu.VMEM((CHUNKS, piece, width), BF),
            pltpu.SemaphoreType.DMA((5 + 6 * CHUNKS,)),
            pltpu.SemaphoreType.DMA((sems,)),
            pltpu.SemaphoreType.DMA((sems,)),
        ],
        compiler_params=pltpu.CompilerParams(
            collective_id=1, has_side_effects=True, vmem_limit_bytes=VMEM_MOST
        ),
        name="middle",
    )(gated, weights, own, cot, gain)


def gains_kernel(n, m, mine, total, first, second, send_sem, recv_sem):
    barrier = pltpu.get_barrier_semaphore()
    groups = (("dp", m, first), ("mp", n, second))
    for axis, size, _ in groups:
        me = lax.axis_index(axis)
        for k in range(1, size):
            peer = lax.rem(me + k, size)
            pl.semaphore_signal(barrier, inc=1, device_id={axis: peer}, device_id_type=MESH)
    pl.semaphore_wait(barrier, n + m - 2)
    source = mine
    for base, (axis, size, held) in zip((0, m), groups):
        me = lax.axis_index(axis)
        held[me] = source[...]

        def copy(k, slot):
            return pltpu.make_async_remote_copy(
                src_ref=source,
                dst_ref=held.at[slot],
                send_sem=send_sem.at[base + k],
                recv_sem=recv_sem.at[base + k],
                device_id={axis: lax.rem(me + k, size)},
                device_id_type=MESH,
            )

        sent = [copy(k, me) for k in range(1, size)]
        for c in sent:
            c.start()
        for k in range(1, size):
            copy(k, lax.rem(me - k + size, size)).wait_recv()
        value = held[0]
        for k in range(1, size):
            value = value + held[k]
        for c in sent:
            c.wait_send()
        total[...] = value
        source = total


def sum_gains(values, n, m):
    flat = values.reshape(-1, LANES)
    return pl.pallas_call(
        functools.partial(gains_kernel, n, m),
        out_shape=jax.ShapeDtypeStruct(flat.shape, F32),
        in_specs=[VM],
        out_specs=VM,
        scratch_shapes=[
            pltpu.VMEM((m,) + flat.shape, F32),
            pltpu.VMEM((n,) + flat.shape, F32),
            pltpu.SemaphoreType.DMA((n + m,)),
            pltpu.SemaphoreType.DMA((n + m,)),
        ],
        compiler_params=pltpu.CompilerParams(collective_id=3, has_side_effects=True),
        name="sum_gains",
    )(flat).reshape(values.shape)


def last_kernel(
    n, grads, weight, out, grads_v, weight_v, part, lefts, rights, copy_sem, send_sem, recv_sem
):
    line = Line(n, send_sem, recv_sem)
    count, width = out.shape
    piece = count // CHUNKS
    per = n * piece
    load = [
        pltpu.make_async_copy(
            grads.at[pl.ds(h * per, per)], grads_v.at[pl.ds(h * per, per)], copy_sem.at[h]
        )
        for h in range(CHUNKS)
    ]
    load_weight = pltpu.make_async_copy(weight, weight_v, copy_sem.at[CHUNKS])
    for item in load + [load_weight]:
        item.start()
    line.enter()
    for h in range(CHUNKS):
        no_neighbour_zero(n, line.place, lefts.at[h, n - 2], rights.at[h, n - 2])
    scatters = [
        Scatter(
            line,
            lambda k, h=h: part.at[pl.ds(h * per + k * piece, piece)],
            lambda s, h=h: lefts.at[h, s - 1],
            lambda s, h=h: rights.at[h, s - 1],
            add_into,
        )
        for h in range(CHUNKS)
    ]

    def finish(h):
        scatters[h].finish()

        def step(at):
            src = at(h * per)
            out[at(h * piece), :] = (
                part[src, :].astype(F32)
                + lefts[h, n - 2, at(), :].astype(F32)
                + rights[h, n - 2, at(), :].astype(F32)
            )

        blocks(piece, step)

    load_weight.wait()
    for h in range(CHUNKS):
        load[h].wait()
        rows = pl.ds(h * per, per)
        product_tiles(part.at[rows], grads_v.at[rows], weight_v, 2 * LANES)
        scatters[h].step()
    for _ in range(n - 2):
        for h in range(CHUNKS):
            scatters[h].step()
    for h in range(CHUNKS):
        finish(h)
    for h in range(CHUNKS):
        scatters[h].drain()


def last_call(grads, weight, n):
    tokens, deep = grads.shape
    width = weight.shape[1]
    rows = tokens // n
    sems = CHUNKS * 2 * (n - 1)
    hop = (CHUNKS, n - 1, rows // CHUNKS, width)
    return pl.pallas_call(
        functools.partial(last_kernel, n),
        out_shape=jax.ShapeDtypeStruct((rows, width), F32),
        in_specs=[ANY, ANY],
        out_specs=VM,
        scratch_shapes=[
            pltpu.VMEM((tokens, deep), BF),
            pltpu.VMEM((deep, width), BF),
            pltpu.VMEM((tokens, width), BF),
            pltpu.VMEM(hop, BF),
            pltpu.VMEM(hop, BF),
            pltpu.SemaphoreType.DMA((CHUNKS + 1,)),
            pltpu.SemaphoreType.DMA((sems,)),
            pltpu.SemaphoreType.DMA((sems,)),
        ],
        compiler_params=pltpu.CompilerParams(
            collective_id=2, has_side_effects=True, vmem_limit_bytes=VMEM_MOST
        ),
        name="last",
    )(grads, weight)


def pad_rows(array, count):
    return jnp.pad(array, ((0, count - array.shape[0]), (0, 0)))


def pad_columns(array, count):
    return jnp.pad(array, ((0, 0), (0, count - array.shape[1])))


def body(
    inputs,
    segments,
    first_norm_gain,
    w_query,
    w_key,
    w_value,
    w_gate,
    w_out,
    second_norm_gain,
    w_glu_gate,
    w_glu_up,
    w_down,
    cotangent,
):
    n = lax.axis_size("mp")
    place = lax.axis_index("mp")
    heads = H // n
    head_start = place * heads
    rows, width = inputs.shape
    shard = w_query.shape[0]
    piece = rows // CHUNKS
    nk, nv, nf = heads * HK, heads * HV, w_down.shape[0]
    n_one = 2 * nk + 2 * nv
    one_wide = -(-n_one // (2 * LANES)) * 2 * LANES
    v_wide, f_wide = -(-nv // LANES) * LANES, -(-nf // LANES) * LANES
    f_tiles = f_wide // LANES

    pack_one = pad_rows(
        jnp.concatenate([w_query.T, w_key.T, w_value.T, w_gate.T], axis=0), one_wide
    )
    weight_one = lax.all_gather(pack_one, "dp", axis=1, tiled=True)
    glu_pack = jnp.stack(
        [
            pad_rows(w_glu_gate.T, f_wide).reshape(f_tiles, LANES, shard),
            pad_rows(w_glu_up.T, f_wide).reshape(f_tiles, LANES, shard),
        ],
        axis=1,
    ).reshape(2 * f_wide, shard)
    pack_two = jnp.concatenate([glu_pack, pad_rows(w_down, f_wide), pad_rows(w_out, v_wide)], axis=0)
    pack_two, weight_one = lax.optimization_barrier((pack_two, weight_one))
    weight_two = lax.all_gather(pack_two, "dp", axis=1, tiled=True)
    out_weight = weight_two[3 * f_wide :]

    first_hat, first_scale = layer_norm(inputs.astype(F32), epsilon)
    rows_one = gather_rows((first_hat * first_norm_gain).astype(BF), n)
    tokens = rows_one.shape[0]

    slot_shard = lax.rem(place - jnp.arange(n) + n, n)
    places = (
        slot_shard[None, :, None] * rows
        + jnp.arange(CHUNKS)[:, None, None] * piece
        + jnp.arange(piece)[None, None, :]
    ).reshape(tokens)
    seg = segments.reshape(n, CHUNKS, piece)[::-1]
    seg = lax.dynamic_slice_in_dim(jnp.concatenate([seg, seg], axis=0), n - 1 - place, n, axis=0)
    seg = seg.transpose(1, 0, 2).reshape(tokens)

    query_key = dot_nt(rows_one, weight_one[: 2 * nk]).astype(BF)
    value = dot_nt(rows_one, weight_one[2 * nk : 2 * nk + nv]).astype(BF)
    gate_pre = dot_nt(rows_one, weight_one[2 * nk + nv : n_one])
    query = query_key[:, :nk].reshape(tokens, heads, HK)
    key = query_key[:, nk:].reshape(tokens, heads, HK)
    value = value.reshape(tokens, heads, HV)

    distance = places[:, None] - places[None, :]
    allowed = (distance >= 0) & (seg[:, None] == seg[None, :])
    log_gamma = jnp.log1p(-jnp.exp2(-5.0 - (head_start + jnp.arange(heads)).astype(F32)))
    exponent = jnp.where(
        allowed[None], distance[None].astype(F32) * log_gamma[:, None, None], 0.0
    )
    mask = jnp.where(allowed[None], jnp.exp(exponent), 0.0) * HK ** (-0.5)

    scores = (jnp.einsum("thk,shk->hts", query, key, preferred_element_type=F32) * mask).astype(BF)
    retained = jnp.einsum("hts,shv->thv", scores, value, preferred_element_type=F32)
    normalized, scale_group = layer_norm(retained, group_epsilon)
    normal_flat = normalized.reshape(tokens, nv)
    swish = jax.nn.silu(gate_pre)
    gated = pad_columns((swish * normal_flat).astype(BF), v_wide)

    rows_two, cot_rows, mid_rows, hidden, d_glu, outputs, middle_grad, second_gain = middle_call(
        gated, weight_two, inputs, cotangent, second_norm_gain[None], n
    )

    grads_two = jnp.concatenate([dot_tn(d_glu, rows_two), dot_tn(hidden, cot_rows)], axis=0).astype(BF)
    summed_two = lax.psum_scatter(grads_two, "dp", scatter_dimension=1, tiled=True).astype(F32)
    glu_sum = summed_two[: 2 * f_wide].reshape(f_tiles, 2, LANES, shard)

    d_gated = dot_nt(mid_rows, out_weight[:nv])
    sigmoid_gate = jax.nn.sigmoid(gate_pre)
    d_gate_pre = (
        d_gated * normal_flat * (sigmoid_gate + gate_pre * sigmoid_gate * (1.0 - sigmoid_gate))
    ).astype(BF)
    d_normalized = (d_gated * swish).reshape(tokens, heads, HV)
    d_retained = norm_back(d_normalized, normalized, scale_group).astype(BF)
    grads_out = jnp.concatenate(
        [dot_tn(gated[:, :nv], mid_rows).astype(BF), dot_tn(d_gate_pre, rows_one).astype(BF)], axis=0
    )
    summed_out = lax.psum_scatter(grads_out, "dp", scatter_dimension=1, tiled=True).astype(F32)

    d_value = jnp.einsum("hts,thv->shv", scores, d_retained, preferred_element_type=F32).astype(BF)
    d_scores = (
        jnp.einsum("thv,shv->hts", d_retained, value, preferred_element_type=F32) * mask
    ).astype(BF)
    d_query = jnp.einsum("hts,shk->thk", d_scores, key, preferred_element_type=F32).astype(BF)
    d_key = jnp.einsum("hts,thk->shk", d_scores, query, preferred_element_type=F32).astype(BF)
    d_qkv = jnp.concatenate(
        [d_query.reshape(tokens, nk), d_key.reshape(tokens, nk), d_value.reshape(tokens, nv)], axis=1
    )
    grads_one = dot_tn(d_qkv, rows_one).astype(BF)
    summed_one = lax.psum_scatter(grads_one, "dp", scatter_dimension=1, tiled=True).astype(F32)

    d_one = pad_columns(jnp.concatenate([d_qkv, d_gate_pre], axis=1), one_wide)
    first_grad = last_call(d_one, weight_one, n)
    first_gain = jnp.sum(first_hat * first_grad, axis=0)
    input_gradient = middle_grad + norm_back(first_grad * first_norm_gain, first_hat, first_scale)

    gains = sum_gains(
        jnp.stack([first_gain, jnp.sum(second_gain, axis=0)]), n, lax.axis_size("dp")
    )
    return (
        outputs,
        input_gradient,
        gains[0],
        summed_one[:nk].T,
        summed_one[nk : 2 * nk].T,
        summed_one[2 * nk :].T,
        summed_out[nv:].T,
        summed_out[:nv],
        gains[1],
        glu_sum[:, 0].reshape(f_wide, shard)[:nf].T,
        glu_sum[:, 1].reshape(f_wide, shard)[:nf].T,
        summed_two[2 * f_wide : 2 * f_wide + nf],
    )


def solution(mesh):
    split = P(("dp", "mp"), None)
    wide, tall = P("dp", "mp"), P("mp", "dp")
    return jax.shard_map(
        body,
        mesh=mesh,
        in_specs=(
            split, P("dp", None), P(), wide, wide, wide, wide, tall, P(), wide, wide, tall, split,
        ),
        out_specs=(
            split, split, P(), wide, wide, wide, wide, tall, P(), wide, wide, tall,
        ),
        check_vma=False,
    )
```

```python
import functools

import jax
import jax.numpy as jnp
from jax import lax
from jax.experimental import pallas as pl
from jax.experimental.pallas import tpu as pltpu
from jax.sharding import PartitionSpec as P

H = 8
HK = 256
HV = 432
LEN = 1024
CHUNKS = 4
LANES = 128
VMEM_MOST = 66_000_000

epsilon = 1e-05
group_epsilon = 1.0
BF = jnp.bfloat16
F32 = jnp.float32


def layer_norm(values_in, offset):
    centre = jnp.mean(values_in, axis=-1, keepdims=True)
    centred = values_in - centre
    variance = jnp.mean(centred * centred, axis=-1, keepdims=True)
    scaling = lax.rsqrt(variance + offset)
    return (centred * scaling, scaling)


def norm_back(grad_hat, normed_hat, scaling):
    first_mean = jnp.mean(grad_hat, axis=-1, keepdims=True)
    second_mean = jnp.mean(grad_hat * normed_hat, axis=-1, keepdims=True)
    return scaling * (grad_hat - first_mean - normed_hat * second_mean)


def glu_act(gate_pre, up_pre):
    return jax.nn.gelu(gate_pre, approximate=True) * up_pre


def dot_nt(a, b):
    return lax.dot_general(a, b, (((1,), (1,)), ((), ())), preferred_element_type=F32)


def dot_nn(a, b):
    return lax.dot_general(a, b, (((1,), (0,)), ((), ())), preferred_element_type=F32)


def dot_tn(a, b):
    return lax.dot_general(a, b, (((0,), (0,)), ((), ())), preferred_element_type=F32)


MESH = pl.DeviceIdType.MESH


class Line:
    def __init__(self, n, send_sem, recv_sem):
        self.n, self.send_sem, self.recv_sem = n, send_sem, recv_sem
        self.place = lax.axis_index("mp")
        self.used = 0
        self.sent = []

    def enter(self, others=None):
        barrier = pltpu.get_barrier_semaphore()
        n, place = self.n, self.place

        @pl.when(place >= 1)
        def _():
            pl.semaphore_signal(barrier, inc=1, device_id={"mp": place - 1}, device_id_type=MESH)

        @pl.when(place <= n - 2)
        def _():
            pl.semaphore_signal(barrier, inc=1, device_id={"mp": place + 1}, device_id_type=MESH)

        peers = jnp.minimum(place, 1) + jnp.minimum(n - 1 - place, 1)
        if others is not None:
            axis, indices = others
            for index in indices:
                pl.semaphore_signal(barrier, inc=1, device_id={axis: index}, device_id_type=MESH)
            peers = peers + len(indices)
        pl.semaphore_wait(barrier, peers)

    def copy(self, src, dst, index, toward):
        return pltpu.make_async_remote_copy(
            src_ref=src,
            dst_ref=dst,
            send_sem=self.send_sem.at[index],
            recv_sem=self.recv_sem.at[index],
            device_id={"mp": self.place + toward},
            device_id_type=MESH,
        )

    def leave(self):
        for condition, copy in self.sent:
            pl.when(condition)(copy.wait_send)


class Gather:
    def __init__(self, line, slot):
        self.line, self.slot, self.step_no = line, slot, 0
        self.base = line.used
        line.used += 2 * (line.n - 1)
        n = line.n
        self.right = [
            line.copy(slot(s - 1), slot(s), self.base + s - 1, 1) for s in range(1, n)
        ]
        self.left = [
            line.copy(slot((n - s + 1) % n), slot(n - s), self.base + n - 2 + s, -1)
            for s in range(1, n)
        ]

    def arrive(self, s):
        n, place = self.line.n, self.line.place
        pl.when(place >= s)(self.right[s - 1].wait_recv)
        pl.when(place <= n - 1 - s)(self.left[s - 1].wait_recv)

    def step(self):
        self.step_no += 1
        s, n, place = self.step_no, self.line.n, self.line.place
        if s > 1:
            self.arrive(s - 1)
        if s < n:
            to_right = (place >= s - 1) & (place <= n - 2)
            to_left = (place <= n - s) & (place >= 1)
            pl.when(to_right)(self.right[s - 1].start)
            pl.when(to_left)(self.left[s - 1].start)
            self.line.sent += [(to_right, self.right[s - 1]), (to_left, self.left[s - 1])]


class Scatter:
    def __init__(self, line, slot, from_left, from_right, add):
        self.line, self.slot, self.add, self.step_no = line, slot, add, 0
        self.from_left, self.from_right = from_left, from_right
        self.base = line.used
        line.used += 2 * (line.n - 1)
        n = line.n
        self.right = [
            line.copy(slot(s), from_left(s), self.base + s - 1, 1) for s in range(1, n)
        ]
        self.left = [
            line.copy(slot(n - s), from_right(s), self.base + n - 2 + s, -1) for s in range(1, n)
        ]
        self.mine = []

    def step(self):
        self.step_no += 1
        s, n, place = self.step_no, self.line.n, self.line.place
        to_right, to_left = place <= s - 1, place >= n - s
        if s > 1:

            @pl.when(to_right & (place >= 1))
            def _():
                self.right[s - 2].wait_recv()
                self.add(self.slot(s), self.from_left(s - 1))

            @pl.when(to_left & (place <= n - 2))
            def _():
                self.left[s - 2].wait_recv()
                self.add(self.slot(n - s), self.from_right(s - 1))

        pl.when(to_right)(self.right[s - 1].start)
        pl.when(to_left)(self.left[s - 1].start)
        self.mine += [(to_right, self.right[s - 1]), (to_left, self.left[s - 1])]

    def finish(self):
        n, place = self.line.n, self.line.place

        @pl.when(place >= 1)
        def _():
            self.right[n - 2].wait_recv()

        @pl.when(place <= n - 2)
        def _():
            self.left[n - 2].wait_recv()

    def drain(self):
        for condition, copy in self.mine:
            pl.when(condition)(copy.wait_send)


ANY = pl.BlockSpec(memory_space=pl.ANY)
VM = pl.BlockSpec(memory_space=pltpu.VMEM)
BLOCK = 16


def blocks(count, step):
    def run(i, carry):
        step(lambda base=0: pl.ds(pl.multiple_of(base + i * BLOCK, BLOCK), BLOCK))
        return carry

    lax.fori_loop(0, count // BLOCK, run, 0)


def add_into(target, extra):
    def step(at):
        target[at(), :] = (target[at(), :].astype(F32) + extra[at(), :].astype(F32)).astype(BF)

    blocks(target.shape[0], step)


def product_tiles(target, left, right, tile):
    def step(j, carry):
        at = pl.ds(pl.multiple_of(j * tile, tile), tile)
        target[:, at] = dot_nn(left[...], right[:, at]).astype(BF)
        return carry

    lax.fori_loop(0, right.shape[1] // tile, step, 0)


class Doubling:
    def __init__(self, m, own, out, rows, bits, base, send_sem, recv_sem):
        self.d = lax.axis_index("dp")
        self.own, self.out, self.rows, self.bits, self.base = own, out, rows, bits, base
        self.send_sem, self.recv_sem = send_sem, recv_sem
        self.shard = own.shape[1]
        self.done = 0
        self.sent = []

    def flip(self, d, bit):
        return d + bit * (1 - 2 * (lax.div(d, bit) % 2))

    def block(self, d):
        return self.out.at[self.rows, pl.ds(pl.multiple_of(d * self.shard, self.shard), self.shard)]

    def copies(self, level, landing):
        owners = [self.d]
        for bit in self.bits[:level]:
            owners += [self.flip(d, bit) for d in owners]
        bit = self.bits[level]
        partner = self.flip(self.d, bit)
        out = []
        for i, d in enumerate(owners):
            d = self.flip(d, bit) if landing else d
            src = self.own.at[self.rows] if i == 0 and not landing else self.block(d)
            index = self.base + (1 << level) - 1 + i
            out.append(
                pltpu.make_async_remote_copy(
                    src_ref=src,
                    dst_ref=self.block(d),
                    send_sem=self.send_sem.at[index],
                    recv_sem=self.recv_sem.at[index],
                    device_id={"dp": partner},
                    device_id_type=MESH,
                )
            )
        return out

    def step(self):
        level = self.done
        if level > 0:
            for c in self.copies(level - 1, True):
                c.wait_recv()
        if level < len(self.bits):
            out = self.copies(level, False)
            for c in out:
                c.start()
            self.sent += out
        self.done += 1

    def leave(self):
        for c in self.sent:
            c.wait_send()


def bits_of(m):
    bits = [1 << b for b in range(m.bit_length() - 1)]
    assert 1 << len(bits) == m
    return bits


PARTS = 2


def gather_kernel(n, m, own, pack, out, weight, send_sem, recv_sem, copy_sem, wide_send, wide_recv):
    line = Line(n, send_sem, recv_sem)
    piece = own.shape[0] // CHUNKS
    per = n * piece
    shard = pack.shape[1]
    d = lax.axis_index("dp")
    bits = bits_of(m)
    outer = bits[1:]
    height = pack.shape[0] // (2 * PARTS)
    doubling = []
    for i in range(2 * PARTS):
        order = (outer if i % 2 == 0 else outer[::-1]) + bits[:1]
        doubling.append(
            Doubling(
                m, pack, weight, pl.ds(i * height, height), order, i * (m - 1), wide_send, wide_recv
            )
        )
    first = doubling[0]
    line.enter(["dp", [first.flip(d, bit) for bit in bits]])
    local, gathers = [], []
    columns = pl.ds(pl.multiple_of(d * shard, shard), shard)
    keep = pltpu.make_async_copy(pack, weight.at[:, columns], copy_sem.at[CHUNKS])
    for h in range(CHUNKS):
        mine = own.at[pl.ds(h * piece, piece)]
        local.append(
            pltpu.make_async_copy(mine, out.at[pl.ds(h * per, piece)], copy_sem.at[h])
        )

        def slot(k, h=h, mine=mine):
            return mine if k == 0 else out.at[pl.ds(h * per + k * piece, piece)]

        gathers.append(Gather(line, slot))
    local.append(keep)

    def line_step(items):
        for item in items:
            item.step()

    half = CHUNKS // 2
    line_step(gathers)
    line_step(doubling)
    for item in local:
        item.start()
    for level in range(1, max(n, len(bits) + 1)):
        for side in range(2):
            if level <= len(bits):
                line_step(doubling[side * PARTS : (side + 1) * PARTS])
            if level < n:
                line_step(gathers[side * half : (side + 1) * half])
    for item in local:
        item.wait()
    for item in gathers:
        assert item.step_no == n
    for item in doubling:
        assert item.done == len(bits) + 1
        item.leave()
    line.leave()


def gather_rows(own, pack, n, m):
    rows, width = own.shape
    count = CHUNKS * 2 * (n - 1)
    wide = 2 * PARTS * (m - 1)
    return pl.pallas_call(
        functools.partial(gather_kernel, n, m),
        out_shape=(
            jax.ShapeDtypeStruct((n * rows, width), own.dtype),
            jax.ShapeDtypeStruct((pack.shape[0], m * pack.shape[1]), pack.dtype),
        ),
        in_specs=[VM, VM],
        out_specs=(ANY, ANY),
        scratch_shapes=[
            pltpu.SemaphoreType.DMA((count,)),
            pltpu.SemaphoreType.DMA((count,)),
            pltpu.SemaphoreType.DMA((CHUNKS + 1,)),
            pltpu.SemaphoreType.DMA((wide,)),
            pltpu.SemaphoreType.DMA((wide,)),
        ],
        compiler_params=pltpu.CompilerParams(collective_id=0, has_side_effects=True),
        name="gather_rows",
    )(own, pack)


def no_neighbour_zero(n, place, from_left, from_right):
    @pl.when(place == 0)
    def _():
        from_left[...] = jnp.zeros_like(from_left)

    @pl.when(place == n - 1)
    def _():
        from_right[...] = jnp.zeros_like(from_right)


(COT, OUT, ONE, END_ONE, TWO, GLU, GRAD, GRAD_SUM, END_GRAD, MID, DOWN, DOWN_SUM, END_DOWN) = range(13)

DUE = {
    OUT: (-2.23, 1.66, 0), ONE: (-1.99, 1.12, 1.03), END_ONE: (1.46, 1.37, 0), TWO: (0.73, 1.15, 0.94),
    COT: (0.35, 1.39, 1.02), GLU: (1.14, -1.37, 1.55), GRAD: (3.09, 2.02, 0),
    GRAD_SUM: (3.48, 1.71, 0.74), END_GRAD: (7.02, -2.12, 0), MID: (5.68, 0.86, 1.11),
    DOWN: (1.3, 0.36, 0), DOWN_SUM: (1.87, 1.35, 0.95), END_DOWN: (7.9, 2.17, 0),
}
TUNED = {
    (4, 4): [
        0, 4, 8, 0, 5, 8, 1, 0, 8, 9, 6, 1, 12, 9, 16, 9, 10, 16, 0, 3,
        10, 16, 7, 11, 1, 13, 17, 16, 20, 10, 20, 11, 1, 17, 40, 14, 2, 11, 18, 24,
        17, 2, 28, 44, 15, 19, 17, 21, 2, 18, 28, 44, 21, 41, 18, 19, 3, 2, 45, 28,
        25, 29, 18, 45, 22, 3, 29, 22, 42, 29, 32, 19, 46, 26, 36, 46, 3, 33, 19, 44,
        30, 23, 36, 23, 37, 45, 30, 46, 30, 37, 43, 27, 31, 47, 36, 34, 38, 36, 31, 47,
        50, 37, 37, 38, 31, 48, 47, 35, 38, 39, 49, 39, 38, 39, 51, 39,
    ],
}


def middle_order(n):
    if (n, CHUNKS) in TUNED:
        return [divmod(code, CHUNKS) for code in TUNED[n, CHUNKS]]
    count = {k: 1 for k in DUE}
    count.update({COT: n, TWO: n, MID: n, ONE: n - 1, GRAD_SUM: n - 1, DOWN_SUM: n - 1, GLU: 2})
    needs = {
        ONE: [OUT], END_ONE: [ONE], TWO: [END_ONE], GLU: [TWO, COT], GRAD: [GLU], GRAD_SUM: [GRAD],
        END_GRAD: [GRAD_SUM], MID: [END_GRAD], DOWN: [GLU], DOWN_SUM: [DOWN], END_DOWN: [DOWN_SUM],
    }
    todo = sorted(
        (first + h * later + s * 3 / (n - 1) * each, k, h, s)
        for k, (first, later, each) in DUE.items()
        for h in range(CHUNKS)
        for s in range(count[k])
    )
    taken, order = {}, []
    while todo:
        for item in todo:
            _, k, h, s = item
            ready = taken.get((k, h), 0) == s and all(
                taken.get((need, h), 0) == count[need] for need in needs.get(k, [])
            )
            if ready:
                break
        todo.remove(item)
        taken[k, h] = s + 1
        order.append((k, h))
    return order


def middle_kernel(
    n, gated, weights, own, cot, gain,
    rows_out, cot_out, mid_out, hidden_out, glu_out, outputs, d_middle, gain_out,
    gated_v, wo_v, wg_v, wd_v, own_v, cot_v, rows_v, hidden_v, glu_v, part, part_two,
    left_a, right_a, left_b, right_b, middle, stage, copy_sem, send_sem, recv_sem,
):
    line = Line(n, send_sem, recv_sem)
    place = line.place
    count, width = own.shape
    piece = count // CHUNKS
    per = n * piece
    wide = hidden_v.shape[1]
    copies = []

    def local(src, dst):
        c = pltpu.make_async_copy(src, dst, copy_sem.at[len(copies)])
        copies.append(c)
        c.start()
        return c

    def rows_at(ref, h, k=0, size=piece):
        return ref.at[pl.ds(h * per + k * piece, size)]

    load_cot = [
        local(cot.at[pl.ds(h * piece, piece)], rows_at(cot_v, h)) for h in range(CHUNKS)
    ]
    load_gated = local(gated, gated_v)
    load_wo = local(weights.at[pl.ds(3 * wide, wo_v.shape[0])], wo_v)
    load_own = local(own, own_v)
    load_wg = local(weights.at[pl.ds(0, 2 * wide)], wg_v)
    load_wd = local(weights.at[pl.ds(2 * wide, wide)], wd_v)
    line.enter()
    for h in range(CHUNKS):
        no_neighbour_zero(n, place, left_a.at[h, n - 2], right_a.at[h, n - 2])
        no_neighbour_zero(n, place, left_b.at[h, n - 2], right_b.at[h, n - 2])
    gain_out[...] = jnp.zeros_like(gain_out)

    def scatter(buf, lefts, rights, h):
        return Scatter(
            line,
            lambda k: rows_at(buf, h, k),
            lambda s: lefts.at[h, s - 1],
            lambda s: rights.at[h, s - 1],
            add_into,
        )

    gather_cot = [Gather(line, functools.partial(rows_at, cot_v, h)) for h in range(CHUNKS)]
    gather_two = [Gather(line, functools.partial(rows_at, rows_v, h)) for h in range(CHUNKS)]

    def mid_slot(h, k):
        return stage.at[h] if k == 0 else rows_at(mid_out, h, k)

    gather_mid = [Gather(line, functools.partial(mid_slot, h)) for h in range(CHUNKS)]
    scatter_one = [scatter(part, left_a, right_a, h) for h in range(CHUNKS)]
    scatter_two = [scatter(part_two, left_b, right_b, h) for h in range(CHUNKS)]
    scatter_grad = [scatter(part, left_a, right_a, h) for h in range(CHUNKS)]

    def chunk(ref, h):
        return ref.at[pl.ds(h * per, per)]

    def out_product(h):
        product_tiles(chunk(part, h), chunk(gated_v, h), wo_v, 2 * LANES)

    def finish_one(h):
        scatter_one[h].finish()

        def step(at):
            src = at(h * per)
            mine = at(h * piece)
            total = (
                own_v[mine, :].astype(F32)
                + part[src, :].astype(F32)
                + left_a[h, n - 2, at(), :].astype(F32)
                + right_a[h, n - 2, at(), :].astype(F32)
            )
            middle[mine, :] = total
            hat, _ = layer_norm(total, epsilon)
            rows_v[src, :] = (hat * gain[...]).astype(BF)

        blocks(piece, step)

    def glu_tiles(h, first, last):
        def step(j, carry):
            pair = pl.ds(pl.multiple_of(j * 2 * LANES, 2 * LANES), 2 * LANES)
            at = pl.ds(pl.multiple_of(j * LANES, LANES), LANES)
            whole = pl.ds(h * per, per)
            both = dot_nt(rows_v[whole, :], wg_v[pair, :])
            d_hidden = dot_nt(cot_v[whole, :], wd_v[at, :])
            u, up = both[:, :LANES], both[:, LANES:]
            c = 0.7978845608028654
            t = jnp.tanh(c * (u + 0.044715 * (u * u * u)))
            half = 0.5 * (1.0 + t)
            act = u * half
            slope = half + 0.5 * u * (1.0 - t * t) * (c * (1.0 + 3 * 0.044715 * (u * u)))
            hidden_v[whole, at] = (act * up).astype(BF)
            glu_v[whole, pair] = jnp.concatenate(
                [(d_hidden * up * slope).astype(BF), (d_hidden * act).astype(BF)], axis=1
            )
            return carry

        lax.fori_loop(first, last, step, 0)

    def grad_product(h):
        product_tiles(chunk(part, h), chunk(glu_v, h), wg_v, 2 * LANES)

    def down_product(h):
        product_tiles(chunk(part_two, h), chunk(hidden_v, h), wd_v, 2 * LANES)

    def finish_grad(h):
        scatter_grad[h].finish()

        def step(at):
            src = at(h * per)
            mine = at(h * piece)
            grad = (
                part[src, :].astype(F32)
                + left_a[h, n - 2, at(), :].astype(F32)
                + right_a[h, n - 2, at(), :].astype(F32)
            )
            hat, scale = layer_norm(middle[mine, :], epsilon)
            gain_out[...] += jnp.sum((hat * grad).reshape(BLOCK // 8, 8, width), axis=0)
            d_mid = cot_v[src, :].astype(F32) + norm_back(grad * gain[...], hat, scale)
            d_middle[mine, :] = d_mid
            stage[h, at(), :] = d_mid.astype(BF)

        blocks(piece, step)
        local(stage.at[h], rows_at(mid_out, h))

    def finish_two(h):
        scatter_two[h].finish()

        def step(at):
            src = at(h * per)
            mine = at(h * piece)
            outputs[mine, :] = (
                middle[mine, :]
                + part_two[src, :].astype(F32)
                + left_b[h, n - 2, at(), :].astype(F32)
                + right_b[h, n - 2, at(), :].astype(F32)
            ).astype(BF)

        blocks(piece, step)

    tiles = wide // LANES
    cut = tiles // 2

    def wait_for(items):
        for item in items:
            item.wait()
        items.clear()

    first_loads, own_load = [load_gated, load_wo], [load_own]
    later_loads = [load_wg, load_wd]

    def out_action(h):
        wait_for(first_loads)
        out_product(h)

    def finish_one_action(h):
        wait_for(own_load)
        finish_one(h)

    def glu_action(h):
        wait_for(later_loads)
        if h in begun:
            glu_tiles(h, cut, tiles)
        else:
            begun.add(h)
            glu_tiles(h, 0, cut)

    def grad_action(h):
        scatter_one[h].drain()
        grad_product(h)

    begun = set()
    actions = {
        COT: lambda h: gather_cot[h].step(),
        OUT: out_action,
        ONE: lambda h: scatter_one[h].step(),
        END_ONE: finish_one_action,
        TWO: lambda h: gather_two[h].step(),
        GLU: glu_action,
        GRAD: grad_action,
        GRAD_SUM: lambda h: scatter_grad[h].step(),
        END_GRAD: finish_grad,
        MID: lambda h: gather_mid[h].step(),
        DOWN: down_product,
        DOWN_SUM: lambda h: scatter_two[h].step(),
        END_DOWN: finish_two,
    }
    for item in load_cot:
        item.wait()
    for kind, h in middle_order(n):
        actions[kind](h)
    for c in range(CHUNKS):
        local(chunk(rows_v, c), chunk(rows_out, c))
        local(chunk(cot_v, c), chunk(cot_out, c))
        local(chunk(hidden_v, c), chunk(hidden_out, c))
        local(chunk(glu_v, c), chunk(glu_out, c))
    for item in gather_cot + gather_two + gather_mid:
        assert item.step_no == n
    for item in scatter_one + scatter_two + scatter_grad:
        assert item.step_no == n - 1
    for group in (scatter_grad, scatter_two):
        for item in group:
            item.drain()
    for item in copies[CHUNKS + 5 :]:
        item.wait()
    line.leave()


def middle_call(gated, weights, own, cot, gain, n):
    rows, width = own.shape
    tokens, nv = gated.shape
    wide = (weights.shape[0] - nv) // 3
    piece = rows // CHUNKS
    sems = CHUNKS * 6 * 2 * (n - 1)
    hop = (CHUNKS, n - 1, piece, width)
    shape = jax.ShapeDtypeStruct
    return pl.pallas_call(
        functools.partial(middle_kernel, n),
        out_shape=(
            shape((tokens, width), BF),
            shape((tokens, width), BF),
            shape((tokens, width), BF),
            shape((tokens, wide), BF),
            shape((tokens, 2 * wide), BF),
            shape((rows, width), BF),
            shape((rows, width), F32),
            shape((8, width), F32),
        ),
        in_specs=[ANY] * 4 + [VM],
        out_specs=(ANY,) * 5 + (VM,) * 3,
        scratch_shapes=[
            pltpu.VMEM((tokens, nv), BF),
            pltpu.VMEM((nv, width), BF),
            pltpu.VMEM((2 * wide, width), BF),
            pltpu.VMEM((wide, width), BF),
            pltpu.VMEM((rows, width), BF),
            pltpu.VMEM((tokens, width), BF),
            pltpu.VMEM((tokens, width), BF),
            pltpu.VMEM((tokens, wide), BF),
            pltpu.VMEM((tokens, 2 * wide), BF),
            pltpu.VMEM((tokens, width), BF),
            pltpu.VMEM((tokens, width), BF),
            pltpu.VMEM(hop, BF),
            pltpu.VMEM(hop, BF),
            pltpu.VMEM(hop, BF),
            pltpu.VMEM(hop, BF),
            pltpu.VMEM((rows, width), F32),
            pltpu.VMEM((CHUNKS, piece, width), BF),
            pltpu.SemaphoreType.DMA((5 + 6 * CHUNKS,)),
            pltpu.SemaphoreType.DMA((sems,)),
            pltpu.SemaphoreType.DMA((sems,)),
        ],
        compiler_params=pltpu.CompilerParams(
            collective_id=1, has_side_effects=True, vmem_limit_bytes=VMEM_MOST
        ),
        name="middle",
    )(gated, weights, own, cot, gain)


def gains_kernel(n, m, mine, total, first, second, send_sem, recv_sem):
    barrier = pltpu.get_barrier_semaphore()
    groups = (("dp", m, first), ("mp", n, second))
    for axis, size, _ in groups:
        me = lax.axis_index(axis)
        for k in range(1, size):
            peer = lax.rem(me + k, size)
            pl.semaphore_signal(barrier, inc=1, device_id={axis: peer}, device_id_type=MESH)
    pl.semaphore_wait(barrier, n + m - 2)
    source = mine
    for base, (axis, size, held) in zip((0, m), groups):
        me = lax.axis_index(axis)
        held[me] = source[...]

        def copy(k, slot):
            return pltpu.make_async_remote_copy(
                src_ref=source,
                dst_ref=held.at[slot],
                send_sem=send_sem.at[base + k],
                recv_sem=recv_sem.at[base + k],
                device_id={axis: lax.rem(me + k, size)},
                device_id_type=MESH,
            )

        sent = [copy(k, me) for k in range(1, size)]
        for c in sent:
            c.start()
        for k in range(1, size):
            copy(k, lax.rem(me - k + size, size)).wait_recv()
        value = held[0]
        for k in range(1, size):
            value = value + held[k]
        for c in sent:
            c.wait_send()
        total[...] = value
        source = total


def sum_gains(values, n, m):
    flat = values.reshape(-1, LANES)
    return pl.pallas_call(
        functools.partial(gains_kernel, n, m),
        out_shape=jax.ShapeDtypeStruct(flat.shape, F32),
        in_specs=[VM],
        out_specs=VM,
        scratch_shapes=[
            pltpu.VMEM((m,) + flat.shape, F32),
            pltpu.VMEM((n,) + flat.shape, F32),
            pltpu.SemaphoreType.DMA((n + m,)),
            pltpu.SemaphoreType.DMA((n + m,)),
        ],
        compiler_params=pltpu.CompilerParams(collective_id=3, has_side_effects=True),
        name="sum_gains",
    )(flat).reshape(values.shape)


def last_kernel(
    n, grads, weight, out, grads_v, weight_v, part, lefts, rights, copy_sem, send_sem, recv_sem
):
    line = Line(n, send_sem, recv_sem)
    count, width = out.shape
    piece = count // CHUNKS
    per = n * piece
    load = [
        pltpu.make_async_copy(
            grads.at[pl.ds(h * per, per)], grads_v.at[pl.ds(h * per, per)], copy_sem.at[h]
        )
        for h in range(CHUNKS)
    ]
    load_weight = pltpu.make_async_copy(weight, weight_v, copy_sem.at[CHUNKS])
    for item in load + [load_weight]:
        item.start()
    line.enter()
    for h in range(CHUNKS):
        no_neighbour_zero(n, line.place, lefts.at[h, n - 2], rights.at[h, n - 2])
    scatters = [
        Scatter(
            line,
            lambda k, h=h: part.at[pl.ds(h * per + k * piece, piece)],
            lambda s, h=h: lefts.at[h, s - 1],
            lambda s, h=h: rights.at[h, s - 1],
            add_into,
        )
        for h in range(CHUNKS)
    ]

    def finish(h):
        scatters[h].finish()

        def step(at):
            src = at(h * per)
            out[at(h * piece), :] = (
                part[src, :].astype(F32)
                + lefts[h, n - 2, at(), :].astype(F32)
                + rights[h, n - 2, at(), :].astype(F32)
            )

        blocks(piece, step)

    load_weight.wait()
    for h in range(CHUNKS):
        load[h].wait()
        rows = pl.ds(h * per, per)
        product_tiles(part.at[rows], grads_v.at[rows], weight_v, 2 * LANES)
        scatters[h].step()
    for _ in range(n - 2):
        for h in range(CHUNKS):
            scatters[h].step()
    for h in range(CHUNKS):
        finish(h)
    for h in range(CHUNKS):
        scatters[h].drain()


def last_call(grads, weight, n):
    tokens, deep = grads.shape
    width = weight.shape[1]
    rows = tokens // n
    sems = CHUNKS * 2 * (n - 1)
    hop = (CHUNKS, n - 1, rows // CHUNKS, width)
    return pl.pallas_call(
        functools.partial(last_kernel, n),
        out_shape=jax.ShapeDtypeStruct((rows, width), F32),
        in_specs=[ANY, ANY],
        out_specs=VM,
        scratch_shapes=[
            pltpu.VMEM((tokens, deep), BF),
            pltpu.VMEM((deep, width), BF),
            pltpu.VMEM((tokens, width), BF),
            pltpu.VMEM(hop, BF),
            pltpu.VMEM(hop, BF),
            pltpu.SemaphoreType.DMA((CHUNKS + 1,)),
            pltpu.SemaphoreType.DMA((sems,)),
            pltpu.SemaphoreType.DMA((sems,)),
        ],
        compiler_params=pltpu.CompilerParams(
            collective_id=2, has_side_effects=True, vmem_limit_bytes=VMEM_MOST
        ),
        name="last",
    )(grads, weight)


def pad_rows(array, count):
    return jnp.pad(array, ((0, count - array.shape[0]), (0, 0)))


def pad_columns(array, count):
    return jnp.pad(array, ((0, 0), (0, count - array.shape[1])))


def body(
    inputs,
    segments,
    first_norm_gain,
    w_query,
    w_key,
    w_value,
    w_gate,
    w_out,
    second_norm_gain,
    w_glu_gate,
    w_glu_up,
    w_down,
    cotangent,
):
    n = lax.axis_size("mp")
    place = lax.axis_index("mp")
    heads = H // n
    head_start = place * heads
    rows, width = inputs.shape
    shard = w_query.shape[0]
    piece = rows // CHUNKS
    nk, nv, nf = heads * HK, heads * HV, w_down.shape[0]
    n_one = 2 * nk + 2 * nv
    one_wide = -(-n_one // (2 * LANES)) * 2 * LANES
    v_wide, f_wide = -(-nv // LANES) * LANES, -(-nf // LANES) * LANES
    f_tiles = f_wide // LANES

    pack_one = pad_rows(
        jnp.concatenate([w_query.T, w_key.T, w_value.T, w_gate.T], axis=0), one_wide
    )
    glu_pack = jnp.stack(
        [
            pad_rows(w_glu_gate.T, f_wide).reshape(f_tiles, LANES, shard),
            pad_rows(w_glu_up.T, f_wide).reshape(f_tiles, LANES, shard),
        ],
        axis=1,
    ).reshape(2 * f_wide, shard)
    pack_two = jnp.concatenate([glu_pack, pad_rows(w_down, f_wide), pad_rows(w_out, v_wide)], axis=0)
    weight_two = lax.all_gather(pack_two, "dp", axis=1, tiled=True)
    out_weight = weight_two[3 * f_wide :]

    first_hat, first_scale = layer_norm(inputs.astype(F32), epsilon)
    rows_one, weight_one = gather_rows(
        (first_hat * first_norm_gain).astype(BF), pack_one, n, lax.axis_size("dp")
    )
    tokens = rows_one.shape[0]

    slot_shard = lax.rem(place - jnp.arange(n) + n, n)
    places = (
        slot_shard[None, :, None] * rows
        + jnp.arange(CHUNKS)[:, None, None] * piece
        + jnp.arange(piece)[None, None, :]
    ).reshape(tokens)
    seg = segments.reshape(n, CHUNKS, piece)[::-1]
    seg = lax.dynamic_slice_in_dim(jnp.concatenate([seg, seg], axis=0), n - 1 - place, n, axis=0)
    seg = seg.transpose(1, 0, 2).reshape(tokens)

    query_key = dot_nt(rows_one, weight_one[: 2 * nk]).astype(BF)
    value = dot_nt(rows_one, weight_one[2 * nk : 2 * nk + nv]).astype(BF)
    gate_pre = dot_nt(rows_one, weight_one[2 * nk + nv : n_one])
    query = query_key[:, :nk].reshape(tokens, heads, HK)
    key = query_key[:, nk:].reshape(tokens, heads, HK)
    value = value.reshape(tokens, heads, HV)

    distance = places[:, None] - places[None, :]
    allowed = (distance >= 0) & (seg[:, None] == seg[None, :])
    log_gamma = jnp.log1p(-jnp.exp2(-5.0 - (head_start + jnp.arange(heads)).astype(F32)))
    exponent = jnp.where(
        allowed[None], distance[None].astype(F32) * log_gamma[:, None, None], 0.0
    )
    mask = jnp.where(allowed[None], jnp.exp(exponent), 0.0) * HK ** (-0.5)

    scores = (jnp.einsum("thk,shk->hts", query, key, preferred_element_type=F32) * mask).astype(BF)
    retained = jnp.einsum("hts,shv->thv", scores, value, preferred_element_type=F32)
    normalized, scale_group = layer_norm(retained, group_epsilon)
    normal_flat = normalized.reshape(tokens, nv)
    swish = jax.nn.silu(gate_pre)
    gated = pad_columns((swish * normal_flat).astype(BF), v_wide)

    rows_two, cot_rows, mid_rows, hidden, d_glu, outputs, middle_grad, second_gain = middle_call(
        gated, weight_two, inputs, cotangent, second_norm_gain[None], n
    )

    grads_two = jnp.concatenate([dot_tn(d_glu, rows_two), dot_tn(hidden, cot_rows)], axis=0).astype(BF)
    summed_two = lax.psum_scatter(grads_two, "dp", scatter_dimension=1, tiled=True).astype(F32)
    glu_sum = summed_two[: 2 * f_wide].reshape(f_tiles, 2, LANES, shard)

    d_gated = dot_nt(mid_rows, out_weight[:nv])
    sigmoid_gate = jax.nn.sigmoid(gate_pre)
    d_gate_pre = (
        d_gated * normal_flat * (sigmoid_gate + gate_pre * sigmoid_gate * (1.0 - sigmoid_gate))
    ).astype(BF)
    d_normalized = (d_gated * swish).reshape(tokens, heads, HV)
    d_retained = norm_back(d_normalized, normalized, scale_group).astype(BF)
    grads_out = jnp.concatenate(
        [dot_tn(gated[:, :nv], mid_rows).astype(BF), dot_tn(d_gate_pre, rows_one).astype(BF)], axis=0
    )
    summed_out = lax.psum_scatter(grads_out, "dp", scatter_dimension=1, tiled=True).astype(F32)

    d_value = jnp.einsum("hts,thv->shv", scores, d_retained, preferred_element_type=F32).astype(BF)
    d_scores = (
        jnp.einsum("thv,shv->hts", d_retained, value, preferred_element_type=F32) * mask
    ).astype(BF)
    d_query = jnp.einsum("hts,shk->thk", d_scores, key, preferred_element_type=F32).astype(BF)
    d_key = jnp.einsum("hts,thk->shk", d_scores, query, preferred_element_type=F32).astype(BF)
    d_qkv = jnp.concatenate(
        [d_query.reshape(tokens, nk), d_key.reshape(tokens, nk), d_value.reshape(tokens, nv)], axis=1
    )
    grads_one = dot_tn(d_qkv, rows_one).astype(BF)
    summed_one = lax.psum_scatter(grads_one, "dp", scatter_dimension=1, tiled=True).astype(F32)

    d_one = pad_columns(jnp.concatenate([d_qkv, d_gate_pre], axis=1), one_wide)
    first_grad = last_call(d_one, weight_one, n)
    first_gain = jnp.sum(first_hat * first_grad, axis=0)
    input_gradient = middle_grad + norm_back(first_grad * first_norm_gain, first_hat, first_scale)

    gains = sum_gains(
        jnp.stack([first_gain, jnp.sum(second_gain, axis=0)]), n, lax.axis_size("dp")
    )
    return (
        outputs,
        input_gradient,
        gains[0],
        summed_one[:nk].T,
        summed_one[nk : 2 * nk].T,
        summed_one[2 * nk :].T,
        summed_out[nv:].T,
        summed_out[:nv],
        gains[1],
        glu_sum[:, 0].reshape(f_wide, shard)[:nf].T,
        glu_sum[:, 1].reshape(f_wide, shard)[:nf].T,
        summed_two[2 * f_wide : 2 * f_wide + nf],
    )


def solution(mesh):
    split = P(("dp", "mp"), None)
    wide, tall = P("dp", "mp"), P("mp", "dp")
    return jax.shard_map(
        body,
        mesh=mesh,
        in_specs=(
            split, P("dp", None), P(), wide, wide, wide, wide, tall, P(), wide, wide, tall, split,
        ),
        out_specs=(
            split, split, P(), wide, wide, wide, wide, tall, P(), wide, wide, tall,
        ),
        check_vma=False,
    )
```

```python
import functools

import jax
import jax.numpy as jnp
from jax import lax
from jax.experimental import pallas as pl
from jax.experimental.pallas import tpu as pltpu
from jax.sharding import PartitionSpec as P

H = 8
HK = 256
HV = 432
LEN = 1024
CHUNKS = 4
FRONT = CHUNKS // 2
LANES = 128
VMEM_MOST = 66_000_000

epsilon = 1e-05
group_epsilon = 1.0
BF = jnp.bfloat16
F32 = jnp.float32


def layer_norm(values_in, offset):
    centre = jnp.mean(values_in, axis=-1, keepdims=True)
    centred = values_in - centre
    variance = jnp.mean(centred * centred, axis=-1, keepdims=True)
    scaling = lax.rsqrt(variance + offset)
    return (centred * scaling, scaling)


def norm_back(grad_hat, normed_hat, scaling):
    first_mean = jnp.mean(grad_hat, axis=-1, keepdims=True)
    second_mean = jnp.mean(grad_hat * normed_hat, axis=-1, keepdims=True)
    return scaling * (grad_hat - first_mean - normed_hat * second_mean)


def glu_act(gate_pre, up_pre):
    return jax.nn.gelu(gate_pre, approximate=True) * up_pre


def dot_nt(a, b):
    return lax.dot_general(a, b, (((1,), (1,)), ((), ())), preferred_element_type=F32)


def dot_nn(a, b):
    return lax.dot_general(a, b, (((1,), (0,)), ((), ())), preferred_element_type=F32)


def dot_tn(a, b):
    return lax.dot_general(a, b, (((0,), (0,)), ((), ())), preferred_element_type=F32)


MESH = pl.DeviceIdType.MESH


class Line:
    def __init__(self, n, send_sem, recv_sem):
        self.n, self.send_sem, self.recv_sem = n, send_sem, recv_sem
        self.place = lax.axis_index("mp")
        self.used = 0
        self.sent = []

    def enter(self, others=None):
        barrier = pltpu.get_barrier_semaphore()
        n, place = self.n, self.place

        @pl.when(place >= 1)
        def _():
            pl.semaphore_signal(barrier, inc=1, device_id={"mp": place - 1}, device_id_type=MESH)

        @pl.when(place <= n - 2)
        def _():
            pl.semaphore_signal(barrier, inc=1, device_id={"mp": place + 1}, device_id_type=MESH)

        peers = jnp.minimum(place, 1) + jnp.minimum(n - 1 - place, 1)
        if others is not None:
            axis, indices = others
            for index in indices:
                pl.semaphore_signal(barrier, inc=1, device_id={axis: index}, device_id_type=MESH)
            peers = peers + len(indices)
        pl.semaphore_wait(barrier, peers)

    def copy(self, src, dst, index, toward):
        return pltpu.make_async_remote_copy(
            src_ref=src,
            dst_ref=dst,
            send_sem=self.send_sem.at[index],
            recv_sem=self.recv_sem.at[index],
            device_id={"mp": self.place + toward},
            device_id_type=MESH,
        )

    def leave(self):
        for condition, copy in self.sent:
            pl.when(condition)(copy.wait_send)


class Gather:
    def __init__(self, line, slot):
        self.line, self.slot, self.step_no = line, slot, 0
        self.base = line.used
        line.used += 2 * (line.n - 1)
        n = line.n
        self.right = [
            line.copy(slot(s - 1), slot(s), self.base + s - 1, 1) for s in range(1, n)
        ]
        self.left = [
            line.copy(slot((n - s + 1) % n), slot(n - s), self.base + n - 2 + s, -1)
            for s in range(1, n)
        ]

    def arrive(self, s):
        n, place = self.line.n, self.line.place
        pl.when(place >= s)(self.right[s - 1].wait_recv)
        pl.when(place <= n - 1 - s)(self.left[s - 1].wait_recv)

    def step(self):
        self.step_no += 1
        s, n, place = self.step_no, self.line.n, self.line.place
        if s > 1:
            self.arrive(s - 1)
        if s < n:
            to_right = (place >= s - 1) & (place <= n - 2)
            to_left = (place <= n - s) & (place >= 1)
            pl.when(to_right)(self.right[s - 1].start)
            pl.when(to_left)(self.left[s - 1].start)
            self.line.sent += [(to_right, self.right[s - 1]), (to_left, self.left[s - 1])]


class Scatter:
    def __init__(self, line, slot, from_left, from_right, add):
        self.line, self.slot, self.add, self.step_no = line, slot, add, 0
        self.from_left, self.from_right = from_left, from_right
        self.base = line.used
        line.used += 2 * (line.n - 1)
        n = line.n
        self.right = [
            line.copy(slot(s), from_left(s), self.base + s - 1, 1) for s in range(1, n)
        ]
        self.left = [
            line.copy(slot(n - s), from_right(s), self.base + n - 2 + s, -1) for s in range(1, n)
        ]
        self.mine = []

    def step(self):
        self.step_no += 1
        s, n, place = self.step_no, self.line.n, self.line.place
        to_right, to_left = place <= s - 1, place >= n - s
        if s > 1:

            @pl.when(to_right & (place >= 1))
            def _():
                self.right[s - 2].wait_recv()
                self.add(self.slot(s), self.from_left(s - 1))

            @pl.when(to_left & (place <= n - 2))
            def _():
                self.left[s - 2].wait_recv()
                self.add(self.slot(n - s), self.from_right(s - 1))

        pl.when(to_right)(self.right[s - 1].start)
        pl.when(to_left)(self.left[s - 1].start)
        self.mine += [(to_right, self.right[s - 1]), (to_left, self.left[s - 1])]

    def finish(self):
        n, place = self.line.n, self.line.place

        @pl.when(place >= 1)
        def _():
            self.right[n - 2].wait_recv()

        @pl.when(place <= n - 2)
        def _():
            self.left[n - 2].wait_recv()

    def drain(self):
        for condition, copy in self.mine:
            pl.when(condition)(copy.wait_send)


ANY = pl.BlockSpec(memory_space=pl.ANY)
VM = pl.BlockSpec(memory_space=pltpu.VMEM)
BLOCK = 16


def blocks(count, step):
    def run(i, carry):
        step(lambda base=0: pl.ds(pl.multiple_of(base + i * BLOCK, BLOCK), BLOCK))
        return carry

    lax.fori_loop(0, count // BLOCK, run, 0)


def add_into(target, extra):
    def step(at):
        target[at(), :] = (target[at(), :].astype(F32) + extra[at(), :].astype(F32)).astype(BF)

    blocks(target.shape[0], step)


def product_tiles(target, left, right, tile):
    def step(j, carry):
        at = pl.ds(pl.multiple_of(j * tile, tile), tile)
        target[:, at] = dot_nn(left[...], right[:, at]).astype(BF)
        return carry

    lax.fori_loop(0, right.shape[1] // tile, step, 0)


class Doubling:
    def __init__(self, m, own, out, rows, bits, base, send_sem, recv_sem):
        self.d = lax.axis_index("dp")
        self.own, self.out, self.rows, self.bits, self.base = own, out, rows, bits, base
        self.send_sem, self.recv_sem = send_sem, recv_sem
        self.shard = own.shape[1]
        self.done = 0
        self.sent = []

    def flip(self, d, bit):
        return d + bit * (1 - 2 * (lax.div(d, bit) % 2))

    def block(self, d):
        return self.out.at[self.rows, pl.ds(pl.multiple_of(d * self.shard, self.shard), self.shard)]

    def copies(self, level, landing):
        owners = [self.d]
        for bit in self.bits[:level]:
            owners += [self.flip(d, bit) for d in owners]
        bit = self.bits[level]
        partner = self.flip(self.d, bit)
        out = []
        for i, d in enumerate(owners):
            d = self.flip(d, bit) if landing else d
            src = self.own.at[self.rows] if i == 0 and not landing else self.block(d)
            index = self.base + (1 << level) - 1 + i
            out.append(
                pltpu.make_async_remote_copy(
                    src_ref=src,
                    dst_ref=self.block(d),
                    send_sem=self.send_sem.at[index],
                    recv_sem=self.recv_sem.at[index],
                    device_id={"dp": partner},
                    device_id_type=MESH,
                )
            )
        return out

    def step(self):
        level = self.done
        if level > 0:
            for c in self.copies(level - 1, True):
                c.wait_recv()
        if level < len(self.bits):
            out = self.copies(level, False)
            for c in out:
                c.start()
            self.sent += out
        self.done += 1

    def leave(self):
        for c in self.sent:
            c.wait_send()


def bits_of(m):
    bits = [1 << b for b in range(m.bit_length() - 1)]
    assert 1 << len(bits) == m
    return bits


PARTS = 2


def gather_kernel(n, m, own, pack, out, weight, send_sem, recv_sem, copy_sem, wide_send, wide_recv):
    line = Line(n, send_sem, recv_sem)
    piece = own.shape[0] // CHUNKS
    per = n * piece
    shard = pack.shape[1]
    d = lax.axis_index("dp")
    bits = bits_of(m)
    outer = bits[1:]
    height = pack.shape[0] // (2 * PARTS)
    doubling = []
    for i in range(2 * PARTS):
        order = (outer if i % 2 == 0 else outer[::-1]) + bits[:1]
        doubling.append(
            Doubling(
                m, pack, weight, pl.ds(i * height, height), order, i * (m - 1), wide_send, wide_recv
            )
        )
    first = doubling[0]
    line.enter(["dp", [first.flip(d, bit) for bit in bits]])
    local, gathers = [], []
    columns = pl.ds(pl.multiple_of(d * shard, shard), shard)
    keep = pltpu.make_async_copy(pack, weight.at[:, columns], copy_sem.at[CHUNKS])
    for h in range(CHUNKS):
        mine = own.at[pl.ds(h * piece, piece)]
        local.append(
            pltpu.make_async_copy(mine, out.at[pl.ds(h * per, piece)], copy_sem.at[h])
        )

        def slot(k, h=h, mine=mine):
            return mine if k == 0 else out.at[pl.ds(h * per + k * piece, piece)]

        gathers.append(Gather(line, slot))
    local.append(keep)

    def line_step(items):
        for item in items:
            item.step()

    half = CHUNKS // 2
    line_step(gathers)
    line_step(doubling)
    for item in local:
        item.start()
    for level in range(1, max(n, len(bits) + 1)):
        for side in range(2):
            if level <= len(bits):
                line_step(doubling[side * PARTS : (side + 1) * PARTS])
            if level < n:
                line_step(gathers[side * half : (side + 1) * half])
    for item in local:
        item.wait()
    for item in gathers:
        assert item.step_no == n
    for item in doubling:
        assert item.done == len(bits) + 1
        item.leave()
    line.leave()


def gather_rows(own, pack, n, m):
    rows, width = own.shape
    count = CHUNKS * 2 * (n - 1)
    wide = 2 * PARTS * (m - 1)
    return pl.pallas_call(
        functools.partial(gather_kernel, n, m),
        out_shape=(
            jax.ShapeDtypeStruct((n * rows, width), own.dtype),
            jax.ShapeDtypeStruct((pack.shape[0], m * pack.shape[1]), pack.dtype),
        ),
        in_specs=[VM, VM],
        out_specs=(ANY, ANY),
        scratch_shapes=[
            pltpu.SemaphoreType.DMA((count,)),
            pltpu.SemaphoreType.DMA((count,)),
            pltpu.SemaphoreType.DMA((CHUNKS + 1,)),
            pltpu.SemaphoreType.DMA((wide,)),
            pltpu.SemaphoreType.DMA((wide,)),
        ],
        compiler_params=pltpu.CompilerParams(collective_id=0, has_side_effects=True),
        name="gather_rows",
    )(own, pack)


def no_neighbour_zero(n, place, from_left, from_right):
    @pl.when(place == 0)
    def _():
        from_left[...] = jnp.zeros_like(from_left)

    @pl.when(place == n - 1)
    def _():
        from_right[...] = jnp.zeros_like(from_right)


(COT, OUT, ONE, END_ONE, TWO, GLU, GRAD, GRAD_SUM, END_GRAD, MID, DOWN, DOWN_SUM, END_DOWN) = range(13)

DUE = {
    OUT: (-2.23, 1.66, 0), ONE: (-1.99, 1.12, 1.03), END_ONE: (1.46, 1.37, 0), TWO: (0.73, 1.15, 0.94),
    COT: (0.35, 1.39, 1.02), GLU: (1.14, -1.37, 1.55), GRAD: (3.09, 2.02, 0),
    GRAD_SUM: (3.48, 1.71, 0.74), END_GRAD: (7.02, -2.12, 0), MID: (5.68, 0.86, 1.11),
    DOWN: (1.3, 0.36, 0), DOWN_SUM: (1.87, 1.35, 0.95), END_DOWN: (7.9, 2.17, 0),
}
TUNED = {
    (4, 4): [
        2, 4, 8, 8, 5, 2, 8, 6, 9, 10, 2, 9, 12, 16, 7, 9, 11, 16, 13, 10,
        11, 16, 16, 17, 2, 20, 11, 10, 20, 17, 15, 19, 14, 24, 17, 18, 40, 28, 17, 21,
        18, 28, 18, 3, 21, 28, 25, 19, 18, 29, 22, 29, 32, 3, 36, 44, 19, 22, 26, 36,
        30, 41, 30, 3, 42, 44, 19, 3, 29, 30, 23, 44, 23, 36, 34, 33, 38, 37, 27, 31,
        38, 31, 37, 38, 31, 45, 45, 35, 39, 36, 45, 39, 49, 48, 37, 43, 37, 39, 39, 38,
    ],
}


def middle_order(n):
    if (n, CHUNKS) in TUNED:
        return [divmod(code, CHUNKS) for code in TUNED[n, CHUNKS]]
    count = {k: 1 for k in DUE}
    count.update({COT: n, TWO: n, MID: n, ONE: n - 1, GRAD_SUM: n - 1, DOWN_SUM: n - 1, GLU: 2})
    needs = {
        ONE: [OUT], END_ONE: [ONE], TWO: [END_ONE], GLU: [TWO, COT], GRAD: [GLU], GRAD_SUM: [GRAD],
        END_GRAD: [GRAD_SUM], MID: [END_GRAD], DOWN: [GLU], DOWN_SUM: [DOWN], END_DOWN: [DOWN_SUM],
    }
    todo = sorted(
        (first + h * later + s * 3 / (n - 1) * each, k, h, s)
        for k, (first, later, each) in DUE.items()
        for h in range(CHUNKS)
        for s in range(count[k])
        if not (k == COT and h < FRONT or k in (DOWN_SUM, END_DOWN) and h >= FRONT)
    )
    taken, order = {}, []
    while todo:
        for item in todo:
            _, k, h, s = item
            ready = taken.get((k, h), 0) == s and all(
                taken.get((need, h), 0) == count[need] or (need == COT and h < FRONT)
                for need in needs.get(k, [])
            )
            if ready:
                break
        todo.remove(item)
        taken[k, h] = s + 1
        order.append((k, h))
    return order


def middle_kernel(
    n, gated, weights, own, cot, cot_front, gain,
    rows_out, cot_out, mid_out, hidden_out, glu_out, down_out, outputs, middle_out, d_middle,
    gain_out,
    gated_v, wo_v, wg_v, wd_v, own_v, cot_v, rows_v, hidden_v, glu_v, part, part_two,
    left_a, right_a, left_b, right_b, middle, stage, copy_sem, send_sem, recv_sem,
):
    line = Line(n, send_sem, recv_sem)
    place = line.place
    count, width = own.shape
    piece = count // CHUNKS
    per = n * piece
    wide = hidden_v.shape[1]
    copies = []

    def local(src, dst):
        c = pltpu.make_async_copy(src, dst, copy_sem.at[len(copies)])
        copies.append(c)
        c.start()
        return c

    def rows_at(ref, h, k=0, size=piece):
        return ref.at[pl.ds(h * per + k * piece, size)]

    load_cot = [
        local(cot.at[pl.ds(h * piece, piece)], rows_at(cot_v, h)) for h in range(FRONT, CHUNKS)
    ]
    front = pl.ds(0, FRONT * per)
    load_cot.append(local(cot_front, cot_v.at[front]))
    load_gated = local(gated, gated_v)
    load_wo = local(weights.at[pl.ds(3 * wide, wo_v.shape[0])], wo_v)
    load_own = local(own, own_v)
    load_wg = local(weights.at[pl.ds(0, 2 * wide)], wg_v)
    load_wd = local(weights.at[pl.ds(2 * wide, wide)], wd_v)
    line.enter()
    for h in range(CHUNKS):
        no_neighbour_zero(n, place, left_a.at[h, n - 2], right_a.at[h, n - 2])
    for h in range(FRONT):
        no_neighbour_zero(n, place, left_b.at[h, n - 2], right_b.at[h, n - 2])
    gain_out[...] = jnp.zeros_like(gain_out)

    def scatter(buf, lefts, rights, h):
        return Scatter(
            line,
            lambda k: rows_at(buf, h, k),
            lambda s: lefts.at[h, s - 1],
            lambda s: rights.at[h, s - 1],
            add_into,
        )

    gather_cot = {
        h: Gather(line, functools.partial(rows_at, cot_v, h)) for h in range(FRONT, CHUNKS)
    }
    gather_two = [Gather(line, functools.partial(rows_at, rows_v, h)) for h in range(CHUNKS)]

    def mid_slot(h, k):
        return stage.at[h] if k == 0 else rows_at(mid_out, h, k)

    gather_mid = [Gather(line, functools.partial(mid_slot, h)) for h in range(CHUNKS)]
    scatter_one = [scatter(part, left_a, right_a, h) for h in range(CHUNKS)]
    scatter_two = [scatter(part_two, left_b, right_b, h) for h in range(FRONT)]
    scatter_grad = [scatter(part, left_a, right_a, h) for h in range(CHUNKS)]

    def chunk(ref, h):
        return ref.at[pl.ds(h * per, per)]

    def out_product(h):
        heads, _, size = gated_v.shape
        target, whole = chunk(part, h), pl.ds(h * per, per)

        def step(j, carry):
            at = pl.ds(pl.multiple_of(j * 2 * LANES, 2 * LANES), 2 * LANES)
            target[:, at] = sum(
                dot_nn(gated_v[i, whole, :], wo_v[pl.ds(i * size, size), at]) for i in range(heads)
            ).astype(BF)
            return carry

        lax.fori_loop(0, width // (2 * LANES), step, 0)

    def finish_one(h):
        scatter_one[h].finish()

        def step(at):
            src = at(h * per)
            mine = at(h * piece)
            total = (
                own_v[mine, :].astype(F32)
                + part[src, :].astype(F32)
                + left_a[h, n - 2, at(), :].astype(F32)
                + right_a[h, n - 2, at(), :].astype(F32)
            )
            middle[mine, :] = total
            hat, _ = layer_norm(total, epsilon)
            rows_v[src, :] = (hat * gain[...]).astype(BF)

        blocks(piece, step)

    def glu_tiles(h, first, last):
        def step(j, carry):
            pair = pl.ds(pl.multiple_of(j * 2 * LANES, 2 * LANES), 2 * LANES)
            at = pl.ds(pl.multiple_of(j * LANES, LANES), LANES)
            whole = pl.ds(h * per, per)
            both = dot_nt(rows_v[whole, :], wg_v[pair, :])
            d_hidden = dot_nt(cot_v[whole, :], wd_v[at, :])
            u, up = both[:, :LANES], both[:, LANES:]
            c = 0.7978845608028654
            t = jnp.tanh(c * (u + 0.044715 * (u * u * u)))
            half = 0.5 * (1.0 + t)
            act = u * half
            slope = half + 0.5 * u * (1.0 - t * t) * (c * (1.0 + 3 * 0.044715 * (u * u)))
            hidden_v[whole, at] = (act * up).astype(BF)
            glu_v[whole, pair] = jnp.concatenate(
                [(d_hidden * up * slope).astype(BF), (d_hidden * act).astype(BF)], axis=1
            )
            return carry

        lax.fori_loop(first, last, step, 0)

    def grad_product(h):
        product_tiles(chunk(part, h), chunk(glu_v, h), wg_v, 2 * LANES)

    def down_product(h):
        product_tiles(chunk(part_two, h), chunk(hidden_v, h), wd_v, 2 * LANES)

    def finish_grad(h):
        scatter_grad[h].finish()

        def step(at):
            src = at(h * per)
            mine = at(h * piece)
            grad = (
                part[src, :].astype(F32)
                + left_a[h, n - 2, at(), :].astype(F32)
                + right_a[h, n - 2, at(), :].astype(F32)
            )
            hat, scale = layer_norm(middle[mine, :], epsilon)
            gain_out[...] += jnp.sum((hat * grad).reshape(BLOCK // 8, 8, width), axis=0)
            d_mid = cot_v[src, :].astype(F32) + norm_back(grad * gain[...], hat, scale)
            d_middle[mine, :] = d_mid
            stage[h, at(), :] = d_mid.astype(BF)

        blocks(piece, step)
        local(stage.at[h], rows_at(mid_out, h))

    def finish_two(h):
        scatter_two[h].finish()

        def step(at):
            src = at(h * per)
            mine = at(h * piece)
            outputs[mine, :] = (
                middle[mine, :]
                + part_two[src, :].astype(F32)
                + left_b[h, n - 2, at(), :].astype(F32)
                + right_b[h, n - 2, at(), :].astype(F32)
            ).astype(BF)

        blocks(piece, step)

    tiles = wide // LANES
    cut = tiles // 2

    def wait_for(items):
        for item in items:
            item.wait()
        items.clear()

    first_loads, own_load = [load_gated, load_wo], [load_own]
    later_loads = [load_wg, load_wd]

    def out_action(h):
        wait_for(first_loads)
        out_product(h)

    def finish_one_action(h):
        wait_for(own_load)
        finish_one(h)

    def glu_action(h):
        wait_for(later_loads)
        if h in begun:
            glu_tiles(h, cut, tiles)
        else:
            begun.add(h)
            glu_tiles(h, 0, cut)

    def grad_action(h):
        scatter_one[h].drain()
        grad_product(h)

    begun = set()
    actions = {
        COT: lambda h: gather_cot[h].step(),
        OUT: out_action,
        ONE: lambda h: scatter_one[h].step(),
        END_ONE: finish_one_action,
        TWO: lambda h: gather_two[h].step(),
        GLU: glu_action,
        GRAD: grad_action,
        GRAD_SUM: lambda h: scatter_grad[h].step(),
        END_GRAD: finish_grad,
        MID: lambda h: gather_mid[h].step(),
        DOWN: down_product,
        DOWN_SUM: lambda h: scatter_two[h].step(),
        END_DOWN: finish_two,
    }
    for item in load_cot:
        item.wait()
    for kind, h in middle_order(n):
        actions[kind](h)
    for c in range(CHUNKS):
        local(chunk(rows_v, c), chunk(rows_out, c))
        local(chunk(cot_v, c), chunk(cot_out, c))
        local(chunk(hidden_v, c), chunk(hidden_out, c))
        local(chunk(glu_v, c), chunk(glu_out, c))
    local(part_two.at[pl.ds(FRONT * per, down_out.shape[0])], down_out)
    local(middle.at[pl.ds(FRONT * piece, middle_out.shape[0])], middle_out)
    for item in list(gather_cot.values()) + gather_two + gather_mid:
        assert item.step_no == n
    for item in scatter_one + scatter_two + scatter_grad:
        assert item.step_no == n - 1
    for group in (scatter_grad, scatter_two):
        for item in group:
            item.drain()
    for item in copies[CHUNKS - FRONT + 6 :]:
        item.wait()
    line.leave()


def middle_call(gated, weights, own, cot, cot_front, gain, n):
    rows, width = own.shape
    heads, tokens, size = gated.shape
    nv = heads * size
    wide = (weights.shape[0] - -(-nv // LANES) * LANES) // 3
    piece = rows // CHUNKS
    back = CHUNKS - FRONT
    sems = CHUNKS * 5 * 2 * (n - 1)
    hop = (CHUNKS, n - 1, piece, width)
    shape = jax.ShapeDtypeStruct
    return pl.pallas_call(
        functools.partial(middle_kernel, n),
        out_shape=(
            shape((tokens, width), BF),
            shape((tokens, width), BF),
            shape((tokens, width), BF),
            shape((tokens, wide), BF),
            shape((tokens, 2 * wide), BF),
            shape((back * n * piece, width), BF),
            shape((FRONT * piece, width), BF),
            shape((back * piece, width), F32),
            shape((rows, width), F32),
            shape((8, width), F32),
        ),
        in_specs=[ANY] * 5 + [VM],
        out_specs=(ANY,) * 6 + (VM, ANY, VM, VM),
        scratch_shapes=[
            pltpu.VMEM((heads, tokens, size), BF),
            pltpu.VMEM((nv, width), BF),
            pltpu.VMEM((2 * wide, width), BF),
            pltpu.VMEM((wide, width), BF),
            pltpu.VMEM((rows, width), BF),
            pltpu.VMEM((tokens, width), BF),
            pltpu.VMEM((tokens, width), BF),
            pltpu.VMEM((tokens, wide), BF),
            pltpu.VMEM((tokens, 2 * wide), BF),
            pltpu.VMEM((tokens, width), BF),
            pltpu.VMEM((tokens, width), BF),
            pltpu.VMEM(hop, BF),
            pltpu.VMEM(hop, BF),
            pltpu.VMEM((FRONT,) + hop[1:], BF),
            pltpu.VMEM((FRONT,) + hop[1:], BF),
            pltpu.VMEM((rows, width), F32),
            pltpu.VMEM((CHUNKS, piece, width), BF),
            pltpu.SemaphoreType.DMA((8 + 6 * CHUNKS - FRONT,)),
            pltpu.SemaphoreType.DMA((sems,)),
            pltpu.SemaphoreType.DMA((sems,)),
        ],
        compiler_params=pltpu.CompilerParams(
            collective_id=1, has_side_effects=True, vmem_limit_bytes=VMEM_MOST
        ),
        name="middle",
    )(gated, weights, own, cot, cot_front, gain)


def gains_kernel(n, m, mine, total, first, second, send_sem, recv_sem):
    barrier = pltpu.get_barrier_semaphore()
    groups = (("dp", m, first), ("mp", n, second))
    for axis, size, _ in groups:
        me = lax.axis_index(axis)
        for k in range(1, size):
            peer = lax.rem(me + k, size)
            pl.semaphore_signal(barrier, inc=1, device_id={axis: peer}, device_id_type=MESH)
    pl.semaphore_wait(barrier, n + m - 2)
    source = mine
    for base, (axis, size, held) in zip((0, m), groups):
        me = lax.axis_index(axis)
        held[me] = source[...]

        def copy(k, slot):
            return pltpu.make_async_remote_copy(
                src_ref=source,
                dst_ref=held.at[slot],
                send_sem=send_sem.at[base + k],
                recv_sem=recv_sem.at[base + k],
                device_id={axis: lax.rem(me + k, size)},
                device_id_type=MESH,
            )

        sent = [copy(k, me) for k in range(1, size)]
        for c in sent:
            c.start()
        for k in range(1, size):
            copy(k, lax.rem(me - k + size, size)).wait_recv()
        value = held[0]
        for k in range(1, size):
            value = value + held[k]
        for c in sent:
            c.wait_send()
        total[...] = value
        source = total


def sum_gains(values, n, m):
    flat = values.reshape(-1, LANES)
    return pl.pallas_call(
        functools.partial(gains_kernel, n, m),
        out_shape=jax.ShapeDtypeStruct(flat.shape, F32),
        in_specs=[VM],
        out_specs=VM,
        scratch_shapes=[
            pltpu.VMEM((m,) + flat.shape, F32),
            pltpu.VMEM((n,) + flat.shape, F32),
            pltpu.SemaphoreType.DMA((n + m,)),
            pltpu.SemaphoreType.DMA((n + m,)),
        ],
        compiler_params=pltpu.CompilerParams(collective_id=3, has_side_effects=True),
        name="sum_gains",
    )(flat).reshape(values.shape)


def last_kernel(
    n, d_qk, d_value, d_gate, weight, out,
    qk_v, value_v, gate_v, weight_v, part, lefts, rights, copy_sem, send_sem, recv_sem
):
    line = Line(n, send_sem, recv_sem)
    count, width = out.shape
    piece = count // CHUNKS
    per = n * piece
    heads, _, size = value_v.shape
    wide = qk_v.shape[1]
    load = [
        pltpu.make_async_copy(src, dst, copy_sem.at[i])
        for i, (src, dst) in enumerate(
            [(weight, weight_v), (d_qk, qk_v), (d_value, value_v), (d_gate, gate_v)]
        )
    ]
    for item in load:
        item.start()
    line.enter()
    for h in range(CHUNKS):
        no_neighbour_zero(n, line.place, lefts.at[h, n - 2], rights.at[h, n - 2])
    scatters = [
        Scatter(
            line,
            lambda k, h=h: part.at[pl.ds(h * per + k * piece, piece)],
            lambda s, h=h: lefts.at[h, s - 1],
            lambda s, h=h: rights.at[h, s - 1],
            add_into,
        )
        for h in range(CHUNKS)
    ]

    def product(h):
        rows = pl.ds(h * per, per)

        def step(j, carry):
            at = pl.ds(pl.multiple_of(j * 2 * LANES, 2 * LANES), 2 * LANES)
            total = dot_nn(qk_v[rows, :], weight_v[pl.ds(0, wide), at])
            for i in range(heads):
                base = wide + i * size
                total += dot_nn(value_v[i, rows, :], weight_v[pl.ds(base, size), at])
                base += heads * size
                total += dot_nn(gate_v[i, rows, :], weight_v[pl.ds(base, size), at])
            part[rows, at] = total.astype(BF)
            return carry

        lax.fori_loop(0, width // (2 * LANES), step, 0)

    def finish(h):
        scatters[h].finish()

        def step(at):
            out[at(h * piece), :] = (
                part[at(h * per), :].astype(F32)
                + lefts[h, n - 2, at(), :].astype(F32)
                + rights[h, n - 2, at(), :].astype(F32)
            )

        blocks(piece, step)

    for item in load:
        item.wait()
    for h in range(CHUNKS):
        product(h)
        scatters[h].step()
    for _ in range(n - 2):
        for h in range(CHUNKS):
            scatters[h].step()
    for h in range(CHUNKS):
        finish(h)
    for h in range(CHUNKS):
        scatters[h].drain()


def last_call(d_qk, d_value, d_gate, weight, n):
    tokens = d_qk.shape[0]
    width = weight.shape[1]
    rows = tokens // n
    sems = CHUNKS * 2 * (n - 1)
    hop = (CHUNKS, n - 1, rows // CHUNKS, width)
    return pl.pallas_call(
        functools.partial(last_kernel, n),
        out_shape=jax.ShapeDtypeStruct((rows, width), F32),
        in_specs=[ANY] * 4,
        out_specs=VM,
        scratch_shapes=[
            pltpu.VMEM(d_qk.shape, BF),
            pltpu.VMEM(d_value.shape, BF),
            pltpu.VMEM(d_gate.shape, BF),
            pltpu.VMEM(weight.shape, BF),
            pltpu.VMEM((tokens, width), BF),
            pltpu.VMEM(hop, BF),
            pltpu.VMEM(hop, BF),
            pltpu.SemaphoreType.DMA((4,)),
            pltpu.SemaphoreType.DMA((sems,)),
            pltpu.SemaphoreType.DMA((sems,)),
        ],
        compiler_params=pltpu.CompilerParams(
            collective_id=2, has_side_effects=True, vmem_limit_bytes=VMEM_MOST
        ),
        name="last",
    )(d_qk, d_value, d_gate, weight)


TILE = 256


def tiles_of(count, step):
    def run(i, carry):
        step(pl.ds(pl.multiple_of(i * TILE, TILE), TILE))
        return carry

    lax.fori_loop(0, count // TILE, run, 0)


def in_order(units, steps):
    taken = 0
    for i, unit in enumerate(units):
        unit()
        upto = (i + 1) * len(steps) // len(units)
        for step in steps[taken:upto]:
            step()
        taken = upto


def forward_kernel(
    n, rows, weight, cot, col, row,
    query_o, key_o, value_o, gate_o, norm_o, scale_o, scores_o, gated_o, cot_o,
    rows_v, weight_v, query_v, key_v, value_v, gate_v, norm_v, scale_v, scores_v, gated_v, cot_v,
    copy_sem, send_sem, recv_sem,
):
    line = Line(n, send_sem, recv_sem)
    heads, tokens, deep = query_v.shape
    size = value_v.shape[2]
    per = cot_v.shape[0] // FRONT
    piece = per // n
    copies = []

    def local(src, dst):
        c = pltpu.make_async_copy(src, dst, copy_sem.at[len(copies)])
        copies.append(c)
        c.start()
        return c

    load_cot = [
        local(cot.at[pl.ds(h * piece, piece)], cot_v.at[pl.ds(h * per, piece)])
        for h in range(FRONT)
    ]
    load_rows, load_weight = local(rows, rows_v), local(weight, weight_v)
    line.enter()
    gathers = [
        Gather(line, lambda k, h=h: cot_v.at[pl.ds(h * per + k * piece, piece)])
        for h in range(FRONT)
    ]
    for item in load_cot:
        item.wait()
    for g in gathers:
        g.step()
    load_rows.wait()
    load_weight.wait()

    def project(target, h, base, width):
        def step(at):
            target[h, at, :] = dot_nt(rows_v[at, :], weight_v[pl.ds(base, width), :]).astype(
                target.dtype
            )

        return lambda: tiles_of(tokens, step)

    def attend(h):
        def step(at):
            allowed = (col[at, 0:1] >= row[0:1, :]) & (col[at, 1:2] == row[1:2, :])
            scores = dot_nt(query_v[h, at, :], key_v[h]) * col[at, 2 + h : 3 + h]
            scores = jnp.where(allowed, scores * row[2 + h : 3 + h, :], 0.0).astype(BF)
            scores_v[h, at, :] = scores
            hat, scale = layer_norm(dot_nn(scores, value_v[h]), group_epsilon)
            norm_v[h, at, :] = hat
            scale_v[h, at, :] = scale
            gate = gate_v[h, at, :]
            gated_v[h, at, :] = (gate * jax.nn.sigmoid(gate) * hat).astype(BF)

        return lambda: tiles_of(tokens, step)

    values, gates = 2 * heads * deep, 2 * heads * deep + heads * size
    units = []
    for h in range(heads):
        units += [
            project(query_v, h, h * deep, deep),
            project(key_v, h, (heads + h) * deep, deep),
            project(value_v, h, values + h * size, size),
            project(gate_v, h, gates + h * size, size),
            attend(h),
        ]
    in_order(units, [g.step for _ in range(n - 1) for g in gathers])
    count = len(copies)
    for src, dst in (
        (query_v, query_o), (key_v, key_o), (value_v, value_o), (gate_v, gate_o),
        (norm_v, norm_o), (scale_v, scale_o), (scores_v, scores_o), (gated_v, gated_o),
        (cot_v, cot_o),
    ):
        local(src, dst)
    for item in copies[count:]:
        item.wait()
    line.leave()


def forward_call(rows, weight, cot, col, row, n, heads):
    tokens, width = rows.shape
    shape = jax.ShapeDtypeStruct
    outs = (
        shape((heads, tokens, HK), BF),
        shape((heads, tokens, HK), BF),
        shape((heads, tokens, HV), BF),
        shape((heads, tokens, HV), F32),
        shape((heads, tokens, HV), F32),
        shape((heads, tokens, 1), F32),
        shape((heads, tokens, tokens), BF),
        shape((heads, tokens, HV), BF),
        shape((tokens * FRONT // CHUNKS, width), BF),
    )
    sems = FRONT * 2 * (n - 1)
    return pl.pallas_call(
        functools.partial(forward_kernel, n),
        out_shape=outs,
        in_specs=[ANY] * 3 + [VM] * 2,
        out_specs=(ANY,) * len(outs),
        scratch_shapes=[pltpu.VMEM(rows.shape, BF), pltpu.VMEM(weight.shape, BF)]
        + [pltpu.VMEM(o.shape, o.dtype) for o in outs]
        + [
            pltpu.SemaphoreType.DMA((FRONT + 2 + len(outs),)),
            pltpu.SemaphoreType.DMA((sems,)),
            pltpu.SemaphoreType.DMA((sems,)),
        ],
        compiler_params=pltpu.CompilerParams(
            collective_id=4, has_side_effects=True, vmem_limit_bytes=VMEM_MOST
        ),
        name="forward",
    )(rows, weight, cot, col, row)


def backward_kernel(
    n, mid, weights, gate, norm, scale, scores, query, key, value, down, middle, col, row,
    qk_o, value_o, gate_o, outputs,
    mid_v, wo_v, gate_v, norm_v, scale_v, scores_v, query_v, key_v, value_v, part, middle_v,
    d_qk, d_value, d_gate, d_kept, d_scores, lefts, rights, copy_sem, send_sem, recv_sem,
):
    line = Line(n, send_sem, recv_sem)
    heads, tokens, deep = query_v.shape
    size = value_v.shape[2]
    back = CHUNKS - FRONT
    per = part.shape[0] // back
    piece = per // n
    copies = []

    def local(src, dst):
        c = pltpu.make_async_copy(src, dst, copy_sem.at[len(copies)])
        copies.append(c)
        c.start()
        return c

    load_part = local(down, part)
    loads = [
        local(src, dst)
        for src, dst in (
            (mid, mid_v), (weights.at[pl.ds(weights.shape[0] - wo_v.shape[0], wo_v.shape[0])], wo_v),
            (gate, gate_v), (norm, norm_v), (scale, scale_v), (value, value_v), (key, key_v),
            (query, query_v), (scores, scores_v), (middle, middle_v),
        )
    ]
    line.enter()
    for h in range(back):
        no_neighbour_zero(n, line.place, lefts.at[h, n - 2], rights.at[h, n - 2])
    scatters = [
        Scatter(
            line,
            lambda k, h=h: part.at[pl.ds(h * per + k * piece, piece)],
            lambda s, h=h: lefts.at[h, s - 1],
            lambda s, h=h: rights.at[h, s - 1],
            add_into,
        )
        for h in range(back)
    ]
    load_part.wait()
    for item in scatters:
        item.step()
    for item in loads:
        item.wait()

    def gates(h):
        def step(at):
            grad = dot_nt(mid_v[at, :], wo_v[pl.ds(h * size, size), :])
            pre, hat = gate_v[h, at, :], norm_v[h, at, :]
            s = jax.nn.sigmoid(pre)
            d_gate[h, at, :] = (grad * hat * (s + pre * s * (1.0 - s))).astype(BF)
            d_kept[h, at, :] = norm_back(grad * (pre * s), hat, scale_v[h, at, :]).astype(BF)

        return lambda: tiles_of(tokens, step)

    def by_row(h):
        def step(at):
            allowed = (col[at, 0:1] >= row[0:1, :]) & (col[at, 1:2] == row[1:2, :])
            grad = dot_nt(d_kept[h, at, :], value_v[h]) * col[at, 2 + h : 3 + h]
            grad = jnp.where(allowed, grad * row[2 + h : 3 + h, :], 0.0).astype(BF)
            d_scores[at, :] = grad
            d_qk[at, pl.ds(h * deep, deep)] = dot_nn(grad, key_v[h]).astype(BF)

        return lambda: tiles_of(tokens, step)

    def by_column(h):
        def step(at):
            d_value[h, at, :] = dot_tn(scores_v[h, :, at], d_kept[h]).astype(BF)
            d_qk[at, pl.ds((heads + h) * deep, deep)] = dot_tn(d_scores[:, at], query_v[h]).astype(
                BF
            )

        return lambda: tiles_of(tokens, step)

    units = []
    for h in range(heads):
        units += [gates(h), by_row(h), by_column(h)]
    in_order(units, [item.step for _ in range(n - 2) for item in scatters])
    count = len(copies)
    local(d_qk, qk_o)
    local(d_value, value_o)
    local(d_gate, gate_o)
    for h in range(back):
        scatters[h].finish()

        def step(at):
            outputs[at(h * piece), :] = (
                middle_v[at(h * piece), :]
                + part[at(h * per), :].astype(F32)
                + lefts[h, n - 2, at(), :].astype(F32)
                + rights[h, n - 2, at(), :].astype(F32)
            ).astype(BF)

        blocks(piece, step)
    for item in copies[count:]:
        item.wait()
    for item in scatters:
        item.drain()


def backward_call(mid, weights, gate, norm, scale, scores, query, key, value, down, middle, col, row, n):
    tokens, width = mid.shape
    heads, _, size = value.shape
    back = CHUNKS - FRONT
    nv = heads * size
    shape = jax.ShapeDtypeStruct
    outs = (
        shape((tokens, 2 * heads * HK), BF),
        shape(value.shape, BF),
        shape(value.shape, BF),
        shape(middle.shape, BF),
    )
    ins = (gate, norm, scale, scores, query, key, value, down, middle)
    hop = (back, n - 1, middle.shape[0] // back, width)
    sems = back * 2 * (n - 1)
    wo_rows = -(-nv // LANES) * LANES
    return pl.pallas_call(
        functools.partial(backward_kernel, n),
        out_shape=outs,
        in_specs=[ANY] * 11 + [VM] * 2,
        out_specs=(ANY,) * 3 + (VM,),
        scratch_shapes=[pltpu.VMEM(mid.shape, BF), pltpu.VMEM((wo_rows, width), BF)]
        + [pltpu.VMEM(a.shape, a.dtype) for a in ins]
        + [pltpu.VMEM(o.shape, o.dtype) for o in outs[:3]]
        + [
            pltpu.VMEM(value.shape, BF),
            pltpu.VMEM((tokens, tokens), BF),
            pltpu.VMEM(hop, BF),
            pltpu.VMEM(hop, BF),
            pltpu.SemaphoreType.DMA((14,)),
            pltpu.SemaphoreType.DMA((sems,)),
            pltpu.SemaphoreType.DMA((sems,)),
        ],
        compiler_params=pltpu.CompilerParams(
            collective_id=5, has_side_effects=True, vmem_limit_bytes=VMEM_MOST
        ),
        name="backward",
    )(mid, weights, *ins, col, row)


def products_kernel(plan, arrays, *refs):
    ins, out = refs[:arrays], refs[arrays]
    held, result, copy_sem = refs[arrays + 1 : 2 * arrays + 1], refs[-2], refs[-1]
    loads = [pltpu.make_async_copy(a, b, copy_sem.at[i]) for i, (a, b) in enumerate(zip(ins, held))]
    for item in loads:
        item.start()
    waited, stores, base = set(), [], 0
    for left, head, start, size, right in plan:
        for i in (left, right):
            if i not in waited:
                loads[i].wait()
                waited.add(i)
        target = pl.ds(base, size)

        def step(j, carry):
            at = pl.ds(pl.multiple_of(j * 4 * LANES, 4 * LANES), 4 * LANES)
            source = held[left][head] if head is not None else held[left][:, pl.ds(start, size)]
            result[target, at] = dot_tn(source, held[right][:, at]).astype(BF)
            return carry

        lax.fori_loop(0, result.shape[1] // (4 * LANES), step, 0)
        store = pltpu.make_async_copy(
            result.at[target], out.at[target], copy_sem.at[arrays + len(stores)]
        )
        store.start()
        stores.append(store)
        base += size
    for item in stores:
        item.wait()


def weight_products(plan, arrays, name):
    rows = sum(p[3] for p in plan)
    width = arrays[plan[0][4]].shape[1]
    return pl.pallas_call(
        functools.partial(products_kernel, plan, len(arrays)),
        out_shape=jax.ShapeDtypeStruct((rows, width), BF),
        in_specs=[ANY] * len(arrays),
        out_specs=ANY,
        scratch_shapes=[pltpu.VMEM(a.shape, a.dtype) for a in arrays]
        + [pltpu.VMEM((rows, width), BF), pltpu.SemaphoreType.DMA((len(arrays) + len(plan),))],
        compiler_params=pltpu.CompilerParams(vmem_limit_bytes=VMEM_MOST),
        name=name,
    )(*arrays)


def pad_rows(array, count):
    return jnp.pad(array, ((0, count - array.shape[0]), (0, 0)))


def pad_columns(array, count):
    return jnp.pad(array, ((0, 0), (0, count - array.shape[1])))


def body(
    inputs,
    segments,
    first_norm_gain,
    w_query,
    w_key,
    w_value,
    w_gate,
    w_out,
    second_norm_gain,
    w_glu_gate,
    w_glu_up,
    w_down,
    cotangent,
):
    n = lax.axis_size("mp")
    place = lax.axis_index("mp")
    heads = H // n
    head_start = place * heads
    rows, width = inputs.shape
    shard = w_query.shape[0]
    piece = rows // CHUNKS
    nk, nv, nf = heads * HK, heads * HV, w_down.shape[0]
    n_one = 2 * nk + 2 * nv
    one_wide = -(-n_one // (2 * LANES)) * 2 * LANES
    v_wide, f_wide = -(-nv // LANES) * LANES, -(-nf // LANES) * LANES
    f_tiles = f_wide // LANES

    pack_one = pad_rows(
        jnp.concatenate([w_query.T, w_key.T, w_value.T, w_gate.T], axis=0), one_wide
    )
    glu_pack = jnp.stack(
        [
            pad_rows(w_glu_gate.T, f_wide).reshape(f_tiles, LANES, shard),
            pad_rows(w_glu_up.T, f_wide).reshape(f_tiles, LANES, shard),
        ],
        axis=1,
    ).reshape(2 * f_wide, shard)
    pack_two = jnp.concatenate([glu_pack, pad_rows(w_down, f_wide), pad_rows(w_out, v_wide)], axis=0)
    weight_two = lax.all_gather(pack_two, "dp", axis=1, tiled=True)
    out_weight = weight_two[3 * f_wide :]

    first_hat, first_scale = layer_norm(inputs.astype(F32), epsilon)
    rows_one, weight_one = gather_rows(
        (first_hat * first_norm_gain).astype(BF), pack_one, n, lax.axis_size("dp")
    )
    tokens = rows_one.shape[0]

    slot_shard = lax.rem(place - jnp.arange(n) + n, n)
    places = (
        slot_shard[None, :, None] * rows
        + jnp.arange(CHUNKS)[:, None, None] * piece
        + jnp.arange(piece)[None, None, :]
    ).reshape(tokens)
    seg = segments.reshape(n, CHUNKS, piece)[::-1]
    seg = lax.dynamic_slice_in_dim(jnp.concatenate([seg, seg], axis=0), n - 1 - place, n, axis=0)
    seg = seg.transpose(1, 0, 2).reshape(tokens)

    log_gamma = jnp.log1p(-jnp.exp2(-5.0 - (head_start + jnp.arange(heads)).astype(F32)))
    spot = places.astype(F32)
    powers = spot[None] * log_gamma[:, None]
    marks = jnp.stack([spot, seg.astype(F32)])
    col = jnp.concatenate([marks, jnp.exp(powers)], axis=0).T
    row = jnp.concatenate([marks, jnp.exp(-powers) * HK ** (-0.5)], axis=0)

    query, key, value, gate_pre, normalized, scale_group, scores, gated, cot_front = forward_call(
        rows_one, weight_one, cotangent, col, row, n, heads
    )
    (
        rows_two, cot_rows, mid_rows, hidden, d_glu, down, outputs_front, middle, middle_grad,
        second_gain,
    ) = middle_call(gated, weight_two, inputs, cotangent, cot_front, second_norm_gain[None], n)

    plan = [(0, None, t * f_wide, f_wide, 1) for t in range(2)] + [(2, None, 0, f_wide, 3)]
    grads_two = weight_products(plan, (d_glu, rows_two, hidden, cot_rows), "products_two")
    summed_two = lax.psum_scatter(grads_two, "dp", scatter_dimension=1, tiled=True).astype(F32)
    glu_sum = summed_two[: 2 * f_wide].reshape(f_tiles, 2, LANES, shard)

    d_qk, d_value, d_gate, outputs_back = backward_call(
        mid_rows, weight_two, gate_pre, normalized, scale_group, scores, query, key, value,
        down, middle, col, row, n,
    )
    plan = [(0, h, 0, HV, 1) for h in range(heads)] + [(2, h, 0, HV, 3) for h in range(heads)]
    plan += [(4, None, t * nk, nk, 3) for t in range(2)]
    plan += [(5, h, 0, HV, 3) for h in range(heads)]
    grads_one = weight_products(
        plan, (gated, mid_rows, d_gate, rows_one, d_qk, d_value), "products_one"
    )
    summed_one = lax.psum_scatter(grads_one, "dp", scatter_dimension=1, tiled=True).astype(F32)

    first_grad = last_call(d_qk, d_value, d_gate, weight_one, n)
    first_gain = jnp.sum(first_hat * first_grad, axis=0)
    input_gradient = middle_grad + norm_back(first_grad * first_norm_gain, first_hat, first_scale)

    gains = sum_gains(
        jnp.stack([first_gain, jnp.sum(second_gain, axis=0)]), n, lax.axis_size("dp")
    )
    at = 2 * nv
    return (
        jnp.concatenate([outputs_front, outputs_back], axis=0),
        input_gradient,
        gains[0],
        summed_one[at : at + nk].T,
        summed_one[at + nk : at + 2 * nk].T,
        summed_one[at + 2 * nk :].T,
        summed_one[nv : 2 * nv].T,
        summed_one[:nv],
        gains[1],
        glu_sum[:, 0].reshape(f_wide, shard)[:nf].T,
        glu_sum[:, 1].reshape(f_wide, shard)[:nf].T,
        summed_two[2 * f_wide : 2 * f_wide + nf],
    )


def solution(mesh):
    split = P(("dp", "mp"), None)
    wide, tall = P("dp", "mp"), P("mp", "dp")
    return jax.shard_map(
        body,
        mesh=mesh,
        in_specs=(
            split, P("dp", None), P(), wide, wide, wide, wide, tall, P(), wide, wide, tall, split,
        ),
        out_specs=(
            split, split, P(), wide, wide, wide, wide, tall, P(), wide, wide, tall,
        ),
        check_vma=False,
    )
```

```python
import functools

import jax
import jax.numpy as jnp
from jax import lax
from jax.experimental import pallas as pl
from jax.experimental.pallas import tpu as pltpu
from jax.sharding import PartitionSpec as P

H = 8
HK = 256
HV = 432
LEN = 1024
CHUNKS = 4
FRONT = CHUNKS // 2
DOWNS = CHUNKS // 4
LANES = 128
VMEM_MOST = 66_000_000

epsilon = 1e-05
group_epsilon = 1.0
BF = jnp.bfloat16
F32 = jnp.float32


def layer_norm(values_in, offset):
    centre = jnp.mean(values_in, axis=-1, keepdims=True)
    centred = values_in - centre
    variance = jnp.mean(centred * centred, axis=-1, keepdims=True)
    scaling = lax.rsqrt(variance + offset)
    return (centred * scaling, scaling)


def norm_back(grad_hat, normed_hat, scaling):
    first_mean = jnp.mean(grad_hat, axis=-1, keepdims=True)
    second_mean = jnp.mean(grad_hat * normed_hat, axis=-1, keepdims=True)
    return scaling * (grad_hat - first_mean - normed_hat * second_mean)


def glu_act(gate_pre, up_pre):
    return jax.nn.gelu(gate_pre, approximate=True) * up_pre


def dot_nt(a, b):
    return lax.dot_general(a, b, (((1,), (1,)), ((), ())), preferred_element_type=F32)


def dot_nn(a, b):
    return lax.dot_general(a, b, (((1,), (0,)), ((), ())), preferred_element_type=F32)


def dot_tn(a, b):
    return lax.dot_general(a, b, (((0,), (0,)), ((), ())), preferred_element_type=F32)


MESH = pl.DeviceIdType.MESH


class Line:
    def __init__(self, n, send_sem, recv_sem):
        self.n, self.send_sem, self.recv_sem = n, send_sem, recv_sem
        self.place = lax.axis_index("mp")
        self.used = 0
        self.sent = []

    def enter(self, others=None):
        barrier = pltpu.get_barrier_semaphore()
        n, place = self.n, self.place

        @pl.when(place >= 1)
        def _():
            pl.semaphore_signal(barrier, inc=1, device_id={"mp": place - 1}, device_id_type=MESH)

        @pl.when(place <= n - 2)
        def _():
            pl.semaphore_signal(barrier, inc=1, device_id={"mp": place + 1}, device_id_type=MESH)

        peers = jnp.minimum(place, 1) + jnp.minimum(n - 1 - place, 1)
        if others is not None:
            axis, indices = others
            for index in indices:
                pl.semaphore_signal(barrier, inc=1, device_id={axis: index}, device_id_type=MESH)
            peers = peers + len(indices)
        pl.semaphore_wait(barrier, peers)

    def copy(self, src, dst, index, toward):
        return pltpu.make_async_remote_copy(
            src_ref=src,
            dst_ref=dst,
            send_sem=self.send_sem.at[index],
            recv_sem=self.recv_sem.at[index],
            device_id={"mp": self.place + toward},
            device_id_type=MESH,
        )

    def leave(self):
        for condition, copy in self.sent:
            pl.when(condition)(copy.wait_send)


class Gather:
    def __init__(self, line, slot):
        self.line, self.slot, self.step_no = line, slot, 0
        self.base = line.used
        line.used += 2 * (line.n - 1)
        n = line.n
        self.right = [
            line.copy(slot(s - 1), slot(s), self.base + s - 1, 1) for s in range(1, n)
        ]
        self.left = [
            line.copy(slot((n - s + 1) % n), slot(n - s), self.base + n - 2 + s, -1)
            for s in range(1, n)
        ]

    def arrive(self, s):
        n, place = self.line.n, self.line.place
        pl.when(place >= s)(self.right[s - 1].wait_recv)
        pl.when(place <= n - 1 - s)(self.left[s - 1].wait_recv)

    def step(self):
        self.step_no += 1
        s, n, place = self.step_no, self.line.n, self.line.place
        if s > 1:
            self.arrive(s - 1)
        if s < n:
            to_right = (place >= s - 1) & (place <= n - 2)
            to_left = (place <= n - s) & (place >= 1)
            pl.when(to_right)(self.right[s - 1].start)
            pl.when(to_left)(self.left[s - 1].start)
            self.line.sent += [(to_right, self.right[s - 1]), (to_left, self.left[s - 1])]


class Scatter:
    def __init__(self, line, slot, from_left, from_right, add):
        self.line, self.slot, self.add, self.step_no = line, slot, add, 0
        self.from_left, self.from_right = from_left, from_right
        self.base = line.used
        line.used += 2 * (line.n - 1)
        n = line.n
        self.right = [
            line.copy(slot(s), from_left(s), self.base + s - 1, 1) for s in range(1, n)
        ]
        self.left = [
            line.copy(slot(n - s), from_right(s), self.base + n - 2 + s, -1) for s in range(1, n)
        ]
        self.mine = []

    def step(self):
        self.step_no += 1
        s, n, place = self.step_no, self.line.n, self.line.place
        to_right, to_left = place <= s - 1, place >= n - s
        if s > 1:

            @pl.when(to_right & (place >= 1))
            def _():
                self.right[s - 2].wait_recv()
                self.add(self.slot(s), self.from_left(s - 1))

            @pl.when(to_left & (place <= n - 2))
            def _():
                self.left[s - 2].wait_recv()
                self.add(self.slot(n - s), self.from_right(s - 1))

        pl.when(to_right)(self.right[s - 1].start)
        pl.when(to_left)(self.left[s - 1].start)
        self.mine += [(to_right, self.right[s - 1]), (to_left, self.left[s - 1])]

    def finish(self):
        n, place = self.line.n, self.line.place

        @pl.when(place >= 1)
        def _():
            self.right[n - 2].wait_recv()

        @pl.when(place <= n - 2)
        def _():
            self.left[n - 2].wait_recv()

    def drain(self):
        for condition, copy in self.mine:
            pl.when(condition)(copy.wait_send)


ANY = pl.BlockSpec(memory_space=pl.ANY)
VM = pl.BlockSpec(memory_space=pltpu.VMEM)
BLOCK = 16


def blocks(count, step):
    def run(i, carry):
        step(lambda base=0: pl.ds(pl.multiple_of(base + i * BLOCK, BLOCK), BLOCK))
        return carry

    lax.fori_loop(0, count // BLOCK, run, 0)


def add_into(target, extra):
    def step(at):
        target[at(), :] = (target[at(), :].astype(F32) + extra[at(), :].astype(F32)).astype(BF)

    blocks(target.shape[0], step)


def product_tiles(target, left, right, tile):
    def step(j, carry):
        at = pl.ds(pl.multiple_of(j * tile, tile), tile)
        target[:, at] = dot_nn(left[...], right[:, at]).astype(BF)
        return carry

    lax.fori_loop(0, right.shape[1] // tile, step, 0)


class Doubling:
    def __init__(self, m, own, out, rows, bits, base, send_sem, recv_sem):
        self.d = lax.axis_index("dp")
        self.own, self.out, self.rows, self.bits, self.base = own, out, rows, bits, base
        self.send_sem, self.recv_sem = send_sem, recv_sem
        self.shard = own.shape[1]
        self.done = 0
        self.sent = []

    def flip(self, d, bit):
        return d + bit * (1 - 2 * (lax.div(d, bit) % 2))

    def block(self, d):
        return self.out.at[self.rows, pl.ds(pl.multiple_of(d * self.shard, self.shard), self.shard)]

    def copies(self, level, landing):
        owners = [self.d]
        for bit in self.bits[:level]:
            owners += [self.flip(d, bit) for d in owners]
        bit = self.bits[level]
        partner = self.flip(self.d, bit)
        out = []
        for i, d in enumerate(owners):
            d = self.flip(d, bit) if landing else d
            src = self.own.at[self.rows] if i == 0 and not landing else self.block(d)
            index = self.base + (1 << level) - 1 + i
            out.append(
                pltpu.make_async_remote_copy(
                    src_ref=src,
                    dst_ref=self.block(d),
                    send_sem=self.send_sem.at[index],
                    recv_sem=self.recv_sem.at[index],
                    device_id={"dp": partner},
                    device_id_type=MESH,
                )
            )
        return out

    def step(self):
        level = self.done
        if level > 0:
            for c in self.copies(level - 1, True):
                c.wait_recv()
        if level < len(self.bits):
            out = self.copies(level, False)
            for c in out:
                c.start()
            self.sent += out
        self.done += 1

    def leave(self):
        for c in self.sent:
            c.wait_send()


def bits_of(m):
    bits = [1 << b for b in range(m.bit_length() - 1)]
    assert 1 << len(bits) == m
    return bits


PARTS = 2


def weight_gather(m, pack, weight, send_sem, recv_sem):
    bits = bits_of(m)
    outer = bits[1:]
    height = pack.shape[0] // (2 * PARTS)
    doubling = []
    for i in range(2 * PARTS):
        order = (outer if i % 2 == 0 else outer[::-1]) + bits[:1]
        rows = pl.ds(i * height, height)
        doubling.append(Doubling(m, pack, weight, rows, order, i * (m - 1), send_sem, recv_sem))
    first = doubling[0]
    return doubling, [first.flip(first.d, bit) for bit in bits]


def own_columns(pack, weight):
    shard = pack.shape[1]
    at = pl.multiple_of(lax.axis_index("dp") * shard, shard)
    return weight.at[:, pl.ds(at, shard)]


def gather_kernel(n, m, own, pack, out, weight, send_sem, recv_sem, copy_sem, wide_send, wide_recv):
    line = Line(n, send_sem, recv_sem)
    piece = own.shape[0] // CHUNKS
    per = n * piece
    bits = bits_of(m)
    doubling, peers = weight_gather(m, pack, weight, wide_send, wide_recv)
    line.enter(["dp", peers])
    local, gathers = [], []
    keep = pltpu.make_async_copy(pack, own_columns(pack, weight), copy_sem.at[CHUNKS])
    for h in range(CHUNKS):
        mine = own.at[pl.ds(h * piece, piece)]
        local.append(
            pltpu.make_async_copy(mine, out.at[pl.ds(h * per, piece)], copy_sem.at[h])
        )

        def slot(k, h=h, mine=mine):
            return mine if k == 0 else out.at[pl.ds(h * per + k * piece, piece)]

        gathers.append(Gather(line, slot))
    local.append(keep)

    def line_step(items):
        for item in items:
            item.step()

    half = CHUNKS // 2
    line_step(gathers)
    line_step(doubling)
    for item in local:
        item.start()
    for level in range(1, max(n, len(bits) + 1)):
        for side in range(2):
            if level <= len(bits):
                line_step(doubling[side * PARTS : (side + 1) * PARTS])
            if level < n:
                line_step(gathers[side * half : (side + 1) * half])
    for item in local:
        item.wait()
    for item in gathers:
        assert item.step_no == n
    for item in doubling:
        assert item.done == len(bits) + 1
        item.leave()
    line.leave()


def gather_rows(own, pack, n, m):
    rows, width = own.shape
    count = CHUNKS * 2 * (n - 1)
    wide = 2 * PARTS * (m - 1)
    return pl.pallas_call(
        functools.partial(gather_kernel, n, m),
        out_shape=(
            jax.ShapeDtypeStruct((n * rows, width), own.dtype),
            jax.ShapeDtypeStruct((pack.shape[0], m * pack.shape[1]), pack.dtype),
        ),
        in_specs=[VM, VM],
        out_specs=(ANY, ANY),
        scratch_shapes=[
            pltpu.SemaphoreType.DMA((count,)),
            pltpu.SemaphoreType.DMA((count,)),
            pltpu.SemaphoreType.DMA((CHUNKS + 1,)),
            pltpu.SemaphoreType.DMA((wide,)),
            pltpu.SemaphoreType.DMA((wide,)),
        ],
        compiler_params=pltpu.CompilerParams(collective_id=0, has_side_effects=True),
        name="gather_rows",
    )(own, pack)


def no_neighbour_zero(n, place, from_left, from_right):
    @pl.when(place == 0)
    def _():
        from_left[...] = jnp.zeros_like(from_left)

    @pl.when(place == n - 1)
    def _():
        from_right[...] = jnp.zeros_like(from_right)


(COT, OUT, ONE, END_ONE, TWO, GLU, GRAD, GRAD_SUM, END_GRAD, MID, DOWN, DOWN_SUM, END_DOWN) = range(13)

DUE = {
    OUT: (-2.23, 1.66, 0), ONE: (-1.99, 1.12, 1.03), END_ONE: (1.46, 1.37, 0), TWO: (0.73, 1.15, 0.94),
    COT: (0.35, 1.39, 1.02), GLU: (1.14, -1.37, 1.55), GRAD: (3.09, 2.02, 0),
    GRAD_SUM: (3.48, 1.71, 0.74), END_GRAD: (7.02, -2.12, 0), MID: (5.68, 0.86, 1.11),
    DOWN: (1.3, 0.36, 0), DOWN_SUM: (1.87, 1.35, 0.95), END_DOWN: (7.9, 2.17, 0),
}
TUNED = {
    (4, 4): [
        3, 5, 4, 8, 8, 2, 8, 2, 7, 9, 12, 16, 9, 6, 16, 9, 10, 16, 3, 13,
        11, 17, 16, 20, 10, 11, 2, 17, 20, 10, 17, 40, 11, 24, 14, 18, 2, 28, 17, 3,
        21, 18, 28, 15, 19, 21, 25, 29, 44, 18, 18, 28, 19, 22, 29, 44, 22, 19, 32, 3,
        36, 26, 30, 19, 29, 23, 36, 23, 36, 30, 33, 37, 30, 27, 31, 44, 34, 37, 38, 43,
        37, 31, 41, 38, 48, 36, 42, 31, 37, 38, 35, 39, 38, 39, 39, 39,
    ],
}


def middle_order(n):
    if (n, CHUNKS) in TUNED:
        return [divmod(code, CHUNKS) for code in TUNED[n, CHUNKS]]
    count = {k: 1 for k in DUE}
    count.update({COT: n, TWO: n, MID: n, ONE: n - 1, GRAD_SUM: n - 1, DOWN_SUM: n - 1, GLU: 2})
    needs = {
        ONE: [OUT], END_ONE: [ONE], TWO: [END_ONE], GLU: [TWO, COT], GRAD: [GLU], GRAD_SUM: [GRAD],
        END_GRAD: [GRAD_SUM], MID: [END_GRAD], DOWN: [GLU], DOWN_SUM: [DOWN], END_DOWN: [DOWN_SUM],
    }
    todo = sorted(
        (first + h * later + s * 3 / (n - 1) * each, k, h, s)
        for k, (first, later, each) in DUE.items()
        for h in range(CHUNKS)
        for s in range(count[k])
        if not (k == COT and h < FRONT or k in (DOWN_SUM, END_DOWN) and h >= DOWNS)
    )
    taken, order = {}, []
    while todo:
        for item in todo:
            _, k, h, s = item
            ready = taken.get((k, h), 0) == s and all(
                taken.get((need, h), 0) == count[need] or (need == COT and h < FRONT)
                for need in needs.get(k, [])
            )
            if ready:
                break
        todo.remove(item)
        taken[k, h] = s + 1
        order.append((k, h))
    return order


def middle_kernel(
    n, gated, weights, out_weight, own, cot, cot_front, gain,
    rows_out, cot_out, mid_out, hidden_out, glu_out, down_out, outputs, middle_out, d_middle,
    gain_out,
    gated_v, wo_v, wg_v, wd_v, own_v, cot_v, rows_v, hidden_v, glu_v, part, part_two,
    left_a, right_a, left_b, right_b, middle, stage, copy_sem, send_sem, recv_sem,
):
    line = Line(n, send_sem, recv_sem)
    place = line.place
    count, width = own.shape
    piece = count // CHUNKS
    per = n * piece
    wide = hidden_v.shape[1]
    copies = []

    def local(src, dst):
        c = pltpu.make_async_copy(src, dst, copy_sem.at[len(copies)])
        copies.append(c)
        c.start()
        return c

    def rows_at(ref, h, k=0, size=piece):
        return ref.at[pl.ds(h * per + k * piece, size)]

    load_cot = [
        local(cot.at[pl.ds(h * piece, piece)], rows_at(cot_v, h)) for h in range(FRONT, CHUNKS)
    ]
    front = pl.ds(0, FRONT * per)
    load_cot.append(local(cot_front, cot_v.at[front]))
    load_gated = local(gated, gated_v)
    load_wo = local(
        out_weight.at[pl.ds(out_weight.shape[0] - wo_v.shape[0], wo_v.shape[0])], wo_v
    )
    load_own = local(own, own_v)
    load_wg = local(weights.at[pl.ds(0, 2 * wide)], wg_v)
    load_wd = local(weights.at[pl.ds(2 * wide, wide)], wd_v)
    line.enter()
    for h in range(CHUNKS):
        no_neighbour_zero(n, place, left_a.at[h, n - 2], right_a.at[h, n - 2])
    for h in range(DOWNS):
        no_neighbour_zero(n, place, left_b.at[h, n - 2], right_b.at[h, n - 2])
    gain_out[...] = jnp.zeros_like(gain_out)

    def scatter(buf, lefts, rights, h):
        return Scatter(
            line,
            lambda k: rows_at(buf, h, k),
            lambda s: lefts.at[h, s - 1],
            lambda s: rights.at[h, s - 1],
            add_into,
        )

    gather_cot = {
        h: Gather(line, functools.partial(rows_at, cot_v, h)) for h in range(FRONT, CHUNKS)
    }
    gather_two = [Gather(line, functools.partial(rows_at, rows_v, h)) for h in range(CHUNKS)]

    def mid_slot(h, k):
        return stage.at[h] if k == 0 else rows_at(mid_out, h, k)

    gather_mid = [Gather(line, functools.partial(mid_slot, h)) for h in range(CHUNKS)]
    scatter_one = [scatter(part, left_a, right_a, h) for h in range(CHUNKS)]
    scatter_two = [scatter(part_two, left_b, right_b, h) for h in range(DOWNS)]
    scatter_grad = [scatter(part, left_a, right_a, h) for h in range(CHUNKS)]

    def chunk(ref, h):
        return ref.at[pl.ds(h * per, per)]

    def out_product(h):
        heads, _, size = gated_v.shape
        target, whole = chunk(part, h), pl.ds(h * per, per)

        def step(j, carry):
            at = pl.ds(pl.multiple_of(j * 2 * LANES, 2 * LANES), 2 * LANES)
            target[:, at] = sum(
                dot_nn(gated_v[i, whole, :], wo_v[pl.ds(i * size, size), at]) for i in range(heads)
            ).astype(BF)
            return carry

        lax.fori_loop(0, width // (2 * LANES), step, 0)

    def finish_one(h):
        scatter_one[h].finish()

        def step(at):
            src = at(h * per)
            mine = at(h * piece)
            total = (
                own_v[mine, :].astype(F32)
                + part[src, :].astype(F32)
                + left_a[h, n - 2, at(), :].astype(F32)
                + right_a[h, n - 2, at(), :].astype(F32)
            )
            middle[mine, :] = total
            hat, _ = layer_norm(total, epsilon)
            rows_v[src, :] = (hat * gain[...]).astype(BF)

        blocks(piece, step)

    def glu_tiles(h, first, last):
        def step(j, carry):
            pair = pl.ds(pl.multiple_of(j * 2 * LANES, 2 * LANES), 2 * LANES)
            at = pl.ds(pl.multiple_of(j * LANES, LANES), LANES)
            whole = pl.ds(h * per, per)
            both = dot_nt(rows_v[whole, :], wg_v[pair, :])
            d_hidden = dot_nt(cot_v[whole, :], wd_v[at, :])
            u, up = both[:, :LANES], both[:, LANES:]
            c = 0.7978845608028654
            t = jnp.tanh(c * (u + 0.044715 * (u * u * u)))
            half = 0.5 * (1.0 + t)
            act = u * half
            slope = half + 0.5 * u * (1.0 - t * t) * (c * (1.0 + 3 * 0.044715 * (u * u)))
            hidden_v[whole, at] = (act * up).astype(BF)
            glu_v[whole, pair] = jnp.concatenate(
                [(d_hidden * up * slope).astype(BF), (d_hidden * act).astype(BF)], axis=1
            )
            return carry

        lax.fori_loop(first, last, step, 0)

    def grad_product(h):
        product_tiles(chunk(part, h), chunk(glu_v, h), wg_v, 2 * LANES)

    def down_product(h):
        product_tiles(chunk(part_two, h), chunk(hidden_v, h), wd_v, 2 * LANES)

    def finish_grad(h):
        scatter_grad[h].finish()

        def step(at):
            src = at(h * per)
            mine = at(h * piece)
            grad = (
                part[src, :].astype(F32)
                + left_a[h, n - 2, at(), :].astype(F32)
                + right_a[h, n - 2, at(), :].astype(F32)
            )
            hat, scale = layer_norm(middle[mine, :], epsilon)
            gain_out[...] += jnp.sum((hat * grad).reshape(BLOCK // 8, 8, width), axis=0)
            d_mid = cot_v[src, :].astype(F32) + norm_back(grad * gain[...], hat, scale)
            d_middle[mine, :] = d_mid
            stage[h, at(), :] = d_mid.astype(BF)

        blocks(piece, step)
        local(stage.at[h], rows_at(mid_out, h))

    def finish_two(h):
        scatter_two[h].finish()

        def step(at):
            src = at(h * per)
            mine = at(h * piece)
            outputs[mine, :] = (
                middle[mine, :]
                + part_two[src, :].astype(F32)
                + left_b[h, n - 2, at(), :].astype(F32)
                + right_b[h, n - 2, at(), :].astype(F32)
            ).astype(BF)

        blocks(piece, step)

    tiles = wide // LANES
    cut = tiles // 2

    def wait_for(items):
        for item in items:
            item.wait()
        items.clear()

    first_loads, own_load = [load_gated, load_wo], [load_own]
    later_loads = [load_wg, load_wd]

    def out_action(h):
        wait_for(first_loads)
        out_product(h)

    def finish_one_action(h):
        wait_for(own_load)
        finish_one(h)

    def glu_action(h):
        wait_for(later_loads)
        if h in begun:
            glu_tiles(h, cut, tiles)
        else:
            begun.add(h)
            glu_tiles(h, 0, cut)

    def grad_action(h):
        scatter_one[h].drain()
        grad_product(h)

    begun = set()
    actions = {
        COT: lambda h: gather_cot[h].step(),
        OUT: out_action,
        ONE: lambda h: scatter_one[h].step(),
        END_ONE: finish_one_action,
        TWO: lambda h: gather_two[h].step(),
        GLU: glu_action,
        GRAD: grad_action,
        GRAD_SUM: lambda h: scatter_grad[h].step(),
        END_GRAD: finish_grad,
        MID: lambda h: gather_mid[h].step(),
        DOWN: down_product,
        DOWN_SUM: lambda h: scatter_two[h].step(),
        END_DOWN: finish_two,
    }
    for item in load_cot:
        item.wait()
    for kind, h in middle_order(n):
        actions[kind](h)
    for c in range(CHUNKS):
        local(chunk(rows_v, c), chunk(rows_out, c))
        local(chunk(cot_v, c), chunk(cot_out, c))
        local(chunk(hidden_v, c), chunk(hidden_out, c))
        local(chunk(glu_v, c), chunk(glu_out, c))
    local(part_two.at[pl.ds(DOWNS * per, down_out.shape[0])], down_out)
    local(middle.at[pl.ds(DOWNS * piece, middle_out.shape[0])], middle_out)
    for item in list(gather_cot.values()) + gather_two + gather_mid:
        assert item.step_no == n
    for item in scatter_one + scatter_two + scatter_grad:
        assert item.step_no == n - 1
    for group in (scatter_grad, scatter_two):
        for item in group:
            item.drain()
    for item in copies[CHUNKS - FRONT + 6 :]:
        item.wait()
    line.leave()


def middle_call(gated, weights, out_weight, own, cot, cot_front, gain, n):
    rows, width = own.shape
    heads, tokens, size = gated.shape
    nv = heads * size
    wide = weights.shape[0] // 3
    piece = rows // CHUNKS
    back = CHUNKS - DOWNS
    sems = CHUNKS * 5 * 2 * (n - 1)
    hop = (CHUNKS, n - 1, piece, width)
    shape = jax.ShapeDtypeStruct
    return pl.pallas_call(
        functools.partial(middle_kernel, n),
        out_shape=(
            shape((tokens, width), BF),
            shape((tokens, width), BF),
            shape((tokens, width), BF),
            shape((tokens, wide), BF),
            shape((tokens, 2 * wide), BF),
            shape((back * n * piece, width), BF),
            shape((DOWNS * piece, width), BF),
            shape((back * piece, width), F32),
            shape((rows, width), F32),
            shape((8, width), F32),
        ),
        in_specs=[ANY] * 6 + [VM],
        out_specs=(ANY,) * 6 + (VM, ANY, VM, VM),
        scratch_shapes=[
            pltpu.VMEM((heads, tokens, size), BF),
            pltpu.VMEM((nv, width), BF),
            pltpu.VMEM((2 * wide, width), BF),
            pltpu.VMEM((wide, width), BF),
            pltpu.VMEM((rows, width), BF),
            pltpu.VMEM((tokens, width), BF),
            pltpu.VMEM((tokens, width), BF),
            pltpu.VMEM((tokens, wide), BF),
            pltpu.VMEM((tokens, 2 * wide), BF),
            pltpu.VMEM((tokens, width), BF),
            pltpu.VMEM((tokens, width), BF),
            pltpu.VMEM(hop, BF),
            pltpu.VMEM(hop, BF),
            pltpu.VMEM((DOWNS,) + hop[1:], BF),
            pltpu.VMEM((DOWNS,) + hop[1:], BF),
            pltpu.VMEM((rows, width), F32),
            pltpu.VMEM((CHUNKS, piece, width), BF),
            pltpu.SemaphoreType.DMA((8 + 6 * CHUNKS - FRONT,)),
            pltpu.SemaphoreType.DMA((sems,)),
            pltpu.SemaphoreType.DMA((sems,)),
        ],
        compiler_params=pltpu.CompilerParams(
            collective_id=1, has_side_effects=True, vmem_limit_bytes=VMEM_MOST
        ),
        name="middle",
    )(gated, weights, out_weight, own, cot, cot_front, gain)


class Halving:
    def __init__(self, grads, rows, bits, base, kept, held, out, send_sem, recv_sem, load_sem):
        self.d = lax.axis_index("dp")
        self.grads, self.rows, self.bits, self.base = grads, rows, bits, base
        self.kept, self.held, self.out = kept, held, out
        self.send_sem, self.recv_sem, self.load_sem = send_sem, recv_sem, load_sem
        self.shard = out.shape[1]
        self.masks = [0]
        for bit in bits[:0:-1]:
            self.masks += [k + bit for k in self.masks]
        self.done, self.sent, self.loads = 0, [], []

    def flip(self, d, mask):
        for bit in self.bits:
            if mask & bit:
                d = d + bit * (1 - 2 * (lax.div(d, bit) % 2))
        return d

    def block(self, d):
        return self.grads.at[self.rows, pl.ds(pl.multiple_of(d * self.shard, self.shard), self.shard)]

    def count(self, level):
        return 1 << (len(self.bits) - 1 - level)

    def copies(self, level):
        bit = self.bits[level]
        partner = self.flip(self.d, bit)
        out = []
        for i in range(self.count(level)):
            if level == 0:
                src = self.block(self.flip(partner, self.masks[i]))
            else:
                src = self.kept.at[self.count(level) + i, self.rows]
            index = self.base + len(out) + sum(self.count(k) for k in range(level))
            out.append(
                pltpu.make_async_remote_copy(
                    src_ref=src,
                    dst_ref=self.held[level].at[i, self.rows],
                    send_sem=self.send_sem.at[index],
                    recv_sem=self.recv_sem.at[index],
                    device_id={"dp": partner},
                    device_id_type=MESH,
                )
            )
        return out

    def load(self):
        for i, mask in enumerate(self.masks):
            c = pltpu.make_async_copy(
                self.block(self.flip(self.d, mask)), self.kept.at[i, self.rows], self.load_sem.at[i]
            )
            c.start()
            self.loads.append(c)

    def add(self, level):
        last = level == len(self.bits) - 1
        start, size = self.rows.start, self.rows.size
        for i in range(self.count(level)):

            def step(at):
                total = self.kept[i, at(start), :].astype(F32) + self.held[level][
                    i, at(start), :
                ].astype(F32)
                if last:
                    self.out[at(start), :] = total
                else:
                    self.kept[i, at(start), :] = total.astype(BF)

            blocks(size, step)

    def step(self):
        level = self.done
        if level > 0:
            for c in self.loads:
                c.wait()
            self.loads = []
            for c in self.sent[-1]:
                c.wait_recv()
            self.add(level - 1)
        if level < len(self.bits):
            out = self.copies(level)
            for c in out:
                c.start()
            self.sent.append(out)
        self.done += 1

    def leave(self):
        for group in self.sent:
            for c in group:
                c.wait_send()


def exchange(groups, mine, total, send_sem, recv_sem):
    source, base = mine, 0
    for axis, size, held in groups:
        me = lax.axis_index(axis)
        held[me] = source[...]

        def copy(k, slot):
            return pltpu.make_async_remote_copy(
                src_ref=source,
                dst_ref=held.at[slot],
                send_sem=send_sem.at[base + k],
                recv_sem=recv_sem.at[base + k],
                device_id={axis: lax.rem(me + k, size)},
                device_id_type=MESH,
            )

        sent = [copy(k, me) for k in range(1, size)]
        for c in sent:
            c.start()
        for k in range(1, size):
            copy(k, lax.rem(me - k + size, size)).wait_recv()
        value = held[0]
        for k in range(1, size):
            value = value + held[k]
        for c in sent:
            c.wait_send()
        total[...] = value
        source, base = total, base + size


def last_kernel(
    n, m, d_qk, d_value, d_gate, weight, grads, inputs, gain, d_middle, second_gain,
    out, gains, summed,
    qk_v, value_v, gate_v, weight_v, inputs_v, middle_v, part, lefts, rights, kept, *rest
):
    bits = bits_of(m)
    held, (gain_sum, mine, first, second) = rest[: len(bits)], rest[len(bits) : len(bits) + 4]
    copy_sem, send_sem, recv_sem, wide_send, wide_recv, load_sem, gain_send, gain_recv = rest[
        len(bits) + 4 :
    ]
    line = Line(n, send_sem, recv_sem)
    count, width = out.shape
    piece = count // CHUNKS
    per = n * piece
    heads, _, size = value_v.shape
    wide = qk_v.shape[1]
    load = [
        pltpu.make_async_copy(src, dst, copy_sem.at[i])
        for i, (src, dst) in enumerate(
            [
                (weight.at[pl.ds(0, weight_v.shape[0])], weight_v), (d_qk, qk_v),
                (d_value, value_v), (d_gate, gate_v), (inputs, inputs_v), (d_middle, middle_v),
            ]
        )
    ]
    for item in load:
        item.start()
    barrier = pltpu.get_barrier_semaphore()
    for axis, extent in (("dp", m), ("mp", n)):
        me = lax.axis_index(axis)
        for k in range(1, extent):
            peer = lax.rem(me + k, extent)
            pl.semaphore_signal(barrier, inc=1, device_id={axis: peer}, device_id_type=MESH)
    pl.semaphore_wait(barrier, n + m - 2)

    height = grads.shape[0] // (2 * PARTS)
    halving = []
    for i in range(2 * PARTS):
        order = bits[:1] + (bits[1:] if i % 2 == 0 else bits[:0:-1])
        halving.append(
            Halving(
                grads, pl.ds(i * height, height), order, i * (m - 1), kept, held, summed,
                wide_send, wide_recv, load_sem.at[i],
            )
        )
    for item in halving:
        item.step()
    for item in halving:
        item.load()
    for h in range(CHUNKS):
        no_neighbour_zero(n, line.place, lefts.at[h, n - 2], rights.at[h, n - 2])
    gain_sum[...] = jnp.zeros_like(gain_sum)
    scatters = [
        Scatter(
            line,
            lambda k, h=h: part.at[pl.ds(h * per + k * piece, piece)],
            lambda s, h=h: lefts.at[h, s - 1],
            lambda s, h=h: rights.at[h, s - 1],
            add_into,
        )
        for h in range(CHUNKS)
    ]

    def product(h):
        rows = pl.ds(h * per, per)

        def step(j, carry):
            at = pl.ds(pl.multiple_of(j * 2 * LANES, 2 * LANES), 2 * LANES)
            total = dot_nn(qk_v[rows, :], weight_v[pl.ds(0, wide), at])
            for i in range(heads):
                base = wide + i * size
                total += dot_nn(value_v[i, rows, :], weight_v[pl.ds(base, size), at])
                base += heads * size
                total += dot_nn(gate_v[i, rows, :], weight_v[pl.ds(base, size), at])
            part[rows, at] = total.astype(BF)
            return carry

        lax.fori_loop(0, width // (2 * LANES), step, 0)

    def finish(h):
        scatters[h].finish()

        def step(at):
            own = at(h * piece)
            grad = (
                part[at(h * per), :].astype(F32)
                + lefts[h, n - 2, at(), :].astype(F32)
                + rights[h, n - 2, at(), :].astype(F32)
            )
            hat, scale = layer_norm(inputs_v[own, :].astype(F32), epsilon)
            gain_sum[...] += jnp.sum((hat * grad).reshape(BLOCK // 8, 8, width), axis=0)
            out[own, :] = middle_v[own, :] + norm_back(grad * gain[...], hat, scale)

        blocks(piece, step)

    for item in load:
        item.wait()
    for h in range(CHUNKS):
        product(h)
        scatters[h].step()
    for s in range(n - 2):
        for h in range(CHUNKS):
            if s < len(bits) and h < len(halving):
                halving[h].step()
            scatters[h].step()
    while halving[0].done < len(bits):
        for item in halving:
            item.step()
    for h in range(CHUNKS):
        finish(h)
    groups = [("dp", m, first), ("mp", n, second)]
    for i, source in enumerate((gain_sum, second_gain)):
        flat = jnp.sum(source[...], axis=0, keepdims=True)
        for j in range(width // LANES):
            mine[pl.ds(i * (width // LANES) + j, 1), :] = flat[:, j * LANES : (j + 1) * LANES]
    exchange(groups, mine, gains, gain_send, gain_recv)
    for item in halving:
        while item.done <= len(bits):
            item.step()
        item.leave()
    for h in range(CHUNKS):
        scatters[h].drain()


def last_call(d_qk, d_value, d_gate, weight, grads, inputs, gain, d_middle, second_gain, n, m):
    tokens = d_qk.shape[0]
    rows, width = inputs.shape
    heads = d_value.shape[0]
    shard = width // m
    sems = CHUNKS * 2 * (n - 1)
    wide = 2 * PARTS * (m - 1)
    hop = (CHUNKS, n - 1, rows // CHUNKS, width)
    flat = (2 * width // LANES, LANES)
    levels = [m >> (1 + k) for k in range(len(bits_of(m)))]
    shape = jax.ShapeDtypeStruct
    return pl.pallas_call(
        functools.partial(last_kernel, n, m),
        out_shape=(
            shape((rows, width), F32), shape(flat, F32), shape((grads.shape[0], shard), F32),
        ),
        in_specs=[ANY] * 6 + [VM, ANY, VM],
        out_specs=(VM,) * 3,
        scratch_shapes=[
            pltpu.VMEM(d_qk.shape, BF),
            pltpu.VMEM(d_value.shape, BF),
            pltpu.VMEM(d_gate.shape, BF),
            pltpu.VMEM((2 * heads * (HK + HV), width), BF),
            pltpu.VMEM((rows, width), BF),
            pltpu.VMEM((rows, width), F32),
            pltpu.VMEM((tokens, width), BF),
            pltpu.VMEM(hop, BF),
            pltpu.VMEM(hop, BF),
            pltpu.VMEM((m // 2, grads.shape[0], shard), BF),
        ]
        + [pltpu.VMEM((count, grads.shape[0], shard), BF) for count in levels]
        + [
            pltpu.VMEM((8, width), F32),
            pltpu.VMEM(flat, F32),
            pltpu.VMEM((m,) + flat, F32),
            pltpu.VMEM((n,) + flat, F32),
            pltpu.SemaphoreType.DMA((6,)),
            pltpu.SemaphoreType.DMA((sems,)),
            pltpu.SemaphoreType.DMA((sems,)),
            pltpu.SemaphoreType.DMA((wide,)),
            pltpu.SemaphoreType.DMA((wide,)),
            pltpu.SemaphoreType.DMA((2 * PARTS, m // 2)),
            pltpu.SemaphoreType.DMA((n + m,)),
            pltpu.SemaphoreType.DMA((n + m,)),
        ],
        compiler_params=pltpu.CompilerParams(
            collective_id=2, has_side_effects=True, vmem_limit_bytes=VMEM_MOST
        ),
        name="last",
    )(d_qk, d_value, d_gate, weight, grads, inputs, gain, d_middle, second_gain)


TILE = 256


def tiles_of(count, step):
    def run(i, carry):
        step(pl.ds(pl.multiple_of(i * TILE, TILE), TILE))
        return carry

    lax.fori_loop(0, count // TILE, run, 0)


def in_order(units, steps):
    taken = 0
    for i, unit in enumerate(units):
        unit()
        upto = (i + 1) * len(steps) // len(units)
        for step in steps[taken:upto]:
            step()
        taken = upto


def forward_kernel(
    n, m, rows, weight, cot, col, row, pack,
    query_o, key_o, value_o, gate_o, norm_o, scale_o, scores_o, gated_o, cot_o, second_o,
    rows_v, weight_v, query_v, key_v, value_v, gate_v, norm_v, scale_v, scores_v, gated_v, cot_v,
    copy_sem, send_sem, recv_sem, wide_send, wide_recv,
):
    line = Line(n, send_sem, recv_sem)
    heads, tokens, deep = query_v.shape
    size = value_v.shape[2]
    per = cot_v.shape[0] // FRONT
    piece = per // n
    copies = []

    def local(src, dst):
        c = pltpu.make_async_copy(src, dst, copy_sem.at[len(copies)])
        copies.append(c)
        c.start()
        return c

    load_cot = [
        local(cot.at[pl.ds(h * piece, piece)], cot_v.at[pl.ds(h * per, piece)])
        for h in range(FRONT)
    ]
    load_rows = local(rows, rows_v)
    load_weight = local(weight.at[pl.ds(0, weight_v.shape[0])], weight_v)
    doubling, peers = weight_gather(m, pack, second_o, wide_send, wide_recv)
    line.enter(["dp", peers])
    gathers = [
        Gather(line, lambda k, h=h: cot_v.at[pl.ds(h * per + k * piece, piece)])
        for h in range(FRONT)
    ]
    for item in load_cot:
        item.wait()
    for g in gathers + doubling:
        g.step()
    local(pack, own_columns(pack, second_o))
    load_rows.wait()
    load_weight.wait()

    def project(target, h, base, width):
        def step(at):
            target[h, at, :] = dot_nt(rows_v[at, :], weight_v[pl.ds(base, width), :]).astype(
                target.dtype
            )

        return lambda: tiles_of(tokens, step)

    def attend(h):
        def step(at):
            allowed = (col[at, 0:1] >= row[0:1, :]) & (col[at, 1:2] == row[1:2, :])
            scores = dot_nt(query_v[h, at, :], key_v[h]) * col[at, 2 + h : 3 + h]
            scores = jnp.where(allowed, scores * row[2 + h : 3 + h, :], 0.0).astype(BF)
            scores_v[h, at, :] = scores
            hat, scale = layer_norm(dot_nn(scores, value_v[h]), group_epsilon)
            norm_v[h, at, :] = hat
            scale_v[h, at, :] = scale
            gate = gate_v[h, at, :]
            gated_v[h, at, :] = (gate * jax.nn.sigmoid(gate) * hat).astype(BF)

        return lambda: tiles_of(tokens, step)

    values, gates = 2 * heads * deep, 2 * heads * deep + heads * size
    units = []
    for h in range(heads):
        units += [
            project(query_v, h, h * deep, deep),
            project(key_v, h, (heads + h) * deep, deep),
            project(value_v, h, values + h * size, size),
            project(gate_v, h, gates + h * size, size),
            attend(h),
        ]
    steps = [g.step for _ in range(n - 1) for g in gathers]
    wide_steps = [g.step for _ in range(len(bits_of(m))) for g in doubling]
    mixed = []
    for i in range(max(len(steps), len(wide_steps))):
        mixed += steps[i : i + 1] + wide_steps[i : i + 1]
    late = mixed[-2 * PARTS :]
    in_order(units, mixed[: -2 * PARTS])
    count = len(copies) - 1
    for src, dst in (
        (query_v, query_o), (key_v, key_o), (value_v, value_o), (gate_v, gate_o),
        (norm_v, norm_o), (scale_v, scale_o), (scores_v, scores_o), (gated_v, gated_o),
        (cot_v, cot_o),
    ):
        local(src, dst)
    for step in late:
        step()
    for item in copies[count:]:
        item.wait()
    for item in doubling:
        assert item.done == len(bits_of(m)) + 1
        item.leave()
    line.leave()


def forward_call(rows, weight, cot, col, row, pack, n, m, heads):
    tokens, width = rows.shape
    shape = jax.ShapeDtypeStruct
    outs = (
        shape((heads, tokens, HK), BF),
        shape((heads, tokens, HK), BF),
        shape((heads, tokens, HV), BF),
        shape((heads, tokens, HV), F32),
        shape((heads, tokens, HV), F32),
        shape((heads, tokens, 1), F32),
        shape((heads, tokens, tokens), BF),
        shape((heads, tokens, HV), BF),
        shape((tokens * FRONT // CHUNKS, width), BF),
        shape((pack.shape[0], m * pack.shape[1]), BF),
    )
    attention_rows = 2 * heads * (HK + HV)
    wide = 2 * PARTS * (m - 1)
    sems = FRONT * 2 * (n - 1)
    return pl.pallas_call(
        functools.partial(forward_kernel, n, m),
        out_shape=outs,
        in_specs=[ANY] * 3 + [VM] * 3,
        out_specs=(ANY,) * len(outs),
        scratch_shapes=[pltpu.VMEM(rows.shape, BF), pltpu.VMEM((attention_rows, width), BF)]
        + [pltpu.VMEM(o.shape, o.dtype) for o in outs[:-1]]
        + [
            pltpu.SemaphoreType.DMA((FRONT + 2 + len(outs),)),
            pltpu.SemaphoreType.DMA((sems,)),
            pltpu.SemaphoreType.DMA((sems,)),
            pltpu.SemaphoreType.DMA((wide,)),
            pltpu.SemaphoreType.DMA((wide,)),
        ],
        compiler_params=pltpu.CompilerParams(
            collective_id=4, has_side_effects=True, vmem_limit_bytes=VMEM_MOST
        ),
        name="forward",
    )(rows, weight, cot, col, row, pack)


def backward_kernel(
    n, mid, weights, gate, norm, scale, scores, query, key, value, down, middle, col, row,
    qk_o, value_o, gate_o, outputs,
    mid_v, wo_v, gate_v, norm_v, scale_v, scores_v, query_v, key_v, value_v, part, middle_v,
    d_qk, d_value, d_gate, d_kept, d_scores, lefts, rights, copy_sem, send_sem, recv_sem,
):
    line = Line(n, send_sem, recv_sem)
    heads, tokens, deep = query_v.shape
    size = value_v.shape[2]
    back = CHUNKS - DOWNS
    per = part.shape[0] // back
    piece = per // n
    copies = []

    def local(src, dst):
        c = pltpu.make_async_copy(src, dst, copy_sem.at[len(copies)])
        copies.append(c)
        c.start()
        return c

    load_part = local(down, part)
    loads = [
        local(src, dst)
        for src, dst in (
            (mid, mid_v), (weights.at[pl.ds(weights.shape[0] - wo_v.shape[0], wo_v.shape[0])], wo_v),
            (gate, gate_v), (norm, norm_v), (scale, scale_v), (value, value_v), (key, key_v),
            (query, query_v), (scores, scores_v), (middle, middle_v),
        )
    ]
    line.enter()
    for h in range(back):
        no_neighbour_zero(n, line.place, lefts.at[h, n - 2], rights.at[h, n - 2])
    scatters = [
        Scatter(
            line,
            lambda k, h=h: part.at[pl.ds(h * per + k * piece, piece)],
            lambda s, h=h: lefts.at[h, s - 1],
            lambda s, h=h: rights.at[h, s - 1],
            add_into,
        )
        for h in range(back)
    ]
    load_part.wait()
    for item in scatters:
        item.step()
    for item in loads:
        item.wait()

    def gates(h):
        def step(at):
            grad = dot_nt(mid_v[at, :], wo_v[pl.ds(h * size, size), :])
            pre, hat = gate_v[h, at, :], norm_v[h, at, :]
            s = jax.nn.sigmoid(pre)
            d_gate[h, at, :] = (grad * hat * (s + pre * s * (1.0 - s))).astype(BF)
            d_kept[h, at, :] = norm_back(grad * (pre * s), hat, scale_v[h, at, :]).astype(BF)

        return lambda: tiles_of(tokens, step)

    def by_row(h):
        def step(at):
            allowed = (col[at, 0:1] >= row[0:1, :]) & (col[at, 1:2] == row[1:2, :])
            grad = dot_nt(d_kept[h, at, :], value_v[h]) * col[at, 2 + h : 3 + h]
            grad = jnp.where(allowed, grad * row[2 + h : 3 + h, :], 0.0).astype(BF)
            d_scores[at, :] = grad
            d_qk[at, pl.ds(h * deep, deep)] = dot_nn(grad, key_v[h]).astype(BF)

        return lambda: tiles_of(tokens, step)

    def by_column(h):
        def step(at):
            d_value[h, at, :] = dot_tn(scores_v[h, :, at], d_kept[h]).astype(BF)
            d_qk[at, pl.ds((heads + h) * deep, deep)] = dot_tn(d_scores[:, at], query_v[h]).astype(
                BF
            )

        return lambda: tiles_of(tokens, step)

    units = []
    for h in range(heads):
        units += [gates(h), by_row(h), by_column(h)]
    in_order(units, [item.step for _ in range(n - 2) for item in scatters])
    count = len(copies)
    local(d_qk, qk_o)
    local(d_value, value_o)
    local(d_gate, gate_o)
    for h in range(back):
        scatters[h].finish()

        def step(at):
            outputs[at(h * piece), :] = (
                middle_v[at(h * piece), :]
                + part[at(h * per), :].astype(F32)
                + lefts[h, n - 2, at(), :].astype(F32)
                + rights[h, n - 2, at(), :].astype(F32)
            ).astype(BF)

        blocks(piece, step)
    for item in copies[count:]:
        item.wait()
    for item in scatters:
        item.drain()


def backward_call(mid, weights, gate, norm, scale, scores, query, key, value, down, middle, col, row, n):
    tokens, width = mid.shape
    heads, _, size = value.shape
    back = CHUNKS - DOWNS
    nv = heads * size
    shape = jax.ShapeDtypeStruct
    outs = (
        shape((tokens, 2 * heads * HK), BF),
        shape(value.shape, BF),
        shape(value.shape, BF),
        shape(middle.shape, BF),
    )
    ins = (gate, norm, scale, scores, query, key, value, down, middle)
    hop = (back, n - 1, middle.shape[0] // back, width)
    sems = back * 2 * (n - 1)
    return pl.pallas_call(
        functools.partial(backward_kernel, n),
        out_shape=outs,
        in_specs=[ANY] * 11 + [VM] * 2,
        out_specs=(ANY,) * 3 + (VM,),
        scratch_shapes=[pltpu.VMEM(mid.shape, BF), pltpu.VMEM((nv, width), BF)]
        + [pltpu.VMEM(a.shape, a.dtype) for a in ins]
        + [pltpu.VMEM(o.shape, o.dtype) for o in outs[:3]]
        + [
            pltpu.VMEM(value.shape, BF),
            pltpu.VMEM((tokens, tokens), BF),
            pltpu.VMEM(hop, BF),
            pltpu.VMEM(hop, BF),
            pltpu.SemaphoreType.DMA((14,)),
            pltpu.SemaphoreType.DMA((sems,)),
            pltpu.SemaphoreType.DMA((sems,)),
        ],
        compiler_params=pltpu.CompilerParams(
            collective_id=5, has_side_effects=True, vmem_limit_bytes=VMEM_MOST
        ),
        name="backward",
    )(mid, weights, *ins, col, row)


def products_kernel(plan, arrays, *refs):
    ins, out = refs[:arrays], refs[arrays]
    held, result, copy_sem = refs[arrays + 1 : 2 * arrays + 1], refs[-2], refs[-1]
    loads = [pltpu.make_async_copy(a, b, copy_sem.at[i]) for i, (a, b) in enumerate(zip(ins, held))]
    for item in loads:
        item.start()
    waited, stores, base = set(), [], 0
    for left, head, start, size, right in plan:
        for i in (left, right):
            if i not in waited:
                loads[i].wait()
                waited.add(i)
        target = pl.ds(base, size)

        def step(j, carry):
            at = pl.ds(pl.multiple_of(j * 4 * LANES, 4 * LANES), 4 * LANES)
            source = held[left][head] if head is not None else held[left][:, pl.ds(start, size)]
            result[target, at] = dot_tn(source, held[right][:, at]).astype(BF)
            return carry

        lax.fori_loop(0, result.shape[1] // (4 * LANES), step, 0)
        store = pltpu.make_async_copy(
            result.at[target], out.at[target], copy_sem.at[arrays + len(stores)]
        )
        store.start()
        stores.append(store)
        base += size
    spare = result.shape[0] - base
    if spare:
        target = pl.ds(base, spare)
        result[target, :] = jnp.zeros((spare, result.shape[1]), BF)
        store = pltpu.make_async_copy(
            result.at[target], out.at[target], copy_sem.at[arrays + len(stores)]
        )
        store.start()
        stores.append(store)
    for item in stores:
        item.wait()


def weight_products(plan, arrays, name, rows):
    width = arrays[plan[0][4]].shape[1]
    return pl.pallas_call(
        functools.partial(products_kernel, plan, len(arrays)),
        out_shape=jax.ShapeDtypeStruct((rows, width), BF),
        in_specs=[ANY] * len(arrays),
        out_specs=ANY,
        scratch_shapes=[pltpu.VMEM(a.shape, a.dtype) for a in arrays]
        + [pltpu.VMEM((rows, width), BF), pltpu.SemaphoreType.DMA((len(arrays) + len(plan) + 1,))],
        compiler_params=pltpu.CompilerParams(vmem_limit_bytes=VMEM_MOST),
        name=name,
    )(*arrays)


def pad_rows(array, count):
    return jnp.pad(array, ((0, count - array.shape[0]), (0, 0)))


def pad_columns(array, count):
    return jnp.pad(array, ((0, 0), (0, count - array.shape[1])))


def body(
    inputs,
    segments,
    first_norm_gain,
    w_query,
    w_key,
    w_value,
    w_gate,
    w_out,
    second_norm_gain,
    w_glu_gate,
    w_glu_up,
    w_down,
    cotangent,
):
    n = lax.axis_size("mp")
    place = lax.axis_index("mp")
    heads = H // n
    head_start = place * heads
    rows, width = inputs.shape
    shard = w_query.shape[0]
    piece = rows // CHUNKS
    nk, nv, nf = heads * HK, heads * HV, w_down.shape[0]
    f_wide = -(-nf // LANES) * LANES
    f_tiles = f_wide // LANES
    grain = 2 * PARTS * BLOCK
    one_rows = -(-(2 * nk + 3 * nv) // grain) * grain
    gap = one_rows - 2 * nk - 3 * nv
    m = lax.axis_size("dp")

    pack_one = jnp.concatenate(
        [w_query.T, w_key.T, w_value.T, w_gate.T, jnp.zeros((gap, shard), BF), w_out], axis=0
    )
    glu_pack = jnp.stack(
        [
            pad_rows(w_glu_gate.T, f_wide).reshape(f_tiles, LANES, shard),
            pad_rows(w_glu_up.T, f_wide).reshape(f_tiles, LANES, shard),
        ],
        axis=1,
    ).reshape(2 * f_wide, shard)
    pack_two = jnp.concatenate([glu_pack, pad_rows(w_down, f_wide)], axis=0)

    first_hat, _ = layer_norm(inputs.astype(F32), epsilon)
    rows_one, weight_one = gather_rows((first_hat * first_norm_gain).astype(BF), pack_one, n, m)
    tokens = rows_one.shape[0]

    slot_shard = lax.rem(place - jnp.arange(n) + n, n)
    places = (
        slot_shard[None, :, None] * rows
        + jnp.arange(CHUNKS)[:, None, None] * piece
        + jnp.arange(piece)[None, None, :]
    ).reshape(tokens)
    seg = segments.reshape(n, CHUNKS, piece)[::-1]
    seg = lax.dynamic_slice_in_dim(jnp.concatenate([seg, seg], axis=0), n - 1 - place, n, axis=0)
    seg = seg.transpose(1, 0, 2).reshape(tokens)

    log_gamma = jnp.log1p(-jnp.exp2(-5.0 - (head_start + jnp.arange(heads)).astype(F32)))
    spot = places.astype(F32)
    powers = spot[None] * log_gamma[:, None]
    marks = jnp.stack([spot, seg.astype(F32)])
    col = jnp.concatenate([marks, jnp.exp(powers)], axis=0).T
    row = jnp.concatenate([marks, jnp.exp(-powers) * HK ** (-0.5)], axis=0)

    (
        query, key, value, gate_pre, normalized, scale_group, scores, gated, cot_front, weight_two,
    ) = forward_call(rows_one, weight_one, cotangent, col, row, pack_two, n, m, heads)
    (
        rows_two, cot_rows, mid_rows, hidden, d_glu, down, outputs_front, middle, middle_grad,
        second_gain,
    ) = middle_call(
        gated, weight_two, weight_one, inputs, cotangent, cot_front, second_norm_gain[None], n
    )

    plan = [(0, None, t * f_wide, f_wide, 1) for t in range(2)] + [(2, None, 0, f_wide, 3)]
    grads_two = weight_products(plan, (d_glu, rows_two, hidden, cot_rows), "products_two", 3 * f_wide)
    summed_two = lax.psum_scatter(grads_two, "dp", scatter_dimension=1, tiled=True).astype(F32)
    glu_sum = summed_two[: 2 * f_wide].reshape(f_tiles, 2, LANES, shard)

    d_qk, d_value, d_gate, outputs_back = backward_call(
        mid_rows, weight_one, gate_pre, normalized, scale_group, scores, query, key, value,
        down, middle, col, row, n,
    )
    plan = [(0, h, 0, HV, 1) for h in range(heads)] + [(2, h, 0, HV, 3) for h in range(heads)]
    plan += [(4, None, t * nk, nk, 3) for t in range(2)]
    plan += [(5, h, 0, HV, 3) for h in range(heads)]
    grads_one = weight_products(
        plan, (gated, mid_rows, d_gate, rows_one, d_qk, d_value), "products_one", one_rows
    )
    input_gradient, gains, summed_one = last_call(
        d_qk, d_value, d_gate, weight_one, grads_one, inputs, first_norm_gain[None], middle_grad,
        second_gain, n, m,
    )
    gains = gains.reshape(2, width)
    at = 2 * nv
    return (
        jnp.concatenate([outputs_front, outputs_back], axis=0),
        input_gradient,
        gains[0],
        summed_one[at : at + nk].T,
        summed_one[at + nk : at + 2 * nk].T,
        summed_one[at + 2 * nk : at + 2 * nk + nv].T,
        summed_one[nv : 2 * nv].T,
        summed_one[:nv],
        gains[1],
        glu_sum[:, 0].reshape(f_wide, shard)[:nf].T,
        glu_sum[:, 1].reshape(f_wide, shard)[:nf].T,
        summed_two[2 * f_wide : 2 * f_wide + nf],
    )


def solution(mesh):
    split = P(("dp", "mp"), None)
    wide, tall = P("dp", "mp"), P("mp", "dp")
    return jax.shard_map(
        body,
        mesh=mesh,
        in_specs=(
            split, P("dp", None), P(), wide, wide, wide, wide, tall, P(), wide, wide, tall, split,
        ),
        out_specs=(
            split, split, P(), wide, wide, wide, wide, tall, P(), wide, wide, tall,
        ),
        check_vma=False,
    )
```

```python
import functools

import jax
import jax.numpy as jnp
from jax import lax
from jax.experimental import pallas as pl
from jax.experimental.pallas import tpu as pltpu
from jax.sharding import PartitionSpec as P

H = 8
HK = 256
HV = 432
LEN = 1024
CHUNKS = 4
FRONT = CHUNKS // 2
DOWNS = CHUNKS // 4
LANES = 128
VMEM_MOST = 66_000_000

epsilon = 1e-05
group_epsilon = 1.0
BF = jnp.bfloat16
F32 = jnp.float32


def layer_norm(values_in, offset):
    centre = jnp.mean(values_in, axis=-1, keepdims=True)
    centred = values_in - centre
    variance = jnp.mean(centred * centred, axis=-1, keepdims=True)
    scaling = lax.rsqrt(variance + offset)
    return (centred * scaling, scaling)


def norm_back(grad_hat, normed_hat, scaling):
    first_mean = jnp.mean(grad_hat, axis=-1, keepdims=True)
    second_mean = jnp.mean(grad_hat * normed_hat, axis=-1, keepdims=True)
    return scaling * (grad_hat - first_mean - normed_hat * second_mean)


def glu_act(gate_pre, up_pre):
    return jax.nn.gelu(gate_pre, approximate=True) * up_pre


def dot_nt(a, b):
    return lax.dot_general(a, b, (((1,), (1,)), ((), ())), preferred_element_type=F32)


def dot_nn(a, b):
    return lax.dot_general(a, b, (((1,), (0,)), ((), ())), preferred_element_type=F32)


def dot_tn(a, b):
    return lax.dot_general(a, b, (((0,), (0,)), ((), ())), preferred_element_type=F32)


MESH = pl.DeviceIdType.MESH


class Line:
    def __init__(self, n, send_sem, recv_sem):
        self.n, self.send_sem, self.recv_sem = n, send_sem, recv_sem
        self.place = lax.axis_index("mp")
        self.used = 0
        self.sent = []

    def enter(self, others=None):
        barrier = pltpu.get_barrier_semaphore()
        n, place = self.n, self.place

        @pl.when(place >= 1)
        def _():
            pl.semaphore_signal(barrier, inc=1, device_id={"mp": place - 1}, device_id_type=MESH)

        @pl.when(place <= n - 2)
        def _():
            pl.semaphore_signal(barrier, inc=1, device_id={"mp": place + 1}, device_id_type=MESH)

        peers = jnp.minimum(place, 1) + jnp.minimum(n - 1 - place, 1)
        if others is not None:
            axis, indices = others
            for index in indices:
                pl.semaphore_signal(barrier, inc=1, device_id={axis: index}, device_id_type=MESH)
            peers = peers + len(indices)
        pl.semaphore_wait(barrier, peers)

    def copy(self, src, dst, index, toward):
        return pltpu.make_async_remote_copy(
            src_ref=src,
            dst_ref=dst,
            send_sem=self.send_sem.at[index],
            recv_sem=self.recv_sem.at[index],
            device_id={"mp": self.place + toward},
            device_id_type=MESH,
        )

    def leave(self):
        for condition, copy in self.sent:
            pl.when(condition)(copy.wait_send)


class Gather:
    def __init__(self, line, slot):
        self.line, self.slot, self.step_no = line, slot, 0
        self.base = line.used
        line.used += 2 * (line.n - 1)
        n = line.n
        self.right = [
            line.copy(slot(s - 1), slot(s), self.base + s - 1, 1) for s in range(1, n)
        ]
        self.left = [
            line.copy(slot((n - s + 1) % n), slot(n - s), self.base + n - 2 + s, -1)
            for s in range(1, n)
        ]

    def arrive(self, s):
        n, place = self.line.n, self.line.place
        pl.when(place >= s)(self.right[s - 1].wait_recv)
        pl.when(place <= n - 1 - s)(self.left[s - 1].wait_recv)

    def step(self):
        self.step_no += 1
        s, n, place = self.step_no, self.line.n, self.line.place
        if s > 1:
            self.arrive(s - 1)
        if s < n:
            to_right = (place >= s - 1) & (place <= n - 2)
            to_left = (place <= n - s) & (place >= 1)
            pl.when(to_right)(self.right[s - 1].start)
            pl.when(to_left)(self.left[s - 1].start)
            self.line.sent += [(to_right, self.right[s - 1]), (to_left, self.left[s - 1])]


class Scatter:
    def __init__(self, line, slot, from_left, from_right, add):
        self.line, self.slot, self.add, self.step_no = line, slot, add, 0
        self.from_left, self.from_right = from_left, from_right
        self.base = line.used
        line.used += 2 * (line.n - 1)
        n = line.n
        self.right = [
            line.copy(slot(s), from_left(s), self.base + s - 1, 1) for s in range(1, n)
        ]
        self.left = [
            line.copy(slot(n - s), from_right(s), self.base + n - 2 + s, -1) for s in range(1, n)
        ]
        self.mine = []

    def step(self):
        self.step_no += 1
        s, n, place = self.step_no, self.line.n, self.line.place
        to_right, to_left = place <= s - 1, place >= n - s
        if s > 1:

            @pl.when(to_right & (place >= 1))
            def _():
                self.right[s - 2].wait_recv()
                self.add(self.slot(s), self.from_left(s - 1))

            @pl.when(to_left & (place <= n - 2))
            def _():
                self.left[s - 2].wait_recv()
                self.add(self.slot(n - s), self.from_right(s - 1))

        pl.when(to_right)(self.right[s - 1].start)
        pl.when(to_left)(self.left[s - 1].start)
        self.mine += [(to_right, self.right[s - 1]), (to_left, self.left[s - 1])]

    def finish(self):
        n, place = self.line.n, self.line.place

        @pl.when(place >= 1)
        def _():
            self.right[n - 2].wait_recv()

        @pl.when(place <= n - 2)
        def _():
            self.left[n - 2].wait_recv()

    def drain(self):
        for condition, copy in self.mine:
            pl.when(condition)(copy.wait_send)


ANY = pl.BlockSpec(memory_space=pl.ANY)
VM = pl.BlockSpec(memory_space=pltpu.VMEM)
BLOCK = 16


def blocks(count, step):
    def run(i, carry):
        step(lambda base=0: pl.ds(pl.multiple_of(base + i * BLOCK, BLOCK), BLOCK))
        return carry

    lax.fori_loop(0, count // BLOCK, run, 0)


def add_into(target, extra):
    def step(at):
        target[at(), :] = (target[at(), :].astype(F32) + extra[at(), :].astype(F32)).astype(BF)

    blocks(target.shape[0], step)


def product_tiles(target, left, right, tile):
    def step(j, carry):
        at = pl.ds(pl.multiple_of(j * tile, tile), tile)
        target[:, at] = dot_nn(left[...], right[:, at]).astype(BF)
        return carry

    lax.fori_loop(0, right.shape[1] // tile, step, 0)


class Doubling:
    def __init__(self, m, own, out, rows, bits, base, send_sem, recv_sem):
        self.d = lax.axis_index("dp")
        self.own, self.out, self.rows, self.bits, self.base = own, out, rows, bits, base
        self.send_sem, self.recv_sem = send_sem, recv_sem
        self.shard = own.shape[1]
        self.done = 0
        self.sent = []

    def flip(self, d, bit):
        return d + bit * (1 - 2 * (lax.div(d, bit) % 2))

    def block(self, d):
        return self.out.at[self.rows, pl.ds(pl.multiple_of(d * self.shard, self.shard), self.shard)]

    def copies(self, level, landing):
        owners = [self.d]
        for bit in self.bits[:level]:
            owners += [self.flip(d, bit) for d in owners]
        bit = self.bits[level]
        partner = self.flip(self.d, bit)
        out = []
        for i, d in enumerate(owners):
            d = self.flip(d, bit) if landing else d
            src = self.own.at[self.rows] if i == 0 and not landing else self.block(d)
            index = self.base + (1 << level) - 1 + i
            out.append(
                pltpu.make_async_remote_copy(
                    src_ref=src,
                    dst_ref=self.block(d),
                    send_sem=self.send_sem.at[index],
                    recv_sem=self.recv_sem.at[index],
                    device_id={"dp": partner},
                    device_id_type=MESH,
                )
            )
        return out

    def step(self):
        level = self.done
        if level > 0:
            for c in self.copies(level - 1, True):
                c.wait_recv()
        if level < len(self.bits):
            out = self.copies(level, False)
            for c in out:
                c.start()
            self.sent += out
        self.done += 1

    def leave(self):
        for c in self.sent:
            c.wait_send()


def bits_of(m):
    bits = [1 << b for b in range(m.bit_length() - 1)]
    assert 1 << len(bits) == m
    return bits


PARTS = 2


def weight_gather(m, pack, weight, send_sem, recv_sem):
    bits = bits_of(m)
    outer = bits[1:]
    height = pack.shape[0] // (2 * PARTS)
    doubling = []
    for i in range(2 * PARTS):
        order = (outer if i % 2 == 0 else outer[::-1]) + bits[:1]
        rows = pl.ds(i * height, height)
        doubling.append(Doubling(m, pack, weight, rows, order, i * (m - 1), send_sem, recv_sem))
    first = doubling[0]
    return doubling, [first.flip(first.d, bit) for bit in bits]


def own_columns(pack, weight):
    shard = pack.shape[1]
    at = pl.multiple_of(lax.axis_index("dp") * shard, shard)
    return weight.at[:, pl.ds(at, shard)]


def gather_kernel(n, m, own, pack, out, weight, send_sem, recv_sem, copy_sem, wide_send, wide_recv):
    line = Line(n, send_sem, recv_sem)
    piece = own.shape[0] // CHUNKS
    per = n * piece
    bits = bits_of(m)
    doubling, peers = weight_gather(m, pack, weight, wide_send, wide_recv)
    line.enter(["dp", peers])
    local, gathers = [], []
    keep = pltpu.make_async_copy(pack, own_columns(pack, weight), copy_sem.at[CHUNKS])
    for h in range(CHUNKS):
        mine = own.at[pl.ds(h * piece, piece)]
        local.append(
            pltpu.make_async_copy(mine, out.at[pl.ds(h * per, piece)], copy_sem.at[h])
        )

        def slot(k, h=h, mine=mine):
            return mine if k == 0 else out.at[pl.ds(h * per + k * piece, piece)]

        gathers.append(Gather(line, slot))
    local.append(keep)

    def line_step(items):
        for item in items:
            item.step()

    half = CHUNKS // 2
    line_step(gathers)
    line_step(doubling)
    for item in local:
        item.start()
    for level in range(1, max(n, len(bits) + 1)):
        for side in range(2):
            if level <= len(bits):
                line_step(doubling[side * PARTS : (side + 1) * PARTS])
            if level < n:
                line_step(gathers[side * half : (side + 1) * half])
    for item in local:
        item.wait()
    for item in gathers:
        assert item.step_no == n
    for item in doubling:
        assert item.done == len(bits) + 1
        item.leave()
    line.leave()


def gather_rows(own, pack, n, m):
    rows, width = own.shape
    count = CHUNKS * 2 * (n - 1)
    wide = 2 * PARTS * (m - 1)
    return pl.pallas_call(
        functools.partial(gather_kernel, n, m),
        out_shape=(
            jax.ShapeDtypeStruct((n * rows, width), own.dtype),
            jax.ShapeDtypeStruct((pack.shape[0], m * pack.shape[1]), pack.dtype),
        ),
        in_specs=[VM, VM],
        out_specs=(ANY, ANY),
        scratch_shapes=[
            pltpu.SemaphoreType.DMA((count,)),
            pltpu.SemaphoreType.DMA((count,)),
            pltpu.SemaphoreType.DMA((CHUNKS + 1,)),
            pltpu.SemaphoreType.DMA((wide,)),
            pltpu.SemaphoreType.DMA((wide,)),
        ],
        compiler_params=pltpu.CompilerParams(collective_id=0, has_side_effects=True),
        name="gather_rows",
    )(own, pack)


def no_neighbour_zero(n, place, from_left, from_right):
    @pl.when(place == 0)
    def _():
        from_left[...] = jnp.zeros_like(from_left)

    @pl.when(place == n - 1)
    def _():
        from_right[...] = jnp.zeros_like(from_right)


(COT, OUT, ONE, END_ONE, TWO, GLU, GRAD, GRAD_SUM, END_GRAD, MID, DOWN, DOWN_SUM, END_DOWN, PRODUCTS) = range(14)

DUE = {
    OUT: (-2.23, 1.66, 0), ONE: (-1.99, 1.12, 1.03), END_ONE: (1.46, 1.37, 0), TWO: (0.73, 1.15, 0.94),
    COT: (0.35, 1.39, 1.02), GLU: (1.14, -1.37, 1.55), GRAD: (3.09, 2.02, 0),
    GRAD_SUM: (3.48, 1.71, 0.74), END_GRAD: (7.02, -2.12, 0), MID: (5.68, 0.86, 1.11),
    DOWN: (1.3, 0.36, 0), DOWN_SUM: (1.87, 1.35, 0.95), END_DOWN: (7.9, 2.17, 0),
    PRODUCTS: (7.5, 0, 0.4),
}
TUNED = {
    (4, 4): [
        2, 4, 5, 8, 8, 2, 7, 9, 8, 11, 2, 9, 2, 12, 16, 9, 16, 11, 6, 16,
        13, 10, 16, 17, 20, 10, 11, 17, 20, 10, 24, 17, 15, 3, 14, 28, 18, 17, 21, 19,
        21, 18, 19, 25, 28, 29, 18, 40, 3, 29, 19, 28, 44, 18, 22, 29, 3, 22, 19, 32,
        36, 26, 30, 3, 33, 37, 23, 36, 30, 23, 44, 37, 30, 43, 27, 44, 36, 34, 37, 31,
        31, 38, 48, 52, 31, 41, 38, 52, 35, 39, 36, 42, 38, 52, 37, 39, 38, 39, 39,
    ],
}


def middle_order(n):
    if (n, CHUNKS) in TUNED:
        return [divmod(code, CHUNKS) for code in TUNED[n, CHUNKS]]
    count = {k: 1 for k in DUE}
    count.update({COT: n, TWO: n, MID: n, ONE: n - 1, GRAD_SUM: n - 1, DOWN_SUM: n - 1, GLU: 2, PRODUCTS: 3})
    needs = {
        ONE: [OUT], END_ONE: [ONE], TWO: [END_ONE], GLU: [TWO, COT], GRAD: [GLU], GRAD_SUM: [GRAD],
        END_GRAD: [GRAD_SUM], MID: [END_GRAD], DOWN: [GLU], DOWN_SUM: [DOWN], END_DOWN: [DOWN_SUM],
    }
    todo = sorted(
        (first + h * later + s * 3 / (n - 1) * each, k, h, s)
        for k, (first, later, each) in DUE.items()
        for h in range(CHUNKS)
        for s in range(count[k])
        if not (k == PRODUCTS and h > 0 or k == COT and h < FRONT or k in (DOWN_SUM, END_DOWN) and h >= DOWNS)
    )
    taken, order = {}, []
    while todo:
        for item in todo:
            _, k, h, s = item
            ready = taken.get((k, h), 0) == s and (
                k != PRODUCTS or all(taken.get((GLU, c), 0) == 2 for c in range(CHUNKS))
            )
            ready = ready and all(
                taken.get((need, h), 0) == count[need] or (need == COT and h < FRONT)
                for need in needs.get(k, [])
            )
            if ready:
                break
        todo.remove(item)
        taken[k, h] = s + 1
        order.append((k, h))
    return order


def middle_kernel(
    n, gated, weights, out_weight, own, cot, cot_front, gain,
    mid_out, products_out, down_out, outputs, middle_out, d_middle, gain_out,
    gated_v, wo_v, wg_v, wd_v, own_v, cot_v, rows_v, hidden_v, glu_v, part, part_two,
    left_a, right_a, left_b, right_b, middle, stage, result, copy_sem, send_sem, recv_sem,
):
    line = Line(n, send_sem, recv_sem)
    place = line.place
    count, width = own.shape
    piece = count // CHUNKS
    per = n * piece
    wide = hidden_v.shape[1]
    copies = []

    def local(src, dst):
        c = pltpu.make_async_copy(src, dst, copy_sem.at[len(copies)])
        copies.append(c)
        c.start()
        return c

    def rows_at(ref, h, k=0, size=piece):
        return ref.at[pl.ds(h * per + k * piece, size)]

    load_cot = [
        local(cot.at[pl.ds(h * piece, piece)], rows_at(cot_v, h)) for h in range(FRONT, CHUNKS)
    ]
    front = pl.ds(0, FRONT * per)
    load_cot.append(local(cot_front, cot_v.at[front]))
    load_gated = local(gated, gated_v)
    load_wo = local(
        out_weight.at[pl.ds(out_weight.shape[0] - wo_v.shape[0], wo_v.shape[0])], wo_v
    )
    load_own = local(own, own_v)
    load_wg = local(weights.at[pl.ds(0, 2 * wide)], wg_v)
    load_wd = local(weights.at[pl.ds(2 * wide, wide)], wd_v)
    line.enter()
    for h in range(CHUNKS):
        no_neighbour_zero(n, place, left_a.at[h, n - 2], right_a.at[h, n - 2])
    for h in range(DOWNS):
        no_neighbour_zero(n, place, left_b.at[h, n - 2], right_b.at[h, n - 2])
    gain_out[...] = jnp.zeros_like(gain_out)

    def scatter(buf, lefts, rights, h):
        return Scatter(
            line,
            lambda k: rows_at(buf, h, k),
            lambda s: lefts.at[h, s - 1],
            lambda s: rights.at[h, s - 1],
            add_into,
        )

    gather_cot = {
        h: Gather(line, functools.partial(rows_at, cot_v, h)) for h in range(FRONT, CHUNKS)
    }
    gather_two = [Gather(line, functools.partial(rows_at, rows_v, h)) for h in range(CHUNKS)]

    def mid_slot(h, k):
        return stage.at[h] if k == 0 else rows_at(mid_out, h, k)

    gather_mid = [Gather(line, functools.partial(mid_slot, h)) for h in range(CHUNKS)]
    scatter_one = [scatter(part, left_a, right_a, h) for h in range(CHUNKS)]
    scatter_two = [scatter(part_two, left_b, right_b, h) for h in range(DOWNS)]
    scatter_grad = [scatter(part, left_a, right_a, h) for h in range(CHUNKS)]

    def chunk(ref, h):
        return ref.at[pl.ds(h * per, per)]

    def out_product(h):
        heads, _, size = gated_v.shape
        target, whole = chunk(part, h), pl.ds(h * per, per)

        def step(j, carry):
            at = pl.ds(pl.multiple_of(j * 2 * LANES, 2 * LANES), 2 * LANES)
            target[:, at] = sum(
                dot_nn(gated_v[i, whole, :], wo_v[pl.ds(i * size, size), at]) for i in range(heads)
            ).astype(BF)
            return carry

        lax.fori_loop(0, width // (2 * LANES), step, 0)

    def finish_one(h):
        scatter_one[h].finish()

        def step(at):
            src = at(h * per)
            mine = at(h * piece)
            total = (
                own_v[mine, :].astype(F32)
                + part[src, :].astype(F32)
                + left_a[h, n - 2, at(), :].astype(F32)
                + right_a[h, n - 2, at(), :].astype(F32)
            )
            middle[mine, :] = total
            hat, _ = layer_norm(total, epsilon)
            rows_v[src, :] = (hat * gain[...]).astype(BF)

        blocks(piece, step)

    def glu_tiles(h, first, last):
        def step(j, carry):
            pair = pl.ds(pl.multiple_of(j * 2 * LANES, 2 * LANES), 2 * LANES)
            at = pl.ds(pl.multiple_of(j * LANES, LANES), LANES)
            whole = pl.ds(h * per, per)
            both = dot_nt(rows_v[whole, :], wg_v[pair, :])
            d_hidden = dot_nt(cot_v[whole, :], wd_v[at, :])
            u, up = both[:, :LANES], both[:, LANES:]
            c = 0.7978845608028654
            t = jnp.tanh(c * (u + 0.044715 * (u * u * u)))
            half = 0.5 * (1.0 + t)
            act = u * half
            slope = half + 0.5 * u * (1.0 - t * t) * (c * (1.0 + 3 * 0.044715 * (u * u)))
            hidden_v[whole, at] = (act * up).astype(BF)
            glu_v[whole, pair] = jnp.concatenate(
                [(d_hidden * up * slope).astype(BF), (d_hidden * act).astype(BF)], axis=1
            )
            return carry

        lax.fori_loop(first, last, step, 0)

    def grad_product(h):
        product_tiles(chunk(part, h), chunk(glu_v, h), wg_v, 2 * LANES)

    def down_product(h):
        product_tiles(chunk(part_two, h), chunk(hidden_v, h), wd_v, 2 * LANES)

    def finish_grad(h):
        scatter_grad[h].finish()

        def step(at):
            src = at(h * per)
            mine = at(h * piece)
            grad = (
                part[src, :].astype(F32)
                + left_a[h, n - 2, at(), :].astype(F32)
                + right_a[h, n - 2, at(), :].astype(F32)
            )
            hat, scale = layer_norm(middle[mine, :], epsilon)
            gain_out[...] += jnp.sum((hat * grad).reshape(BLOCK // 8, 8, width), axis=0)
            d_mid = cot_v[src, :].astype(F32) + norm_back(grad * gain[...], hat, scale)
            d_middle[mine, :] = d_mid
            stage[h, at(), :] = d_mid.astype(BF)

        blocks(piece, step)
        local(stage.at[h], rows_at(mid_out, h))

    def finish_two(h):
        scatter_two[h].finish()

        def step(at):
            src = at(h * per)
            mine = at(h * piece)
            outputs[mine, :] = (
                middle[mine, :]
                + part_two[src, :].astype(F32)
                + left_b[h, n - 2, at(), :].astype(F32)
                + right_b[h, n - 2, at(), :].astype(F32)
            ).astype(BF)

        blocks(piece, step)

    tiles = wide // LANES
    cut = tiles // 2

    def wait_for(items):
        for item in items:
            item.wait()
        items.clear()

    first_loads, own_load = [load_gated, load_wo], [load_own]
    later_loads = [load_wg, load_wd]

    def out_action(h):
        wait_for(first_loads)
        out_product(h)

    def finish_one_action(h):
        wait_for(own_load)
        finish_one(h)

    def glu_action(h):
        wait_for(later_loads)
        if h in begun:
            glu_tiles(h, cut, tiles)
        else:
            begun.add(h)
            glu_tiles(h, 0, cut)

    def grad_action(h):
        scatter_one[h].drain()
        grad_product(h)

    def products_action(_):
        k = len(products)
        if k >= 2:
            products[k - 2].wait()
        left = hidden_v.at[...] if k == 2 else glu_v.at[:, pl.ds(k * wide, wide)]
        right = cot_v if k == 2 else rows_v
        target = result.at[k % 2]

        def step(j, carry):
            at = pl.ds(pl.multiple_of(j * 2 * LANES, 2 * LANES), 2 * LANES)
            target[:, at] = dot_tn(left[...], right[:, at]).astype(BF)
            return carry

        lax.fori_loop(0, width // (2 * LANES), step, 0)
        store = pltpu.make_async_copy(
            target, products_out.at[pl.ds(k * wide, wide)], copy_sem.at[spare + k]
        )
        store.start()
        products.append(store)

    products, spare = [], copy_sem.shape[0] - 3
    begun = set()
    actions = {
        COT: lambda h: gather_cot[h].step(),
        OUT: out_action,
        ONE: lambda h: scatter_one[h].step(),
        END_ONE: finish_one_action,
        TWO: lambda h: gather_two[h].step(),
        GLU: glu_action,
        GRAD: grad_action,
        GRAD_SUM: lambda h: scatter_grad[h].step(),
        END_GRAD: finish_grad,
        MID: lambda h: gather_mid[h].step(),
        DOWN: down_product,
        DOWN_SUM: lambda h: scatter_two[h].step(),
        END_DOWN: finish_two,
        PRODUCTS: products_action,
    }
    for item in load_cot:
        item.wait()
    for kind, h in middle_order(n):
        actions[kind](h)
    local(part_two.at[pl.ds(DOWNS * per, down_out.shape[0])], down_out)
    local(middle.at[pl.ds(DOWNS * piece, middle_out.shape[0])], middle_out)
    for item in list(gather_cot.values()) + gather_two + gather_mid:
        assert item.step_no == n
    for item in scatter_one + scatter_two + scatter_grad:
        assert item.step_no == n - 1
    for group in (scatter_grad, scatter_two):
        for item in group:
            item.drain()
    for item in copies[CHUNKS - FRONT + 6 :] + products[1:]:
        item.wait()
    assert len(products) == 3
    line.leave()


def middle_call(gated, weights, out_weight, own, cot, cot_front, gain, n):
    rows, width = own.shape
    heads, tokens, size = gated.shape
    nv = heads * size
    wide = weights.shape[0] // 3
    piece = rows // CHUNKS
    back = CHUNKS - DOWNS
    sems = CHUNKS * 5 * 2 * (n - 1)
    hop = (CHUNKS, n - 1, piece, width)
    shape = jax.ShapeDtypeStruct
    return pl.pallas_call(
        functools.partial(middle_kernel, n),
        out_shape=(
            shape((tokens, width), BF),
            shape((3 * wide, width), BF),
            shape((back * n * piece, width), BF),
            shape((DOWNS * piece, width), BF),
            shape((back * piece, width), F32),
            shape((rows, width), F32),
            shape((8, width), F32),
        ),
        in_specs=[ANY] * 6 + [VM],
        out_specs=(ANY,) * 3 + (VM, ANY, VM, VM),
        scratch_shapes=[
            pltpu.VMEM((heads, tokens, size), BF),
            pltpu.VMEM((nv, width), BF),
            pltpu.VMEM((2 * wide, width), BF),
            pltpu.VMEM((wide, width), BF),
            pltpu.VMEM((rows, width), BF),
            pltpu.VMEM((tokens, width), BF),
            pltpu.VMEM((tokens, width), BF),
            pltpu.VMEM((tokens, wide), BF),
            pltpu.VMEM((tokens, 2 * wide), BF),
            pltpu.VMEM((tokens, width), BF),
            pltpu.VMEM((tokens, width), BF),
            pltpu.VMEM(hop, BF),
            pltpu.VMEM(hop, BF),
            pltpu.VMEM((DOWNS,) + hop[1:], BF),
            pltpu.VMEM((DOWNS,) + hop[1:], BF),
            pltpu.VMEM((rows, width), F32),
            pltpu.VMEM((CHUNKS, piece, width), BF),
            pltpu.VMEM((2, wide, width), BF),
            pltpu.SemaphoreType.DMA((11 + 2 * CHUNKS - FRONT,)),
            pltpu.SemaphoreType.DMA((sems,)),
            pltpu.SemaphoreType.DMA((sems,)),
        ],
        compiler_params=pltpu.CompilerParams(
            collective_id=1, has_side_effects=True, vmem_limit_bytes=VMEM_MOST
        ),
        name="middle",
    )(gated, weights, out_weight, own, cot, cot_front, gain)


class Halving:
    def __init__(self, grads, rows, bits, base, kept, held, out, send_sem, recv_sem, load_sem):
        self.d = lax.axis_index("dp")
        self.grads, self.rows, self.bits, self.base = grads, rows, bits, base
        self.kept, self.held, self.out = kept, held, out
        self.send_sem, self.recv_sem, self.load_sem = send_sem, recv_sem, load_sem
        self.shard = out.shape[1]
        self.masks = [0]
        for bit in bits[:0:-1]:
            self.masks += [k + bit for k in self.masks]
        self.done, self.sent, self.loads = 0, [], []

    def flip(self, d, mask):
        for bit in self.bits:
            if mask & bit:
                d = d + bit * (1 - 2 * (lax.div(d, bit) % 2))
        return d

    def block(self, d):
        return self.grads.at[self.rows, pl.ds(pl.multiple_of(d * self.shard, self.shard), self.shard)]

    def count(self, level):
        return 1 << (len(self.bits) - 1 - level)

    def copies(self, level):
        bit = self.bits[level]
        partner = self.flip(self.d, bit)
        out = []
        for i in range(self.count(level)):
            if level == 0:
                src = self.block(self.flip(partner, self.masks[i]))
            else:
                src = self.kept.at[self.count(level) + i, self.rows]
            index = self.base + len(out) + sum(self.count(k) for k in range(level))
            out.append(
                pltpu.make_async_remote_copy(
                    src_ref=src,
                    dst_ref=self.held[level].at[i, self.rows],
                    send_sem=self.send_sem.at[index],
                    recv_sem=self.recv_sem.at[index],
                    device_id={"dp": partner},
                    device_id_type=MESH,
                )
            )
        return out

    def load(self):
        for i, mask in enumerate(self.masks):
            c = pltpu.make_async_copy(
                self.block(self.flip(self.d, mask)), self.kept.at[i, self.rows], self.load_sem.at[i]
            )
            c.start()
            self.loads.append(c)

    def add(self, level):
        last = level == len(self.bits) - 1
        start, size = self.rows.start, self.rows.size
        for i in range(self.count(level)):

            def step(at):
                total = self.kept[i, at(start), :].astype(F32) + self.held[level][
                    i, at(start), :
                ].astype(F32)
                if last:
                    self.out[at(start), :] = total
                else:
                    self.kept[i, at(start), :] = total.astype(BF)

            blocks(size, step)

    def step(self):
        level = self.done
        if level > 0:
            for c in self.loads:
                c.wait()
            self.loads = []
            for c in self.sent[-1]:
                c.wait_recv()
            self.add(level - 1)
        if level < len(self.bits):
            out = self.copies(level)
            for c in out:
                c.start()
            self.sent.append(out)
        self.done += 1

    def leave(self):
        for group in self.sent:
            for c in group:
                c.wait_send()


def grad_scatter(m, grads, kept, held, summed, send_sem, recv_sem, load_sem):
    bits = bits_of(m)
    height = grads.shape[0] // (2 * PARTS)
    out = []
    for i in range(2 * PARTS):
        order = bits[:1] + (bits[1:] if i % 2 == 0 else bits[:0:-1])
        rows = pl.ds(i * height, height)
        out.append(
            Halving(
                grads, rows, order, i * (m - 1), kept, held, summed, send_sem, recv_sem, load_sem.at[i]
            )
        )
    return out, [out[0].flip(out[0].d, bit) for bit in bits]


def scatter_scratch(m, rows, shard):
    wide = 2 * PARTS * (m - 1)
    counts = [m // 2] + [m >> (1 + k) for k in range(len(bits_of(m)))]
    return [pltpu.VMEM((count, rows, shard), BF) for count in counts] + [
        pltpu.VMEM((rows, shard), F32),
        pltpu.SemaphoreType.DMA((wide,)),
        pltpu.SemaphoreType.DMA((wide,)),
        pltpu.SemaphoreType.DMA((2 * PARTS, m // 2)),
    ]


def exchange(groups, mine, total, send_sem, recv_sem):
    source, base = mine, 0
    for axis, size, held in groups:
        me = lax.axis_index(axis)
        held[me] = source[...]

        def copy(k, slot):
            return pltpu.make_async_remote_copy(
                src_ref=source,
                dst_ref=held.at[slot],
                send_sem=send_sem.at[base + k],
                recv_sem=recv_sem.at[base + k],
                device_id={axis: lax.rem(me + k, size)},
                device_id_type=MESH,
            )

        sent = [copy(k, me) for k in range(1, size)]
        for c in sent:
            c.start()
        for k in range(1, size):
            copy(k, lax.rem(me - k + size, size)).wait_recv()
        value = held[0]
        for k in range(1, size):
            value = value + held[k]
        for c in sent:
            c.wait_send()
        total[...] = value
        source, base = total, base + size


def last_kernel(
    n, m, d_qk, d_value, d_gate, weight, grads, inputs, gain, d_middle, second_gain,
    out, gains, grad_query, grad_key, grad_out, grad_gate, grad_value,
    qk_v, value_v, gate_v, weight_v, inputs_v, middle_v, part, lefts, rights, *rest
):
    bits = bits_of(m)
    kept, held = rest[0], rest[1 : 1 + len(bits)]
    summed, wide_send, wide_recv, load_sem = rest[1 + len(bits) : 5 + len(bits)]
    gain_sum, mine, first, second = rest[5 + len(bits) : 9 + len(bits)]
    copy_sem, send_sem, recv_sem, gain_send, gain_recv = rest[9 + len(bits) :]
    line = Line(n, send_sem, recv_sem)
    count, width = out.shape
    piece = count // CHUNKS
    per = n * piece
    heads, _, size = value_v.shape
    wide = qk_v.shape[1]
    load = [
        pltpu.make_async_copy(src, dst, copy_sem.at[i])
        for i, (src, dst) in enumerate(
            [
                (weight.at[pl.ds(0, weight_v.shape[0])], weight_v), (d_qk, qk_v),
                (d_value, value_v), (d_gate, gate_v), (inputs, inputs_v), (d_middle, middle_v),
            ]
        )
    ]
    for item in load:
        item.start()
    barrier = pltpu.get_barrier_semaphore()
    for axis, extent in (("dp", m), ("mp", n)):
        me = lax.axis_index(axis)
        for k in range(1, extent):
            peer = lax.rem(me + k, extent)
            pl.semaphore_signal(barrier, inc=1, device_id={axis: peer}, device_id_type=MESH)
    pl.semaphore_wait(barrier, n + m - 2)

    halving, _ = grad_scatter(m, grads, kept, held, summed, wide_send, wide_recv, load_sem)
    for item in halving:
        item.step()
    for item in halving:
        item.load()
    for h in range(CHUNKS):
        no_neighbour_zero(n, line.place, lefts.at[h, n - 2], rights.at[h, n - 2])
    gain_sum[...] = jnp.zeros_like(gain_sum)
    scatters = [
        Scatter(
            line,
            lambda k, h=h: part.at[pl.ds(h * per + k * piece, piece)],
            lambda s, h=h: lefts.at[h, s - 1],
            lambda s, h=h: rights.at[h, s - 1],
            add_into,
        )
        for h in range(CHUNKS)
    ]

    def product(h):
        rows = pl.ds(h * per, per)

        def step(j, carry):
            at = pl.ds(pl.multiple_of(j * 2 * LANES, 2 * LANES), 2 * LANES)
            total = dot_nn(qk_v[rows, :], weight_v[pl.ds(0, wide), at])
            for i in range(heads):
                base = wide + i * size
                total += dot_nn(value_v[i, rows, :], weight_v[pl.ds(base, size), at])
                base += heads * size
                total += dot_nn(gate_v[i, rows, :], weight_v[pl.ds(base, size), at])
            part[rows, at] = total.astype(BF)
            return carry

        lax.fori_loop(0, width // (2 * LANES), step, 0)

    def finish(h):
        scatters[h].finish()

        def step(at):
            own = at(h * piece)
            grad = (
                part[at(h * per), :].astype(F32)
                + lefts[h, n - 2, at(), :].astype(F32)
                + rights[h, n - 2, at(), :].astype(F32)
            )
            hat, scale = layer_norm(inputs_v[own, :].astype(F32), epsilon)
            gain_sum[...] += jnp.sum((hat * grad).reshape(BLOCK // 8, 8, width), axis=0)
            out[own, :] = middle_v[own, :] + norm_back(grad * gain[...], hat, scale)

        blocks(piece, step)

    for item in load:
        item.wait()
    for h in range(CHUNKS):
        product(h)
        scatters[h].step()
    for s in range(n - 2):
        for h in range(CHUNKS):
            if s < len(bits) and h < len(halving):
                halving[h].step()
            scatters[h].step()
    while halving[0].done < len(bits):
        for item in halving:
            item.step()
    for h in range(CHUNKS):
        finish(h)
    groups = [("dp", m, first), ("mp", n, second)]
    for i, source in enumerate((gain_sum, second_gain)):
        flat = jnp.sum(source[...], axis=0, keepdims=True)
        for j in range(width // LANES):
            mine[pl.ds(i * (width // LANES) + j, 1), :] = flat[:, j * LANES : (j + 1) * LANES]
    for item in halving:
        while item.done <= len(bits):
            item.step()
    stores, base = [], 0
    for target in (grad_out, grad_gate):
        source = summed.at[pl.ds(base, target.shape[0])]
        stores.append(pltpu.make_async_copy(source, target, copy_sem.at[len(load) + len(stores)]))
        base += target.shape[0]
    deep = grad_query.shape[1]
    value_base = base + 2 * deep
    source = summed.at[pl.ds(value_base, grad_value.shape[0])]
    stores.append(pltpu.make_async_copy(source, grad_value, copy_sem.at[len(load) + len(stores)]))
    for store in stores:
        store.start()
    for target in (grad_query, grad_key):
        for j in range(deep // LANES):
            target[:, j * LANES : (j + 1) * LANES] = summed[pl.ds(base, LANES), :].T
            base += LANES
    exchange(groups, mine, gains, gain_send, gain_recv)
    for item in halving:
        item.leave()
    for store in stores:
        store.wait()
    for h in range(CHUNKS):
        scatters[h].drain()


def last_call(d_qk, d_value, d_gate, weight, grads, inputs, gain, d_middle, second_gain, n, m):
    tokens = d_qk.shape[0]
    rows, width = inputs.shape
    heads = d_value.shape[0]
    shard = width // m
    sems = CHUNKS * 2 * (n - 1)
    hop = (CHUNKS, n - 1, rows // CHUNKS, width)
    flat = (2 * width // LANES, LANES)
    shape = jax.ShapeDtypeStruct
    return pl.pallas_call(
        functools.partial(last_kernel, n, m),
        out_shape=(
            shape((rows, width), F32),
            shape(flat, F32),
            shape((shard, heads * HK), F32),
            shape((shard, heads * HK), F32),
        )
        + (shape((heads * HV, shard), F32),) * 3,
        in_specs=[ANY] * 6 + [VM, ANY, VM],
        out_specs=(VM,) * 4 + (ANY,) * 3,
        scratch_shapes=[
            pltpu.VMEM(d_qk.shape, BF),
            pltpu.VMEM(d_value.shape, BF),
            pltpu.VMEM(d_gate.shape, BF),
            pltpu.VMEM((2 * heads * (HK + HV), width), BF),
            pltpu.VMEM((rows, width), BF),
            pltpu.VMEM((rows, width), F32),
            pltpu.VMEM((tokens, width), BF),
            pltpu.VMEM(hop, BF),
            pltpu.VMEM(hop, BF),
        ]
        + scatter_scratch(m, grads.shape[0], shard)
        + [
            pltpu.VMEM((8, width), F32),
            pltpu.VMEM(flat, F32),
            pltpu.VMEM((m,) + flat, F32),
            pltpu.VMEM((n,) + flat, F32),
            pltpu.SemaphoreType.DMA((9,)),
            pltpu.SemaphoreType.DMA((sems,)),
            pltpu.SemaphoreType.DMA((sems,)),
            pltpu.SemaphoreType.DMA((n + m,)),
            pltpu.SemaphoreType.DMA((n + m,)),
        ],
        compiler_params=pltpu.CompilerParams(
            collective_id=2, has_side_effects=True, vmem_limit_bytes=VMEM_MOST
        ),
        name="last",
    )(d_qk, d_value, d_gate, weight, grads, inputs, gain, d_middle, second_gain)


TILE = 256


def tiles_of(count, step):
    def run(i, carry):
        step(pl.ds(pl.multiple_of(i * TILE, TILE), TILE))
        return carry

    lax.fori_loop(0, count // TILE, run, 0)


def in_order(units, steps):
    taken = 0
    for i, unit in enumerate(units):
        unit()
        upto = (i + 1) * len(steps) // len(units)
        for step in steps[taken:upto]:
            step()
        taken = upto


def forward_kernel(
    n, m, rows, weight, cot, col, row, pack,
    query_o, key_o, value_o, gate_o, norm_o, scale_o, scores_o, gated_o, cot_o, second_o,
    rows_v, weight_v, query_v, key_v, value_v, gate_v, norm_v, scale_v, scores_v, gated_v, cot_v,
    copy_sem, send_sem, recv_sem, wide_send, wide_recv,
):
    line = Line(n, send_sem, recv_sem)
    heads, tokens, deep = query_v.shape
    size = value_v.shape[2]
    per = cot_v.shape[0] // FRONT
    piece = per // n
    copies = []

    def local(src, dst):
        c = pltpu.make_async_copy(src, dst, copy_sem.at[len(copies)])
        copies.append(c)
        c.start()
        return c

    load_cot = [
        local(cot.at[pl.ds(h * piece, piece)], cot_v.at[pl.ds(h * per, piece)])
        for h in range(FRONT)
    ]
    load_rows = local(rows, rows_v)
    load_weight = local(weight.at[pl.ds(0, weight_v.shape[0])], weight_v)
    doubling, peers = weight_gather(m, pack, second_o, wide_send, wide_recv)
    line.enter(["dp", peers])
    gathers = [
        Gather(line, lambda k, h=h: cot_v.at[pl.ds(h * per + k * piece, piece)])
        for h in range(FRONT)
    ]
    for item in load_cot:
        item.wait()
    for g in gathers + doubling:
        g.step()
    local(pack, own_columns(pack, second_o))
    load_rows.wait()
    load_weight.wait()

    def project(target, h, base, width):
        def step(at):
            target[h, at, :] = dot_nt(rows_v[at, :], weight_v[pl.ds(base, width), :]).astype(
                target.dtype
            )

        return lambda: tiles_of(tokens, step)

    def attend(h):
        def step(at):
            allowed = (col[at, 0:1] >= row[0:1, :]) & (col[at, 1:2] == row[1:2, :])
            scores = dot_nt(query_v[h, at, :], key_v[h]) * col[at, 2 + h : 3 + h]
            scores = jnp.where(allowed, scores * row[2 + h : 3 + h, :], 0.0).astype(BF)
            scores_v[h, at, :] = scores
            hat, scale = layer_norm(dot_nn(scores, value_v[h]), group_epsilon)
            norm_v[h, at, :] = hat
            scale_v[h, at, :] = scale
            gate = gate_v[h, at, :]
            gated_v[h, at, :] = (gate * jax.nn.sigmoid(gate) * hat).astype(BF)

        return lambda: tiles_of(tokens, step)

    values, gates = 2 * heads * deep, 2 * heads * deep + heads * size
    units = []
    for h in range(heads):
        units += [
            project(query_v, h, h * deep, deep),
            project(key_v, h, (heads + h) * deep, deep),
            project(value_v, h, values + h * size, size),
            project(gate_v, h, gates + h * size, size),
            attend(h),
        ]
    steps = [g.step for _ in range(n - 1) for g in gathers]
    wide_steps = [g.step for _ in range(len(bits_of(m))) for g in doubling]
    mixed = []
    for i in range(max(len(steps), len(wide_steps))):
        mixed += steps[i : i + 1] + wide_steps[i : i + 1]
    late = mixed[-2 * PARTS :]
    in_order(units, mixed[: -2 * PARTS])
    count = len(copies) - 1
    for src, dst in (
        (query_v, query_o), (key_v, key_o), (value_v, value_o), (gate_v, gate_o),
        (norm_v, norm_o), (scale_v, scale_o), (scores_v, scores_o), (gated_v, gated_o),
        (cot_v, cot_o),
    ):
        local(src, dst)
    for step in late:
        step()
    for item in copies[count:]:
        item.wait()
    for item in doubling:
        assert item.done == len(bits_of(m)) + 1
        item.leave()
    line.leave()


def forward_call(rows, weight, cot, col, row, pack, n, m, heads):
    tokens, width = rows.shape
    shape = jax.ShapeDtypeStruct
    outs = (
        shape((heads, tokens, HK), BF),
        shape((heads, tokens, HK), BF),
        shape((heads, tokens, HV), BF),
        shape((heads, tokens, HV), F32),
        shape((heads, tokens, HV), F32),
        shape((heads, tokens, 1), F32),
        shape((heads, tokens, tokens), BF),
        shape((heads, tokens, HV), BF),
        shape((tokens * FRONT // CHUNKS, width), BF),
        shape((pack.shape[0], m * pack.shape[1]), BF),
    )
    attention_rows = 2 * heads * (HK + HV)
    wide = 2 * PARTS * (m - 1)
    sems = FRONT * 2 * (n - 1)
    return pl.pallas_call(
        functools.partial(forward_kernel, n, m),
        out_shape=outs,
        in_specs=[ANY] * 3 + [VM] * 3,
        out_specs=(ANY,) * len(outs),
        scratch_shapes=[pltpu.VMEM(rows.shape, BF), pltpu.VMEM((attention_rows, width), BF)]
        + [pltpu.VMEM(o.shape, o.dtype) for o in outs[:-1]]
        + [
            pltpu.SemaphoreType.DMA((FRONT + 2 + len(outs),)),
            pltpu.SemaphoreType.DMA((sems,)),
            pltpu.SemaphoreType.DMA((sems,)),
            pltpu.SemaphoreType.DMA((wide,)),
            pltpu.SemaphoreType.DMA((wide,)),
        ],
        compiler_params=pltpu.CompilerParams(
            collective_id=4, has_side_effects=True, vmem_limit_bytes=VMEM_MOST
        ),
        name="forward",
    )(rows, weight, cot, col, row, pack)


def backward_kernel(
    n, m, mid, weights, gate, norm, scale, scores, query, key, value, down, middle, grads, col, row,
    qk_o, value_o, gate_o, glu_gate_o, glu_up_o, down_o, outputs,
    mid_v, wo_v, gate_v, norm_v, scale_v, scores_v, query_v, key_v, value_v, part, middle_v,
    d_qk, d_value, d_gate, d_kept, d_scores, lefts, rights, *rest
):
    bits = bits_of(m)
    kept, held = rest[0], rest[1 : 1 + len(bits)]
    summed, wide_send, wide_recv, load_sem = rest[1 + len(bits) : 5 + len(bits)]
    copy_sem, send_sem, recv_sem = rest[5 + len(bits) :]
    line = Line(n, send_sem, recv_sem)
    heads, tokens, deep = query_v.shape
    size = value_v.shape[2]
    back = CHUNKS - DOWNS
    per = part.shape[0] // back
    piece = per // n
    copies = []

    def local(src, dst):
        c = pltpu.make_async_copy(src, dst, copy_sem.at[len(copies)])
        copies.append(c)
        c.start()
        return c

    load_part = local(down, part)
    loads = [
        local(src, dst)
        for src, dst in (
            (mid, mid_v), (weights.at[pl.ds(weights.shape[0] - wo_v.shape[0], wo_v.shape[0])], wo_v),
            (gate, gate_v), (norm, norm_v), (scale, scale_v), (value, value_v), (key, key_v),
            (query, query_v), (scores, scores_v), (middle, middle_v),
        )
    ]
    halving, peers = grad_scatter(m, grads, kept, held, summed, wide_send, wide_recv, load_sem)
    line.enter(["dp", peers])
    for item in halving:
        item.step()
    for item in halving:
        item.load()
    for h in range(back):
        no_neighbour_zero(n, line.place, lefts.at[h, n - 2], rights.at[h, n - 2])
    scatters = [
        Scatter(
            line,
            lambda k, h=h: part.at[pl.ds(h * per + k * piece, piece)],
            lambda s, h=h: lefts.at[h, s - 1],
            lambda s, h=h: rights.at[h, s - 1],
            add_into,
        )
        for h in range(back)
    ]
    load_part.wait()
    for item in scatters:
        item.step()
    for item in loads:
        item.wait()

    def gates(h):
        def step(at):
            grad = dot_nt(mid_v[at, :], wo_v[pl.ds(h * size, size), :])
            pre, hat = gate_v[h, at, :], norm_v[h, at, :]
            s = jax.nn.sigmoid(pre)
            d_gate[h, at, :] = (grad * hat * (s + pre * s * (1.0 - s))).astype(BF)
            d_kept[h, at, :] = norm_back(grad * (pre * s), hat, scale_v[h, at, :]).astype(BF)

        return lambda: tiles_of(tokens, step)

    def by_row(h):
        def step(at):
            allowed = (col[at, 0:1] >= row[0:1, :]) & (col[at, 1:2] == row[1:2, :])
            grad = dot_nt(d_kept[h, at, :], value_v[h]) * col[at, 2 + h : 3 + h]
            grad = jnp.where(allowed, grad * row[2 + h : 3 + h, :], 0.0).astype(BF)
            d_scores[at, :] = grad
            d_qk[at, pl.ds(h * deep, deep)] = dot_nn(grad, key_v[h]).astype(BF)

        return lambda: tiles_of(tokens, step)

    def by_column(h):
        def step(at):
            d_value[h, at, :] = dot_tn(scores_v[h, :, at], d_kept[h]).astype(BF)
            d_qk[at, pl.ds((heads + h) * deep, deep)] = dot_tn(d_scores[:, at], query_v[h]).astype(
                BF
            )

        return lambda: tiles_of(tokens, step)

    units = []
    for h in range(heads):
        units += [gates(h), by_row(h), by_column(h)]
    steps = [item.step for _ in range(n - 2) for item in scatters]
    wide_steps = [item.step for _ in bits for item in halving]
    mixed = []
    for i in range(max(len(steps), len(wide_steps))):
        mixed += steps[i : i + 1] + wide_steps[i : i + 1]
    late = mixed[-2 * PARTS :]
    in_order(units, mixed[: -2 * PARTS])
    count = len(copies)
    local(d_qk, qk_o)
    local(d_value, value_o)
    local(d_gate, gate_o)
    for step in late:
        step()
    size = down_o.shape[0]
    wide = grads.shape[0] // 3
    for t in range(wide // LANES):
        have = min(LANES, size - t * LANES)
        for i, target in enumerate((glu_gate_o, glu_up_o)):
            local(
                summed.at[pl.ds((2 * t + i) * LANES, have)], target.at[pl.ds(t * LANES, have)]
            )
    local(summed.at[pl.ds(2 * wide, size)], down_o)
    for item in halving:
        assert item.done == len(bits) + 1
        item.leave()
    for h in range(back):
        scatters[h].finish()

        def step(at):
            outputs[at(h * piece), :] = (
                middle_v[at(h * piece), :]
                + part[at(h * per), :].astype(F32)
                + lefts[h, n - 2, at(), :].astype(F32)
                + rights[h, n - 2, at(), :].astype(F32)
            ).astype(BF)

        blocks(piece, step)
    for item in copies[count:]:
        item.wait()
    for item in scatters:
        item.drain()


def backward_call(mid, weights, gate, norm, scale, scores, query, key, value, down, middle, grads, size_two, col, row, n, m):
    tokens, width = mid.shape
    heads, _, size = value.shape
    back = CHUNKS - DOWNS
    nv = heads * size
    shard = width // m
    shape = jax.ShapeDtypeStruct
    outs = (
        shape((tokens, 2 * heads * HK), BF),
        shape(value.shape, BF),
        shape(value.shape, BF),
    ) + (shape((size_two, shard), F32),) * 3 + (shape(middle.shape, BF),)
    ins = (gate, norm, scale, scores, query, key, value, down, middle)
    hop = (back, n - 1, middle.shape[0] // back, width)
    sems = back * 2 * (n - 1)
    return pl.pallas_call(
        functools.partial(backward_kernel, n, m),
        out_shape=outs,
        in_specs=[ANY] * 12 + [VM] * 2,
        out_specs=(ANY,) * 6 + (VM,),
        scratch_shapes=[pltpu.VMEM(mid.shape, BF), pltpu.VMEM((nv, width), BF)]
        + [pltpu.VMEM(a.shape, a.dtype) for a in ins]
        + [pltpu.VMEM(o.shape, o.dtype) for o in outs[:3]]
        + [
            pltpu.VMEM(value.shape, BF),
            pltpu.VMEM((tokens, tokens), BF),
            pltpu.VMEM(hop, BF),
            pltpu.VMEM(hop, BF),
        ]
        + scatter_scratch(m, grads.shape[0], shard)
        + [
            pltpu.SemaphoreType.DMA((15 + 2 * (grads.shape[0] // (3 * LANES)),)),
            pltpu.SemaphoreType.DMA((sems,)),
            pltpu.SemaphoreType.DMA((sems,)),
        ],
        compiler_params=pltpu.CompilerParams(
            collective_id=5, has_side_effects=True, vmem_limit_bytes=VMEM_MOST
        ),
        name="backward",
    )(mid, weights, *ins, grads, col, row)


def products_kernel(plan, arrays, *refs):
    ins, out = refs[:arrays], refs[arrays]
    held, result, copy_sem = refs[arrays + 1 : 2 * arrays + 1], refs[-2], refs[-1]
    loads = [pltpu.make_async_copy(a, b, copy_sem.at[i]) for i, (a, b) in enumerate(zip(ins, held))]
    for item in loads:
        item.start()
    waited, stores, base = set(), [], 0
    for left, head, start, size, right in plan:
        for i in (left, right):
            if i not in waited:
                loads[i].wait()
                waited.add(i)
        target = pl.ds(base, size)

        def step(j, carry):
            at = pl.ds(pl.multiple_of(j * 4 * LANES, 4 * LANES), 4 * LANES)
            source = held[left][head] if head is not None else held[left][:, pl.ds(start, size)]
            result[target, at] = dot_tn(source, held[right][:, at]).astype(BF)
            return carry

        lax.fori_loop(0, result.shape[1] // (4 * LANES), step, 0)
        store = pltpu.make_async_copy(
            result.at[target], out.at[target], copy_sem.at[arrays + len(stores)]
        )
        store.start()
        stores.append(store)
        base += size
    spare = result.shape[0] - base
    if spare:
        target = pl.ds(base, spare)
        result[target, :] = jnp.zeros((spare, result.shape[1]), BF)
        store = pltpu.make_async_copy(
            result.at[target], out.at[target], copy_sem.at[arrays + len(stores)]
        )
        store.start()
        stores.append(store)
    for item in stores:
        item.wait()


def weight_products(plan, arrays, name, rows):
    width = arrays[plan[0][4]].shape[1]
    return pl.pallas_call(
        functools.partial(products_kernel, plan, len(arrays)),
        out_shape=jax.ShapeDtypeStruct((rows, width), BF),
        in_specs=[ANY] * len(arrays),
        out_specs=ANY,
        scratch_shapes=[pltpu.VMEM(a.shape, a.dtype) for a in arrays]
        + [pltpu.VMEM((rows, width), BF), pltpu.SemaphoreType.DMA((len(arrays) + len(plan) + 1,))],
        compiler_params=pltpu.CompilerParams(vmem_limit_bytes=VMEM_MOST),
        name=name,
    )(*arrays)


def pad_rows(array, count):
    return jnp.pad(array, ((0, count - array.shape[0]), (0, 0)))


def pad_columns(array, count):
    return jnp.pad(array, ((0, 0), (0, count - array.shape[1])))


def body(
    inputs,
    segments,
    first_norm_gain,
    w_query,
    w_key,
    w_value,
    w_gate,
    w_out,
    second_norm_gain,
    w_glu_gate,
    w_glu_up,
    w_down,
    cotangent,
):
    n = lax.axis_size("mp")
    place = lax.axis_index("mp")
    heads = H // n
    head_start = place * heads
    rows, width = inputs.shape
    shard = w_query.shape[0]
    piece = rows // CHUNKS
    nk, nv, nf = heads * HK, heads * HV, w_down.shape[0]
    f_wide = -(-nf // LANES) * LANES
    f_tiles = f_wide // LANES
    grain = 2 * PARTS * BLOCK
    one_rows = -(-(2 * nk + 3 * nv) // grain) * grain
    gap = one_rows - 2 * nk - 3 * nv
    m = lax.axis_size("dp")

    pack_one = jnp.concatenate(
        [w_query.T, w_key.T, w_value.T, w_gate.T, jnp.zeros((gap, shard), BF), w_out], axis=0
    )
    glu_pack = jnp.stack(
        [
            pad_rows(w_glu_gate.T, f_wide).reshape(f_tiles, LANES, shard),
            pad_rows(w_glu_up.T, f_wide).reshape(f_tiles, LANES, shard),
        ],
        axis=1,
    ).reshape(2 * f_wide, shard)
    pack_two = jnp.concatenate([glu_pack, pad_rows(w_down, f_wide)], axis=0)

    first_hat, _ = layer_norm(inputs.astype(F32), epsilon)
    rows_one, weight_one = gather_rows((first_hat * first_norm_gain).astype(BF), pack_one, n, m)
    tokens = rows_one.shape[0]

    slot_shard = lax.rem(place - jnp.arange(n) + n, n)
    places = (
        slot_shard[None, :, None] * rows
        + jnp.arange(CHUNKS)[:, None, None] * piece
        + jnp.arange(piece)[None, None, :]
    ).reshape(tokens)
    seg = segments.reshape(n, CHUNKS, piece)[::-1]
    seg = lax.dynamic_slice_in_dim(jnp.concatenate([seg, seg], axis=0), n - 1 - place, n, axis=0)
    seg = seg.transpose(1, 0, 2).reshape(tokens)

    log_gamma = jnp.log1p(-jnp.exp2(-5.0 - (head_start + jnp.arange(heads)).astype(F32)))
    spot = places.astype(F32)
    powers = spot[None] * log_gamma[:, None]
    marks = jnp.stack([spot, seg.astype(F32)])
    col = jnp.concatenate([marks, jnp.exp(powers)], axis=0).T
    row = jnp.concatenate([marks, jnp.exp(-powers) * HK ** (-0.5)], axis=0)

    (
        query, key, value, gate_pre, normalized, scale_group, scores, gated, cot_front, weight_two,
    ) = forward_call(rows_one, weight_one, cotangent, col, row, pack_two, n, m, heads)
    mid_rows, grads_two, down, outputs_front, middle, middle_grad, second_gain = middle_call(
        gated, weight_two, weight_one, inputs, cotangent, cot_front, second_norm_gain[None], n
    )
    d_qk, d_value, d_gate, grad_glu_gate, grad_glu_up, grad_down, outputs_back = backward_call(
        mid_rows, weight_one, gate_pre, normalized, scale_group, scores, query, key, value,
        down, middle, grads_two, nf, col, row, n, m,
    )
    plan = [(0, h, 0, HV, 1) for h in range(heads)] + [(2, h, 0, HV, 3) for h in range(heads)]
    plan += [(4, None, t * nk, nk, 3) for t in range(2)]
    plan += [(5, h, 0, HV, 3) for h in range(heads)]
    grads_one = weight_products(
        plan, (gated, mid_rows, d_gate, rows_one, d_qk, d_value), "products_one", one_rows
    )
    input_gradient, gains, grad_query, grad_key, grad_out, grad_gate, grad_value = last_call(
        d_qk, d_value, d_gate, weight_one, grads_one, inputs, first_norm_gain[None], middle_grad,
        second_gain, n, m,
    )
    gains = gains.reshape(2, width)
    return (
        jnp.concatenate([outputs_front, outputs_back], axis=0),
        input_gradient,
        gains[0],
        grad_query,
        grad_key,
        grad_value.T,
        grad_gate.T,
        grad_out,
        gains[1],
        grad_glu_gate.T,
        grad_glu_up.T,
        grad_down,
    )


def solution(mesh):
    split = P(("dp", "mp"), None)
    wide, tall = P("dp", "mp"), P("mp", "dp")
    return jax.shard_map(
        body,
        mesh=mesh,
        in_specs=(
            split, P("dp", None), P(), wide, wide, wide, wide, tall, P(), wide, wide, tall, split,
        ),
        out_specs=(
            split, split, P(), wide, wide, wide, wide, tall, P(), wide, wide, tall,
        ),
        check_vma=False,
    )
```

```python
import functools

import jax
import jax.numpy as jnp
from jax import lax
from jax.experimental import pallas as pl
from jax.experimental.pallas import tpu as pltpu
from jax.sharding import PartitionSpec as P

H = 8
HK = 256
HV = 432
LEN = 1024
CHUNKS = 4
FRONT = CHUNKS // 2
DOWNS = CHUNKS // 4
ENDS = CHUNKS // 4
LANES = 128
VMEM_MOST = 66_000_000

epsilon = 1e-05
group_epsilon = 1.0
BF = jnp.bfloat16
F32 = jnp.float32


def layer_norm(values_in, offset):
    centre = jnp.mean(values_in, axis=-1, keepdims=True)
    centred = values_in - centre
    variance = jnp.mean(centred * centred, axis=-1, keepdims=True)
    scaling = lax.rsqrt(variance + offset)
    return (centred * scaling, scaling)


def norm_back(grad_hat, normed_hat, scaling):
    first_mean = jnp.mean(grad_hat, axis=-1, keepdims=True)
    second_mean = jnp.mean(grad_hat * normed_hat, axis=-1, keepdims=True)
    return scaling * (grad_hat - first_mean - normed_hat * second_mean)


def glu_act(gate_pre, up_pre):
    return jax.nn.gelu(gate_pre, approximate=True) * up_pre


def dot_nt(a, b):
    return lax.dot_general(a, b, (((1,), (1,)), ((), ())), preferred_element_type=F32)


def dot_nn(a, b):
    return lax.dot_general(a, b, (((1,), (0,)), ((), ())), preferred_element_type=F32)


def dot_tn(a, b):
    return lax.dot_general(a, b, (((0,), (0,)), ((), ())), preferred_element_type=F32)


MESH = pl.DeviceIdType.MESH


class Line:
    def __init__(self, n, send_sem, recv_sem):
        self.n, self.send_sem, self.recv_sem = n, send_sem, recv_sem
        self.place = lax.axis_index("mp")
        self.used = 0
        self.sent = []

    def enter(self, others=None):
        barrier = pltpu.get_barrier_semaphore()
        n, place = self.n, self.place

        @pl.when(place >= 1)
        def _():
            pl.semaphore_signal(barrier, inc=1, device_id={"mp": place - 1}, device_id_type=MESH)

        @pl.when(place <= n - 2)
        def _():
            pl.semaphore_signal(barrier, inc=1, device_id={"mp": place + 1}, device_id_type=MESH)

        peers = jnp.minimum(place, 1) + jnp.minimum(n - 1 - place, 1)
        if others is not None:
            axis, indices = others
            for index in indices:
                pl.semaphore_signal(barrier, inc=1, device_id={axis: index}, device_id_type=MESH)
            peers = peers + len(indices)
        pl.semaphore_wait(barrier, peers)

    def copy(self, src, dst, index, toward):
        return pltpu.make_async_remote_copy(
            src_ref=src,
            dst_ref=dst,
            send_sem=self.send_sem.at[index],
            recv_sem=self.recv_sem.at[index],
            device_id={"mp": self.place + toward},
            device_id_type=MESH,
        )

    def leave(self):
        for condition, copy in self.sent:
            pl.when(condition)(copy.wait_send)


class Gather:
    def __init__(self, line, slot):
        self.line, self.slot, self.step_no = line, slot, 0
        self.base = line.used
        line.used += 2 * (line.n - 1)
        n = line.n
        self.right = [
            line.copy(slot(s - 1), slot(s), self.base + s - 1, 1) for s in range(1, n)
        ]
        self.left = [
            line.copy(slot((n - s + 1) % n), slot(n - s), self.base + n - 2 + s, -1)
            for s in range(1, n)
        ]

    def arrive(self, s):
        n, place = self.line.n, self.line.place
        pl.when(place >= s)(self.right[s - 1].wait_recv)
        pl.when(place <= n - 1 - s)(self.left[s - 1].wait_recv)

    def step(self):
        self.step_no += 1
        s, n, place = self.step_no, self.line.n, self.line.place
        if s > 1:
            self.arrive(s - 1)
        if s < n:
            to_right = (place >= s - 1) & (place <= n - 2)
            to_left = (place <= n - s) & (place >= 1)
            pl.when(to_right)(self.right[s - 1].start)
            pl.when(to_left)(self.left[s - 1].start)
            self.line.sent += [(to_right, self.right[s - 1]), (to_left, self.left[s - 1])]


class Scatter:
    def __init__(self, line, slot, from_left, from_right, add):
        self.line, self.slot, self.add, self.step_no = line, slot, add, 0
        self.from_left, self.from_right = from_left, from_right
        self.base = line.used
        line.used += 2 * (line.n - 1)
        n = line.n
        self.right = [
            line.copy(slot(s), from_left(s), self.base + s - 1, 1) for s in range(1, n)
        ]
        self.left = [
            line.copy(slot(n - s), from_right(s), self.base + n - 2 + s, -1) for s in range(1, n)
        ]
        self.mine = []

    def step(self):
        self.step_no += 1
        s, n, place = self.step_no, self.line.n, self.line.place
        to_right, to_left = place <= s - 1, place >= n - s
        if s > 1:

            @pl.when(to_right & (place >= 1))
            def _():
                self.right[s - 2].wait_recv()
                self.add(self.slot(s), self.from_left(s - 1))

            @pl.when(to_left & (place <= n - 2))
            def _():
                self.left[s - 2].wait_recv()
                self.add(self.slot(n - s), self.from_right(s - 1))

        pl.when(to_right)(self.right[s - 1].start)
        pl.when(to_left)(self.left[s - 1].start)
        self.mine += [(to_right, self.right[s - 1]), (to_left, self.left[s - 1])]

    def finish(self):
        n, place = self.line.n, self.line.place

        @pl.when(place >= 1)
        def _():
            self.right[n - 2].wait_recv()

        @pl.when(place <= n - 2)
        def _():
            self.left[n - 2].wait_recv()

    def drain(self):
        for condition, copy in self.mine:
            pl.when(condition)(copy.wait_send)


ANY = pl.BlockSpec(memory_space=pl.ANY)
VM = pl.BlockSpec(memory_space=pltpu.VMEM)
BLOCK = 16


def blocks(count, step):
    def run(i, carry):
        step(lambda base=0: pl.ds(pl.multiple_of(base + i * BLOCK, BLOCK), BLOCK))
        return carry

    lax.fori_loop(0, count // BLOCK, run, 0)


def add_into(target, extra):
    def step(at):
        target[at(), :] = (target[at(), :].astype(F32) + extra[at(), :].astype(F32)).astype(BF)

    blocks(target.shape[0], step)


def product_tiles(target, left, right, tile):
    def step(j, carry):
        at = pl.ds(pl.multiple_of(j * tile, tile), tile)
        target[:, at] = dot_nn(left[...], right[:, at]).astype(BF)
        return carry

    lax.fori_loop(0, right.shape[1] // tile, step, 0)


class Doubling:
    def __init__(self, m, own, out, rows, bits, base, send_sem, recv_sem):
        self.d = lax.axis_index("dp")
        self.own, self.out, self.rows, self.bits, self.base = own, out, rows, bits, base
        self.send_sem, self.recv_sem = send_sem, recv_sem
        self.shard = own.shape[1]
        self.done = 0
        self.sent = []

    def flip(self, d, bit):
        return d + bit * (1 - 2 * (lax.div(d, bit) % 2))

    def block(self, d):
        return self.out.at[self.rows, pl.ds(pl.multiple_of(d * self.shard, self.shard), self.shard)]

    def copies(self, level, landing):
        owners = [self.d]
        for bit in self.bits[:level]:
            owners += [self.flip(d, bit) for d in owners]
        bit = self.bits[level]
        partner = self.flip(self.d, bit)
        out = []
        for i, d in enumerate(owners):
            d = self.flip(d, bit) if landing else d
            src = self.own.at[self.rows] if i == 0 and not landing else self.block(d)
            index = self.base + (1 << level) - 1 + i
            out.append(
                pltpu.make_async_remote_copy(
                    src_ref=src,
                    dst_ref=self.block(d),
                    send_sem=self.send_sem.at[index],
                    recv_sem=self.recv_sem.at[index],
                    device_id={"dp": partner},
                    device_id_type=MESH,
                )
            )
        return out

    def step(self):
        level = self.done
        if level > 0:
            for c in self.copies(level - 1, True):
                c.wait_recv()
        if level < len(self.bits):
            out = self.copies(level, False)
            for c in out:
                c.start()
            self.sent += out
        self.done += 1

    def leave(self):
        for c in self.sent:
            c.wait_send()


def bits_of(m):
    bits = [1 << b for b in range(m.bit_length() - 1)]
    assert 1 << len(bits) == m
    return bits


PARTS = 2


def weight_gather(m, pack, weight, send_sem, recv_sem):
    bits = bits_of(m)
    outer = bits[1:]
    height = pack.shape[0] // (2 * PARTS)
    doubling = []
    for i in range(2 * PARTS):
        order = (outer if i % 2 == 0 else outer[::-1]) + bits[:1]
        rows = pl.ds(i * height, height)
        doubling.append(Doubling(m, pack, weight, rows, order, i * (m - 1), send_sem, recv_sem))
    first = doubling[0]
    return doubling, [first.flip(first.d, bit) for bit in bits]


def own_columns(pack, weight):
    shard = pack.shape[1]
    at = pl.multiple_of(lax.axis_index("dp") * shard, shard)
    return weight.at[:, pl.ds(at, shard)]


def gather_kernel(n, m, own, pack, out, weight, send_sem, recv_sem, copy_sem, wide_send, wide_recv):
    line = Line(n, send_sem, recv_sem)
    piece = own.shape[0] // CHUNKS
    per = n * piece
    bits = bits_of(m)
    doubling, peers = weight_gather(m, pack, weight, wide_send, wide_recv)
    line.enter(["dp", peers])
    local, gathers = [], []
    keep = pltpu.make_async_copy(pack, own_columns(pack, weight), copy_sem.at[CHUNKS])
    for h in range(CHUNKS):
        mine = own.at[pl.ds(h * piece, piece)]
        local.append(
            pltpu.make_async_copy(mine, out.at[pl.ds(h * per, piece)], copy_sem.at[h])
        )

        def slot(k, h=h, mine=mine):
            return mine if k == 0 else out.at[pl.ds(h * per + k * piece, piece)]

        gathers.append(Gather(line, slot))
    local.append(keep)

    def line_step(items):
        for item in items:
            item.step()

    half = CHUNKS // 2
    line_step(gathers)
    line_step(doubling)
    for item in local:
        item.start()
    for level in range(1, max(n, len(bits) + 1)):
        for side in range(2):
            if level <= len(bits):
                line_step(doubling[side * PARTS : (side + 1) * PARTS])
            if level < n:
                line_step(gathers[side * half : (side + 1) * half])
    for item in local:
        item.wait()
    for item in gathers:
        assert item.step_no == n
    for item in doubling:
        assert item.done == len(bits) + 1
        item.leave()
    line.leave()


def gather_rows(own, pack, n, m):
    rows, width = own.shape
    count = CHUNKS * 2 * (n - 1)
    wide = 2 * PARTS * (m - 1)
    return pl.pallas_call(
        functools.partial(gather_kernel, n, m),
        out_shape=(
            jax.ShapeDtypeStruct((n * rows, width), own.dtype),
            jax.ShapeDtypeStruct((pack.shape[0], m * pack.shape[1]), pack.dtype),
        ),
        in_specs=[VM, VM],
        out_specs=(ANY, ANY),
        scratch_shapes=[
            pltpu.SemaphoreType.DMA((count,)),
            pltpu.SemaphoreType.DMA((count,)),
            pltpu.SemaphoreType.DMA((CHUNKS + 1,)),
            pltpu.SemaphoreType.DMA((wide,)),
            pltpu.SemaphoreType.DMA((wide,)),
        ],
        compiler_params=pltpu.CompilerParams(collective_id=0, has_side_effects=True),
        name="gather_rows",
    )(own, pack)


def no_neighbour_zero(n, place, from_left, from_right):
    @pl.when(place == 0)
    def _():
        from_left[...] = jnp.zeros_like(from_left)

    @pl.when(place == n - 1)
    def _():
        from_right[...] = jnp.zeros_like(from_right)


(COT, OUT, ONE, END_ONE, TWO, GLU, GRAD, GRAD_SUM, END_GRAD, MID, DOWN, DOWN_SUM, END_DOWN, PRODUCTS, WIDE) = range(15)

DUE = {
    OUT: (-2.23, 1.66, 0), ONE: (-1.99, 1.12, 1.03), END_ONE: (1.46, 1.37, 0), TWO: (0.73, 1.15, 0.94),
    COT: (0.35, 1.39, 1.02), GLU: (1.14, -1.37, 1.55), GRAD: (3.09, 2.02, 0),
    GRAD_SUM: (3.48, 1.71, 0.74), END_GRAD: (7.02, -2.12, 0), MID: (5.68, 0.86, 1.11),
    DOWN: (1.3, 0.36, 0), DOWN_SUM: (1.87, 1.35, 0.95), END_DOWN: (7.9, 2.17, 0),
    PRODUCTS: (7.5, 0, 0.4), WIDE: (-4, 0.05, 1.5),
}
TUNED = {
    (4, 4, 3): [
        58, 2, 4, 57, 59, 8, 56, 2, 5, 57, 8, 58, 8, 9, 3, 59, 7, 12, 56, 2,
        16, 9, 58, 6, 16, 9, 57, 10, 59, 56, 16, 13, 11, 17, 57, 3, 10, 16, 58, 17,
        11, 56, 59, 20, 10, 20, 17, 24, 11, 14, 28, 18, 3, 15, 28, 18, 19, 2, 17, 21,
        28, 21, 40, 44, 18, 19, 25, 32, 29, 36, 18, 22, 29, 19, 44, 22, 29, 26, 36, 30,
        44, 19, 3, 23, 33, 36, 37, 30, 23, 27, 37, 31, 30, 52, 37, 31, 34, 38, 42, 41,
        48, 31, 38, 52, 35, 39, 38, 39, 36, 37, 38, 52, 39, 43, 39,
    ],
}


def middle_order(n, levels):
    if (n, CHUNKS, levels) in TUNED:
        return [divmod(code, CHUNKS) for code in TUNED[n, CHUNKS, levels]]
    count = {k: 1 for k in DUE}
    count.update({COT: n, TWO: n, MID: n, ONE: n - 1, GRAD_SUM: n - 1, DOWN_SUM: n - 1, GLU: 2, PRODUCTS: 3, WIDE: levels + 1})
    needs = {
        ONE: [OUT], END_ONE: [ONE], TWO: [END_ONE], GLU: [TWO, COT], GRAD: [GLU], GRAD_SUM: [GRAD],
        END_GRAD: [GRAD_SUM], MID: [END_GRAD], DOWN: [GLU], DOWN_SUM: [DOWN], END_DOWN: [DOWN_SUM],
    }
    todo = sorted(
        (first + h * later + s * 3 / (n - 1) * each, k, h, s)
        for k, (first, later, each) in DUE.items()
        for h in range(CHUNKS)
        for s in range(count[k])
        if not (k == PRODUCTS and h > 0 or k == COT and h < FRONT or k in (DOWN_SUM, END_DOWN) and h >= DOWNS)
    )
    taken, order = {}, []
    while todo:
        for item in todo:
            _, k, h, s = item
            ready = taken.get((k, h), 0) == s and (
                k != PRODUCTS or all(taken.get((GLU, c), 0) == 2 for c in range(CHUNKS))
            )
            ready = ready and (
                k != GLU or all(taken.get((WIDE, c), 0) == levels + 1 for c in range(2 * PARTS))
            )
            ready = ready and all(
                taken.get((need, h), 0) == count[need] or (need == COT and h < FRONT)
                for need in needs.get(k, [])
            )
            if ready:
                break
        todo.remove(item)
        taken[k, h] = s + 1
        order.append((k, h))
    return order


def middle_kernel(
    n, m, gated, pack, out_weight, own, cot, cot_front, gain,
    mid_out, glu_out, product_out, down_out, outputs, middle_out, d_middle, gain_out,
    gated_v, wo_v, weights_v, own_v, cot_v, rows_v, hidden_v, glu_v, part, part_two,
    left_a, right_a, left_b, right_b, middle, stage, result, copy_sem, send_sem, recv_sem,
    wide_send, wide_recv,
):
    line = Line(n, send_sem, recv_sem)
    place = line.place
    count, width = own.shape
    piece = count // CHUNKS
    per = n * piece
    wide = hidden_v.shape[1]
    copies = []

    def local(src, dst):
        c = pltpu.make_async_copy(src, dst, copy_sem.at[len(copies)])
        copies.append(c)
        c.start()
        return c

    def rows_at(ref, h, k=0, size=piece):
        return ref.at[pl.ds(h * per + k * piece, size)]

    load_cot = [
        local(cot.at[pl.ds(h * piece, piece)], rows_at(cot_v, h)) for h in range(FRONT, CHUNKS)
    ]
    front = pl.ds(0, FRONT * per)
    load_cot.append(local(cot_front, cot_v.at[front]))
    load_gated = local(gated, gated_v)
    load_wo = local(
        out_weight.at[pl.ds(out_weight.shape[0] - wo_v.shape[0], wo_v.shape[0])], wo_v
    )
    load_own = local(own, own_v)
    load_pack = local(pack, own_columns(pack, weights_v))
    wg_v, wd_v = weights_v.at[pl.ds(0, 2 * wide)], weights_v.at[pl.ds(2 * wide, wide)]
    doubling, peers = weight_gather(m, pack, weights_v, wide_send, wide_recv)
    line.enter(["dp", peers])
    for h in range(CHUNKS):
        no_neighbour_zero(n, place, left_a.at[h, n - 2], right_a.at[h, n - 2])
    for h in range(DOWNS):
        no_neighbour_zero(n, place, left_b.at[h, n - 2], right_b.at[h, n - 2])
    gain_out[...] = jnp.zeros_like(gain_out)

    def scatter(buf, lefts, rights, h):
        return Scatter(
            line,
            lambda k: rows_at(buf, h, k),
            lambda s: lefts.at[h, s - 1],
            lambda s: rights.at[h, s - 1],
            add_into,
        )

    gather_cot = {
        h: Gather(line, functools.partial(rows_at, cot_v, h)) for h in range(FRONT, CHUNKS)
    }
    gather_two = [Gather(line, functools.partial(rows_at, rows_v, h)) for h in range(CHUNKS)]

    def mid_slot(h, k):
        return stage.at[h] if k == 0 else rows_at(mid_out, h, k)

    gather_mid = [Gather(line, functools.partial(mid_slot, h)) for h in range(CHUNKS)]
    scatter_one = [scatter(part, left_a, right_a, h) for h in range(CHUNKS)]
    scatter_two = [scatter(part_two, left_b, right_b, h) for h in range(DOWNS)]
    scatter_grad = [scatter(part, left_a, right_a, h) for h in range(CHUNKS)]

    def chunk(ref, h):
        return ref.at[pl.ds(h * per, per)]

    def out_product(h):
        heads, _, size = gated_v.shape
        target, whole = chunk(part, h), pl.ds(h * per, per)

        def step(j, carry):
            at = pl.ds(pl.multiple_of(j * 2 * LANES, 2 * LANES), 2 * LANES)
            target[:, at] = sum(
                dot_nn(gated_v[i, whole, :], wo_v[pl.ds(i * size, size), at]) for i in range(heads)
            ).astype(BF)
            return carry

        lax.fori_loop(0, width // (2 * LANES), step, 0)

    def finish_one(h):
        scatter_one[h].finish()

        def step(at):
            src = at(h * per)
            mine = at(h * piece)
            total = (
                own_v[mine, :].astype(F32)
                + part[src, :].astype(F32)
                + left_a[h, n - 2, at(), :].astype(F32)
                + right_a[h, n - 2, at(), :].astype(F32)
            )
            middle[mine, :] = total
            hat, _ = layer_norm(total, epsilon)
            rows_v[src, :] = (hat * gain[...]).astype(BF)

        blocks(piece, step)

    def glu_tiles(h, first, last):
        def step(j, carry):
            pair = pl.ds(pl.multiple_of(j * 2 * LANES, 2 * LANES), 2 * LANES)
            at = pl.ds(pl.multiple_of(j * LANES, LANES), LANES)
            whole = pl.ds(h * per, per)
            both = dot_nt(rows_v[whole, :], wg_v[pair, :])
            d_hidden = dot_nt(cot_v[whole, :], wd_v[at, :])
            u, up = both[:, :LANES], both[:, LANES:]
            c = 0.7978845608028654
            t = jnp.tanh(c * (u + 0.044715 * (u * u * u)))
            half = 0.5 * (1.0 + t)
            act = u * half
            slope = half + 0.5 * u * (1.0 - t * t) * (c * (1.0 + 3 * 0.044715 * (u * u)))
            hidden_v[whole, at] = (act * up).astype(BF)
            glu_v[whole, pair] = jnp.concatenate(
                [(d_hidden * up * slope).astype(BF), (d_hidden * act).astype(BF)], axis=1
            )
            return carry

        lax.fori_loop(first, last, step, 0)

    def grad_product(h):
        product_tiles(chunk(part, h), chunk(glu_v, h), wg_v, 2 * LANES)

    def down_product(h):
        product_tiles(chunk(part_two, h), chunk(hidden_v, h), wd_v, 2 * LANES)

    def finish_grad(h):
        scatter_grad[h].finish()

        def step(at):
            src = at(h * per)
            mine = at(h * piece)
            grad = (
                part[src, :].astype(F32)
                + left_a[h, n - 2, at(), :].astype(F32)
                + right_a[h, n - 2, at(), :].astype(F32)
            )
            hat, scale = layer_norm(middle[mine, :], epsilon)
            gain_out[...] += jnp.sum((hat * grad).reshape(BLOCK // 8, 8, width), axis=0)
            d_mid = cot_v[src, :].astype(F32) + norm_back(grad * gain[...], hat, scale)
            d_middle[mine, :] = d_mid
            stage[h, at(), :] = d_mid.astype(BF)

        blocks(piece, step)
        local(stage.at[h], rows_at(mid_out, h))

    def finish_two(h):
        scatter_two[h].finish()

        def step(at):
            src = at(h * per)
            mine = at(h * piece)
            outputs[mine, :] = (
                middle[mine, :]
                + part_two[src, :].astype(F32)
                + left_b[h, n - 2, at(), :].astype(F32)
                + right_b[h, n - 2, at(), :].astype(F32)
            ).astype(BF)

        blocks(piece, step)

    tiles = wide // LANES
    cut = tiles // 2

    def wait_for(items):
        for item in items:
            item.wait()
        items.clear()

    first_loads, own_load = [load_gated, load_wo], [load_own]
    later_loads = [load_pack]

    def out_action(h):
        wait_for(first_loads)
        out_product(h)

    def finish_one_action(h):
        wait_for(own_load)
        finish_one(h)

    def glu_action(h):
        wait_for(later_loads)
        assert all(item.done == len(bits_of(m)) + 1 for item in doubling)
        if h in begun:
            glu_tiles(h, cut, tiles)
        else:
            begun.add(h)
            glu_tiles(h, 0, cut)

    def grad_action(h):
        scatter_one[h].drain()
        grad_product(h)

    def products_action(_):
        k = len(products)
        if k >= 2:
            products[k - 2].wait()
        left = hidden_v.at[...] if k == 2 else glu_v.at[:, pl.ds(k * wide, wide)]
        right = cot_v if k == 2 else rows_v
        target = result.at[k % 2]

        def step(j, carry):
            at = pl.ds(pl.multiple_of(j * 2 * LANES, 2 * LANES), 2 * LANES)
            target[:, at] = dot_tn(left[...], right[:, at]).astype(BF)
            return carry

        lax.fori_loop(0, width // (2 * LANES), step, 0)
        place_out = product_out if k == 2 else glu_out.at[pl.ds(k * wide, wide)]
        store = pltpu.make_async_copy(target, place_out, copy_sem.at[spare + k])
        store.start()
        products.append(store)

    products, spare = [], copy_sem.shape[0] - 3
    begun = set()
    actions = {
        COT: lambda h: gather_cot[h].step(),
        OUT: out_action,
        ONE: lambda h: scatter_one[h].step(),
        END_ONE: finish_one_action,
        TWO: lambda h: gather_two[h].step(),
        GLU: glu_action,
        GRAD: grad_action,
        GRAD_SUM: lambda h: scatter_grad[h].step(),
        END_GRAD: finish_grad,
        MID: lambda h: gather_mid[h].step(),
        DOWN: down_product,
        DOWN_SUM: lambda h: scatter_two[h].step(),
        END_DOWN: finish_two,
        PRODUCTS: products_action,
        WIDE: lambda h: doubling[h].step(),
    }
    for item in load_cot:
        item.wait()
    for kind, h in middle_order(n, len(bits_of(m))):
        actions[kind](h)
    local(part_two.at[pl.ds(DOWNS * per, down_out.shape[0])], down_out)
    local(middle.at[pl.ds(DOWNS * piece, middle_out.shape[0])], middle_out)
    for item in list(gather_cot.values()) + gather_two + gather_mid:
        assert item.step_no == n
    for item in scatter_one + scatter_two + scatter_grad:
        assert item.step_no == n - 1
    for group in (scatter_grad, scatter_two):
        for item in group:
            item.drain()
    for item in copies[CHUNKS - FRONT + 5 :] + products[1:]:
        item.wait()
    assert len(products) == 3
    for item in doubling:
        item.leave()
    line.leave()


def middle_call(gated, pack, out_weight, own, cot, cot_front, gain, n, m):
    rows, width = own.shape
    heads, tokens, size = gated.shape
    nv = heads * size
    wide = pack.shape[0] // 3
    piece = rows // CHUNKS
    back = CHUNKS - DOWNS
    sems = CHUNKS * 5 * 2 * (n - 1)
    hop = (CHUNKS, n - 1, piece, width)
    shape = jax.ShapeDtypeStruct
    return pl.pallas_call(
        functools.partial(middle_kernel, n, m),
        out_shape=(
            shape((tokens, width), BF),
            shape((2 * wide, width), BF),
            shape((wide, width), BF),
            shape((back * n * piece, width), BF),
            shape((DOWNS * piece, width), BF),
            shape((back * piece, width), F32),
            shape((rows, width), F32),
            shape((8, width), F32),
        ),
        in_specs=[ANY, VM] + [ANY] * 4 + [VM],
        out_specs=(ANY,) * 4 + (VM, ANY, VM, VM),
        scratch_shapes=[
            pltpu.VMEM((heads, tokens, size), BF),
            pltpu.VMEM((nv, width), BF),
            pltpu.VMEM((3 * wide, width), BF),
            pltpu.VMEM((rows, width), BF),
            pltpu.VMEM((tokens, width), BF),
            pltpu.VMEM((tokens, width), BF),
            pltpu.VMEM((tokens, wide), BF),
            pltpu.VMEM((tokens, 2 * wide), BF),
            pltpu.VMEM((tokens, width), BF),
            pltpu.VMEM((tokens, width), BF),
            pltpu.VMEM(hop, BF),
            pltpu.VMEM(hop, BF),
            pltpu.VMEM((DOWNS,) + hop[1:], BF),
            pltpu.VMEM((DOWNS,) + hop[1:], BF),
            pltpu.VMEM((rows, width), F32),
            pltpu.VMEM((CHUNKS, piece, width), BF),
            pltpu.VMEM((2, wide, width), BF),
            pltpu.SemaphoreType.DMA((11 + 2 * CHUNKS - FRONT,)),
            pltpu.SemaphoreType.DMA((sems,)),
            pltpu.SemaphoreType.DMA((sems,)),
            pltpu.SemaphoreType.DMA((2 * PARTS * (m - 1),)),
            pltpu.SemaphoreType.DMA((2 * PARTS * (m - 1),)),
        ],
        compiler_params=pltpu.CompilerParams(
            collective_id=1, has_side_effects=True, vmem_limit_bytes=VMEM_MOST
        ),
        name="middle",
    )(gated, pack, out_weight, own, cot, cot_front, gain)


class Halving:
    def __init__(self, grads, rows, bits, base, kept, held, out, send_sem, recv_sem, load_sem):
        self.d = lax.axis_index("dp")
        self.grads, self.rows, self.bits, self.base = grads, rows, bits, base
        self.kept, self.held, self.out = kept, held, out
        self.send_sem, self.recv_sem, self.load_sem = send_sem, recv_sem, load_sem
        self.shard = out.shape[1]
        self.masks = [0]
        for bit in bits[:0:-1]:
            self.masks += [k + bit for k in self.masks]
        self.done, self.sent, self.loads = 0, [], []

    def flip(self, d, mask):
        for bit in self.bits:
            if mask & bit:
                d = d + bit * (1 - 2 * (lax.div(d, bit) % 2))
        return d

    def block(self, d):
        return self.grads.at[self.rows, pl.ds(pl.multiple_of(d * self.shard, self.shard), self.shard)]

    def count(self, level):
        return 1 << (len(self.bits) - 1 - level)

    def copies(self, level):
        bit = self.bits[level]
        partner = self.flip(self.d, bit)
        out = []
        for i in range(self.count(level)):
            if level == 0:
                src = self.block(self.flip(partner, self.masks[i]))
            else:
                src = self.kept.at[self.count(level) + i, self.rows]
            index = self.base + len(out) + sum(self.count(k) for k in range(level))
            out.append(
                pltpu.make_async_remote_copy(
                    src_ref=src,
                    dst_ref=self.held[level].at[i, self.rows],
                    send_sem=self.send_sem.at[index],
                    recv_sem=self.recv_sem.at[index],
                    device_id={"dp": partner},
                    device_id_type=MESH,
                )
            )
        return out

    def load(self):
        for i, mask in enumerate(self.masks):
            c = pltpu.make_async_copy(
                self.block(self.flip(self.d, mask)), self.kept.at[i, self.rows], self.load_sem.at[i]
            )
            c.start()
            self.loads.append(c)

    def add(self, level):
        last = level == len(self.bits) - 1
        start, size = self.rows.start, self.rows.size
        for i in range(self.count(level)):

            def step(at):
                total = self.kept[i, at(start), :].astype(F32) + self.held[level][
                    i, at(start), :
                ].astype(F32)
                if last:
                    self.out[at(start), :] = total
                else:
                    self.kept[i, at(start), :] = total.astype(BF)

            blocks(size, step)

    def step(self):
        level = self.done
        if level > 0:
            for c in self.loads:
                c.wait()
            self.loads = []
            for c in self.sent[-1]:
                c.wait_recv()
            self.add(level - 1)
        if level < len(self.bits):
            out = self.copies(level)
            for c in out:
                c.start()
            self.sent.append(out)
        self.done += 1

    def leave(self):
        for group in self.sent:
            for c in group:
                c.wait_send()


def grad_scatter(m, grads, kept, held, summed, send_sem, recv_sem, load_sem):
    bits = bits_of(m)
    height = grads.shape[0] // (2 * PARTS)
    out = []
    for i in range(2 * PARTS):
        order = bits[:1] + (bits[1:] if i % 2 == 0 else bits[:0:-1])
        rows = pl.ds(i * height, height)
        out.append(
            Halving(
                grads, rows, order, i * (m - 1), kept, held, summed, send_sem, recv_sem, load_sem.at[i]
            )
        )
    return out, [out[0].flip(out[0].d, bit) for bit in bits]


def scatter_scratch(m, rows, shard):
    wide = 2 * PARTS * (m - 1)
    counts = [m // 2] + [m >> (1 + k) for k in range(len(bits_of(m)))]
    return [pltpu.VMEM((count, rows, shard), BF) for count in counts] + [
        pltpu.VMEM((rows, shard), F32),
        pltpu.SemaphoreType.DMA((wide,)),
        pltpu.SemaphoreType.DMA((wide,)),
        pltpu.SemaphoreType.DMA((2 * PARTS, m // 2)),
    ]


def exchange(groups, mine, total, send_sem, recv_sem):
    source, base = mine, 0
    for axis, size, held in groups:
        me = lax.axis_index(axis)
        held[me] = source[...]

        def copy(k, slot):
            return pltpu.make_async_remote_copy(
                src_ref=source,
                dst_ref=held.at[slot],
                send_sem=send_sem.at[base + k],
                recv_sem=recv_sem.at[base + k],
                device_id={axis: lax.rem(me + k, size)},
                device_id_type=MESH,
            )

        sent = [copy(k, me) for k in range(1, size)]
        for c in sent:
            c.start()
        for k in range(1, size):
            copy(k, lax.rem(me - k + size, size)).wait_recv()
        value = held[0]
        for k in range(1, size):
            value = value + held[k]
        for c in sent:
            c.wait_send()
        total[...] = value
        source, base = total, base + size


def last_kernel(
    n, m, d_qk, d_value, d_gate, weight, grads, inputs, gain, d_middle, second_gain,
    out, gains, grad_query, grad_key, grad_out, grad_gate, grad_value,
    qk_v, value_v, gate_v, weight_v, inputs_v, middle_v, part, lefts, rights, *rest
):
    bits = bits_of(m)
    kept, held = rest[0], rest[1 : 1 + len(bits)]
    summed, wide_send, wide_recv, load_sem = rest[1 + len(bits) : 5 + len(bits)]
    gain_sum, mine, first, second = rest[5 + len(bits) : 9 + len(bits)]
    copy_sem, send_sem, recv_sem, gain_send, gain_recv = rest[9 + len(bits) :]
    line = Line(n, send_sem, recv_sem)
    count, width = out.shape
    piece = count // CHUNKS
    per = n * piece
    heads, _, size = value_v.shape
    wide = qk_v.shape[1]
    load = [
        pltpu.make_async_copy(src, dst, copy_sem.at[i])
        for i, (src, dst) in enumerate(
            [
                (weight.at[pl.ds(0, weight_v.shape[0])], weight_v), (d_qk, qk_v),
                (d_value, value_v), (d_gate, gate_v), (inputs, inputs_v), (d_middle, middle_v),
            ]
        )
    ]
    for item in load:
        item.start()
    barrier = pltpu.get_barrier_semaphore()
    for axis, extent in (("dp", m), ("mp", n)):
        me = lax.axis_index(axis)
        for k in range(1, extent):
            peer = lax.rem(me + k, extent)
            pl.semaphore_signal(barrier, inc=1, device_id={axis: peer}, device_id_type=MESH)
    pl.semaphore_wait(barrier, n + m - 2)

    halving, _ = grad_scatter(m, grads, kept, held, summed, wide_send, wide_recv, load_sem)
    for item in halving:
        item.step()
    for item in halving:
        item.load()
    for h in range(CHUNKS):
        no_neighbour_zero(n, line.place, lefts.at[h, n - 2], rights.at[h, n - 2])
    gain_sum[...] = jnp.zeros_like(gain_sum)
    scatters = [
        Scatter(
            line,
            lambda k, h=h: part.at[pl.ds(h * per + k * piece, piece)],
            lambda s, h=h: lefts.at[h, s - 1],
            lambda s, h=h: rights.at[h, s - 1],
            add_into,
        )
        for h in range(CHUNKS)
    ]

    def product(h):
        rows = pl.ds(h * per, per)

        def step(j, carry):
            at = pl.ds(pl.multiple_of(j * 2 * LANES, 2 * LANES), 2 * LANES)
            total = dot_nn(qk_v[rows, :], weight_v[pl.ds(0, wide), at])
            for i in range(heads):
                base = wide + i * size
                total += dot_nn(value_v[i, rows, :], weight_v[pl.ds(base, size), at])
                base += heads * size
                total += dot_nn(gate_v[i, rows, :], weight_v[pl.ds(base, size), at])
            part[rows, at] = total.astype(BF)
            return carry

        lax.fori_loop(0, width // (2 * LANES), step, 0)

    def finish(h):
        scatters[h].finish()

        def step(at):
            own = at(h * piece)
            grad = (
                part[at(h * per), :].astype(F32)
                + lefts[h, n - 2, at(), :].astype(F32)
                + rights[h, n - 2, at(), :].astype(F32)
            )
            hat, scale = layer_norm(inputs_v[own, :].astype(F32), epsilon)
            gain_sum[...] += jnp.sum((hat * grad).reshape(BLOCK // 8, 8, width), axis=0)
            out[own, :] = middle_v[own, :] + norm_back(grad * gain[...], hat, scale)

        blocks(piece, step)

    for item in load:
        item.wait()
    for h in range(CHUNKS):
        product(h)
        scatters[h].step()
    for s in range(n - 2):
        for h in range(CHUNKS):
            if s < len(bits) and h < len(halving):
                halving[h].step()
            scatters[h].step()
    while halving[0].done < len(bits):
        for item in halving:
            item.step()
    for h in range(CHUNKS):
        finish(h)
    groups = [("dp", m, first), ("mp", n, second)]
    for i, source in enumerate((gain_sum, second_gain)):
        flat = jnp.sum(source[...], axis=0, keepdims=True)
        for j in range(width // LANES):
            mine[pl.ds(i * (width // LANES) + j, 1), :] = flat[:, j * LANES : (j + 1) * LANES]
    for item in halving:
        while item.done <= len(bits):
            item.step()
    stores, base = [], 0
    for target in (grad_out, grad_gate):
        source = summed.at[pl.ds(base, target.shape[0])]
        stores.append(pltpu.make_async_copy(source, target, copy_sem.at[len(load) + len(stores)]))
        base += target.shape[0]
    deep = grad_query.shape[1]
    value_base = base + 2 * deep
    source = summed.at[pl.ds(value_base, grad_value.shape[0])]
    stores.append(pltpu.make_async_copy(source, grad_value, copy_sem.at[len(load) + len(stores)]))
    for store in stores:
        store.start()
    for target in (grad_query, grad_key):
        for j in range(deep // LANES):
            target[:, j * LANES : (j + 1) * LANES] = summed[pl.ds(base, LANES), :].T
            base += LANES
    exchange(groups, mine, gains, gain_send, gain_recv)
    for item in halving:
        item.leave()
    for store in stores:
        store.wait()
    for h in range(CHUNKS):
        scatters[h].drain()


def last_call(d_qk, d_value, d_gate, weight, grads, inputs, gain, d_middle, second_gain, n, m):
    tokens = d_qk.shape[0]
    rows, width = inputs.shape
    heads = d_value.shape[0]
    shard = width // m
    sems = CHUNKS * 2 * (n - 1)
    hop = (CHUNKS, n - 1, rows // CHUNKS, width)
    flat = (2 * width // LANES, LANES)
    shape = jax.ShapeDtypeStruct
    return pl.pallas_call(
        functools.partial(last_kernel, n, m),
        out_shape=(
            shape((rows, width), F32),
            shape(flat, F32),
            shape((shard, heads * HK), F32),
            shape((shard, heads * HK), F32),
        )
        + (shape((heads * HV, shard), F32),) * 3,
        in_specs=[ANY] * 6 + [VM, ANY, VM],
        out_specs=(VM,) * 4 + (ANY,) * 3,
        scratch_shapes=[
            pltpu.VMEM(d_qk.shape, BF),
            pltpu.VMEM(d_value.shape, BF),
            pltpu.VMEM(d_gate.shape, BF),
            pltpu.VMEM((2 * heads * (HK + HV), width), BF),
            pltpu.VMEM((rows, width), BF),
            pltpu.VMEM((rows, width), F32),
            pltpu.VMEM((tokens, width), BF),
            pltpu.VMEM(hop, BF),
            pltpu.VMEM(hop, BF),
        ]
        + scatter_scratch(m, grads.shape[0], shard)
        + [
            pltpu.VMEM((8, width), F32),
            pltpu.VMEM(flat, F32),
            pltpu.VMEM((m,) + flat, F32),
            pltpu.VMEM((n,) + flat, F32),
            pltpu.SemaphoreType.DMA((9,)),
            pltpu.SemaphoreType.DMA((sems,)),
            pltpu.SemaphoreType.DMA((sems,)),
            pltpu.SemaphoreType.DMA((n + m,)),
            pltpu.SemaphoreType.DMA((n + m,)),
        ],
        compiler_params=pltpu.CompilerParams(
            collective_id=2, has_side_effects=True, vmem_limit_bytes=VMEM_MOST
        ),
        name="last",
    )(d_qk, d_value, d_gate, weight, grads, inputs, gain, d_middle, second_gain)


TILE = 256


def tiles_of(count, step):
    def run(i, carry):
        step(pl.ds(pl.multiple_of(i * TILE, TILE), TILE))
        return carry

    lax.fori_loop(0, count // TILE, run, 0)


def in_order(units, steps):
    taken = 0
    for i, unit in enumerate(units):
        unit()
        upto = (i + 1) * len(steps) // len(units)
        for step in steps[taken:upto]:
            step()
        taken = upto


def forward_kernel(
    n, rows, weight, cot, col, row,
    query_o, key_o, value_o, gate_o, norm_o, scale_o, scores_o, gated_o, cot_o,
    rows_v, weight_v, query_v, key_v, value_v, gate_v, norm_v, scale_v, scores_v, gated_v, cot_v,
    copy_sem, send_sem, recv_sem,
):
    line = Line(n, send_sem, recv_sem)
    heads, tokens, deep = query_v.shape
    size = value_v.shape[2]
    per = cot_v.shape[0] // FRONT
    piece = per // n
    copies = []

    def local(src, dst):
        c = pltpu.make_async_copy(src, dst, copy_sem.at[len(copies)])
        copies.append(c)
        c.start()
        return c

    load_cot = [
        local(cot.at[pl.ds(h * piece, piece)], cot_v.at[pl.ds(h * per, piece)])
        for h in range(FRONT)
    ]
    load_rows = local(rows, rows_v)
    load_weight = local(weight.at[pl.ds(0, weight_v.shape[0])], weight_v)
    line.enter()
    gathers = [
        Gather(line, lambda k, h=h: cot_v.at[pl.ds(h * per + k * piece, piece)])
        for h in range(FRONT)
    ]
    for item in load_cot:
        item.wait()
    for g in gathers:
        g.step()
    load_rows.wait()
    load_weight.wait()

    def project(target, h, base, width):
        def step(at):
            target[h, at, :] = dot_nt(rows_v[at, :], weight_v[pl.ds(base, width), :]).astype(
                target.dtype
            )

        return lambda: tiles_of(tokens, step)

    def attend(h):
        def step(at):
            allowed = (col[at, 0:1] >= row[0:1, :]) & (col[at, 1:2] == row[1:2, :])
            scores = dot_nt(query_v[h, at, :], key_v[h]) * col[at, 2 + h : 3 + h]
            scores = jnp.where(allowed, scores * row[2 + h : 3 + h, :], 0.0).astype(BF)
            scores_v[h, at, :] = scores
            hat, scale = layer_norm(dot_nn(scores, value_v[h]), group_epsilon)
            norm_v[h, at, :] = hat
            scale_v[h, at, :] = scale
            gate = gate_v[h, at, :]
            gated_v[h, at, :] = (gate * jax.nn.sigmoid(gate) * hat).astype(BF)

        return lambda: tiles_of(tokens, step)

    values, gates = 2 * heads * deep, 2 * heads * deep + heads * size
    units = []
    for h in range(heads):
        units += [
            project(query_v, h, h * deep, deep),
            project(key_v, h, (heads + h) * deep, deep),
            project(value_v, h, values + h * size, size),
            project(gate_v, h, gates + h * size, size),
            attend(h),
        ]
    in_order(units, [g.step for _ in range(n - 1) for g in gathers])
    count = len(copies)
    for src, dst in (
        (query_v, query_o), (key_v, key_o), (value_v, value_o), (gate_v, gate_o),
        (norm_v, norm_o), (scale_v, scale_o), (scores_v, scores_o), (gated_v, gated_o),
        (cot_v, cot_o),
    ):
        local(src, dst)
    for item in copies[count:]:
        item.wait()
    line.leave()


def forward_call(rows, weight, cot, col, row, n, heads):
    tokens, width = rows.shape
    shape = jax.ShapeDtypeStruct
    outs = (
        shape((heads, tokens, HK), BF),
        shape((heads, tokens, HK), BF),
        shape((heads, tokens, HV), BF),
        shape((heads, tokens, HV), F32),
        shape((heads, tokens, HV), F32),
        shape((heads, tokens, 1), F32),
        shape((heads, tokens, tokens), BF),
        shape((heads, tokens, HV), BF),
        shape((tokens * FRONT // CHUNKS, width), BF),
    )
    attention_rows = 2 * heads * (HK + HV)
    sems = FRONT * 2 * (n - 1)
    return pl.pallas_call(
        functools.partial(forward_kernel, n),
        out_shape=outs,
        in_specs=[ANY] * 3 + [VM] * 2,
        out_specs=(ANY,) * len(outs),
        scratch_shapes=[pltpu.VMEM(rows.shape, BF), pltpu.VMEM((attention_rows, width), BF)]
        + [pltpu.VMEM(o.shape, o.dtype) for o in outs]
        + [
            pltpu.SemaphoreType.DMA((FRONT + 2 + len(outs),)),
            pltpu.SemaphoreType.DMA((sems,)),
            pltpu.SemaphoreType.DMA((sems,)),
        ],
        compiler_params=pltpu.CompilerParams(
            collective_id=4, has_side_effects=True, vmem_limit_bytes=VMEM_MOST
        ),
        name="forward",
    )(rows, weight, cot, col, row)


def backward_kernel(
    n, m, mid, weights, gate, norm, scale, scores, query, key, value, down, middle, grads, col, row,
    qk_o, value_o, gate_o, glu_gate_o, glu_up_o, outputs,
    mid_v, wo_v, gate_v, norm_v, scale_v, scores_v, query_v, key_v, value_v, part, middle_v,
    d_qk, d_value, d_gate, d_kept, d_scores, lefts, rights, *rest
):
    bits = bits_of(m)
    kept, held = rest[0], rest[1 : 1 + len(bits)]
    summed, wide_send, wide_recv, load_sem = rest[1 + len(bits) : 5 + len(bits)]
    copy_sem, send_sem, recv_sem = rest[5 + len(bits) :]
    line = Line(n, send_sem, recv_sem)
    heads, tokens, deep = query_v.shape
    size = value_v.shape[2]
    back = CHUNKS - DOWNS - ENDS
    per = part.shape[0] // back
    piece = per // n
    copies = []

    def local(src, dst):
        c = pltpu.make_async_copy(src, dst, copy_sem.at[len(copies)])
        copies.append(c)
        c.start()
        return c

    load_part = local(down.at[pl.ds(0, part.shape[0])], part)
    loads = [
        local(src, dst)
        for src, dst in (
            (mid, mid_v), (weights.at[pl.ds(weights.shape[0] - wo_v.shape[0], wo_v.shape[0])], wo_v),
            (gate, gate_v), (norm, norm_v), (scale, scale_v), (value, value_v), (key, key_v),
            (query, query_v), (scores, scores_v),
            (middle.at[pl.ds(0, middle_v.shape[0])], middle_v),
        )
    ]
    halving, peers = grad_scatter(m, grads, kept, held, summed, wide_send, wide_recv, load_sem)
    line.enter(["dp", peers])
    for item in halving:
        item.step()
    for item in halving:
        item.load()
    for h in range(back):
        no_neighbour_zero(n, line.place, lefts.at[h, n - 2], rights.at[h, n - 2])
    scatters = [
        Scatter(
            line,
            lambda k, h=h: part.at[pl.ds(h * per + k * piece, piece)],
            lambda s, h=h: lefts.at[h, s - 1],
            lambda s, h=h: rights.at[h, s - 1],
            add_into,
        )
        for h in range(back)
    ]
    load_part.wait()
    for item in scatters:
        item.step()
    for item in loads:
        item.wait()

    def gates(h):
        def step(at):
            grad = dot_nt(mid_v[at, :], wo_v[pl.ds(h * size, size), :])
            pre, hat = gate_v[h, at, :], norm_v[h, at, :]
            s = jax.nn.sigmoid(pre)
            d_gate[h, at, :] = (grad * hat * (s + pre * s * (1.0 - s))).astype(BF)
            d_kept[h, at, :] = norm_back(grad * (pre * s), hat, scale_v[h, at, :]).astype(BF)

        return lambda: tiles_of(tokens, step)

    def by_row(h):
        def step(at):
            allowed = (col[at, 0:1] >= row[0:1, :]) & (col[at, 1:2] == row[1:2, :])
            grad = dot_nt(d_kept[h, at, :], value_v[h]) * col[at, 2 + h : 3 + h]
            grad = jnp.where(allowed, grad * row[2 + h : 3 + h, :], 0.0).astype(BF)
            d_scores[at, :] = grad
            d_qk[at, pl.ds(h * deep, deep)] = dot_nn(grad, key_v[h]).astype(BF)

        return lambda: tiles_of(tokens, step)

    def by_column(h):
        def step(at):
            d_value[h, at, :] = dot_tn(scores_v[h, :, at], d_kept[h]).astype(BF)
            d_qk[at, pl.ds((heads + h) * deep, deep)] = dot_tn(d_scores[:, at], query_v[h]).astype(
                BF
            )

        return lambda: tiles_of(tokens, step)

    units = []
    for h in range(heads):
        units += [gates(h), by_row(h), by_column(h)]
    steps = [item.step for _ in range(n - 2) for item in scatters]
    wide_steps = [item.step for _ in bits for item in halving]
    mixed = []
    for i in range(max(len(steps), len(wide_steps))):
        mixed += steps[i : i + 1] + wide_steps[i : i + 1]
    late = mixed[-2 * PARTS :]
    in_order(units, mixed[: -2 * PARTS])
    count = len(copies)
    local(d_qk, qk_o)
    local(d_value, value_o)
    local(d_gate, gate_o)
    for step in late:
        step()
    size = glu_up_o.shape[0]
    wide = grads.shape[0] // 2
    for t in range(wide // LANES):
        have = min(LANES, size - t * LANES)
        for i, target in enumerate((glu_gate_o, glu_up_o)):
            local(
                summed.at[pl.ds((2 * t + i) * LANES, have)], target.at[pl.ds(t * LANES, have)]
            )
    for item in halving:
        assert item.done == len(bits) + 1
        item.leave()
    for h in range(back):
        scatters[h].finish()

        def step(at):
            outputs[at(h * piece), :] = (
                middle_v[at(h * piece), :]
                + part[at(h * per), :].astype(F32)
                + lefts[h, n - 2, at(), :].astype(F32)
                + rights[h, n - 2, at(), :].astype(F32)
            ).astype(BF)

        blocks(piece, step)
    for item in copies[count:]:
        item.wait()
    for item in scatters:
        item.drain()


def backward_call(mid, weights, gate, norm, scale, scores, query, key, value, down, middle, grads, size_two, col, row, n, m):
    tokens, width = mid.shape
    heads, _, size = value.shape
    back = CHUNKS - DOWNS - ENDS
    nv = heads * size
    shard = width // m
    piece = tokens // n // CHUNKS
    shape = jax.ShapeDtypeStruct
    outs = (
        shape((tokens, 2 * heads * HK), BF),
        shape(value.shape, BF),
        shape(value.shape, BF),
    ) + (shape((size_two, shard), F32),) * 2 + (shape((back * piece, width), BF),)
    ins = (gate, norm, scale, scores, query, key, value, down, middle)
    hop = (back, n - 1, piece, width)
    sems = back * 2 * (n - 1)
    return pl.pallas_call(
        functools.partial(backward_kernel, n, m),
        out_shape=outs,
        in_specs=[ANY] * 12 + [VM] * 2,
        out_specs=(ANY,) * 5 + (VM,),
        scratch_shapes=[pltpu.VMEM(mid.shape, BF), pltpu.VMEM((nv, width), BF)]
        + [pltpu.VMEM(a.shape, a.dtype) for a in ins[:-2]]
        + [pltpu.VMEM((back * n * piece, width), BF), pltpu.VMEM((back * piece, width), F32)]
        + [pltpu.VMEM(o.shape, o.dtype) for o in outs[:3]]
        + [
            pltpu.VMEM(value.shape, BF),
            pltpu.VMEM((tokens, tokens), BF),
            pltpu.VMEM(hop, BF),
            pltpu.VMEM(hop, BF),
        ]
        + scatter_scratch(m, grads.shape[0], shard)
        + [
            pltpu.SemaphoreType.DMA((15 + grads.shape[0] // LANES,)),
            pltpu.SemaphoreType.DMA((sems,)),
            pltpu.SemaphoreType.DMA((sems,)),
        ],
        compiler_params=pltpu.CompilerParams(
            collective_id=5, has_side_effects=True, vmem_limit_bytes=VMEM_MOST
        ),
        name="backward",
    )(mid, weights, *ins, grads, col, row)


def products_kernel(n, m, plan, arrays, *refs):
    ins, (down, middle, grads) = refs[:arrays], refs[arrays : arrays + 3]
    out, down_o, outputs = refs[arrays + 3 : arrays + 6]
    held_in = refs[arrays + 6 : 2 * arrays + 6]
    part, middle_v, lefts, rights, result, kept, *rest = refs[2 * arrays + 6 :]
    bits = bits_of(m)
    held = rest[: len(bits)]
    summed, wide_send, wide_recv, load_sem, copy_sem, send_sem, recv_sem = rest[len(bits) :]
    line = Line(n, send_sem, recv_sem)
    count, width = outputs.shape
    piece = count // ENDS
    per = n * piece
    sources = list(zip(ins, held_in))
    sources.append((middle.at[pl.ds(middle.shape[0] - count, count)], middle_v))
    sources.append((down.at[pl.ds(down.shape[0] - n * count, n * count)], part))
    loads = [pltpu.make_async_copy(a, b, copy_sem.at[i]) for i, (a, b) in enumerate(sources)]
    for item in loads[::-1]:
        item.start()
    halving, peers = grad_scatter(m, grads, kept, held, summed, wide_send, wide_recv, load_sem)
    line.enter(["dp", peers])
    for item in halving:
        item.step()
    for item in halving:
        item.load()
    for h in range(ENDS):
        no_neighbour_zero(n, line.place, lefts.at[h, n - 2], rights.at[h, n - 2])
    scatters = [
        Scatter(
            line,
            lambda k, h=h: part.at[pl.ds(h * per + k * piece, piece)],
            lambda s, h=h: lefts.at[h, s - 1],
            lambda s, h=h: rights.at[h, s - 1],
            add_into,
        )
        for h in range(ENDS)
    ]
    loads[-1].wait()
    for item in scatters:
        item.step()
    waited, stores = set(), []

    def product(left, head, start, size, right, base):
        def run():
            for i in (left, right):
                if i not in waited:
                    loads[i].wait()
                    waited.add(i)
            target = pl.ds(base, size)

            def step(j, carry):
                at = pl.ds(pl.multiple_of(j * 4 * LANES, 4 * LANES), 4 * LANES)
                source = (
                    held_in[left][:, pl.ds(start, size)] if head is None else held_in[left][head]
                )
                result[target, at] = dot_tn(source, held_in[right][:, at]).astype(BF)
                return carry

            lax.fori_loop(0, width // (4 * LANES), step, 0)
            store(target)

        return run

    def store(target):
        c = pltpu.make_async_copy(
            result.at[target], out.at[target], copy_sem.at[len(loads) + len(stores)]
        )
        c.start()
        stores.append(c)

    units, base = [], 0
    for item in plan:
        units.append(product(*item, base))
        base += item[3]
    steps = [item.step for _ in range(n - 2) for item in scatters]
    wide_steps = [item.step for _ in bits for item in halving]
    mixed = []
    for i in range(max(len(steps), len(wide_steps))):
        mixed += steps[i : i + 1] + wide_steps[i : i + 1]
    in_order(units, mixed)
    spare = result.shape[0] - base
    if spare:
        result[pl.ds(base, spare), :] = jnp.zeros((spare, width), BF)
        store(pl.ds(base, spare))
    keep = pltpu.make_async_copy(
        summed.at[pl.ds(0, down_o.shape[0])], down_o, copy_sem.at[len(loads) + len(stores)]
    )
    keep.start()
    loads[-2].wait()
    for h in range(ENDS):
        scatters[h].finish()

        def step(at):
            outputs[at(h * piece), :] = (
                middle_v[at(h * piece), :]
                + part[at(h * per), :].astype(F32)
                + lefts[h, n - 2, at(), :].astype(F32)
                + rights[h, n - 2, at(), :].astype(F32)
            ).astype(BF)

        blocks(piece, step)
    for item in halving:
        assert item.done == len(bits) + 1
        item.leave()
    for item in scatters:
        item.drain()
    for item in stores + [keep]:
        item.wait()


def products_call(plan, arrays, down, middle, grads, size_two, rows, n, m):
    width = grads.shape[1]
    shard = width // m
    piece = arrays[1].shape[0] // n // CHUNKS
    sems = ENDS * 2 * (n - 1)
    hop = (ENDS, n - 1, piece, width)
    shape = jax.ShapeDtypeStruct
    return pl.pallas_call(
        functools.partial(products_kernel, n, m, plan, len(arrays)),
        out_shape=(
            shape((rows, width), BF), shape((size_two, shard), F32), shape((ENDS * piece, width), BF),
        ),
        in_specs=[ANY] * (len(arrays) + 3),
        out_specs=(ANY, ANY, VM),
        scratch_shapes=[pltpu.VMEM(a.shape, a.dtype) for a in arrays]
        + [
            pltpu.VMEM((ENDS * n * piece, width), BF),
            pltpu.VMEM((ENDS * piece, width), F32),
            pltpu.VMEM(hop, BF),
            pltpu.VMEM(hop, BF),
            pltpu.VMEM((rows, width), BF),
        ]
        + scatter_scratch(m, grads.shape[0], shard)
        + [
            pltpu.SemaphoreType.DMA((len(arrays) + len(plan) + 4,)),
            pltpu.SemaphoreType.DMA((sems,)),
            pltpu.SemaphoreType.DMA((sems,)),
        ],
        compiler_params=pltpu.CompilerParams(
            collective_id=3, has_side_effects=True, vmem_limit_bytes=VMEM_MOST
        ),
        name="products",
    )(*arrays, down, middle, grads)


def pad_rows(array, count):
    return jnp.pad(array, ((0, count - array.shape[0]), (0, 0)))


def pad_columns(array, count):
    return jnp.pad(array, ((0, 0), (0, count - array.shape[1])))


def body(
    inputs,
    segments,
    first_norm_gain,
    w_query,
    w_key,
    w_value,
    w_gate,
    w_out,
    second_norm_gain,
    w_glu_gate,
    w_glu_up,
    w_down,
    cotangent,
):
    n = lax.axis_size("mp")
    place = lax.axis_index("mp")
    heads = H // n
    head_start = place * heads
    rows, width = inputs.shape
    shard = w_query.shape[0]
    piece = rows // CHUNKS
    nk, nv, nf = heads * HK, heads * HV, w_down.shape[0]
    f_wide = -(-nf // LANES) * LANES
    f_tiles = f_wide // LANES
    grain = 2 * PARTS * BLOCK
    one_rows = -(-(2 * nk + 3 * nv) // grain) * grain
    gap = one_rows - 2 * nk - 3 * nv
    m = lax.axis_size("dp")

    pack_one = jnp.concatenate(
        [w_query.T, w_key.T, w_value.T, w_gate.T, jnp.zeros((gap, shard), BF), w_out], axis=0
    )
    glu_pack = jnp.stack(
        [
            pad_rows(w_glu_gate.T, f_wide).reshape(f_tiles, LANES, shard),
            pad_rows(w_glu_up.T, f_wide).reshape(f_tiles, LANES, shard),
        ],
        axis=1,
    ).reshape(2 * f_wide, shard)
    pack_two = jnp.concatenate([glu_pack, pad_rows(w_down, f_wide)], axis=0)

    first_hat, _ = layer_norm(inputs.astype(F32), epsilon)
    rows_one, weight_one = gather_rows((first_hat * first_norm_gain).astype(BF), pack_one, n, m)
    tokens = rows_one.shape[0]

    slot_shard = lax.rem(place - jnp.arange(n) + n, n)
    places = (
        slot_shard[None, :, None] * rows
        + jnp.arange(CHUNKS)[:, None, None] * piece
        + jnp.arange(piece)[None, None, :]
    ).reshape(tokens)
    seg = segments.reshape(n, CHUNKS, piece)[::-1]
    seg = lax.dynamic_slice_in_dim(jnp.concatenate([seg, seg], axis=0), n - 1 - place, n, axis=0)
    seg = seg.transpose(1, 0, 2).reshape(tokens)

    log_gamma = jnp.log1p(-jnp.exp2(-5.0 - (head_start + jnp.arange(heads)).astype(F32)))
    spot = places.astype(F32)
    powers = spot[None] * log_gamma[:, None]
    marks = jnp.stack([spot, seg.astype(F32)])
    col = jnp.concatenate([marks, jnp.exp(powers)], axis=0).T
    row = jnp.concatenate([marks, jnp.exp(-powers) * HK ** (-0.5)], axis=0)

    (
        query, key, value, gate_pre, normalized, scale_group, scores, gated, cot_front,
    ) = forward_call(rows_one, weight_one, cotangent, col, row, n, heads)
    (
        mid_rows, grads_glu, grads_two, down, outputs_front, middle, middle_grad, second_gain,
    ) = middle_call(
        gated, pack_two, weight_one, inputs, cotangent, cot_front, second_norm_gain[None], n, m
    )
    d_qk, d_value, d_gate, grad_glu_gate, grad_glu_up, outputs_back = backward_call(
        mid_rows, weight_one, gate_pre, normalized, scale_group, scores, query, key, value,
        down, middle, grads_glu, nf, col, row, n, m,
    )
    plan = [(0, h, 0, HV, 1) for h in range(heads)] + [(2, h, 0, HV, 3) for h in range(heads)]
    plan += [(4, None, t * nk, nk, 3) for t in range(2)]
    plan += [(5, h, 0, HV, 3) for h in range(heads)]
    grads_one, grad_down, outputs_end = products_call(
        plan, (gated, mid_rows, d_gate, rows_one, d_qk, d_value), down, middle, grads_two, nf,
        one_rows, n, m,
    )
    input_gradient, gains, grad_query, grad_key, grad_out, grad_gate, grad_value = last_call(
        d_qk, d_value, d_gate, weight_one, grads_one, inputs, first_norm_gain[None], middle_grad,
        second_gain, n, m,
    )
    gains = gains.reshape(2, width)
    return (
        jnp.concatenate([outputs_front, outputs_back, outputs_end], axis=0),
        input_gradient,
        gains[0],
        grad_query,
        grad_key,
        grad_value.T,
        grad_gate.T,
        grad_out,
        gains[1],
        grad_glu_gate.T,
        grad_glu_up.T,
        grad_down,
    )


def solution(mesh):
    split = P(("dp", "mp"), None)
    wide, tall = P("dp", "mp"), P("mp", "dp")
    return jax.shard_map(
        body,
        mesh=mesh,
        in_specs=(
            split, P("dp", None), P(), wide, wide, wide, wide, tall, P(), wide, wide, tall, split,
        ),
        out_specs=(
            split, split, P(), wide, wide, wide, wide, tall, P(), wide, wide, tall,
        ),
        check_vma=False,
    )
```

```python
import functools

import jax
import jax.numpy as jnp
from jax import lax
from jax.experimental import pallas as pl
from jax.experimental.pallas import tpu as pltpu
from jax.sharding import PartitionSpec as P

H = 8
HK = 256
HV = 432
LEN = 1024
CHUNKS = 4
FRONT = CHUNKS // 2
DOWNS = CHUNKS // 4
ENDS = CHUNKS // 4
LANES = 128
VMEM_MOST = 66_000_000

epsilon = 1e-05
group_epsilon = 1.0
BF = jnp.bfloat16
F32 = jnp.float32


def layer_norm(values_in, offset):
    centre = jnp.mean(values_in, axis=-1, keepdims=True)
    centred = values_in - centre
    variance = jnp.mean(centred * centred, axis=-1, keepdims=True)
    scaling = lax.rsqrt(variance + offset)
    return (centred * scaling, scaling)


def norm_back(grad_hat, normed_hat, scaling):
    first_mean = jnp.mean(grad_hat, axis=-1, keepdims=True)
    second_mean = jnp.mean(grad_hat * normed_hat, axis=-1, keepdims=True)
    return scaling * (grad_hat - first_mean - normed_hat * second_mean)


def glu_act(gate_pre, up_pre):
    return jax.nn.gelu(gate_pre, approximate=True) * up_pre


def dot_nt(a, b):
    return lax.dot_general(a, b, (((1,), (1,)), ((), ())), preferred_element_type=F32)


def dot_nn(a, b):
    return lax.dot_general(a, b, (((1,), (0,)), ((), ())), preferred_element_type=F32)


def dot_tn(a, b):
    return lax.dot_general(a, b, (((0,), (0,)), ((), ())), preferred_element_type=F32)


MESH = pl.DeviceIdType.MESH


class Line:
    def __init__(self, n, send_sem, recv_sem):
        self.n, self.send_sem, self.recv_sem = n, send_sem, recv_sem
        self.place = lax.axis_index("mp")
        self.used = 0
        self.sent = []

    def enter(self, others=None):
        barrier = pltpu.get_barrier_semaphore()
        n, place = self.n, self.place

        @pl.when(place >= 1)
        def _():
            pl.semaphore_signal(barrier, inc=1, device_id={"mp": place - 1}, device_id_type=MESH)

        @pl.when(place <= n - 2)
        def _():
            pl.semaphore_signal(barrier, inc=1, device_id={"mp": place + 1}, device_id_type=MESH)

        peers = jnp.minimum(place, 1) + jnp.minimum(n - 1 - place, 1)
        if others is not None:
            axis, indices = others
            for index in indices:
                pl.semaphore_signal(barrier, inc=1, device_id={axis: index}, device_id_type=MESH)
            peers = peers + len(indices)
        pl.semaphore_wait(barrier, peers)

    def copy(self, src, dst, index, toward):
        return pltpu.make_async_remote_copy(
            src_ref=src,
            dst_ref=dst,
            send_sem=self.send_sem.at[index],
            recv_sem=self.recv_sem.at[index],
            device_id={"mp": self.place + toward},
            device_id_type=MESH,
        )

    def leave(self):
        for condition, copy in self.sent:
            pl.when(condition)(copy.wait_send)


class Gather:
    def __init__(self, line, slot):
        self.line, self.slot, self.step_no = line, slot, 0
        self.base = line.used
        line.used += 2 * (line.n - 1)
        n = line.n
        self.right = [
            line.copy(slot(s - 1), slot(s), self.base + s - 1, 1) for s in range(1, n)
        ]
        self.left = [
            line.copy(slot((n - s + 1) % n), slot(n - s), self.base + n - 2 + s, -1)
            for s in range(1, n)
        ]

    def arrive(self, s):
        n, place = self.line.n, self.line.place
        pl.when(place >= s)(self.right[s - 1].wait_recv)
        pl.when(place <= n - 1 - s)(self.left[s - 1].wait_recv)

    def step(self):
        self.step_no += 1
        s, n, place = self.step_no, self.line.n, self.line.place
        if s > 1:
            self.arrive(s - 1)
        if s < n:
            to_right = (place >= s - 1) & (place <= n - 2)
            to_left = (place <= n - s) & (place >= 1)
            pl.when(to_right)(self.right[s - 1].start)
            pl.when(to_left)(self.left[s - 1].start)
            self.line.sent += [(to_right, self.right[s - 1]), (to_left, self.left[s - 1])]


class Scatter:
    def __init__(self, line, slot, from_left, from_right, add):
        self.line, self.slot, self.add, self.step_no = line, slot, add, 0
        self.from_left, self.from_right = from_left, from_right
        self.base = line.used
        line.used += 2 * (line.n - 1)
        n = line.n
        self.right = [
            line.copy(slot(s), from_left(s), self.base + s - 1, 1) for s in range(1, n)
        ]
        self.left = [
            line.copy(slot(n - s), from_right(s), self.base + n - 2 + s, -1) for s in range(1, n)
        ]
        self.mine = []

    def step(self):
        self.step_no += 1
        s, n, place = self.step_no, self.line.n, self.line.place
        to_right, to_left = place <= s - 1, place >= n - s
        if s > 1:

            @pl.when(to_right & (place >= 1))
            def _():
                self.right[s - 2].wait_recv()
                self.add(self.slot(s), self.from_left(s - 1))

            @pl.when(to_left & (place <= n - 2))
            def _():
                self.left[s - 2].wait_recv()
                self.add(self.slot(n - s), self.from_right(s - 1))

        pl.when(to_right)(self.right[s - 1].start)
        pl.when(to_left)(self.left[s - 1].start)
        self.mine += [(to_right, self.right[s - 1]), (to_left, self.left[s - 1])]

    def finish(self):
        n, place = self.line.n, self.line.place

        @pl.when(place >= 1)
        def _():
            self.right[n - 2].wait_recv()

        @pl.when(place <= n - 2)
        def _():
            self.left[n - 2].wait_recv()

    def drain(self):
        for condition, copy in self.mine:
            pl.when(condition)(copy.wait_send)


ANY = pl.BlockSpec(memory_space=pl.ANY)
VM = pl.BlockSpec(memory_space=pltpu.VMEM)
BLOCK = 16


def blocks(count, step):
    def run(i, carry):
        step(lambda base=0: pl.ds(pl.multiple_of(base + i * BLOCK, BLOCK), BLOCK))
        return carry

    lax.fori_loop(0, count // BLOCK, run, 0)


def add_into(target, extra):
    def step(at):
        target[at(), :] = (target[at(), :].astype(F32) + extra[at(), :].astype(F32)).astype(BF)

    blocks(target.shape[0], step)


def product_tiles(target, left, right, tile):
    def step(j, carry):
        at = pl.ds(pl.multiple_of(j * tile, tile), tile)
        target[:, at] = dot_nn(left[...], right[:, at]).astype(BF)
        return carry

    lax.fori_loop(0, right.shape[1] // tile, step, 0)


class Doubling:
    def __init__(self, m, own, out, rows, bits, base, send_sem, recv_sem):
        self.d = lax.axis_index("dp")
        self.own, self.out, self.rows, self.bits, self.base = own, out, rows, bits, base
        self.send_sem, self.recv_sem = send_sem, recv_sem
        self.shard = own.shape[1]
        self.done = 0
        self.sent = []

    def flip(self, d, bit):
        return d + bit * (1 - 2 * (lax.div(d, bit) % 2))

    def block(self, d):
        return self.out.at[self.rows, pl.ds(pl.multiple_of(d * self.shard, self.shard), self.shard)]

    def copies(self, level, landing):
        owners = [self.d]
        for bit in self.bits[:level]:
            owners += [self.flip(d, bit) for d in owners]
        bit = self.bits[level]
        partner = self.flip(self.d, bit)
        out = []
        for i, d in enumerate(owners):
            d = self.flip(d, bit) if landing else d
            src = self.own.at[self.rows] if i == 0 and not landing else self.block(d)
            index = self.base + (1 << level) - 1 + i
            out.append(
                pltpu.make_async_remote_copy(
                    src_ref=src,
                    dst_ref=self.block(d),
                    send_sem=self.send_sem.at[index],
                    recv_sem=self.recv_sem.at[index],
                    device_id={"dp": partner},
                    device_id_type=MESH,
                )
            )
        return out

    def step(self):
        level = self.done
        if level > 0:
            for c in self.copies(level - 1, True):
                c.wait_recv()
        if level < len(self.bits):
            out = self.copies(level, False)
            for c in out:
                c.start()
            self.sent += out
        self.done += 1

    def leave(self):
        for c in self.sent:
            c.wait_send()


def bits_of(m):
    bits = [1 << b for b in range(m.bit_length() - 1)]
    assert 1 << len(bits) == m
    return bits


PARTS = 2


def weight_gather(m, pack, weight, send_sem, recv_sem):
    bits = bits_of(m)
    outer = bits[1:]
    height = pack.shape[0] // (2 * PARTS)
    doubling = []
    for i in range(2 * PARTS):
        order = (outer if i % 2 == 0 else outer[::-1]) + bits[:1]
        rows = pl.ds(i * height, height)
        doubling.append(Doubling(m, pack, weight, rows, order, i * (m - 1), send_sem, recv_sem))
    first = doubling[0]
    return doubling, [first.flip(first.d, bit) for bit in bits]


def own_columns(pack, weight):
    shard = pack.shape[1]
    at = pl.multiple_of(lax.axis_index("dp") * shard, shard)
    return weight.at[:, pl.ds(at, shard)]


def no_neighbour_zero(n, place, from_left, from_right):
    @pl.when(place == 0)
    def _():
        from_left[...] = jnp.zeros_like(from_left)

    @pl.when(place == n - 1)
    def _():
        from_right[...] = jnp.zeros_like(from_right)


(COT, OUT, ONE, END_ONE, TWO, GLU, GRAD, GRAD_SUM, END_GRAD, MID, DOWN, DOWN_SUM, END_DOWN, PRODUCTS, WIDE) = range(15)

DUE = {
    OUT: (-2.23, 1.66, 0), ONE: (-1.99, 1.12, 1.03), END_ONE: (1.46, 1.37, 0), TWO: (0.73, 1.15, 0.94),
    COT: (0.35, 1.39, 1.02), GLU: (1.14, -1.37, 1.55), GRAD: (3.09, 2.02, 0),
    GRAD_SUM: (3.48, 1.71, 0.74), END_GRAD: (7.02, -2.12, 0), MID: (5.68, 0.86, 1.11),
    DOWN: (1.3, 0.36, 0), DOWN_SUM: (1.87, 1.35, 0.95), END_DOWN: (7.9, 2.17, 0),
    PRODUCTS: (7.5, 0, 0.4), WIDE: (-4, 0.05, 1.5),
}
TUNED = {
    (4, 4, 3): [
        2, 58, 7, 57, 4, 59, 8, 56, 5, 2, 8, 57, 58, 56, 8, 9, 3, 6, 59, 12,
        2, 16, 9, 58, 16, 10, 9, 57, 59, 56, 16, 13, 11, 17, 58, 57, 3, 10, 16, 17,
        56, 11, 59, 20, 10, 20, 17, 24, 28, 11, 14, 18, 3, 15, 28, 19, 18, 2, 17, 21,
        28, 21, 40, 44, 18, 19, 25, 32, 29, 36, 18, 22, 29, 19, 44, 22, 29, 26, 36, 30,
        44, 19, 3, 23, 33, 37, 30, 36, 23, 27, 37, 31, 30, 52, 37, 31, 34, 38, 42, 41,
        31, 38, 35, 39, 38, 52, 48, 39, 36, 37, 38, 52, 39, 43, 39,
    ],
}


def middle_order(n, levels):
    if (n, CHUNKS, levels) in TUNED:
        return [divmod(code, CHUNKS) for code in TUNED[n, CHUNKS, levels]]
    count = {k: 1 for k in DUE}
    count.update({COT: n, TWO: n, MID: n, ONE: n - 1, GRAD_SUM: n - 1, DOWN_SUM: n - 1, GLU: 2, PRODUCTS: 3, WIDE: levels + 1})
    needs = {
        ONE: [OUT], END_ONE: [ONE], TWO: [END_ONE], GLU: [TWO, COT], GRAD: [GLU], GRAD_SUM: [GRAD],
        END_GRAD: [GRAD_SUM], MID: [END_GRAD], DOWN: [GLU], DOWN_SUM: [DOWN], END_DOWN: [DOWN_SUM],
    }
    todo = sorted(
        (first + h * later + s * 3 / (n - 1) * each, k, h, s)
        for k, (first, later, each) in DUE.items()
        for h in range(CHUNKS)
        for s in range(count[k])
        if not (k == PRODUCTS and h > 0 or k == COT and h < FRONT or k in (DOWN_SUM, END_DOWN) and h >= DOWNS)
    )
    taken, order = {}, []
    while todo:
        for item in todo:
            _, k, h, s = item
            ready = taken.get((k, h), 0) == s and (
                k != PRODUCTS or all(taken.get((GLU, c), 0) == 2 for c in range(CHUNKS))
            )
            ready = ready and (
                k != GLU or all(taken.get((WIDE, c), 0) == levels + 1 for c in range(2 * PARTS))
            )
            ready = ready and all(
                taken.get((need, h), 0) == count[need] or (need == COT and h < FRONT)
                for need in needs.get(k, [])
            )
            if ready:
                break
        todo.remove(item)
        taken[k, h] = s + 1
        order.append((k, h))
    return order


def middle_kernel(
    n, m, gated, pack, out_weight, own, cot, cot_front, gain,
    mid_out, glu_out, product_out, down_out, outputs, middle_out, d_middle, gain_out,
    gated_v, wo_v, weights_v, own_v, cot_v, rows_v, hidden_v, glu_v, part, part_two,
    left_a, right_a, left_b, right_b, middle, stage, result, copy_sem, send_sem, recv_sem,
    wide_send, wide_recv,
):
    line = Line(n, send_sem, recv_sem)
    place = line.place
    count, width = own.shape
    piece = count // CHUNKS
    per = n * piece
    wide = hidden_v.shape[1]
    copies = []

    def local(src, dst):
        c = pltpu.make_async_copy(src, dst, copy_sem.at[len(copies)])
        copies.append(c)
        c.start()
        return c

    def rows_at(ref, h, k=0, size=piece):
        return ref.at[pl.ds(h * per + k * piece, size)]

    load_cot = [
        local(cot.at[pl.ds(h * piece, piece)], rows_at(cot_v, h)) for h in range(FRONT, CHUNKS)
    ]
    front = pl.ds(0, FRONT * per)
    load_cot.append(local(cot_front, cot_v.at[front]))
    load_gated = local(gated, gated_v)
    load_wo = local(
        out_weight.at[pl.ds(out_weight.shape[0] - wo_v.shape[0], wo_v.shape[0])], wo_v
    )
    load_own = local(own, own_v)
    load_pack = local(pack, own_columns(pack, weights_v))
    wg_v, wd_v = weights_v.at[pl.ds(0, 2 * wide)], weights_v.at[pl.ds(2 * wide, wide)]
    doubling, peers = weight_gather(m, pack, weights_v, wide_send, wide_recv)
    line.enter(["dp", peers])
    for h in range(CHUNKS):
        no_neighbour_zero(n, place, left_a.at[h, n - 2], right_a.at[h, n - 2])
    for h in range(DOWNS):
        no_neighbour_zero(n, place, left_b.at[h, n - 2], right_b.at[h, n - 2])
    gain_out[...] = jnp.zeros_like(gain_out)

    def scatter(buf, lefts, rights, h):
        return Scatter(
            line,
            lambda k: rows_at(buf, h, k),
            lambda s: lefts.at[h, s - 1],
            lambda s: rights.at[h, s - 1],
            add_into,
        )

    gather_cot = {
        h: Gather(line, functools.partial(rows_at, cot_v, h)) for h in range(FRONT, CHUNKS)
    }
    gather_two = [Gather(line, functools.partial(rows_at, rows_v, h)) for h in range(CHUNKS)]

    def mid_slot(h, k):
        return stage.at[h] if k == 0 else rows_at(mid_out, h, k)

    gather_mid = [Gather(line, functools.partial(mid_slot, h)) for h in range(CHUNKS)]
    scatter_one = [scatter(part, left_a, right_a, h) for h in range(CHUNKS)]
    scatter_two = [scatter(part_two, left_b, right_b, h) for h in range(DOWNS)]
    scatter_grad = [scatter(part, left_a, right_a, h) for h in range(CHUNKS)]

    def chunk(ref, h):
        return ref.at[pl.ds(h * per, per)]

    def out_product(h):
        heads, _, size = gated_v.shape
        target, whole = chunk(part, h), pl.ds(h * per, per)

        def step(j, carry):
            at = pl.ds(pl.multiple_of(j * 2 * LANES, 2 * LANES), 2 * LANES)
            target[:, at] = sum(
                dot_nn(gated_v[i, whole, :], wo_v[pl.ds(i * size, size), at]) for i in range(heads)
            ).astype(BF)
            return carry

        lax.fori_loop(0, width // (2 * LANES), step, 0)

    def finish_one(h):
        scatter_one[h].finish()

        def step(at):
            src = at(h * per)
            mine = at(h * piece)
            total = (
                own_v[mine, :].astype(F32)
                + part[src, :].astype(F32)
                + left_a[h, n - 2, at(), :].astype(F32)
                + right_a[h, n - 2, at(), :].astype(F32)
            )
            middle[mine, :] = total
            hat, _ = layer_norm(total, epsilon)
            rows_v[src, :] = (hat * gain[...]).astype(BF)

        blocks(piece, step)

    def glu_tiles(h, first, last):
        def step(j, carry):
            pair = pl.ds(pl.multiple_of(j * 2 * LANES, 2 * LANES), 2 * LANES)
            at = pl.ds(pl.multiple_of(j * LANES, LANES), LANES)
            whole = pl.ds(h * per, per)
            both = dot_nt(rows_v[whole, :], wg_v[pair, :])
            d_hidden = dot_nt(cot_v[whole, :], wd_v[at, :])
            u, up = both[:, :LANES], both[:, LANES:]
            c = 0.7978845608028654
            t = jnp.tanh(c * (u + 0.044715 * (u * u * u)))
            half = 0.5 * (1.0 + t)
            act = u * half
            slope = half + 0.5 * u * (1.0 - t * t) * (c * (1.0 + 3 * 0.044715 * (u * u)))
            hidden_v[whole, at] = (act * up).astype(BF)
            glu_v[whole, pair] = jnp.concatenate(
                [(d_hidden * up * slope).astype(BF), (d_hidden * act).astype(BF)], axis=1
            )
            return carry

        lax.fori_loop(first, last, step, 0)

    def grad_product(h):
        product_tiles(chunk(part, h), chunk(glu_v, h), wg_v, 2 * LANES)

    def down_product(h):
        product_tiles(chunk(part_two, h), chunk(hidden_v, h), wd_v, 2 * LANES)

    def finish_grad(h):
        scatter_grad[h].finish()

        def step(at):
            src = at(h * per)
            mine = at(h * piece)
            grad = (
                part[src, :].astype(F32)
                + left_a[h, n - 2, at(), :].astype(F32)
                + right_a[h, n - 2, at(), :].astype(F32)
            )
            hat, scale = layer_norm(middle[mine, :], epsilon)
            gain_out[...] += jnp.sum((hat * grad).reshape(BLOCK // 8, 8, width), axis=0)
            d_mid = cot_v[src, :].astype(F32) + norm_back(grad * gain[...], hat, scale)
            d_middle[mine, :] = d_mid
            stage[h, at(), :] = d_mid.astype(BF)

        blocks(piece, step)
        local(stage.at[h], rows_at(mid_out, h))

    def finish_two(h):
        scatter_two[h].finish()

        def step(at):
            src = at(h * per)
            mine = at(h * piece)
            outputs[mine, :] = (
                middle[mine, :]
                + part_two[src, :].astype(F32)
                + left_b[h, n - 2, at(), :].astype(F32)
                + right_b[h, n - 2, at(), :].astype(F32)
            ).astype(BF)

        blocks(piece, step)

    tiles = wide // LANES
    cut = tiles // 2

    def wait_for(items):
        for item in items:
            item.wait()
        items.clear()

    first_loads, own_load = [load_gated, load_wo], [load_own]
    later_loads = [load_pack]

    def out_action(h):
        wait_for(first_loads)
        out_product(h)

    def finish_one_action(h):
        wait_for(own_load)
        finish_one(h)

    def glu_action(h):
        wait_for(later_loads)
        assert all(item.done == len(bits_of(m)) + 1 for item in doubling)
        if h in begun:
            glu_tiles(h, cut, tiles)
        else:
            begun.add(h)
            glu_tiles(h, 0, cut)

    def grad_action(h):
        scatter_one[h].drain()
        grad_product(h)

    def products_action(_):
        k = len(products)
        if k >= 2:
            products[k - 2].wait()
        left = hidden_v.at[...] if k == 2 else glu_v.at[:, pl.ds(k * wide, wide)]
        right = cot_v if k == 2 else rows_v
        target = result.at[k % 2]

        def step(j, carry):
            at = pl.ds(pl.multiple_of(j * 2 * LANES, 2 * LANES), 2 * LANES)
            target[:, at] = dot_tn(left[...], right[:, at]).astype(BF)
            return carry

        lax.fori_loop(0, width // (2 * LANES), step, 0)
        place_out = product_out if k == 2 else glu_out.at[pl.ds(k * wide, wide)]
        store = pltpu.make_async_copy(target, place_out, copy_sem.at[spare + k])
        store.start()
        products.append(store)

    products, spare = [], copy_sem.shape[0] - 3
    begun = set()
    actions = {
        COT: lambda h: gather_cot[h].step(),
        OUT: out_action,
        ONE: lambda h: scatter_one[h].step(),
        END_ONE: finish_one_action,
        TWO: lambda h: gather_two[h].step(),
        GLU: glu_action,
        GRAD: grad_action,
        GRAD_SUM: lambda h: scatter_grad[h].step(),
        END_GRAD: finish_grad,
        MID: lambda h: gather_mid[h].step(),
        DOWN: down_product,
        DOWN_SUM: lambda h: scatter_two[h].step(),
        END_DOWN: finish_two,
        PRODUCTS: products_action,
        WIDE: lambda h: doubling[h].step(),
    }
    for item in load_cot:
        item.wait()
    for kind, h in middle_order(n, len(bits_of(m))):
        actions[kind](h)
    local(part_two.at[pl.ds(DOWNS * per, down_out.shape[0])], down_out)
    local(middle.at[pl.ds(DOWNS * piece, middle_out.shape[0])], middle_out)
    for item in list(gather_cot.values()) + gather_two + gather_mid:
        assert item.step_no == n
    for item in scatter_one + scatter_two + scatter_grad:
        assert item.step_no == n - 1
    for group in (scatter_grad, scatter_two):
        for item in group:
            item.drain()
    for item in copies[CHUNKS - FRONT + 5 :] + products[1:]:
        item.wait()
    assert len(products) == 3
    for item in doubling:
        item.leave()
    line.leave()


def middle_call(gated, pack, out_weight, own, cot, cot_front, gain, n, m):
    rows, width = own.shape
    heads, tokens, size = gated.shape
    nv = heads * size
    wide = pack.shape[0] // 3
    piece = rows // CHUNKS
    back = CHUNKS - DOWNS
    sems = CHUNKS * 5 * 2 * (n - 1)
    hop = (CHUNKS, n - 1, piece, width)
    shape = jax.ShapeDtypeStruct
    return pl.pallas_call(
        functools.partial(middle_kernel, n, m),
        out_shape=(
            shape((tokens, width), BF),
            shape((2 * wide, width), BF),
            shape((wide, width), BF),
            shape((back * n * piece, width), BF),
            shape((DOWNS * piece, width), BF),
            shape((back * piece, width), F32),
            shape((rows, width), F32),
            shape((8, width), F32),
        ),
        in_specs=[ANY, VM] + [ANY] * 4 + [VM],
        out_specs=(ANY,) * 4 + (VM, ANY, VM, VM),
        scratch_shapes=[
            pltpu.VMEM((heads, tokens, size), BF),
            pltpu.VMEM((nv, width), BF),
            pltpu.VMEM((3 * wide, width), BF),
            pltpu.VMEM((rows, width), BF),
            pltpu.VMEM((tokens, width), BF),
            pltpu.VMEM((tokens, width), BF),
            pltpu.VMEM((tokens, wide), BF),
            pltpu.VMEM((tokens, 2 * wide), BF),
            pltpu.VMEM((tokens, width), BF),
            pltpu.VMEM((tokens, width), BF),
            pltpu.VMEM(hop, BF),
            pltpu.VMEM(hop, BF),
            pltpu.VMEM((DOWNS,) + hop[1:], BF),
            pltpu.VMEM((DOWNS,) + hop[1:], BF),
            pltpu.VMEM((rows, width), F32),
            pltpu.VMEM((CHUNKS, piece, width), BF),
            pltpu.VMEM((2, wide, width), BF),
            pltpu.SemaphoreType.DMA((11 + 2 * CHUNKS - FRONT,)),
            pltpu.SemaphoreType.DMA((sems,)),
            pltpu.SemaphoreType.DMA((sems,)),
            pltpu.SemaphoreType.DMA((2 * PARTS * (m - 1),)),
            pltpu.SemaphoreType.DMA((2 * PARTS * (m - 1),)),
        ],
        compiler_params=pltpu.CompilerParams(
            collective_id=1, has_side_effects=True, vmem_limit_bytes=VMEM_MOST
        ),
        name="middle",
    )(gated, pack, out_weight, own, cot, cot_front, gain)


class Halving:
    def __init__(self, grads, rows, bits, base, kept, held, out, send_sem, recv_sem, load_sem):
        self.d = lax.axis_index("dp")
        self.grads, self.rows, self.bits, self.base = grads, rows, bits, base
        self.kept, self.held, self.out = kept, held, out
        self.send_sem, self.recv_sem, self.load_sem = send_sem, recv_sem, load_sem
        self.shard = out.shape[1]
        self.masks = [0]
        for bit in bits[:0:-1]:
            self.masks += [k + bit for k in self.masks]
        self.done, self.sent, self.loads = 0, [], []

    def flip(self, d, mask):
        for bit in self.bits:
            if mask & bit:
                d = d + bit * (1 - 2 * (lax.div(d, bit) % 2))
        return d

    def block(self, d):
        return self.grads.at[self.rows, pl.ds(pl.multiple_of(d * self.shard, self.shard), self.shard)]

    def count(self, level):
        return 1 << (len(self.bits) - 1 - level)

    def copies(self, level):
        bit = self.bits[level]
        partner = self.flip(self.d, bit)
        out = []
        for i in range(self.count(level)):
            if level == 0:
                src = self.block(self.flip(partner, self.masks[i]))
            else:
                src = self.kept.at[self.count(level) + i, self.rows]
            index = self.base + len(out) + sum(self.count(k) for k in range(level))
            out.append(
                pltpu.make_async_remote_copy(
                    src_ref=src,
                    dst_ref=self.held[level].at[i, self.rows],
                    send_sem=self.send_sem.at[index],
                    recv_sem=self.recv_sem.at[index],
                    device_id={"dp": partner},
                    device_id_type=MESH,
                )
            )
        return out

    def load(self):
        for i, mask in enumerate(self.masks):
            c = pltpu.make_async_copy(
                self.block(self.flip(self.d, mask)), self.kept.at[i, self.rows], self.load_sem.at[i]
            )
            c.start()
            self.loads.append(c)

    def add(self, level):
        last = level == len(self.bits) - 1
        start, size = self.rows.start, self.rows.size
        for i in range(self.count(level)):

            def step(at):
                total = self.kept[i, at(start), :].astype(F32) + self.held[level][
                    i, at(start), :
                ].astype(F32)
                if last:
                    self.out[at(start), :] = total
                else:
                    self.kept[i, at(start), :] = total.astype(BF)

            blocks(size, step)

    def step(self):
        level = self.done
        if level > 0:
            for c in self.loads:
                c.wait()
            self.loads = []
            for c in self.sent[-1]:
                c.wait_recv()
            self.add(level - 1)
        if level < len(self.bits):
            out = self.copies(level)
            for c in out:
                c.start()
            self.sent.append(out)
        self.done += 1

    def leave(self):
        for group in self.sent:
            for c in group:
                c.wait_send()


def grad_scatter(m, grads, kept, held, summed, send_sem, recv_sem, load_sem):
    bits = bits_of(m)
    height = grads.shape[0] // (2 * PARTS)
    out = []
    for i in range(2 * PARTS):
        order = bits[:1] + (bits[1:] if i % 2 == 0 else bits[:0:-1])
        rows = pl.ds(i * height, height)
        out.append(
            Halving(
                grads, rows, order, i * (m - 1), kept, held, summed, send_sem, recv_sem, load_sem.at[i]
            )
        )
    return out, [out[0].flip(out[0].d, bit) for bit in bits]


def scatter_scratch(m, rows, shard):
    wide = 2 * PARTS * (m - 1)
    counts = [m // 2] + [m >> (1 + k) for k in range(len(bits_of(m)))]
    return [pltpu.VMEM((count, rows, shard), BF) for count in counts] + [
        pltpu.VMEM((rows, shard), F32),
        pltpu.SemaphoreType.DMA((wide,)),
        pltpu.SemaphoreType.DMA((wide,)),
        pltpu.SemaphoreType.DMA((2 * PARTS, m // 2)),
    ]


class Exchange:
    def __init__(self, groups, mine, total, send_sem, recv_sem):
        self.groups, self.source, self.total = groups, mine, total
        self.send_sem, self.recv_sem = send_sem, recv_sem
        self.done, self.base, self.sent = 0, 0, []

    def copy(self, k, slot):
        axis, size, held = self.groups[self.done]
        return pltpu.make_async_remote_copy(
            src_ref=self.source,
            dst_ref=held.at[slot],
            send_sem=self.send_sem.at[self.base + k],
            recv_sem=self.recv_sem.at[self.base + k],
            device_id={axis: lax.rem(lax.axis_index(axis) + k, size)},
            device_id_type=MESH,
        )

    def send(self):
        axis, size, held = self.groups[self.done]
        me = lax.axis_index(axis)
        held[me] = self.source[...]
        self.sent = [self.copy(k, me) for k in range(1, size)]
        for c in self.sent:
            c.start()

    def receive(self):
        axis, size, held = self.groups[self.done]
        me = lax.axis_index(axis)
        for k in range(1, size):
            self.copy(k, lax.rem(me - k + size, size)).wait_recv()
        value = held[0]
        for k in range(1, size):
            value = value + held[k]
        for c in self.sent:
            c.wait_send()
        self.total[...] = value
        self.source, self.base, self.done = self.total, self.base + size, self.done + 1


def last_kernel(
    n, m, d_qk, d_value, d_gate, weight, grads, inputs, gain, d_middle, second_gain, rows,
    out, gains, grad_query, grad_key, grad_out, grad_gate, grad_value,
    qk_v, value_v, gate_v, weight_v, inputs_v, middle_v, part, lefts, rights, *rest
):
    bits = bits_of(m)
    kept, held = rest[0], rest[1 : 1 + len(bits)]
    summed, wide_send, wide_recv, load_sem = rest[1 + len(bits) : 5 + len(bits)]
    gain_sum, mine, first, second, rows_v = rest[5 + len(bits) : 10 + len(bits)]
    copy_sem, send_sem, recv_sem, gain_send, gain_recv = rest[10 + len(bits) :]
    line = Line(n, send_sem, recv_sem)
    count, width = out.shape
    piece = count // CHUNKS
    per = n * piece
    heads, _, size = value_v.shape
    wide = qk_v.shape[1]
    load = [
        pltpu.make_async_copy(src, dst, copy_sem.at[i])
        for i, (src, dst) in enumerate(
            [
                (weight.at[pl.ds(0, weight_v.shape[0])], weight_v), (d_qk, qk_v),
                (d_value, value_v), (d_gate, gate_v), (rows, rows_v), (inputs, inputs_v),
                (d_middle, middle_v),
            ]
        )
    ]
    for item in load:
        item.start()
    barrier = pltpu.get_barrier_semaphore()
    for axis, extent in (("dp", m), ("mp", n)):
        me = lax.axis_index(axis)
        for k in range(1, extent):
            peer = lax.rem(me + k, extent)
            pl.semaphore_signal(barrier, inc=1, device_id={axis: peer}, device_id_type=MESH)
    pl.semaphore_wait(barrier, n + m - 2)

    halving, _ = grad_scatter(m, grads, kept, held, summed, wide_send, wide_recv, load_sem)
    for item in halving:
        item.step()
    for item in halving:
        item.load()
    for h in range(CHUNKS):
        no_neighbour_zero(n, line.place, lefts.at[h, n - 2], rights.at[h, n - 2])
    gain_sum[...] = jnp.zeros_like(gain_sum)
    scatters = [
        Scatter(
            line,
            lambda k, h=h: part.at[pl.ds(h * per + k * piece, piece)],
            lambda s, h=h: lefts.at[h, s - 1],
            lambda s, h=h: rights.at[h, s - 1],
            add_into,
        )
        for h in range(CHUNKS)
    ]

    def product(h):
        rows = pl.ds(h * per, per)

        def step(j, carry):
            at = pl.ds(pl.multiple_of(j * 2 * LANES, 2 * LANES), 2 * LANES)
            total = dot_nn(qk_v[rows, :], weight_v[pl.ds(0, wide), at])
            for i in range(heads):
                base = wide + i * size
                total += dot_nn(value_v[i, rows, :], weight_v[pl.ds(base, size), at])
                base += heads * size
                total += dot_nn(gate_v[i, rows, :], weight_v[pl.ds(base, size), at])
            part[rows, at] = total.astype(BF)
            return carry

        lax.fori_loop(0, width // (2 * LANES), step, 0)

    def finish(h):
        scatters[h].finish()

        def step(at):
            own = at(h * piece)
            grad = (
                part[at(h * per), :].astype(F32)
                + lefts[h, n - 2, at(), :].astype(F32)
                + rights[h, n - 2, at(), :].astype(F32)
            )
            hat, scale = layer_norm(inputs_v[own, :].astype(F32), epsilon)
            out[own, :] = middle_v[own, :] + norm_back(grad * gain[...], hat, scale)

        blocks(piece, step)

    def gain_part(h):
        def step(at):
            here = at(h * per)
            term = rows_v[here, :].astype(F32) * part[here, :].astype(F32)
            gain_sum[...] += jnp.sum(term.reshape(BLOCK // 8, 8, width), axis=0)

        blocks(per, step)

    for item in load[:5]:
        item.wait()
    for h in range(CHUNKS):
        product(h)
        scatters[h].step()
        gain_part(h)
    flats = (
        jnp.sum(gain_sum[...], axis=0, keepdims=True) / gain[...],
        jnp.sum(second_gain[...], axis=0, keepdims=True),
    )
    for i, flat in enumerate(flats):
        for j in range(width // LANES):
            mine[pl.ds(i * (width // LANES) + j, 1), :] = flat[:, j * LANES : (j + 1) * LANES]
    total_gain = Exchange(
        [("dp", m, first), ("mp", n, second)], mine, gains, gain_send, gain_recv
    )
    total_gain.send()
    for item in load[5:]:
        item.wait()
    for s in range(n - 2):
        if s == 1:
            total_gain.receive()
            total_gain.send()
        for h in range(CHUNKS):
            if s < len(bits) and h < len(halving):
                halving[h].step()
            scatters[h].step()
    while halving[0].done < len(bits):
        for item in halving:
            item.step()
    for h in range(CHUNKS):
        finish(h)
    for item in halving:
        while item.done <= len(bits):
            item.step()
    stores, base = [], 0
    for target in (grad_out, grad_gate):
        source = summed.at[pl.ds(base, target.shape[0])]
        stores.append(pltpu.make_async_copy(source, target, copy_sem.at[len(load) + len(stores)]))
        base += target.shape[0]
    deep = grad_query.shape[1]
    value_base = base + 2 * deep
    source = summed.at[pl.ds(value_base, grad_value.shape[0])]
    stores.append(pltpu.make_async_copy(source, grad_value, copy_sem.at[len(load) + len(stores)]))
    for store in stores:
        store.start()
    for target in (grad_query, grad_key):
        for j in range(deep // LANES):
            target[:, j * LANES : (j + 1) * LANES] = summed[pl.ds(base, LANES), :].T
            base += LANES
    total_gain.receive()
    for item in halving:
        item.leave()
    for store in stores:
        store.wait()
    for h in range(CHUNKS):
        scatters[h].drain()


def last_call(
    d_qk, d_value, d_gate, weight, grads, inputs, gain, d_middle, second_gain, rows_one, n, m
):
    tokens = d_qk.shape[0]
    rows, width = inputs.shape
    heads = d_value.shape[0]
    shard = width // m
    sems = CHUNKS * 2 * (n - 1)
    hop = (CHUNKS, n - 1, rows // CHUNKS, width)
    flat = (2 * width // LANES, LANES)
    shape = jax.ShapeDtypeStruct
    return pl.pallas_call(
        functools.partial(last_kernel, n, m),
        out_shape=(
            shape((rows, width), F32),
            shape(flat, F32),
            shape((shard, heads * HK), F32),
            shape((shard, heads * HK), F32),
        )
        + (shape((heads * HV, shard), F32),) * 3,
        in_specs=[ANY] * 6 + [VM, ANY, VM, ANY],
        out_specs=(VM,) * 4 + (ANY,) * 3,
        scratch_shapes=[
            pltpu.VMEM(d_qk.shape, BF),
            pltpu.VMEM(d_value.shape, BF),
            pltpu.VMEM(d_gate.shape, BF),
            pltpu.VMEM((2 * heads * (HK + HV), width), BF),
            pltpu.VMEM((rows, width), BF),
            pltpu.VMEM((rows, width), F32),
            pltpu.VMEM((tokens, width), BF),
            pltpu.VMEM(hop, BF),
            pltpu.VMEM(hop, BF),
        ]
        + scatter_scratch(m, grads.shape[0], shard)
        + [
            pltpu.VMEM((8, width), F32),
            pltpu.VMEM(flat, F32),
            pltpu.VMEM((m,) + flat, F32),
            pltpu.VMEM((n,) + flat, F32),
            pltpu.VMEM((tokens, width), BF),
            pltpu.SemaphoreType.DMA((10,)),
            pltpu.SemaphoreType.DMA((sems,)),
            pltpu.SemaphoreType.DMA((sems,)),
            pltpu.SemaphoreType.DMA((n + m,)),
            pltpu.SemaphoreType.DMA((n + m,)),
        ],
        compiler_params=pltpu.CompilerParams(
            collective_id=2, has_side_effects=True, vmem_limit_bytes=VMEM_MOST
        ),
        name="last",
    )(d_qk, d_value, d_gate, weight, grads, inputs, gain, d_middle, second_gain, rows_one)


TILE = 256


def tiles_of(count, step, start=None):
    def run(i, carry):
        step(pl.ds(pl.multiple_of(i * TILE, TILE), TILE))
        return carry

    if start is None:
        lax.fori_loop(0, count // TILE, run, 0)
    else:
        lax.fori_loop(start, start + count, run, 0)


def in_order(units, steps):
    taken = 0
    for i, unit in enumerate(units):
        unit()
        upto = (i + 1) * len(steps) // len(units)
        for step in steps[taken:upto]:
            step()
        taken = upto


def forward_kernel(
    n, m, own, pack, cot, col, row,
    rows_o, weight_o, query_o, key_o, value_o, gate_o, norm_o, scale_o, scores_o, gated_o, cot_o,
    rows_v, weight_v, both_v, value_v, gate_v, norm_v, scale_v, scores_v, gated_v, cot_v,
    copy_sem, send_sem, recv_sem, wide_send, wide_recv,
):
    line = Line(n, send_sem, recv_sem)
    heads, tokens, size = value_v.shape
    deep = both_v.shape[2]
    per = cot_v.shape[0] // FRONT
    piece = per // n
    copies = []

    def local(src, dst):
        c = pltpu.make_async_copy(src, dst, copy_sem.at[len(copies)])
        copies.append(c)
        c.start()
        return c

    doubling, peers = weight_gather(m, pack, weight_v, wide_send, wide_recv)
    line.enter(["dp", peers])

    def row_slot(h, k):
        if k == 0:
            return own.at[pl.ds(h * piece, piece)]
        return rows_v.at[pl.ds(h * per + k * piece, piece)]

    def cot_slot(h, k):
        return cot_v.at[pl.ds(h * per + k * piece, piece)]

    gathers = [Gather(line, functools.partial(row_slot, h)) for h in range(CHUNKS)]
    cots = [Gather(line, functools.partial(cot_slot, h)) for h in range(FRONT)]
    half = CHUNKS // 2
    levels = len(bits_of(m))

    def go(items):
        for item in items:
            item.step()

    def project(target, first, last, base, width, start, count):
        def step(at):
            def one(j, carry):
                rows = pl.ds(pl.multiple_of(base + j * width, BLOCK), width)
                target[j, at, :] = dot_nt(rows_v[at, :], weight_v[rows, :]).astype(target.dtype)
                return carry

            lax.fori_loop(first, last, one, 0)

        return lambda: tiles_of(count, step, start)

    def attend(h):
        def step(at):
            allowed = (col[at, 0:1] >= row[0:1, :]) & (col[at, 1:2] == row[1:2, :])
            scores = dot_nt(both_v[h, at, :], both_v[heads + h]) * col[at, 2 + h : 3 + h]
            scores = jnp.where(allowed, scores * row[2 + h : 3 + h, :], 0.0).astype(BF)
            scores_v[h, at, :] = scores
            hat, scale = layer_norm(dot_nn(scores, value_v[h]), group_epsilon)
            norm_v[h, at, :] = hat
            scale_v[h, at, :] = scale
            gate = gate_v[h, at, :]
            gated_v[h, at, :] = (gate * jax.nn.sigmoid(gate) * hat).astype(BF)

        return lambda: tiles_of(tokens, step)

    values, gates = 2 * heads * deep, 2 * heads * deep + heads * size
    assert values <= PARTS * (weight_v.shape[0] // (2 * PARTS))
    near, far = gathers[:half], gathers[half:]
    soon, later = doubling[:PARTS], doubling[PARTS:]
    go(near)
    go(soon)
    for h in range(CHUNKS):
        local(row_slot(h, 0), rows_v.at[pl.ds(h * per, piece)])
    local(pack, own_columns(pack, weight_v))
    for h in range(FRONT):
        local(cot.at[pl.ds(h * piece, piece)], cot_slot(h, 0))
    first_copies = list(copies)
    go(near)
    go(soon)
    go(later)
    for _ in range(n - 3):
        go(near)
    go(far)
    for _ in range(levels - 1):
        go(soon)
    go(near)
    for item in first_copies:
        item.wait()
    tail = [g.step for _ in range(n - 2) for g in far]
    tail_wide = [g.step for _ in range(levels - 1) for g in later]
    mixed = []
    for i in range(max(len(tail), len(tail_wide))):
        mixed += tail[i : i + 1] + tail_wide[i : i + 1]
    early = tokens // 2 // TILE
    in_order(
        [
            project(both_v, 0, 2 * heads, 0, deep, t, 1)
            for t in range(early)
        ],
        mixed,
    )
    go(cots)
    go(later)
    go(far)
    units = [
        project(both_v, 0, 2 * heads, 0, deep, early, early),
        project(value_v, 0, heads, values, size, 0, 2 * early),
        project(gate_v, 0, heads, gates, size, 0, early),
        project(gate_v, 0, heads, gates, size, early, early),
    ] + [attend(h) for h in range(heads)]
    count = len(copies)
    local(rows_v, rows_o)
    local(weight_v, weight_o)
    in_order(units, [g.step for _ in range(n - 1) for g in cots])
    for src, dst in (
        (both_v.at[pl.ds(0, heads)], query_o), (both_v.at[pl.ds(heads, heads)], key_o),
        (value_v, value_o), (gate_v, gate_o), (norm_v, norm_o), (scale_v, scale_o),
        (scores_v, scores_o), (gated_v, gated_o), (cot_v, cot_o),
    ):
        local(src, dst)
    for item in copies[count:]:
        item.wait()
    for item in gathers + cots:
        assert item.step_no == n
    for item in doubling:
        assert item.done == levels + 1
        item.leave()
    line.leave()


def forward_call(own, pack, cot, col, row, n, m, heads):
    rows, width = own.shape
    tokens = n * rows
    shape = jax.ShapeDtypeStruct
    outs = (
        shape((tokens, width), BF),
        shape((pack.shape[0], m * pack.shape[1]), BF),
        shape((heads, tokens, HK), BF),
        shape((heads, tokens, HK), BF),
        shape((heads, tokens, HV), BF),
        shape((heads, tokens, HV), F32),
        shape((heads, tokens, HV), F32),
        shape((heads, tokens, 1), F32),
        shape((heads, tokens, tokens), BF),
        shape((heads, tokens, HV), BF),
        shape((tokens * FRONT // CHUNKS, width), BF),
    )
    held = outs[:2] + (shape((2 * heads, tokens, HK), BF),) + outs[4:]
    sems = (CHUNKS + FRONT) * 2 * (n - 1)
    wide = 2 * PARTS * (m - 1)
    return pl.pallas_call(
        functools.partial(forward_kernel, n, m),
        out_shape=outs,
        in_specs=[VM, VM, ANY, VM, VM],
        out_specs=(ANY,) * len(outs),
        scratch_shapes=[pltpu.VMEM(o.shape, o.dtype) for o in held]
        + [
            pltpu.SemaphoreType.DMA((CHUNKS + FRONT + 1 + len(outs),)),
            pltpu.SemaphoreType.DMA((sems,)),
            pltpu.SemaphoreType.DMA((sems,)),
            pltpu.SemaphoreType.DMA((wide,)),
            pltpu.SemaphoreType.DMA((wide,)),
        ],
        compiler_params=pltpu.CompilerParams(
            collective_id=4, has_side_effects=True, vmem_limit_bytes=VMEM_MOST
        ),
        name="forward",
    )(own, pack, cot, col, row)


def backward_kernel(
    n, m, mid, weights, gate, norm, scale, scores, query, key, value, down, middle, grads, col, row,
    qk_o, value_o, gate_o, glu_gate_o, glu_up_o, outputs,
    mid_v, wo_v, gate_v, norm_v, scale_v, scores_v, query_v, key_v, value_v, part, middle_v,
    d_qk, d_value, d_gate, d_kept, d_scores, lefts, rights, *rest
):
    bits = bits_of(m)
    kept, held = rest[0], rest[1 : 1 + len(bits)]
    summed, wide_send, wide_recv, load_sem = rest[1 + len(bits) : 5 + len(bits)]
    copy_sem, send_sem, recv_sem = rest[5 + len(bits) :]
    line = Line(n, send_sem, recv_sem)
    heads, tokens, deep = query_v.shape
    size = value_v.shape[2]
    back = CHUNKS - DOWNS - ENDS
    per = part.shape[0] // back
    piece = per // n
    copies = []

    def local(src, dst):
        c = pltpu.make_async_copy(src, dst, copy_sem.at[len(copies)])
        copies.append(c)
        c.start()
        return c

    load_part = local(down.at[pl.ds(0, part.shape[0])], part)
    loads = [
        local(src, dst)
        for src, dst in (
            (mid, mid_v), (weights.at[pl.ds(weights.shape[0] - wo_v.shape[0], wo_v.shape[0])], wo_v),
            (gate, gate_v), (norm, norm_v), (scale, scale_v), (value, value_v), (key, key_v),
            (query, query_v), (scores, scores_v),
            (middle.at[pl.ds(0, middle_v.shape[0])], middle_v),
        )
    ]
    halving, peers = grad_scatter(m, grads, kept, held, summed, wide_send, wide_recv, load_sem)
    line.enter(["dp", peers])
    for item in halving:
        item.step()
    for item in halving:
        item.load()
    for h in range(back):
        no_neighbour_zero(n, line.place, lefts.at[h, n - 2], rights.at[h, n - 2])
    scatters = [
        Scatter(
            line,
            lambda k, h=h: part.at[pl.ds(h * per + k * piece, piece)],
            lambda s, h=h: lefts.at[h, s - 1],
            lambda s, h=h: rights.at[h, s - 1],
            add_into,
        )
        for h in range(back)
    ]
    load_part.wait()
    for item in scatters:
        item.step()
    for item in loads:
        item.wait()

    def gates(h):
        def step(at):
            grad = dot_nt(mid_v[at, :], wo_v[pl.ds(h * size, size), :])
            pre, hat = gate_v[h, at, :], norm_v[h, at, :]
            s = jax.nn.sigmoid(pre)
            d_gate[h, at, :] = (grad * hat * (s + pre * s * (1.0 - s))).astype(BF)
            d_kept[h, at, :] = norm_back(grad * (pre * s), hat, scale_v[h, at, :]).astype(BF)

        return lambda: tiles_of(tokens, step)

    def by_row(h):
        def step(at):
            allowed = (col[at, 0:1] >= row[0:1, :]) & (col[at, 1:2] == row[1:2, :])
            grad = dot_nt(d_kept[h, at, :], value_v[h]) * col[at, 2 + h : 3 + h]
            grad = jnp.where(allowed, grad * row[2 + h : 3 + h, :], 0.0).astype(BF)
            d_scores[at, :] = grad
            d_qk[at, pl.ds(h * deep, deep)] = dot_nn(grad, key_v[h]).astype(BF)

        return lambda: tiles_of(tokens, step)

    def by_column(h):
        def step(at):
            d_value[h, at, :] = dot_tn(scores_v[h, :, at], d_kept[h]).astype(BF)
            d_qk[at, pl.ds((heads + h) * deep, deep)] = dot_tn(d_scores[:, at], query_v[h]).astype(
                BF
            )

        return lambda: tiles_of(tokens, step)

    units = []
    for h in range(heads):
        units += [gates(h), by_row(h), by_column(h)]
    steps = [item.step for _ in range(n - 2) for item in scatters]
    wide_steps = [item.step for _ in bits for item in halving]
    mixed = []
    for i in range(max(len(steps), len(wide_steps))):
        mixed += steps[i : i + 1] + wide_steps[i : i + 1]
    late = mixed[-2 * PARTS :]
    in_order(units, mixed[: -2 * PARTS])
    count = len(copies)
    local(d_qk, qk_o)
    local(d_value, value_o)
    local(d_gate, gate_o)
    for step in late:
        step()
    size = glu_up_o.shape[0]
    wide = grads.shape[0] // 2
    for t in range(wide // LANES):
        have = min(LANES, size - t * LANES)
        for i, target in enumerate((glu_gate_o, glu_up_o)):
            local(
                summed.at[pl.ds((2 * t + i) * LANES, have)], target.at[pl.ds(t * LANES, have)]
            )
    for item in halving:
        assert item.done == len(bits) + 1
        item.leave()
    for h in range(back):
        scatters[h].finish()

        def step(at):
            outputs[at(h * piece), :] = (
                middle_v[at(h * piece), :]
                + part[at(h * per), :].astype(F32)
                + lefts[h, n - 2, at(), :].astype(F32)
                + rights[h, n - 2, at(), :].astype(F32)
            ).astype(BF)

        blocks(piece, step)
    for item in copies[count:]:
        item.wait()
    for item in scatters:
        item.drain()


def backward_call(mid, weights, gate, norm, scale, scores, query, key, value, down, middle, grads, size_two, col, row, n, m):
    tokens, width = mid.shape
    heads, _, size = value.shape
    back = CHUNKS - DOWNS - ENDS
    nv = heads * size
    shard = width // m
    piece = tokens // n // CHUNKS
    shape = jax.ShapeDtypeStruct
    outs = (
        shape((tokens, 2 * heads * HK), BF),
        shape(value.shape, BF),
        shape(value.shape, BF),
    ) + (shape((size_two, shard), F32),) * 2 + (shape((back * piece, width), BF),)
    ins = (gate, norm, scale, scores, query, key, value, down, middle)
    hop = (back, n - 1, piece, width)
    sems = back * 2 * (n - 1)
    return pl.pallas_call(
        functools.partial(backward_kernel, n, m),
        out_shape=outs,
        in_specs=[ANY] * 12 + [VM] * 2,
        out_specs=(ANY,) * 5 + (VM,),
        scratch_shapes=[pltpu.VMEM(mid.shape, BF), pltpu.VMEM((nv, width), BF)]
        + [pltpu.VMEM(a.shape, a.dtype) for a in ins[:-2]]
        + [pltpu.VMEM((back * n * piece, width), BF), pltpu.VMEM((back * piece, width), F32)]
        + [pltpu.VMEM(o.shape, o.dtype) for o in outs[:3]]
        + [
            pltpu.VMEM(value.shape, BF),
            pltpu.VMEM((tokens, tokens), BF),
            pltpu.VMEM(hop, BF),
            pltpu.VMEM(hop, BF),
        ]
        + scatter_scratch(m, grads.shape[0], shard)
        + [
            pltpu.SemaphoreType.DMA((15 + grads.shape[0] // LANES,)),
            pltpu.SemaphoreType.DMA((sems,)),
            pltpu.SemaphoreType.DMA((sems,)),
        ],
        compiler_params=pltpu.CompilerParams(
            collective_id=5, has_side_effects=True, vmem_limit_bytes=VMEM_MOST
        ),
        name="backward",
    )(mid, weights, *ins, grads, col, row)


def products_kernel(n, m, plan, arrays, *refs):
    ins, (down, middle, grads) = refs[:arrays], refs[arrays : arrays + 3]
    out, down_o, outputs = refs[arrays + 3 : arrays + 6]
    held_in = refs[arrays + 6 : 2 * arrays + 6]
    part, middle_v, lefts, rights, result, kept, *rest = refs[2 * arrays + 6 :]
    bits = bits_of(m)
    held = rest[: len(bits)]
    summed, wide_send, wide_recv, load_sem, copy_sem, send_sem, recv_sem = rest[len(bits) :]
    line = Line(n, send_sem, recv_sem)
    count, width = outputs.shape
    piece = count // ENDS
    per = n * piece
    sources = list(zip(ins, held_in))
    sources.append((middle.at[pl.ds(middle.shape[0] - count, count)], middle_v))
    sources.append((down.at[pl.ds(down.shape[0] - n * count, n * count)], part))
    loads = [pltpu.make_async_copy(a, b, copy_sem.at[i]) for i, (a, b) in enumerate(sources)]
    for item in loads[::-1]:
        item.start()
    halving, peers = grad_scatter(m, grads, kept, held, summed, wide_send, wide_recv, load_sem)
    line.enter(["dp", peers])
    for item in halving:
        item.step()
    for item in halving:
        item.load()
    for h in range(ENDS):
        no_neighbour_zero(n, line.place, lefts.at[h, n - 2], rights.at[h, n - 2])
    scatters = [
        Scatter(
            line,
            lambda k, h=h: part.at[pl.ds(h * per + k * piece, piece)],
            lambda s, h=h: lefts.at[h, s - 1],
            lambda s, h=h: rights.at[h, s - 1],
            add_into,
        )
        for h in range(ENDS)
    ]
    loads[-1].wait()
    for item in scatters:
        item.step()
    waited, stores = set(), []

    def product(left, head, start, size, right, base):
        def run():
            for i in (left, right):
                if i not in waited:
                    loads[i].wait()
                    waited.add(i)
            target = pl.ds(base, size)

            def step(j, carry):
                at = pl.ds(pl.multiple_of(j * 4 * LANES, 4 * LANES), 4 * LANES)
                source = (
                    held_in[left][:, pl.ds(start, size)] if head is None else held_in[left][head]
                )
                result[target, at] = dot_tn(source, held_in[right][:, at]).astype(BF)
                return carry

            lax.fori_loop(0, width // (4 * LANES), step, 0)
            store(target)

        return run

    def store(target):
        c = pltpu.make_async_copy(
            result.at[target], out.at[target], copy_sem.at[len(loads) + len(stores)]
        )
        c.start()
        stores.append(c)

    units, base = [], 0
    for item in plan:
        units.append(product(*item, base))
        base += item[3]
    steps = [item.step for _ in range(n - 2) for item in scatters]
    wide_steps = [item.step for _ in bits for item in halving]
    mixed = []
    for i in range(max(len(steps), len(wide_steps))):
        mixed += steps[i : i + 1] + wide_steps[i : i + 1]
    in_order(units, mixed)
    spare = result.shape[0] - base
    if spare:
        result[pl.ds(base, spare), :] = jnp.zeros((spare, width), BF)
        store(pl.ds(base, spare))
    keep = pltpu.make_async_copy(
        summed.at[pl.ds(0, down_o.shape[0])], down_o, copy_sem.at[len(loads) + len(stores)]
    )
    keep.start()
    loads[-2].wait()
    for h in range(ENDS):
        scatters[h].finish()

        def step(at):
            outputs[at(h * piece), :] = (
                middle_v[at(h * piece), :]
                + part[at(h * per), :].astype(F32)
                + lefts[h, n - 2, at(), :].astype(F32)
                + rights[h, n - 2, at(), :].astype(F32)
            ).astype(BF)

        blocks(piece, step)
    for item in halving:
        assert item.done == len(bits) + 1
        item.leave()
    for item in scatters:
        item.drain()
    for item in stores + [keep]:
        item.wait()


def products_call(plan, arrays, down, middle, grads, size_two, rows, n, m):
    width = grads.shape[1]
    shard = width // m
    piece = arrays[1].shape[0] // n // CHUNKS
    sems = ENDS * 2 * (n - 1)
    hop = (ENDS, n - 1, piece, width)
    shape = jax.ShapeDtypeStruct
    return pl.pallas_call(
        functools.partial(products_kernel, n, m, plan, len(arrays)),
        out_shape=(
            shape((rows, width), BF), shape((size_two, shard), F32), shape((ENDS * piece, width), BF),
        ),
        in_specs=[ANY] * (len(arrays) + 3),
        out_specs=(ANY, ANY, VM),
        scratch_shapes=[pltpu.VMEM(a.shape, a.dtype) for a in arrays]
        + [
            pltpu.VMEM((ENDS * n * piece, width), BF),
            pltpu.VMEM((ENDS * piece, width), F32),
            pltpu.VMEM(hop, BF),
            pltpu.VMEM(hop, BF),
            pltpu.VMEM((rows, width), BF),
        ]
        + scatter_scratch(m, grads.shape[0], shard)
        + [
            pltpu.SemaphoreType.DMA((len(arrays) + len(plan) + 4,)),
            pltpu.SemaphoreType.DMA((sems,)),
            pltpu.SemaphoreType.DMA((sems,)),
        ],
        compiler_params=pltpu.CompilerParams(
            collective_id=3, has_side_effects=True, vmem_limit_bytes=VMEM_MOST
        ),
        name="products",
    )(*arrays, down, middle, grads)


def pad_rows(array, count):
    return jnp.pad(array, ((0, count - array.shape[0]), (0, 0)))


def pad_columns(array, count):
    return jnp.pad(array, ((0, 0), (0, count - array.shape[1])))


def body(
    inputs,
    segments,
    first_norm_gain,
    w_query,
    w_key,
    w_value,
    w_gate,
    w_out,
    second_norm_gain,
    w_glu_gate,
    w_glu_up,
    w_down,
    cotangent,
):
    n = lax.axis_size("mp")
    place = lax.axis_index("mp")
    heads = H // n
    head_start = place * heads
    rows, width = inputs.shape
    shard = w_query.shape[0]
    piece = rows // CHUNKS
    nk, nv, nf = heads * HK, heads * HV, w_down.shape[0]
    f_wide = -(-nf // LANES) * LANES
    f_tiles = f_wide // LANES
    grain = 2 * PARTS * BLOCK
    one_rows = -(-(2 * nk + 3 * nv) // grain) * grain
    gap = one_rows - 2 * nk - 3 * nv
    m = lax.axis_size("dp")

    pack_one = jnp.concatenate(
        [w_query.T, w_key.T, w_value.T, w_gate.T, jnp.zeros((gap, shard), BF), w_out], axis=0
    )
    glu_pack = jnp.stack(
        [
            pad_rows(w_glu_gate.T, f_wide).reshape(f_tiles, LANES, shard),
            pad_rows(w_glu_up.T, f_wide).reshape(f_tiles, LANES, shard),
        ],
        axis=1,
    ).reshape(2 * f_wide, shard)
    pack_two = jnp.concatenate([glu_pack, pad_rows(w_down, f_wide)], axis=0)

    first_hat, _ = layer_norm(inputs.astype(F32), epsilon)
    first_rows = (first_hat * first_norm_gain).astype(BF)
    tokens = n * rows

    slot_shard = lax.rem(place - jnp.arange(n) + n, n)
    places = (
        slot_shard[None, :, None] * rows
        + jnp.arange(CHUNKS)[:, None, None] * piece
        + jnp.arange(piece)[None, None, :]
    ).reshape(tokens)
    seg = segments.reshape(n, CHUNKS, piece)[::-1]
    seg = lax.dynamic_slice_in_dim(jnp.concatenate([seg, seg], axis=0), n - 1 - place, n, axis=0)
    seg = seg.transpose(1, 0, 2).reshape(tokens)

    log_gamma = jnp.log1p(-jnp.exp2(-5.0 - (head_start + jnp.arange(heads)).astype(F32)))
    spot = places.astype(F32)
    powers = spot[None] * log_gamma[:, None]
    marks = jnp.stack([spot, seg.astype(F32)])
    col = jnp.concatenate([marks, jnp.exp(powers)], axis=0).T
    row = jnp.concatenate([marks, jnp.exp(-powers) * HK ** (-0.5)], axis=0)

    (
        rows_one, weight_one, query, key, value, gate_pre, normalized, scale_group, scores, gated,
        cot_front,
    ) = forward_call(first_rows, pack_one, cotangent, col, row, n, m, heads)
    (
        mid_rows, grads_glu, grads_two, down, outputs_front, middle, middle_grad, second_gain,
    ) = middle_call(
        gated, pack_two, weight_one, inputs, cotangent, cot_front, second_norm_gain[None], n, m
    )
    d_qk, d_value, d_gate, grad_glu_gate, grad_glu_up, outputs_back = backward_call(
        mid_rows, weight_one, gate_pre, normalized, scale_group, scores, query, key, value,
        down, middle, grads_glu, nf, col, row, n, m,
    )
    plan = [(0, h, 0, HV, 1) for h in range(heads)] + [(2, h, 0, HV, 3) for h in range(heads)]
    plan += [(4, None, t * nk, nk, 3) for t in range(2)]
    plan += [(5, h, 0, HV, 3) for h in range(heads)]
    grads_one, grad_down, outputs_end = products_call(
        plan, (gated, mid_rows, d_gate, rows_one, d_qk, d_value), down, middle, grads_two, nf,
        one_rows, n, m,
    )
    input_gradient, gains, grad_query, grad_key, grad_out, grad_gate, grad_value = last_call(
        d_qk, d_value, d_gate, weight_one, grads_one, inputs, first_norm_gain[None], middle_grad,
        second_gain, rows_one, n, m,
    )
    gains = gains.reshape(2, width)
    return (
        jnp.concatenate([outputs_front, outputs_back, outputs_end], axis=0),
        input_gradient,
        gains[0],
        grad_query,
        grad_key,
        grad_value.T,
        grad_gate.T,
        grad_out,
        gains[1],
        grad_glu_gate.T,
        grad_glu_up.T,
        grad_down,
    )


def solution(mesh):
    split = P(("dp", "mp"), None)
    wide, tall = P("dp", "mp"), P("mp", "dp")
    return jax.shard_map(
        body,
        mesh=mesh,
        in_specs=(
            split, P("dp", None), P(), wide, wide, wide, wide, tall, P(), wide, wide, tall, split,
        ),
        out_specs=(
            split, split, P(), wide, wide, wide, wide, tall, P(), wide, wide, tall,
        ),
        check_vma=False,
    )
```

```python
import functools

import jax
import jax.numpy as jnp
from jax import lax
from jax.experimental import pallas as pl
from jax.experimental.pallas import tpu as pltpu
from jax.sharding import PartitionSpec as P

H = 8
HK = 256
HV = 432
LEN = 1024
CHUNKS = 4
FRONT = CHUNKS // 2
DOWNS = CHUNKS // 4
ENDS = CHUNKS // 4
LANES = 128
VMEM_MOST = 66_000_000

epsilon = 1e-05
group_epsilon = 1.0
BF = jnp.bfloat16
F32 = jnp.float32


def layer_norm(values_in, offset):
    centre = jnp.mean(values_in, axis=-1, keepdims=True)
    centred = values_in - centre
    variance = jnp.mean(centred * centred, axis=-1, keepdims=True)
    scaling = lax.rsqrt(variance + offset)
    return (centred * scaling, scaling)


def norm_back(grad_hat, normed_hat, scaling):
    first_mean = jnp.mean(grad_hat, axis=-1, keepdims=True)
    second_mean = jnp.mean(grad_hat * normed_hat, axis=-1, keepdims=True)
    return scaling * (grad_hat - first_mean - normed_hat * second_mean)


def glu_act(gate_pre, up_pre):
    return jax.nn.gelu(gate_pre, approximate=True) * up_pre


def dot_nt(a, b):
    return lax.dot_general(a, b, (((1,), (1,)), ((), ())), preferred_element_type=F32)


def dot_nn(a, b):
    return lax.dot_general(a, b, (((1,), (0,)), ((), ())), preferred_element_type=F32)


def dot_tn(a, b):
    return lax.dot_general(a, b, (((0,), (0,)), ((), ())), preferred_element_type=F32)


MESH = pl.DeviceIdType.MESH


class Line:
    def __init__(self, n, send_sem, recv_sem):
        self.n, self.send_sem, self.recv_sem = n, send_sem, recv_sem
        self.place = lax.axis_index("mp")
        self.used = 0
        self.sent = []

    def enter(self, others=None):
        barrier = pltpu.get_barrier_semaphore()
        n, place = self.n, self.place

        @pl.when(place >= 1)
        def _():
            pl.semaphore_signal(barrier, inc=1, device_id={"mp": place - 1}, device_id_type=MESH)

        @pl.when(place <= n - 2)
        def _():
            pl.semaphore_signal(barrier, inc=1, device_id={"mp": place + 1}, device_id_type=MESH)

        peers = jnp.minimum(place, 1) + jnp.minimum(n - 1 - place, 1)
        if others is not None:
            axis, indices = others
            for index in indices:
                pl.semaphore_signal(barrier, inc=1, device_id={axis: index}, device_id_type=MESH)
            peers = peers + len(indices)
        pl.semaphore_wait(barrier, peers)

    def copy(self, src, dst, index, toward):
        return pltpu.make_async_remote_copy(
            src_ref=src,
            dst_ref=dst,
            send_sem=self.send_sem.at[index],
            recv_sem=self.recv_sem.at[index],
            device_id={"mp": self.place + toward},
            device_id_type=MESH,
        )

    def leave(self):
        for condition, copy in self.sent:
            pl.when(condition)(copy.wait_send)


class Gather:
    def __init__(self, line, slot):
        self.line, self.slot, self.step_no = line, slot, 0
        self.base = line.used
        line.used += 2 * (line.n - 1)
        n = line.n
        self.right = [
            line.copy(slot(s - 1), slot(s), self.base + s - 1, 1) for s in range(1, n)
        ]
        self.left = [
            line.copy(slot((n - s + 1) % n), slot(n - s), self.base + n - 2 + s, -1)
            for s in range(1, n)
        ]

    def arrive(self, s):
        n, place = self.line.n, self.line.place
        pl.when(place >= s)(self.right[s - 1].wait_recv)
        pl.when(place <= n - 1 - s)(self.left[s - 1].wait_recv)

    def step(self):
        self.step_no += 1
        s, n, place = self.step_no, self.line.n, self.line.place
        if s > 1:
            self.arrive(s - 1)
        if s < n:
            to_right = (place >= s - 1) & (place <= n - 2)
            to_left = (place <= n - s) & (place >= 1)
            pl.when(to_right)(self.right[s - 1].start)
            pl.when(to_left)(self.left[s - 1].start)
            self.line.sent += [(to_right, self.right[s - 1]), (to_left, self.left[s - 1])]


class Scatter:
    def __init__(self, line, slot, from_left, from_right, add):
        self.line, self.slot, self.add, self.step_no = line, slot, add, 0
        self.from_left, self.from_right = from_left, from_right
        self.base = line.used
        line.used += 2 * (line.n - 1)
        n = line.n
        self.right = [
            line.copy(slot(s), from_left(s), self.base + s - 1, 1) for s in range(1, n)
        ]
        self.left = [
            line.copy(slot(n - s), from_right(s), self.base + n - 2 + s, -1) for s in range(1, n)
        ]
        self.mine = []

    def step(self):
        self.step_no += 1
        s, n, place = self.step_no, self.line.n, self.line.place
        to_right, to_left = place <= s - 1, place >= n - s
        if s > 1:

            @pl.when(to_right & (place >= 1))
            def _():
                self.right[s - 2].wait_recv()
                self.add(self.slot(s), self.from_left(s - 1))

            @pl.when(to_left & (place <= n - 2))
            def _():
                self.left[s - 2].wait_recv()
                self.add(self.slot(n - s), self.from_right(s - 1))

        pl.when(to_right)(self.right[s - 1].start)
        pl.when(to_left)(self.left[s - 1].start)
        self.mine += [(to_right, self.right[s - 1]), (to_left, self.left[s - 1])]

    def finish(self):
        n, place = self.line.n, self.line.place

        @pl.when(place >= 1)
        def _():
            self.right[n - 2].wait_recv()

        @pl.when(place <= n - 2)
        def _():
            self.left[n - 2].wait_recv()

    def drain(self):
        for condition, copy in self.mine:
            pl.when(condition)(copy.wait_send)


ANY = pl.BlockSpec(memory_space=pl.ANY)
VM = pl.BlockSpec(memory_space=pltpu.VMEM)
BLOCK = 16


def blocks(count, step):
    def run(i, carry):
        step(lambda base=0: pl.ds(pl.multiple_of(base + i * BLOCK, BLOCK), BLOCK))
        return carry

    lax.fori_loop(0, count // BLOCK, run, 0)


def add_into(target, extra):
    def step(at):
        target[at(), :] = (target[at(), :].astype(F32) + extra[at(), :].astype(F32)).astype(BF)

    blocks(target.shape[0], step)


def product_tiles(target, left, right, tile):
    def step(j, carry):
        at = pl.ds(pl.multiple_of(j * tile, tile), tile)
        target[:, at] = dot_nn(left[...], right[:, at]).astype(BF)
        return carry

    lax.fori_loop(0, right.shape[1] // tile, step, 0)


class Doubling:
    def __init__(self, m, own, out, rows, bits, base, send_sem, recv_sem):
        self.d = lax.axis_index("dp")
        self.own, self.out, self.rows, self.bits, self.base = own, out, rows, bits, base
        self.send_sem, self.recv_sem = send_sem, recv_sem
        self.shard = own.shape[1]
        self.done = 0
        self.sent = []

    def flip(self, d, bit):
        return d + bit * (1 - 2 * (lax.div(d, bit) % 2))

    def block(self, d):
        return self.out.at[self.rows, pl.ds(pl.multiple_of(d * self.shard, self.shard), self.shard)]

    def copies(self, level, landing):
        owners = [self.d]
        for bit in self.bits[:level]:
            owners += [self.flip(d, bit) for d in owners]
        bit = self.bits[level]
        partner = self.flip(self.d, bit)
        out = []
        for i, d in enumerate(owners):
            d = self.flip(d, bit) if landing else d
            src = self.own.at[self.rows] if i == 0 and not landing else self.block(d)
            index = self.base + (1 << level) - 1 + i
            out.append(
                pltpu.make_async_remote_copy(
                    src_ref=src,
                    dst_ref=self.block(d),
                    send_sem=self.send_sem.at[index],
                    recv_sem=self.recv_sem.at[index],
                    device_id={"dp": partner},
                    device_id_type=MESH,
                )
            )
        return out

    def step(self):
        level = self.done
        if level > 0:
            for c in self.copies(level - 1, True):
                c.wait_recv()
        if level < len(self.bits):
            out = self.copies(level, False)
            for c in out:
                c.start()
            self.sent += out
        self.done += 1

    def leave(self):
        for c in self.sent:
            c.wait_send()


def bits_of(m):
    bits = [1 << b for b in range(m.bit_length() - 1)]
    assert 1 << len(bits) == m
    return bits


PARTS = 2


def weight_gather(m, pack, weight, send_sem, recv_sem):
    bits = bits_of(m)
    outer = bits[1:]
    height = pack.shape[0] // (2 * PARTS)
    doubling = []
    for i in range(2 * PARTS):
        order = (outer if i % 2 == 0 else outer[::-1]) + bits[:1]
        rows = pl.ds(i * height, height)
        doubling.append(Doubling(m, pack, weight, rows, order, i * (m - 1), send_sem, recv_sem))
    first = doubling[0]
    return doubling, [first.flip(first.d, bit) for bit in bits]


def own_columns(pack, weight):
    shard = pack.shape[1]
    at = pl.multiple_of(lax.axis_index("dp") * shard, shard)
    return weight.at[:, pl.ds(at, shard)]


def no_neighbour_zero(n, place, from_left, from_right):
    @pl.when(place == 0)
    def _():
        from_left[...] = jnp.zeros_like(from_left)

    @pl.when(place == n - 1)
    def _():
        from_right[...] = jnp.zeros_like(from_right)


(COT, OUT, ONE, END_ONE, TWO, GLU, GRAD, GRAD_SUM, END_GRAD, MID, DOWN, DOWN_SUM, END_DOWN, PRODUCTS, WIDE) = range(15)

DUE = {
    OUT: (-2.23, 1.66, 0), ONE: (-1.99, 1.12, 1.03), END_ONE: (1.46, 1.37, 0), TWO: (0.73, 1.15, 0.94),
    COT: (0.35, 1.39, 1.02), GLU: (1.14, -1.37, 1.55), GRAD: (3.09, 2.02, 0),
    GRAD_SUM: (3.48, 1.71, 0.74), END_GRAD: (7.02, -2.12, 0), MID: (5.68, 0.86, 1.11),
    DOWN: (1.3, 0.36, 0), DOWN_SUM: (1.87, 1.35, 0.95), END_DOWN: (7.9, 2.17, 0),
    PRODUCTS: (7.5, 0, 0.4), WIDE: (-4, 0.05, 1.5),
}
TUNED = {
    (4, 4, 3): [
        2, 58, 7, 57, 4, 59, 8, 56, 5, 2, 8, 57, 58, 56, 8, 9, 3, 6, 59, 12,
        2, 16, 9, 58, 16, 10, 9, 57, 59, 56, 16, 13, 11, 17, 58, 57, 3, 10, 16, 17,
        56, 11, 59, 20, 10, 20, 17, 24, 28, 11, 14, 18, 3, 15, 28, 19, 18, 2, 17, 21,
        28, 21, 40, 44, 18, 19, 25, 32, 29, 36, 18, 22, 29, 19, 44, 22, 29, 26, 36, 30,
        44, 19, 3, 23, 33, 37, 30, 36, 23, 27, 37, 31, 30, 52, 37, 31, 34, 38, 42, 41,
        31, 38, 35, 39, 38, 52, 48, 39, 36, 37, 38, 52, 39, 43, 39,
    ],
}


def middle_order(n, levels):
    if (n, CHUNKS, levels) in TUNED:
        return [divmod(code, CHUNKS) for code in TUNED[n, CHUNKS, levels]]
    count = {k: 1 for k in DUE}
    count.update({COT: n, TWO: n, MID: n, ONE: n - 1, GRAD_SUM: n - 1, DOWN_SUM: n - 1, GLU: 2, PRODUCTS: 3, WIDE: levels + 1})
    needs = {
        ONE: [OUT], END_ONE: [ONE], TWO: [END_ONE], GLU: [TWO, COT], GRAD: [GLU], GRAD_SUM: [GRAD],
        END_GRAD: [GRAD_SUM], MID: [END_GRAD], DOWN: [GLU], DOWN_SUM: [DOWN], END_DOWN: [DOWN_SUM],
    }
    todo = sorted(
        (first + h * later + s * 3 / (n - 1) * each, k, h, s)
        for k, (first, later, each) in DUE.items()
        for h in range(CHUNKS)
        for s in range(count[k])
        if not (k == PRODUCTS and h > 0 or k == COT and h < FRONT or k in (DOWN_SUM, END_DOWN) and h >= DOWNS)
    )
    taken, order = {}, []
    while todo:
        for item in todo:
            _, k, h, s = item
            ready = taken.get((k, h), 0) == s and (
                k != PRODUCTS or all(taken.get((GLU, c), 0) == 2 for c in range(CHUNKS))
            )
            ready = ready and (
                k != GLU or all(taken.get((WIDE, c), 0) == levels + 1 for c in range(2 * PARTS))
            )
            ready = ready and all(
                taken.get((need, h), 0) == count[need] or (need == COT and h < FRONT)
                for need in needs.get(k, [])
            )
            if ready:
                break
        todo.remove(item)
        taken[k, h] = s + 1
        order.append((k, h))
    return order


def middle_kernel(
    n, m, gated, pack, out_weight, own, cot, cot_front, gain,
    mid_out, glu_out, product_out, down_out, outputs, middle_out, d_middle, gain_out,
    gated_v, wo_v, weights_v, own_v, cot_v, rows_v, hidden_v, glu_v, part, part_two,
    left_a, right_a, left_b, right_b, middle, stage, result, copy_sem, send_sem, recv_sem,
    wide_send, wide_recv,
):
    line = Line(n, send_sem, recv_sem)
    place = line.place
    count, width = own.shape
    piece = count // CHUNKS
    per = n * piece
    wide = hidden_v.shape[1]
    copies = []

    def local(src, dst):
        c = pltpu.make_async_copy(src, dst, copy_sem.at[len(copies)])
        copies.append(c)
        c.start()
        return c

    def rows_at(ref, h, k=0, size=piece):
        return ref.at[pl.ds(h * per + k * piece, size)]

    load_cot = [
        local(cot.at[pl.ds(h * piece, piece)], rows_at(cot_v, h)) for h in range(FRONT, CHUNKS)
    ]
    front = pl.ds(0, FRONT * per)
    load_cot.append(local(cot_front, cot_v.at[front]))
    load_gated = local(gated, gated_v)
    load_wo = local(
        out_weight.at[pl.ds(out_weight.shape[0] - wo_v.shape[0], wo_v.shape[0])], wo_v
    )
    load_own = local(own, own_v)
    load_pack = local(pack, own_columns(pack, weights_v))
    wg_v, wd_v = weights_v.at[pl.ds(0, 2 * wide)], weights_v.at[pl.ds(2 * wide, wide)]
    doubling, peers = weight_gather(m, pack, weights_v, wide_send, wide_recv)
    line.enter(["dp", peers])
    for h in range(CHUNKS):
        no_neighbour_zero(n, place, left_a.at[h, n - 2], right_a.at[h, n - 2])
    for h in range(DOWNS):
        no_neighbour_zero(n, place, left_b.at[h, n - 2], right_b.at[h, n - 2])
    gain_out[...] = jnp.zeros_like(gain_out)

    def scatter(buf, lefts, rights, h):
        return Scatter(
            line,
            lambda k: rows_at(buf, h, k),
            lambda s: lefts.at[h, s - 1],
            lambda s: rights.at[h, s - 1],
            add_into,
        )

    gather_cot = {
        h: Gather(line, functools.partial(rows_at, cot_v, h)) for h in range(FRONT, CHUNKS)
    }
    gather_two = [Gather(line, functools.partial(rows_at, rows_v, h)) for h in range(CHUNKS)]

    def mid_slot(h, k):
        return stage.at[h] if k == 0 else rows_at(mid_out, h, k)

    gather_mid = [Gather(line, functools.partial(mid_slot, h)) for h in range(CHUNKS)]
    scatter_one = [scatter(part, left_a, right_a, h) for h in range(CHUNKS)]
    scatter_two = [scatter(part_two, left_b, right_b, h) for h in range(DOWNS)]
    scatter_grad = [scatter(part, left_a, right_a, h) for h in range(CHUNKS)]

    def chunk(ref, h):
        return ref.at[pl.ds(h * per, per)]

    def out_product(h):
        heads, _, size = gated_v.shape
        target, whole = chunk(part, h), pl.ds(h * per, per)

        def step(j, carry):
            at = pl.ds(pl.multiple_of(j * 2 * LANES, 2 * LANES), 2 * LANES)
            target[:, at] = sum(
                dot_nn(gated_v[i, whole, :], wo_v[pl.ds(i * size, size), at]) for i in range(heads)
            ).astype(BF)
            return carry

        lax.fori_loop(0, width // (2 * LANES), step, 0)

    def finish_one(h):
        scatter_one[h].finish()

        def step(at):
            src = at(h * per)
            mine = at(h * piece)
            total = (
                own_v[mine, :].astype(F32)
                + part[src, :].astype(F32)
                + left_a[h, n - 2, at(), :].astype(F32)
                + right_a[h, n - 2, at(), :].astype(F32)
            )
            middle[mine, :] = total
            hat, _ = layer_norm(total, epsilon)
            rows_v[src, :] = (hat * gain[...]).astype(BF)

        blocks(piece, step)

    def glu_tiles(h, first, last):
        def step(j, carry):
            pair = pl.ds(pl.multiple_of(j * 2 * LANES, 2 * LANES), 2 * LANES)
            at = pl.ds(pl.multiple_of(j * LANES, LANES), LANES)
            whole = pl.ds(h * per, per)
            both = dot_nt(rows_v[whole, :], wg_v[pair, :])
            d_hidden = dot_nt(cot_v[whole, :], wd_v[at, :])
            u, up = both[:, :LANES], both[:, LANES:]
            c = 0.7978845608028654
            t = jnp.tanh(c * (u + 0.044715 * (u * u * u)))
            half = 0.5 * (1.0 + t)
            act = u * half
            slope = half + 0.5 * u * (1.0 - t * t) * (c * (1.0 + 3 * 0.044715 * (u * u)))
            hidden_v[whole, at] = (act * up).astype(BF)
            glu_v[whole, pair] = jnp.concatenate(
                [(d_hidden * up * slope).astype(BF), (d_hidden * act).astype(BF)], axis=1
            )
            return carry

        lax.fori_loop(first, last, step, 0)

    def grad_product(h):
        product_tiles(chunk(part, h), chunk(glu_v, h), wg_v, 2 * LANES)

    def down_product(h):
        product_tiles(chunk(part_two, h), chunk(hidden_v, h), wd_v, 2 * LANES)

    def finish_grad(h):
        scatter_grad[h].finish()

        def step(at):
            src = at(h * per)
            mine = at(h * piece)
            grad = (
                part[src, :].astype(F32)
                + left_a[h, n - 2, at(), :].astype(F32)
                + right_a[h, n - 2, at(), :].astype(F32)
            )
            hat, scale = layer_norm(middle[mine, :], epsilon)
            gain_out[...] += jnp.sum((hat * grad).reshape(BLOCK // 8, 8, width), axis=0)
            d_mid = cot_v[src, :].astype(F32) + norm_back(grad * gain[...], hat, scale)
            d_middle[mine, :] = d_mid
            stage[h, at(), :] = d_mid.astype(BF)

        blocks(piece, step)
        local(stage.at[h], rows_at(mid_out, h))

    def finish_two(h):
        scatter_two[h].finish()

        def step(at):
            src = at(h * per)
            mine = at(h * piece)
            outputs[mine, :] = (
                middle[mine, :]
                + part_two[src, :].astype(F32)
                + left_b[h, n - 2, at(), :].astype(F32)
                + right_b[h, n - 2, at(), :].astype(F32)
            ).astype(BF)

        blocks(piece, step)

    tiles = wide // LANES
    cut = tiles // 2

    def wait_for(items):
        for item in items:
            item.wait()
        items.clear()

    first_loads, own_load = [load_gated, load_wo], [load_own]
    later_loads = [load_pack]

    def out_action(h):
        wait_for(first_loads)
        out_product(h)

    def finish_one_action(h):
        wait_for(own_load)
        finish_one(h)

    def glu_action(h):
        wait_for(later_loads)
        assert all(item.done == len(bits_of(m)) + 1 for item in doubling)
        if h in begun:
            glu_tiles(h, cut, tiles)
        else:
            begun.add(h)
            glu_tiles(h, 0, cut)

    def grad_action(h):
        scatter_one[h].drain()
        grad_product(h)

    def products_action(_):
        k = len(products)
        if k >= 2:
            products[k - 2].wait()
        left = hidden_v.at[...] if k == 2 else glu_v.at[:, pl.ds(k * wide, wide)]
        right = cot_v if k == 2 else rows_v
        target = result.at[k % 2]

        def step(j, carry):
            at = pl.ds(pl.multiple_of(j * 2 * LANES, 2 * LANES), 2 * LANES)
            target[:, at] = dot_tn(left[...], right[:, at]).astype(BF)
            return carry

        lax.fori_loop(0, width // (2 * LANES), step, 0)
        place_out = product_out if k == 2 else glu_out.at[pl.ds(k * wide, wide)]
        store = pltpu.make_async_copy(target, place_out, copy_sem.at[spare + k])
        store.start()
        products.append(store)

    products, spare = [], copy_sem.shape[0] - 3
    begun = set()
    actions = {
        COT: lambda h: gather_cot[h].step(),
        OUT: out_action,
        ONE: lambda h: scatter_one[h].step(),
        END_ONE: finish_one_action,
        TWO: lambda h: gather_two[h].step(),
        GLU: glu_action,
        GRAD: grad_action,
        GRAD_SUM: lambda h: scatter_grad[h].step(),
        END_GRAD: finish_grad,
        MID: lambda h: gather_mid[h].step(),
        DOWN: down_product,
        DOWN_SUM: lambda h: scatter_two[h].step(),
        END_DOWN: finish_two,
        PRODUCTS: products_action,
        WIDE: lambda h: doubling[h].step(),
    }
    for item in load_cot:
        item.wait()
    for kind, h in middle_order(n, len(bits_of(m))):
        actions[kind](h)
    local(part_two.at[pl.ds(DOWNS * per, down_out.shape[0])], down_out)
    local(middle.at[pl.ds(DOWNS * piece, middle_out.shape[0])], middle_out)
    for item in list(gather_cot.values()) + gather_two + gather_mid:
        assert item.step_no == n
    for item in scatter_one + scatter_two + scatter_grad:
        assert item.step_no == n - 1
    for group in (scatter_grad, scatter_two):
        for item in group:
            item.drain()
    for item in copies[CHUNKS - FRONT + 5 :] + products[1:]:
        item.wait()
    assert len(products) == 3
    for item in doubling:
        item.leave()
    line.leave()


def middle_call(gated, pack, out_weight, own, cot, cot_front, gain, n, m):
    rows, width = own.shape
    heads, tokens, size = gated.shape
    nv = heads * size
    wide = pack.shape[0] // 3
    piece = rows // CHUNKS
    back = CHUNKS - DOWNS
    sems = CHUNKS * 5 * 2 * (n - 1)
    hop = (CHUNKS, n - 1, piece, width)
    shape = jax.ShapeDtypeStruct
    return pl.pallas_call(
        functools.partial(middle_kernel, n, m),
        out_shape=(
            shape((tokens, width), BF),
            shape((2 * wide, width), BF),
            shape((wide, width), BF),
            shape((back * n * piece, width), BF),
            shape((DOWNS * piece, width), BF),
            shape((back * piece, width), F32),
            shape((rows, width), F32),
            shape((8, width), F32),
        ),
        in_specs=[ANY, VM] + [ANY] * 4 + [VM],
        out_specs=(ANY,) * 4 + (VM, ANY, VM, VM),
        scratch_shapes=[
            pltpu.VMEM((heads, tokens, size), BF),
            pltpu.VMEM((nv, width), BF),
            pltpu.VMEM((3 * wide, width), BF),
            pltpu.VMEM((rows, width), BF),
            pltpu.VMEM((tokens, width), BF),
            pltpu.VMEM((tokens, width), BF),
            pltpu.VMEM((tokens, wide), BF),
            pltpu.VMEM((tokens, 2 * wide), BF),
            pltpu.VMEM((tokens, width), BF),
            pltpu.VMEM((tokens, width), BF),
            pltpu.VMEM(hop, BF),
            pltpu.VMEM(hop, BF),
            pltpu.VMEM((DOWNS,) + hop[1:], BF),
            pltpu.VMEM((DOWNS,) + hop[1:], BF),
            pltpu.VMEM((rows, width), F32),
            pltpu.VMEM((CHUNKS, piece, width), BF),
            pltpu.VMEM((2, wide, width), BF),
            pltpu.SemaphoreType.DMA((11 + 2 * CHUNKS - FRONT,)),
            pltpu.SemaphoreType.DMA((sems,)),
            pltpu.SemaphoreType.DMA((sems,)),
            pltpu.SemaphoreType.DMA((2 * PARTS * (m - 1),)),
            pltpu.SemaphoreType.DMA((2 * PARTS * (m - 1),)),
        ],
        compiler_params=pltpu.CompilerParams(
            collective_id=1, has_side_effects=True, vmem_limit_bytes=VMEM_MOST
        ),
        name="middle",
    )(gated, pack, out_weight, own, cot, cot_front, gain)


class Halving:
    def __init__(self, grads, rows, bits, base, kept, held, out, send_sem, recv_sem, load_sem):
        self.d = lax.axis_index("dp")
        self.grads, self.rows, self.bits, self.base = grads, rows, bits, base
        self.kept, self.held, self.out = kept, held, out
        self.send_sem, self.recv_sem, self.load_sem = send_sem, recv_sem, load_sem
        self.shard = out.shape[1]
        self.masks = [0]
        for bit in bits[:0:-1]:
            self.masks += [k + bit for k in self.masks]
        self.done, self.sent, self.loads = 0, [], []

    def flip(self, d, mask):
        for bit in self.bits:
            if mask & bit:
                d = d + bit * (1 - 2 * (lax.div(d, bit) % 2))
        return d

    def block(self, d):
        return self.grads.at[self.rows, pl.ds(pl.multiple_of(d * self.shard, self.shard), self.shard)]

    def count(self, level):
        return 1 << (len(self.bits) - 1 - level)

    def copies(self, level):
        bit = self.bits[level]
        partner = self.flip(self.d, bit)
        out = []
        for i in range(self.count(level)):
            if level == 0:
                src = self.block(self.flip(partner, self.masks[i]))
            else:
                src = self.kept.at[self.count(level) + i, self.rows]
            index = self.base + len(out) + sum(self.count(k) for k in range(level))
            out.append(
                pltpu.make_async_remote_copy(
                    src_ref=src,
                    dst_ref=self.held[level].at[i, self.rows],
                    send_sem=self.send_sem.at[index],
                    recv_sem=self.recv_sem.at[index],
                    device_id={"dp": partner},
                    device_id_type=MESH,
                )
            )
        return out

    def load(self):
        for i, mask in enumerate(self.masks):
            c = pltpu.make_async_copy(
                self.block(self.flip(self.d, mask)), self.kept.at[i, self.rows], self.load_sem.at[i]
            )
            c.start()
            self.loads.append(c)

    def add(self, level):
        last = level == len(self.bits) - 1
        start, size = self.rows.start, self.rows.size
        for i in range(self.count(level)):

            def step(at):
                total = self.kept[i, at(start), :].astype(F32) + self.held[level][
                    i, at(start), :
                ].astype(F32)
                if last:
                    self.out[at(start), :] = total
                else:
                    self.kept[i, at(start), :] = total.astype(BF)

            blocks(size, step)

    def step(self):
        level = self.done
        if level > 0:
            for c in self.loads:
                c.wait()
            self.loads = []
            for c in self.sent[-1]:
                c.wait_recv()
            self.add(level - 1)
        if level < len(self.bits):
            out = self.copies(level)
            for c in out:
                c.start()
            self.sent.append(out)
        self.done += 1

    def leave(self):
        for group in self.sent:
            for c in group:
                c.wait_send()


def grad_scatter(m, grads, kept, held, summed, send_sem, recv_sem, load_sem):
    bits = bits_of(m)
    height = grads.shape[0] // (2 * PARTS)
    out = []
    for i in range(2 * PARTS):
        order = bits[:1] + (bits[1:] if i % 2 == 0 else bits[:0:-1])
        rows = pl.ds(i * height, height)
        out.append(
            Halving(
                grads, rows, order, i * (m - 1), kept, held, summed, send_sem, recv_sem, load_sem.at[i]
            )
        )
    return out, [out[0].flip(out[0].d, bit) for bit in bits]


def scatter_scratch(m, rows, shard):
    wide = 2 * PARTS * (m - 1)
    counts = [m // 2] + [m >> (1 + k) for k in range(len(bits_of(m)))]
    return [pltpu.VMEM((count, rows, shard), BF) for count in counts] + [
        pltpu.VMEM((rows, shard), F32),
        pltpu.SemaphoreType.DMA((wide,)),
        pltpu.SemaphoreType.DMA((wide,)),
        pltpu.SemaphoreType.DMA((2 * PARTS, m // 2)),
    ]


class Exchange:
    def __init__(self, groups, mine, total, send_sem, recv_sem):
        self.groups, self.source, self.total = groups, mine, total
        self.send_sem, self.recv_sem = send_sem, recv_sem
        self.done, self.base, self.sent = 0, 0, []

    def copy(self, k, slot):
        axis, size, held = self.groups[self.done]
        return pltpu.make_async_remote_copy(
            src_ref=self.source,
            dst_ref=held.at[slot],
            send_sem=self.send_sem.at[self.base + k],
            recv_sem=self.recv_sem.at[self.base + k],
            device_id={axis: lax.rem(lax.axis_index(axis) + k, size)},
            device_id_type=MESH,
        )

    def send(self):
        axis, size, held = self.groups[self.done]
        me = lax.axis_index(axis)
        held[me] = self.source[...]
        self.sent = [self.copy(k, me) for k in range(1, size)]
        for c in self.sent:
            c.start()

    def receive(self):
        axis, size, held = self.groups[self.done]
        me = lax.axis_index(axis)
        for k in range(1, size):
            self.copy(k, lax.rem(me - k + size, size)).wait_recv()
        value = held[0]
        for k in range(1, size):
            value = value + held[k]
        for c in self.sent:
            c.wait_send()
        self.total[...] = value
        self.source, self.base, self.done = self.total, self.base + size, self.done + 1


def last_kernel(
    n, m, d_qk, d_value, d_gate, weight, grads, inputs, gain, d_middle, second_gain, rows,
    out, gains, grad_query, grad_key, grad_out, grad_gate, grad_value,
    qk_v, value_v, gate_v, weight_v, inputs_v, middle_v, part, lefts, rights, *rest
):
    bits = bits_of(m)
    kept, held = rest[0], rest[1 : 1 + len(bits)]
    summed, wide_send, wide_recv, load_sem = rest[1 + len(bits) : 5 + len(bits)]
    gain_sum, mine, first, second, rows_v = rest[5 + len(bits) : 10 + len(bits)]
    copy_sem, send_sem, recv_sem, gain_send, gain_recv = rest[10 + len(bits) :]
    line = Line(n, send_sem, recv_sem)
    count, width = out.shape
    piece = count // CHUNKS
    per = n * piece
    heads, _, size = value_v.shape
    wide = qk_v.shape[1]
    load = [
        pltpu.make_async_copy(src, dst, copy_sem.at[i])
        for i, (src, dst) in enumerate(
            [
                (weight.at[pl.ds(0, weight_v.shape[0])], weight_v), (d_qk, qk_v),
                (d_value, value_v), (d_gate, gate_v), (rows, rows_v), (inputs, inputs_v),
                (d_middle, middle_v),
            ]
        )
    ]
    for item in load:
        item.start()
    barrier = pltpu.get_barrier_semaphore()
    for axis, extent in (("dp", m), ("mp", n)):
        me = lax.axis_index(axis)
        for k in range(1, extent):
            peer = lax.rem(me + k, extent)
            pl.semaphore_signal(barrier, inc=1, device_id={axis: peer}, device_id_type=MESH)
    pl.semaphore_wait(barrier, n + m - 2)

    halving, _ = grad_scatter(m, grads, kept, held, summed, wide_send, wide_recv, load_sem)
    for item in halving:
        item.step()
    for item in halving:
        item.load()
    for h in range(CHUNKS):
        no_neighbour_zero(n, line.place, lefts.at[h, n - 2], rights.at[h, n - 2])
    gain_sum[...] = jnp.zeros_like(gain_sum)
    scatters = [
        Scatter(
            line,
            lambda k, h=h: part.at[pl.ds(h * per + k * piece, piece)],
            lambda s, h=h: lefts.at[h, s - 1],
            lambda s, h=h: rights.at[h, s - 1],
            add_into,
        )
        for h in range(CHUNKS)
    ]

    def product(h):
        rows = pl.ds(h * per, per)

        def step(j, carry):
            at = pl.ds(pl.multiple_of(j * 2 * LANES, 2 * LANES), 2 * LANES)
            total = dot_nn(qk_v[rows, :], weight_v[pl.ds(0, wide), at])
            for i in range(heads):
                base = wide + i * size
                total += dot_nn(value_v[i, rows, :], weight_v[pl.ds(base, size), at])
                base += heads * size
                total += dot_nn(gate_v[i, rows, :], weight_v[pl.ds(base, size), at])
            part[rows, at] = total.astype(BF)
            return carry

        lax.fori_loop(0, width // (2 * LANES), step, 0)

    def finish(h):
        scatters[h].finish()

        def step(at):
            own = at(h * piece)
            grad = (
                part[at(h * per), :].astype(F32)
                + lefts[h, n - 2, at(), :].astype(F32)
                + rights[h, n - 2, at(), :].astype(F32)
            )
            hat, scale = layer_norm(inputs_v[own, :].astype(F32), epsilon)
            out[own, :] = middle_v[own, :] + norm_back(grad * gain[...], hat, scale)

        blocks(piece, step)

    def gain_part(h):
        def step(at):
            here = at(h * per)
            term = rows_v[here, :].astype(F32) * part[here, :].astype(F32)
            gain_sum[...] += jnp.sum(term.reshape(BLOCK // 8, 8, width), axis=0)

        blocks(per, step)

    for item in load[:5]:
        item.wait()
    for h in range(CHUNKS):
        product(h)
        scatters[h].step()
        gain_part(h)
    flats = (
        jnp.sum(gain_sum[...], axis=0, keepdims=True) / gain[...],
        jnp.sum(second_gain[...], axis=0, keepdims=True),
    )
    for i, flat in enumerate(flats):
        for j in range(width // LANES):
            mine[pl.ds(i * (width // LANES) + j, 1), :] = flat[:, j * LANES : (j + 1) * LANES]
    total_gain = Exchange(
        [("dp", m, first), ("mp", n, second)], mine, gains, gain_send, gain_recv
    )
    total_gain.send()
    for item in load[5:]:
        item.wait()
    for s in range(n - 2):
        if s == 1:
            total_gain.receive()
            total_gain.send()
        for h in range(CHUNKS):
            if s < len(bits) and h < len(halving):
                halving[h].step()
            scatters[h].step()
    while halving[0].done < len(bits):
        for item in halving:
            item.step()
    for h in range(CHUNKS):
        finish(h)
    for item in halving:
        while item.done <= len(bits):
            item.step()
    stores, base = [], 0
    for target in (grad_out, grad_gate):
        source = summed.at[pl.ds(base, target.shape[0])]
        stores.append(pltpu.make_async_copy(source, target, copy_sem.at[len(load) + len(stores)]))
        base += target.shape[0]
    deep = grad_query.shape[1]
    value_base = base + 2 * deep
    source = summed.at[pl.ds(value_base, grad_value.shape[0])]
    stores.append(pltpu.make_async_copy(source, grad_value, copy_sem.at[len(load) + len(stores)]))
    for store in stores:
        store.start()
    for target in (grad_query, grad_key):
        for j in range(deep // LANES):
            target[:, j * LANES : (j + 1) * LANES] = summed[pl.ds(base, LANES), :].T
            base += LANES
    total_gain.receive()
    for item in halving:
        item.leave()
    for store in stores:
        store.wait()
    for h in range(CHUNKS):
        scatters[h].drain()


def last_call(
    d_qk, d_value, d_gate, weight, grads, inputs, gain, d_middle, second_gain, rows_one, n, m
):
    tokens = d_qk.shape[0]
    rows, width = inputs.shape
    heads = d_value.shape[0]
    shard = width // m
    sems = CHUNKS * 2 * (n - 1)
    hop = (CHUNKS, n - 1, rows // CHUNKS, width)
    flat = (2 * width // LANES, LANES)
    shape = jax.ShapeDtypeStruct
    return pl.pallas_call(
        functools.partial(last_kernel, n, m),
        out_shape=(
            shape((rows, width), F32),
            shape(flat, F32),
            shape((shard, heads * HK), F32),
            shape((shard, heads * HK), F32),
        )
        + (shape((heads * HV, shard), F32),) * 3,
        in_specs=[ANY] * 6 + [VM, ANY, VM, ANY],
        out_specs=(VM,) * 4 + (ANY,) * 3,
        scratch_shapes=[
            pltpu.VMEM(d_qk.shape, BF),
            pltpu.VMEM(d_value.shape, BF),
            pltpu.VMEM(d_gate.shape, BF),
            pltpu.VMEM((2 * heads * (HK + HV), width), BF),
            pltpu.VMEM((rows, width), BF),
            pltpu.VMEM((rows, width), F32),
            pltpu.VMEM((tokens, width), BF),
            pltpu.VMEM(hop, BF),
            pltpu.VMEM(hop, BF),
        ]
        + scatter_scratch(m, grads.shape[0], shard)
        + [
            pltpu.VMEM((8, width), F32),
            pltpu.VMEM(flat, F32),
            pltpu.VMEM((m,) + flat, F32),
            pltpu.VMEM((n,) + flat, F32),
            pltpu.VMEM((tokens, width), BF),
            pltpu.SemaphoreType.DMA((10,)),
            pltpu.SemaphoreType.DMA((sems,)),
            pltpu.SemaphoreType.DMA((sems,)),
            pltpu.SemaphoreType.DMA((n + m,)),
            pltpu.SemaphoreType.DMA((n + m,)),
        ],
        compiler_params=pltpu.CompilerParams(
            collective_id=2, has_side_effects=True, vmem_limit_bytes=VMEM_MOST
        ),
        name="last",
    )(d_qk, d_value, d_gate, weight, grads, inputs, gain, d_middle, second_gain, rows_one)


TILE = 256


def tiles_of(count, step, start=None):
    def run(i, carry):
        step(pl.ds(pl.multiple_of(i * TILE, TILE), TILE))
        return carry

    if start is None:
        lax.fori_loop(0, count // TILE, run, 0)
    else:
        lax.fori_loop(start, start + count, run, 0)


def in_order(units, steps):
    taken = 0
    for i, unit in enumerate(units):
        unit()
        upto = (i + 1) * len(steps) // len(units)
        for step in steps[taken:upto]:
            step()
        taken = upto


def forward_kernel(
    n, m, inputs, gain, pack, cot, col, row,
    rows_o, weight_o, query_o, key_o, value_o, gate_o, norm_o, scale_o, scores_o, gated_o, cot_o,
    own, rows_v, weight_v, both_v, value_v, gate_v, norm_v, scale_v, scores_v, gated_v, cot_v,
    copy_sem, send_sem, recv_sem, wide_send, wide_recv,
):
    line = Line(n, send_sem, recv_sem)
    heads, tokens, size = value_v.shape
    deep = both_v.shape[2]
    per = cot_v.shape[0] // FRONT
    piece = per // n
    copies = []

    def local(src, dst):
        c = pltpu.make_async_copy(src, dst, copy_sem.at[len(copies)])
        copies.append(c)
        c.start()
        return c

    doubling, peers = weight_gather(m, pack, weight_v, wide_send, wide_recv)
    line.enter(["dp", peers])

    def row_slot(h, k):
        if k == 0:
            return own.at[pl.ds(h * piece, piece)]
        return rows_v.at[pl.ds(h * per + k * piece, piece)]

    def cot_slot(h, k):
        return cot_v.at[pl.ds(h * per + k * piece, piece)]

    gathers = [Gather(line, functools.partial(row_slot, h)) for h in range(CHUNKS)]
    cots = [Gather(line, functools.partial(cot_slot, h)) for h in range(FRONT)]
    half = CHUNKS // 2
    levels = len(bits_of(m))

    def go(items):
        for item in items:
            item.step()

    def project(target, first, last, base, width, start, count):
        def step(at):
            def one(j, carry):
                rows = pl.ds(pl.multiple_of(base + j * width, BLOCK), width)
                target[j, at, :] = dot_nt(rows_v[at, :], weight_v[rows, :]).astype(target.dtype)
                return carry

            lax.fori_loop(first, last, one, 0)

        return lambda: tiles_of(count, step, start)

    def attend(h):
        def step(at):
            allowed = (col[at, 0:1] >= row[0:1, :]) & (col[at, 1:2] == row[1:2, :])
            scores = dot_nt(both_v[h, at, :], both_v[heads + h]) * col[at, 2 + h : 3 + h]
            scores = jnp.where(allowed, scores * row[2 + h : 3 + h, :], 0.0).astype(BF)
            scores_v[h, at, :] = scores
            hat, scale = layer_norm(dot_nn(scores, value_v[h]), group_epsilon)
            norm_v[h, at, :] = hat
            scale_v[h, at, :] = scale
            gate = gate_v[h, at, :]
            gated_v[h, at, :] = (gate * jax.nn.sigmoid(gate) * hat).astype(BF)

        return lambda: tiles_of(tokens, step)

    values, gates = 2 * heads * deep, 2 * heads * deep + heads * size
    assert values <= PARTS * (weight_v.shape[0] // (2 * PARTS))
    near, far = gathers[:half], gathers[half:]
    soon, later = doubling[:PARTS], doubling[PARTS:]
    def normalize(first, count):
        def step(at):
            hat, _ = layer_norm(inputs[at(first), :].astype(F32), epsilon)
            own[at(first), :] = (hat * gain[...]).astype(BF)

        blocks(count, step)

    go(soon)
    normalize(0, half * piece)
    go(near)
    normalize(half * piece, (CHUNKS - half) * piece)
    for h in range(CHUNKS):
        local(row_slot(h, 0), rows_v.at[pl.ds(h * per, piece)])
    local(pack, own_columns(pack, weight_v))
    for h in range(FRONT):
        local(cot.at[pl.ds(h * piece, piece)], cot_slot(h, 0))
    first_copies = list(copies)
    go(near)
    go(soon)
    go(later)
    for _ in range(n - 3):
        go(near)
    go(far)
    for _ in range(levels - 1):
        go(soon)
    go(near)
    for item in first_copies:
        item.wait()
    tail = [g.step for _ in range(n - 2) for g in far]
    tail_wide = [g.step for _ in range(levels - 1) for g in later]
    mixed = []
    for i in range(max(len(tail), len(tail_wide))):
        mixed += tail[i : i + 1] + tail_wide[i : i + 1]
    early = tokens // 2 // TILE
    in_order(
        [
            project(both_v, 0, 2 * heads, 0, deep, t, 1)
            for t in range(early)
        ],
        mixed,
    )
    go(cots)
    go(later)
    go(far)
    units = [
        project(both_v, 0, 2 * heads, 0, deep, early, early),
        project(value_v, 0, heads, values, size, 0, 2 * early),
        project(gate_v, 0, heads, gates, size, 0, early),
        project(gate_v, 0, heads, gates, size, early, early),
    ] + [attend(h) for h in range(heads)]
    count = len(copies)
    local(rows_v, rows_o)
    local(weight_v, weight_o)
    in_order(units, [g.step for _ in range(n - 1) for g in cots])
    for src, dst in (
        (both_v.at[pl.ds(0, heads)], query_o), (both_v.at[pl.ds(heads, heads)], key_o),
        (value_v, value_o), (gate_v, gate_o), (norm_v, norm_o), (scale_v, scale_o),
        (scores_v, scores_o), (gated_v, gated_o), (cot_v, cot_o),
    ):
        local(src, dst)
    for item in copies[count:]:
        item.wait()
    for item in gathers + cots:
        assert item.step_no == n
    for item in doubling:
        assert item.done == levels + 1
        item.leave()
    line.leave()


def forward_call(inputs, gain, pack, cot, col, row, n, m, heads):
    rows, width = inputs.shape
    tokens = n * rows
    shape = jax.ShapeDtypeStruct
    outs = (
        shape((tokens, width), BF),
        shape((pack.shape[0], m * pack.shape[1]), BF),
        shape((heads, tokens, HK), BF),
        shape((heads, tokens, HK), BF),
        shape((heads, tokens, HV), BF),
        shape((heads, tokens, HV), F32),
        shape((heads, tokens, HV), F32),
        shape((heads, tokens, 1), F32),
        shape((heads, tokens, tokens), BF),
        shape((heads, tokens, HV), BF),
        shape((tokens * FRONT // CHUNKS, width), BF),
    )
    held = outs[:2] + (shape((2 * heads, tokens, HK), BF),) + outs[4:]
    sems = (CHUNKS + FRONT) * 2 * (n - 1)
    wide = 2 * PARTS * (m - 1)
    return pl.pallas_call(
        functools.partial(forward_kernel, n, m),
        out_shape=outs,
        in_specs=[VM, VM, VM, ANY, VM, VM],
        out_specs=(ANY,) * len(outs),
        scratch_shapes=[pltpu.VMEM((rows, width), BF)]
        + [pltpu.VMEM(o.shape, o.dtype) for o in held]
        + [
            pltpu.SemaphoreType.DMA((CHUNKS + FRONT + 1 + len(outs),)),
            pltpu.SemaphoreType.DMA((sems,)),
            pltpu.SemaphoreType.DMA((sems,)),
            pltpu.SemaphoreType.DMA((wide,)),
            pltpu.SemaphoreType.DMA((wide,)),
        ],
        compiler_params=pltpu.CompilerParams(
            collective_id=4, has_side_effects=True, vmem_limit_bytes=VMEM_MOST
        ),
        name="forward",
    )(inputs, gain, pack, cot, col, row)


def backward_kernel(
    n, m, mid, weights, gate, norm, scale, scores, query, key, value, down, middle, grads, col, row,
    qk_o, value_o, gate_o, glu_gate_o, glu_up_o, outputs,
    mid_v, wo_v, gate_v, norm_v, scale_v, scores_v, query_v, key_v, value_v, part, middle_v,
    d_qk, d_value, d_gate, d_kept, d_scores, lefts, rights, *rest
):
    bits = bits_of(m)
    kept, held = rest[0], rest[1 : 1 + len(bits)]
    summed, wide_send, wide_recv, load_sem = rest[1 + len(bits) : 5 + len(bits)]
    copy_sem, send_sem, recv_sem = rest[5 + len(bits) :]
    line = Line(n, send_sem, recv_sem)
    heads, tokens, deep = query_v.shape
    size = value_v.shape[2]
    back = CHUNKS - DOWNS - ENDS
    per = part.shape[0] // back
    piece = per // n
    copies = []

    def local(src, dst):
        c = pltpu.make_async_copy(src, dst, copy_sem.at[len(copies)])
        copies.append(c)
        c.start()
        return c

    load_part = local(down.at[pl.ds(0, part.shape[0])], part)
    loads = [
        local(src, dst)
        for src, dst in (
            (mid, mid_v), (weights.at[pl.ds(weights.shape[0] - wo_v.shape[0], wo_v.shape[0])], wo_v),
            (gate, gate_v), (norm, norm_v), (scale, scale_v), (value, value_v), (key, key_v),
            (query, query_v), (scores, scores_v),
            (middle.at[pl.ds(0, middle_v.shape[0])], middle_v),
        )
    ]
    halving, peers = grad_scatter(m, grads, kept, held, summed, wide_send, wide_recv, load_sem)
    line.enter(["dp", peers])
    for item in halving:
        item.step()
    for item in halving:
        item.load()
    for h in range(back):
        no_neighbour_zero(n, line.place, lefts.at[h, n - 2], rights.at[h, n - 2])
    scatters = [
        Scatter(
            line,
            lambda k, h=h: part.at[pl.ds(h * per + k * piece, piece)],
            lambda s, h=h: lefts.at[h, s - 1],
            lambda s, h=h: rights.at[h, s - 1],
            add_into,
        )
        for h in range(back)
    ]
    load_part.wait()
    for item in scatters:
        item.step()
    for item in loads:
        item.wait()

    def gates(h):
        def step(at):
            grad = dot_nt(mid_v[at, :], wo_v[pl.ds(h * size, size), :])
            pre, hat = gate_v[h, at, :], norm_v[h, at, :]
            s = jax.nn.sigmoid(pre)
            d_gate[h, at, :] = (grad * hat * (s + pre * s * (1.0 - s))).astype(BF)
            d_kept[h, at, :] = norm_back(grad * (pre * s), hat, scale_v[h, at, :]).astype(BF)

        return lambda: tiles_of(tokens, step)

    def by_row(h):
        def step(at):
            allowed = (col[at, 0:1] >= row[0:1, :]) & (col[at, 1:2] == row[1:2, :])
            grad = dot_nt(d_kept[h, at, :], value_v[h]) * col[at, 2 + h : 3 + h]
            grad = jnp.where(allowed, grad * row[2 + h : 3 + h, :], 0.0).astype(BF)
            d_scores[at, :] = grad
            d_qk[at, pl.ds(h * deep, deep)] = dot_nn(grad, key_v[h]).astype(BF)

        return lambda: tiles_of(tokens, step)

    def by_column(h):
        def step(at):
            d_value[h, at, :] = dot_tn(scores_v[h, :, at], d_kept[h]).astype(BF)
            d_qk[at, pl.ds((heads + h) * deep, deep)] = dot_tn(d_scores[:, at], query_v[h]).astype(
                BF
            )

        return lambda: tiles_of(tokens, step)

    units = []
    for h in range(heads):
        units += [gates(h), by_row(h), by_column(h)]
    steps = [item.step for _ in range(n - 2) for item in scatters]
    wide_steps = [item.step for _ in bits for item in halving]
    mixed = []
    for i in range(max(len(steps), len(wide_steps))):
        mixed += steps[i : i + 1] + wide_steps[i : i + 1]
    late = mixed[-2 * PARTS :]
    in_order(units, mixed[: -2 * PARTS])
    count = len(copies)
    local(d_qk, qk_o)
    local(d_value, value_o)
    local(d_gate, gate_o)
    for step in late:
        step()
    size = glu_up_o.shape[0]
    wide = grads.shape[0] // 2
    for t in range(wide // LANES):
        have = min(LANES, size - t * LANES)
        for i, target in enumerate((glu_gate_o, glu_up_o)):
            local(
                summed.at[pl.ds((2 * t + i) * LANES, have)], target.at[pl.ds(t * LANES, have)]
            )
    for item in halving:
        assert item.done == len(bits) + 1
        item.leave()
    for h in range(back):
        scatters[h].finish()

        def step(at):
            outputs[at(h * piece), :] = (
                middle_v[at(h * piece), :]
                + part[at(h * per), :].astype(F32)
                + lefts[h, n - 2, at(), :].astype(F32)
                + rights[h, n - 2, at(), :].astype(F32)
            ).astype(BF)

        blocks(piece, step)
    for item in copies[count:]:
        item.wait()
    for item in scatters:
        item.drain()


def backward_call(mid, weights, gate, norm, scale, scores, query, key, value, down, middle, grads, size_two, col, row, n, m):
    tokens, width = mid.shape
    heads, _, size = value.shape
    back = CHUNKS - DOWNS - ENDS
    nv = heads * size
    shard = width // m
    piece = tokens // n // CHUNKS
    shape = jax.ShapeDtypeStruct
    outs = (
        shape((tokens, 2 * heads * HK), BF),
        shape(value.shape, BF),
        shape(value.shape, BF),
    ) + (shape((size_two, shard), F32),) * 2 + (shape((back * piece, width), BF),)
    ins = (gate, norm, scale, scores, query, key, value, down, middle)
    hop = (back, n - 1, piece, width)
    sems = back * 2 * (n - 1)
    return pl.pallas_call(
        functools.partial(backward_kernel, n, m),
        out_shape=outs,
        in_specs=[ANY] * 12 + [VM] * 2,
        out_specs=(ANY,) * 5 + (VM,),
        scratch_shapes=[pltpu.VMEM(mid.shape, BF), pltpu.VMEM((nv, width), BF)]
        + [pltpu.VMEM(a.shape, a.dtype) for a in ins[:-2]]
        + [pltpu.VMEM((back * n * piece, width), BF), pltpu.VMEM((back * piece, width), F32)]
        + [pltpu.VMEM(o.shape, o.dtype) for o in outs[:3]]
        + [
            pltpu.VMEM(value.shape, BF),
            pltpu.VMEM((tokens, tokens), BF),
            pltpu.VMEM(hop, BF),
            pltpu.VMEM(hop, BF),
        ]
        + scatter_scratch(m, grads.shape[0], shard)
        + [
            pltpu.SemaphoreType.DMA((15 + grads.shape[0] // LANES,)),
            pltpu.SemaphoreType.DMA((sems,)),
            pltpu.SemaphoreType.DMA((sems,)),
        ],
        compiler_params=pltpu.CompilerParams(
            collective_id=5, has_side_effects=True, vmem_limit_bytes=VMEM_MOST
        ),
        name="backward",
    )(mid, weights, *ins, grads, col, row)


def products_kernel(n, m, plan, arrays, *refs):
    ins, (down, middle, grads) = refs[:arrays], refs[arrays : arrays + 3]
    out, down_o, outputs = refs[arrays + 3 : arrays + 6]
    held_in = refs[arrays + 6 : 2 * arrays + 6]
    part, middle_v, lefts, rights, result, kept, *rest = refs[2 * arrays + 6 :]
    bits = bits_of(m)
    held = rest[: len(bits)]
    summed, wide_send, wide_recv, load_sem, copy_sem, send_sem, recv_sem = rest[len(bits) :]
    line = Line(n, send_sem, recv_sem)
    count, width = outputs.shape
    piece = count // ENDS
    per = n * piece
    sources = list(zip(ins, held_in))
    sources.append((middle.at[pl.ds(middle.shape[0] - count, count)], middle_v))
    sources.append((down.at[pl.ds(down.shape[0] - n * count, n * count)], part))
    loads = [pltpu.make_async_copy(a, b, copy_sem.at[i]) for i, (a, b) in enumerate(sources)]
    for item in loads[::-1]:
        item.start()
    halving, peers = grad_scatter(m, grads, kept, held, summed, wide_send, wide_recv, load_sem)
    line.enter(["dp", peers])
    for item in halving:
        item.step()
    for item in halving:
        item.load()
    for h in range(ENDS):
        no_neighbour_zero(n, line.place, lefts.at[h, n - 2], rights.at[h, n - 2])
    scatters = [
        Scatter(
            line,
            lambda k, h=h: part.at[pl.ds(h * per + k * piece, piece)],
            lambda s, h=h: lefts.at[h, s - 1],
            lambda s, h=h: rights.at[h, s - 1],
            add_into,
        )
        for h in range(ENDS)
    ]
    loads[-1].wait()
    for item in scatters:
        item.step()
    waited, stores = set(), []

    def product(left, head, start, size, right, base):
        def run():
            for i in (left, right):
                if i not in waited:
                    loads[i].wait()
                    waited.add(i)
            target = pl.ds(base, size)

            def step(j, carry):
                at = pl.ds(pl.multiple_of(j * 4 * LANES, 4 * LANES), 4 * LANES)
                source = (
                    held_in[left][:, pl.ds(start, size)] if head is None else held_in[left][head]
                )
                result[target, at] = dot_tn(source, held_in[right][:, at]).astype(BF)
                return carry

            lax.fori_loop(0, width // (4 * LANES), step, 0)
            store(target)

        return run

    def store(target):
        c = pltpu.make_async_copy(
            result.at[target], out.at[target], copy_sem.at[len(loads) + len(stores)]
        )
        c.start()
        stores.append(c)

    units, base = [], 0
    for item in plan:
        units.append(product(*item, base))
        base += item[3]
    steps = [item.step for _ in range(n - 2) for item in scatters]
    wide_steps = [item.step for _ in bits for item in halving]
    mixed = []
    for i in range(max(len(steps), len(wide_steps))):
        mixed += steps[i : i + 1] + wide_steps[i : i + 1]
    in_order(units, mixed)
    spare = result.shape[0] - base
    if spare:
        result[pl.ds(base, spare), :] = jnp.zeros((spare, width), BF)
        store(pl.ds(base, spare))
    keep = pltpu.make_async_copy(
        summed.at[pl.ds(0, down_o.shape[0])], down_o, copy_sem.at[len(loads) + len(stores)]
    )
    keep.start()
    loads[-2].wait()
    for h in range(ENDS):
        scatters[h].finish()

        def step(at):
            outputs[at(h * piece), :] = (
                middle_v[at(h * piece), :]
                + part[at(h * per), :].astype(F32)
                + lefts[h, n - 2, at(), :].astype(F32)
                + rights[h, n - 2, at(), :].astype(F32)
            ).astype(BF)

        blocks(piece, step)
    for item in halving:
        assert item.done == len(bits) + 1
        item.leave()
    for item in scatters:
        item.drain()
    for item in stores + [keep]:
        item.wait()


def products_call(plan, arrays, down, middle, grads, size_two, rows, n, m):
    width = grads.shape[1]
    shard = width // m
    piece = arrays[1].shape[0] // n // CHUNKS
    sems = ENDS * 2 * (n - 1)
    hop = (ENDS, n - 1, piece, width)
    shape = jax.ShapeDtypeStruct
    return pl.pallas_call(
        functools.partial(products_kernel, n, m, plan, len(arrays)),
        out_shape=(
            shape((rows, width), BF), shape((size_two, shard), F32), shape((ENDS * piece, width), BF),
        ),
        in_specs=[ANY] * (len(arrays) + 3),
        out_specs=(ANY, ANY, VM),
        scratch_shapes=[pltpu.VMEM(a.shape, a.dtype) for a in arrays]
        + [
            pltpu.VMEM((ENDS * n * piece, width), BF),
            pltpu.VMEM((ENDS * piece, width), F32),
            pltpu.VMEM(hop, BF),
            pltpu.VMEM(hop, BF),
            pltpu.VMEM((rows, width), BF),
        ]
        + scatter_scratch(m, grads.shape[0], shard)
        + [
            pltpu.SemaphoreType.DMA((len(arrays) + len(plan) + 4,)),
            pltpu.SemaphoreType.DMA((sems,)),
            pltpu.SemaphoreType.DMA((sems,)),
        ],
        compiler_params=pltpu.CompilerParams(
            collective_id=3, has_side_effects=True, vmem_limit_bytes=VMEM_MOST
        ),
        name="products",
    )(*arrays, down, middle, grads)


def results_kernel(plan, *refs):
    count = len(plan)
    results = refs[count : -count - 1]
    held, sem = refs[-count - 1 : -1], refs[-1]
    ins = [pltpu.make_async_copy(refs[i], held[i], sem.at[0, i]) for i in range(count)]
    for item in ins:
        item.start()
    outs = []
    for i, (result, start) in enumerate(plan):
        ins[i].wait()
        target = results[result].at[pl.ds(start, held[i].shape[0])]
        outs.append(pltpu.make_async_copy(held[i], target, sem.at[1, i]))
        outs[-1].start()
    for item in outs:
        item.wait()


def write_results(groups):
    plan, arrays, shapes = [], [], []
    for r, group in enumerate(groups):
        start = 0
        for array in group:
            plan.append((r, start))
            arrays.append(array)
            start += array.shape[0]
        shapes.append(jax.ShapeDtypeStruct((start,) + group[0].shape[1:], group[0].dtype))
    return pl.pallas_call(
        functools.partial(results_kernel, plan),
        out_shape=shapes,
        in_specs=[ANY] * len(arrays),
        out_specs=[ANY] * len(shapes),
        scratch_shapes=[pltpu.VMEM(a.shape, a.dtype) for a in arrays]
        + [pltpu.SemaphoreType.DMA((2, len(arrays)))],
        name="results",
    )(*arrays)


def pad_rows(array, count):
    return jnp.pad(array, ((0, count - array.shape[0]), (0, 0)))


def pad_columns(array, count):
    return jnp.pad(array, ((0, 0), (0, count - array.shape[1])))


def body(
    inputs,
    segments,
    first_norm_gain,
    w_query,
    w_key,
    w_value,
    w_gate,
    w_out,
    second_norm_gain,
    w_glu_gate,
    w_glu_up,
    w_down,
    cotangent,
):
    n = lax.axis_size("mp")
    place = lax.axis_index("mp")
    heads = H // n
    head_start = place * heads
    rows, width = inputs.shape
    shard = w_query.shape[0]
    piece = rows // CHUNKS
    nk, nv, nf = heads * HK, heads * HV, w_down.shape[0]
    f_wide = -(-nf // LANES) * LANES
    f_tiles = f_wide // LANES
    grain = 2 * PARTS * BLOCK
    one_rows = -(-(2 * nk + 3 * nv) // grain) * grain
    gap = one_rows - 2 * nk - 3 * nv
    m = lax.axis_size("dp")

    pack_one = jnp.concatenate(
        [w_query.T, w_key.T, w_value.T, w_gate.T, jnp.zeros((gap, shard), BF), w_out], axis=0
    )
    glu_pack = jnp.stack(
        [
            pad_rows(w_glu_gate.T, f_wide).reshape(f_tiles, LANES, shard),
            pad_rows(w_glu_up.T, f_wide).reshape(f_tiles, LANES, shard),
        ],
        axis=1,
    ).reshape(2 * f_wide, shard)
    pack_two = jnp.concatenate([glu_pack, pad_rows(w_down, f_wide)], axis=0)

    tokens = n * rows

    slot_shard = lax.rem(place - jnp.arange(n) + n, n)
    places = (
        slot_shard[None, :, None] * rows
        + jnp.arange(CHUNKS)[:, None, None] * piece
        + jnp.arange(piece)[None, None, :]
    ).reshape(tokens)
    seg = segments.reshape(n, CHUNKS, piece)[::-1]
    seg = lax.dynamic_slice_in_dim(jnp.concatenate([seg, seg], axis=0), n - 1 - place, n, axis=0)
    seg = seg.transpose(1, 0, 2).reshape(tokens)

    log_gamma = jnp.log1p(-jnp.exp2(-5.0 - (head_start + jnp.arange(heads)).astype(F32)))
    spot = places.astype(F32)
    powers = spot[None] * log_gamma[:, None]
    marks = jnp.stack([spot, seg.astype(F32)])
    col = jnp.concatenate([marks, jnp.exp(powers)], axis=0).T
    row = jnp.concatenate([marks, jnp.exp(-powers) * HK ** (-0.5)], axis=0)

    (
        rows_one, weight_one, query, key, value, gate_pre, normalized, scale_group, scores, gated,
        cot_front,
    ) = forward_call(
        inputs, first_norm_gain[None], pack_one, cotangent, col, row, n, m, heads
    )
    (
        mid_rows, grads_glu, grads_two, down, outputs_front, middle, middle_grad, second_gain,
    ) = middle_call(
        gated, pack_two, weight_one, inputs, cotangent, cot_front, second_norm_gain[None], n, m
    )
    d_qk, d_value, d_gate, grad_glu_gate, grad_glu_up, outputs_back = backward_call(
        mid_rows, weight_one, gate_pre, normalized, scale_group, scores, query, key, value,
        down, middle, grads_glu, nf, col, row, n, m,
    )
    plan = [(0, h, 0, HV, 1) for h in range(heads)] + [(2, h, 0, HV, 3) for h in range(heads)]
    plan += [(4, None, t * nk, nk, 3) for t in range(2)]
    plan += [(5, h, 0, HV, 3) for h in range(heads)]
    grads_one, grad_down, outputs_end = products_call(
        plan, (gated, mid_rows, d_gate, rows_one, d_qk, d_value), down, middle, grads_two, nf,
        one_rows, n, m,
    )
    input_gradient, gains, grad_query, grad_key, grad_out, grad_gate, grad_value = last_call(
        d_qk, d_value, d_gate, weight_one, grads_one, inputs, first_norm_gain[None], middle_grad,
        second_gain, rows_one, n, m,
    )
    gains = gains.reshape(2, width)
    (
        outputs, input_gradient, grad_query, grad_key, grad_value, grad_gate, grad_out,
        grad_glu_gate, grad_glu_up, grad_down,
    ) = write_results(
        [
            (outputs_front, outputs_back, outputs_end), (input_gradient,), (grad_query,), (grad_key,),
            (grad_value,), (grad_gate,), (grad_out,), (grad_glu_gate,), (grad_glu_up,), (grad_down,),
        ]
    )
    return (
        outputs,
        input_gradient,
        gains[0],
        grad_query,
        grad_key,
        grad_value.T,
        grad_gate.T,
        grad_out,
        gains[1],
        grad_glu_gate.T,
        grad_glu_up.T,
        grad_down,
    )


def solution(mesh):
    split = P(("dp", "mp"), None)
    wide, tall = P("dp", "mp"), P("mp", "dp")
    return jax.shard_map(
        body,
        mesh=mesh,
        in_specs=(
            split, P("dp", None), P(), wide, wide, wide, wide, tall, P(), wide, wide, tall, split,
        ),
        out_specs=(
            split, split, P(), wide, wide, wide, wide, tall, P(), wide, wide, tall,
        ),
        check_vma=False,
    )
```
